32 devices in a mesh: seq: 2 (over x), shard: 16 (over z, y, core).
Axes of the slice: x: 2, y: 2, z: 4, core: 2. Of those that a mesh axis runs over, the one named last changes fastest.
Arguments:
- hidden_in: bfloat16 [16, 1024, 768], P('shard', 'seq'), may hold values from -6 to 6
- encoded: bfloat16 [16, 1024, 768], P('shard', 'seq'), may hold values from -6 to 6
- cotangent: bfloat16 [16, 1024, 768], P('shard', 'seq'), may hold values from -6 to 6
- buckets: int32 [1024], replicated, may hold values from 0 to 31, as said below
- self_query: bfloat16 [768, 768], P(('seq', 'shard')), may hold values from -0.0390625 to 0.0390625
- self_key: bfloat16 [768, 768], P(('seq', 'shard')), may hold values from -0.21875 to 0.21875
- self_value: bfloat16 [768, 768], P(('seq', 'shard')), may hold values from -0.21875 to 0.21875
- self_out: bfloat16 [768, 768], P(('seq', 'shard')), may hold values from -3 to 3
- cross_query: bfloat16 [768, 768], P(('seq', 'shard')), may hold values from -0.0390625 to 0.0390625
- cross_key: bfloat16 [768, 768], P(('seq', 'shard')), may hold values from -0.21875 to 0.21875
- cross_value: bfloat16 [768, 768], P(('seq', 'shard')), may hold values from -0.21875 to 0.21875
- cross_out: bfloat16 [768, 768], P(('seq', 'shard')), may hold values from -3 to 3
- ff_gate: bfloat16 [768, 2048], P(('seq', 'shard')), may hold values from -0.21875 to 0.21875
- ff_up: bfloat16 [768, 2048], P(('seq', 'shard')), may hold values from -0.21875 to 0.21875
- ff_down: bfloat16 [2048, 768], P(('seq', 'shard')), may hold values from -0.125 to 0.125
- norm_self: bfloat16 [768], P(('seq', 'shard')), may hold values from 0.25 to 1.75
- norm_cross: bfloat16 [768], P(('seq', 'shard')), may hold values from 0.25 to 1.75
- norm_ff: bfloat16 [768], P(('seq', 'shard')), may hold values from 0.25 to 1.75
- bias_table: bfloat16 [384], P(('seq', 'shard')), may hold values from -4 to 4
Outputs:
- hidden_out: bfloat16 [16, 1024, 768], P('shard', 'seq')
- grad_hidden: bfloat16 [16, 1024, 768], P('shard', 'seq')
- grad_encoded: bfloat16 [16, 1024, 768], P('shard', 'seq')
- grad_self_query: float32 [768, 768], P(('seq', 'shard'))
- grad_self_key: float32 [768, 768], P(('seq', 'shard'))
- grad_self_value: float32 [768, 768], P(('seq', 'shard'))
- grad_self_out: float32 [768, 768], P(('seq', 'shard'))
- grad_cross_query: float32 [768, 768], P(('seq', 'shard'))
- grad_cross_key: float32 [768, 768], P(('seq', 'shard'))
- grad_cross_value: float32 [768, 768], P(('seq', 'shard'))
- grad_cross_out: float32 [768, 768], P(('seq', 'shard'))
- grad_ff_gate: float32 [768, 2048], P(('seq', 'shard'))
- grad_ff_up: float32 [768, 2048], P(('seq', 'shard'))
- grad_ff_down: float32 [2048, 768], P(('seq', 'shard'))
- grad_norm_self: float32 [768], P(('seq', 'shard'))
- grad_norm_cross: float32 [768], P(('seq', 'shard'))
- grad_norm_ff: float32 [768], P(('seq', 'shard'))
- grad_bias_table: float32 [384], P(('seq', 'shard'))
The draws below stay inside these ranges and needn't reach their ends.
Inputs may be any that keep to these rules, and one draw needn't show every extreme that they name: `buckets`: bucket of the distance d from a key to a later query, for d = 0 to 1023: never falling as d grows, equal to d for d below 16, and 31 at the largest distance.
All inputs are finite; a program needn't handle non-finite values.
Results may differ from the reference program's by a relative error of at most 0.024.
The reference program's roundings to bfloat16 on the way count: a program that leaves them out, or rounds other values in their place, can miss the bound.
Values may be sent and summed in bfloat16 or wider, within the bound.
A program may use at most 320 MiB of HBM per device.

```python
import jax
import jax.numpy as jnp
from jax import lax

D = 768
H = 12
DH = 64
FF = 2048
BUCKETS = 32
LEN = 1024
BATCH = 16


def draw_buckets(key, part):
    half = BUCKETS // 2
    chosen = jax.random.permutation(key, LEN - half)[:BUCKETS - half].astype(jnp.int32) + half
    distance = jnp.arange(LEN, dtype=jnp.int32)
    counted = jnp.sum((chosen[None, :] <= distance[:, None]).astype(jnp.int32), 1)
    return (jnp.minimum(distance, half - 1) + counted).astype(jnp.int32)


def steps_of(own_key, shape, cuts, low, high):
    level, own = 1.0, jax.random.fold_in(own_key, 6)
    for position, blocks in cuts:
        draws = jnp.exp(jax.random.uniform(jax.random.fold_in(own, position), (blocks,), jnp.float32, low / len(cuts), high / len(cuts)))
        level = level * jnp.repeat(draws, shape[position] // blocks).reshape([-1 if axis == position else 1 for axis in range(len(shape))])
    return level


def bell_draw(own_key, dims, width, limit, shards=(), kind=jnp.bfloat16):
    entries = jax.random.normal(own_key, dims, jnp.float32) * width
    if len(shards) > 0:
        entries = steps_of(own_key, dims, shards, -0.22, 0.18) * entries
    return jnp.clip(entries, min=-limit, max=limit).astype(kind)


def setup_inputs(seed: int = 0) -> dict:
    seeds = jax.random.split(jax.random.key(seed), 20)
    return {
        "hidden_in": bell_draw(seeds[0], (BATCH, LEN, D), 1.0, 6.0, ((0, 16), (1, 2))),
        "encoded": bell_draw(seeds[1], (BATCH, LEN, D), 1.0, 6.0, ((0, 16), (1, 2))),
        "cotangent": bell_draw(seeds[2], (BATCH, LEN, D), 1.0, 6.0, ((0, 16), (1, 2))),
        "buckets": draw_buckets(jax.random.fold_in(seeds[19], 71), 0),
        "self_query": bell_draw(seeds[4], (D, D), (D * 32) ** -0.5, 0.0390625, ((0, 32),)),
        "self_key": bell_draw(seeds[5], (D, D), D ** -0.5, 0.21875, ((0, 32),)),
        "self_value": bell_draw(seeds[6], (D, D), D ** -0.5, 0.21875, ((0, 32),)),
        "self_out": bell_draw(seeds[7], (D, D), (DH // 16) ** -0.5, 3.0, ((0, 32),)),
        "cross_query": bell_draw(seeds[8], (D, D), (D * 32) ** -0.5, 0.0390625, ((0, 32),)),
        "cross_key": bell_draw(seeds[9], (D, D), D ** -0.5, 0.21875, ((0, 32),)),
        "cross_value": bell_draw(seeds[10], (D, D), D ** -0.5, 0.21875, ((0, 32),)),
        "cross_out": bell_draw(seeds[11], (D, D), (DH // 16) ** -0.5, 3.0, ((0, 32),)),
        "ff_gate": bell_draw(seeds[12], (D, FF), D ** -0.5, 0.21875, ((0, 32),)),
        "ff_up": bell_draw(seeds[13], (D, FF), D ** -0.5, 0.21875, ((0, 32),)),
        "ff_down": bell_draw(seeds[14], (FF, D), FF ** -0.5, 0.125, ((0, 32),)),
        "norm_self": jnp.clip(1.0 + 0.15 * jax.random.normal(seeds[15], (D,), jnp.float32), 0.25, 1.75).astype(jnp.bfloat16),
        "norm_cross": jnp.clip(1.0 + 0.15 * jax.random.normal(seeds[16], (D,), jnp.float32), 0.25, 1.75).astype(jnp.bfloat16),
        "norm_ff": jnp.clip(1.0 + 0.15 * jax.random.normal(seeds[17], (D,), jnp.float32), 0.25, 1.75).astype(jnp.bfloat16),
        "bias_table": bell_draw(seeds[18], (H * BUCKETS,), 1.0, 4.0, ((0, 32),)),
    }


@jax.custom_vjp
def low(v):
    return lax.optimization_barrier(v.astype(jnp.bfloat16)).astype(jnp.float32)

@jax.custom_vjp
def low_back(v):
    return v

def low_keep(v):
    return (low(v), None)

def low_pass(kept, grad):
    return (grad,)

def back_keep(v):
    return (v, None)

def back_low(kept, grad):
    return (low(grad),)
low.defvjp(low_keep, low_pass)
low_back.defvjp(back_keep, back_low)
HIGHEST = lax.Precision.HIGHEST
EPSILON = 1e-06
NEGATIVE = -1e+30

def dot_high(left, right):
    return jnp.dot(left, right, precision=HIGHEST)

def normed(value, gain):
    return value * lax.rsqrt(lax.optimization_barrier(jnp.mean(value * value, -1, keepdims=True)) + EPSILON) * gain

def split_heads(value):
    return value.reshape(value.shape[0], H, DH)

def attend(queries, keys_all, values, bias, allowed):
    scores = jnp.einsum('qhd,khd->hqk', split_heads(queries), split_heads(keys_all), precision=HIGHEST)
    if bias is not None:
        scores = jnp.where(allowed[None], scores + bias, NEGATIVE)
    scores = low_back(scores)
    summit = lax.optimization_barrier(jnp.max(scores, -1, keepdims=True))
    exponent = jnp.exp(scores - summit)
    weights = low(exponent / lax.optimization_barrier(jnp.sum(exponent, -1, keepdims=True)))
    mixed = jnp.einsum('hqk,khd->qhd', weights, split_heads(values), precision=HIGHEST)
    return low(low_back(mixed.reshape(queries.shape[0], D)))

def layer(hidden, encoded, params, buckets):
    self_query, self_key, self_value, self_out, cross_query, cross_key, cross_value, cross_out, ff_gate, ff_up, ff_down, norm_self, norm_cross, norm_ff, bias_table = params
    length = hidden.shape[0]
    places = jnp.arange(length, dtype=jnp.int32)
    gap = places[:, None] - places[None, :]
    allowed = gap >= 0
    table = bias_table.reshape(H, BUCKETS)
    bias = table[:, buckets[jnp.maximum(gap, 0).astype(jnp.int32)]]
    first = low(normed(hidden, norm_self))
    queries = low(low_back(dot_high(first, self_query)))
    keys_self = low(low_back(dot_high(first, self_key)))
    values = low(low_back(dot_high(first, self_value)))
    mixed = attend(queries, keys_self, values, bias, allowed)
    after_self = hidden + low_back(dot_high(mixed, self_out))
    second = low(normed(after_self, norm_cross))
    cross_q = low(low_back(dot_high(second, cross_query)))
    cross_k = low(low_back(dot_high(encoded, cross_key)))
    cross_v = low(low_back(dot_high(encoded, cross_value)))
    crossed = attend(cross_q, cross_k, cross_v, None, None)
    after_cross = after_self + low_back(dot_high(crossed, cross_out))
    third = low(normed(after_cross, norm_ff))
    gate = low_back(dot_high(third, ff_gate))
    upper = low_back(dot_high(third, ff_up))
    inner = low(jax.nn.gelu(gate, approximate=True) * upper)
    return after_cross + low_back(dot_high(inner, ff_down))

def reference(hidden_in, encoded, cotangent, buckets, self_query, self_key, self_value, self_out, cross_query, cross_key, cross_value, cross_out, ff_gate, ff_up, ff_down, norm_self, norm_cross, norm_ff, bias_table):
    params = tuple((item.astype(jnp.float32) for item in (self_query, self_key, self_value, self_out, cross_query, cross_key, cross_value, cross_out, ff_gate, ff_up, ff_down, norm_self, norm_cross, norm_ff, bias_table)))

    def one_sequence(totals, inputs):
        hidden, states, incoming = inputs

        def forward(hidden_value, state_value, param_value):
            return layer(hidden_value, state_value, param_value, buckets)
        output, pull = jax.vjp(forward, hidden.astype(jnp.float32), states.astype(jnp.float32), params)
        grad_hid, grad_states, grad_params = pull(incoming.astype(jnp.float32))
        totals = jax.tree.map(lambda running, extra: running + extra, totals, grad_params)
        return (totals, (output.astype(jnp.bfloat16), grad_hid.astype(jnp.bfloat16), grad_states.astype(jnp.bfloat16)))
    zeros = tuple((jnp.zeros_like(item) for item in params))
    totals, (outputs, grad_hid, grad_states) = lax.scan(one_sequence, zeros, (hidden_in, encoded, cotangent))
    return (outputs, grad_hid, grad_states, totals[0], totals[1], totals[2], totals[3], totals[4], totals[5], totals[6], totals[7], totals[8], totals[9], totals[10], totals[11], totals[12], totals[13], totals[14])
```

```python
import functools
import jax
import jax.numpy as jnp
from jax import lax
from jax.experimental import pallas as pl
from jax.experimental.pallas import tpu as pltpu
from jax.sharding import PartitionSpec as P

H = 12
BUCKETS = 32
NEGATIVE = -1e30
EPSILON = 1e-06
F32 = jnp.float32
LOW = jnp.bfloat16
PAIR = 2
TILE = 256


def contract(left, right, left_dim, right_dim):
    return lax.dot_general(
        left, right, (((left_dim,), (right_dim,)), ((), ())), preferred_element_type=F32
    )


def keep_head(value, head):
    size = value.shape[1] // PAIR
    lane = lax.broadcasted_iota(jnp.int32, value.shape, 1)
    inside = (lane >= head * size) & (lane < (head + 1) * size)
    return jnp.where(inside, value, jnp.zeros_like(value))


def toeplitz(row):
    wide = jnp.broadcast_to(row, (TILE, 2 * TILE))
    return pltpu.roll(wide, 0, 1, stride=1, stride_axis=0)[:, :TILE]


def skew_sum(total_ref):
    group = 8
    width = 2 * TILE
    summed = jnp.zeros((group, width), F32)
    for start in range(0, TILE, group):
        rows = total_ref[start : start + group, :]
        wide = jnp.concatenate([rows, jnp.zeros_like(rows)], 1)
        summed = summed + pltpu.roll(wide, (width - start) % width, 1)
    out = summed[0:1]
    for row in range(1, group):
        out = out + pltpu.roll(summed[row : row + 1], width - row, 1)
    return out


def scores_t(keys, query, tiles, last):
    scores = contract(keys, query, 1, 1)
    if tiles is None:
        return scores
    parts = [
        scores[place * TILE : (place + 1) * TILE] + tiles[last - place] for place in range(last + 1)
    ]
    return jnp.concatenate(parts, 0) if len(parts) > 1 else parts[0]


def attend_block(q_ref, k_ref, v_t, o_ref, lse_ref, tiles_ref, start, last, span):
    query = q_ref[start : start + TILE, :]
    size = query.shape[1] // PAIR
    mixed = []
    for head in range(PAIR):
        tiles = None if tiles_ref is None else tiles_ref.at[head]
        scores = scores_t(k_ref[:span, :], keep_head(query, head), tiles, last)
        summit = jnp.max(scores, 0, keepdims=True)
        exponent = jnp.exp(scores - summit)
        total = jnp.sum(exponent, 0, keepdims=True)
        weighted = contract(
            v_t[head * size : (head + 1) * size, :span], exponent.astype(LOW), 1, 0
        )
        mixed.append(weighted / total)
        lse_ref[0, head : head + 1, start : start + TILE] = summit + jnp.log(total)
    o_ref[start : start + TILE, :] = jnp.concatenate(mixed, 0).T.astype(LOW)


def attend_kernel(causal, *refs):
    if causal:
        seq_ref, q_ref, k_ref, v_ref, z_ref, o_ref, lse_ref, tiles_ref = refs
        make_tiles(z_ref, tiles_ref)
    else:
        q_ref, k_ref, v_ref, o_ref, lse_ref = refs
    v_t = v_ref[...].T
    blocks = q_ref.shape[0] // TILE
    keys = k_ref.shape[0]
    if not causal:
        for block in range(blocks):
            attend_block(q_ref, k_ref, v_t, o_ref, lse_ref, None, block * TILE, None, keys)
        return
    for side in range(keys // q_ref.shape[0]):

        @pl.when(seq_ref[0] == side)
        def _(side=side):
            for block in range(blocks):
                last = side * blocks + block
                attend_block(
                    q_ref, k_ref, v_t, o_ref, lse_ref, tiles_ref, block * TILE, last,
                    (last + 1) * TILE,
                )


def make_tiles(z_ref, tiles_ref):
    for head in range(PAIR):
        for off in range(z_ref.shape[2]):
            tiles_ref[head, off] = toeplitz(z_ref[0, head, off : off + 1, :])


def attend(queries, keys_all, values, seq_pos, rows):
    count, width = queries.shape
    length = keys_all.shape[0]
    pairs = H // PAIR
    lanes = width // pairs
    offs = length // TILE
    causal = rows is not None
    col = lambda size: pl.BlockSpec((size, lanes), lambda pair, *_: (0, pair))
    in_specs = [col(count), col(length), col(length)]
    args = [queries, keys_all, values]
    scratch = []
    if causal:
        in_specs.append(pl.BlockSpec((1, PAIR, offs, 2 * TILE), lambda pair, *_: (pair, 0, 0, 0)))
        args = [seq_pos] + args + [rows]
        scratch = [pltpu.VMEM((PAIR, offs, TILE, TILE), F32)]
    work = H * count * length
    return pl.pallas_call(
        functools.partial(attend_kernel, causal),
        grid_spec=pltpu.PrefetchScalarGridSpec(
            num_scalar_prefetch=1 if causal else 0,
            grid=(pairs,),
            in_specs=in_specs,
            out_specs=[
                col(count),
                pl.BlockSpec((1, PAIR, count), lambda pair, *_: (pair, 0, 0)),
            ],
            scratch_shapes=scratch,
        ),
        out_shape=[
            jax.ShapeDtypeStruct((count, width), LOW),
            jax.ShapeDtypeStruct((pairs, PAIR, count), F32),
        ],
        cost_estimate=pl.CostEstimate(
            flops=work * 256 * 2, bytes_accessed=6 * length * width, transcendentals=work
        ),
        name="attend_causal" if causal else "attend_cross",
    )(*args)


def back_block(refs, k_t, prod_t, start, last, span, first, tiles_ref, total_ref):
    q_ref, k_ref, v_ref, g_ref, lse_ref, dq_ref, dk_acc, dv_acc = refs
    query = q_ref[start : start + TILE, :]
    grad = g_ref[start : start + TILE, :]
    size = query.shape[1] // PAIR
    dq_t = []
    dk = dv = None
    for head in range(PAIR):
        own = keep_head(query, head)
        own_grad = keep_head(grad, head)
        tiles = None if tiles_ref is None else tiles_ref.at[head]
        scores = scores_t(k_ref[:span, :], own, tiles, last)
        probs = jnp.exp(scores - lse_ref[0, head : head + 1, start : start + TILE])
        grad_probs = contract(v_ref[:span, :], own_grad, 1, 1)
        delta = jnp.sum(
            prod_t[head * size : (head + 1) * size, start : start + TILE], 0, keepdims=True
        )
        grad_scores = probs * (grad_probs - delta)
        low = grad_scores.astype(LOW)
        dv_new = contract(probs.astype(LOW), own_grad, 1, 0)
        dk_new = contract(low, own, 1, 0)
        dv = dv_new if dv is None else dv + dv_new
        dk = dk_new if dk is None else dk + dk_new
        dq_t.append(contract(k_t[head * size : (head + 1) * size, :span], low, 1, 0))
        if total_ref is not None:
            for place in range(last + 1):
                off = last - place
                piece = grad_scores[place * TILE : (place + 1) * TILE]
                if first:
                    total_ref[head, off] = piece
                elif off == last:
                    total_ref[head, off] = piece
                else:
                    total_ref[head, off] += piece
    dq_ref[start : start + TILE, :] = jnp.concatenate(dq_t, 0).T.astype(LOW)
    if first:
        dk_acc[:span, :] = dk
        dv_acc[:span, :] = dv
        if span < dk_acc.shape[0]:
            dk_acc[span:, :] = jnp.zeros((dk_acc.shape[0] - span, dk_acc.shape[1]), F32)
            dv_acc[span:, :] = jnp.zeros((dv_acc.shape[0] - span, dv_acc.shape[1]), F32)
    else:
        dk_acc[:span, :] += dk
        dv_acc[:span, :] += dv


def back_kernel(causal, *refs):
    if causal:
        (seq_ref, q_ref, k_ref, v_ref, g_ref, o_ref, lse_ref, z_ref,
         dq_ref, dk_ref, dv_ref, row_ref, dk_acc, dv_acc, tiles_ref, total_ref) = refs
        make_tiles(z_ref, tiles_ref)
    else:
        (q_ref, k_ref, v_ref, g_ref, o_ref, lse_ref,
         dq_ref, dk_ref, dv_ref, dk_acc, dv_acc) = refs
        tiles_ref = total_ref = None
    k_t = k_ref[...].T
    prod_t = (g_ref[...].astype(F32) * o_ref[...].astype(F32)).T
    blocks = q_ref.shape[0] // TILE
    keys = k_ref.shape[0]
    main = (q_ref, k_ref, v_ref, g_ref, lse_ref, dq_ref, dk_acc, dv_acc)
    if not causal:
        for block in range(blocks):
            back_block(main, k_t, prod_t, block * TILE, None, keys, block == 0, None, None)
    else:
        for side in range(keys // q_ref.shape[0]):

            @pl.when(seq_ref[0] == side)
            def _(side=side):
                for block in range(blocks):
                    last = side * blocks + block
                    back_block(
                        main, k_t, prod_t, block * TILE, last, (last + 1) * TILE,
                        block == 0, tiles_ref, total_ref,
                    )
                for head in range(PAIR):
                    for off in range(keys // TILE):
                        if off < (side + 1) * blocks:
                            row_ref[0, head, off : off + 1, :] = skew_sum(total_ref.at[head, off])
                        else:
                            row_ref[0, head, off : off + 1, :] = jnp.zeros((1, 2 * TILE), F32)

    dk_ref[...] = dk_acc[...].astype(LOW)
    dv_ref[...] = dv_acc[...].astype(LOW)


def attend_back(queries, keys_all, values, grad_mixed, mixed, lse, seq_pos, rows):
    count, width = queries.shape
    length = keys_all.shape[0]
    pairs = H // PAIR
    lanes = width // pairs
    offs = length // TILE
    causal = rows is not None
    col = lambda size: pl.BlockSpec((size, lanes), lambda pair, *_: (0, pair))
    in_specs = [col(count), col(length), col(length), col(count), col(count),
                pl.BlockSpec((1, PAIR, count), lambda pair, *_: (pair, 0, 0))]
    out_specs = [col(count), col(length), col(length)]
    out_shape = [
        jax.ShapeDtypeStruct((count, width), LOW),
        jax.ShapeDtypeStruct((length, width), LOW),
        jax.ShapeDtypeStruct((length, width), LOW),
    ]
    args = [queries, keys_all, values, grad_mixed, mixed, lse]
    scratch = [pltpu.VMEM((length, lanes), F32), pltpu.VMEM((length, lanes), F32)]
    if causal:
        row_spec = pl.BlockSpec((1, PAIR, offs, 2 * TILE), lambda pair, *_: (pair, 0, 0, 0))
        in_specs.append(row_spec)
        out_specs.append(row_spec)
        out_shape.append(jax.ShapeDtypeStruct((pairs, PAIR, offs, 2 * TILE), F32))
        args = [seq_pos] + args + [rows]
        scratch += [pltpu.VMEM((PAIR, offs, TILE, TILE), F32)] * 2
    work = H * count * length
    return pl.pallas_call(
        functools.partial(back_kernel, causal),
        grid_spec=pltpu.PrefetchScalarGridSpec(
            num_scalar_prefetch=1 if causal else 0,
            grid=(pairs,),
            in_specs=in_specs,
            out_specs=out_specs,
            scratch_shapes=scratch,
        ),
        out_shape=out_shape,
        cost_estimate=pl.CostEstimate(
            flops=work * 640 * 2, bytes_accessed=12 * length * width, transcendentals=work
        ),
        name="attend_causal_back" if causal else "attend_cross_back",
    )(*args)


def bucket_rows(buckets, length):
    offs = length // TILE
    place = jnp.arange(2 * TILE, dtype=jnp.int32)
    step = jnp.where(place < TILE, place, place - 2 * TILE)
    gap = (jnp.arange(offs, dtype=jnp.int32) * TILE)[:, None] + step[None, :]
    marks = jnp.arange(BUCKETS, dtype=jnp.int32)
    begins = jnp.sum((buckets[None, :] < marks[:, None]).astype(jnp.int32), 1)
    ends = jnp.sum((buckets[None, :] <= marks[:, None]).astype(jnp.int32), 1)
    hot = (gap[None] >= begins[:, None, None]) & (gap[None] < ends[:, None, None])
    return (gap, hot.astype(LOW))


def bit_plan():
    bits = []
    for axis in ("seq", "shard"):
        size = lax.axis_size(axis)
        assert size & (size - 1) == 0
        bits += [(axis, place) for place in reversed(range(size.bit_length() - 1))]
    return bits


def bit_orders(bits):
    ends = [0, len(bits) - 2, len(bits) - 1]
    rest = [place for place in range(len(bits)) if place not in ends]
    return (rest + ends, rest + [ends[1], ends[0], ends[2]])


def coords(bits):
    return [lax.rem(lax.axis_index(axis) // (1 << place), 2) for axis, place in bits]


def partner(bits, which):
    axis, place = bits[which]
    index = lax.axis_index(axis)
    mine = lax.rem(index // (1 << place), 2)
    return {axis: index + (1 - 2 * mine) * (1 << place)}


def greet(bits):
    barrier = pltpu.get_barrier_semaphore()
    for which in range(len(bits)):
        pl.semaphore_signal(
            barrier, inc=1, device_id=partner(bits, which), device_id_type=pl.DeviceIdType.MESH
        )
    pl.semaphore_wait(barrier, len(bits))


def send(bits, which, source, target, sems):
    copy = pltpu.make_async_remote_copy(
        src_ref=source,
        dst_ref=target,
        send_sem=sems[0],
        recv_sem=sems[1],
        device_id=partner(bits, which),
        device_id_type=pl.DeviceIdType.MESH,
    )
    copy.start()
    return copy


def gather_kernel(bits, count, *refs):
    sources, outs = refs[:count], refs[count : 2 * count]
    send_sem, recv_sem, own_sem = refs[2 * count :]
    steps = len(bits)
    place = coords(bits)
    orders = bit_orders(bits)
    owns = []
    for item in range(count):
        own = pltpu.make_async_copy(sources[item], outs[item].at[tuple(place)], own_sem.at[item])
        own.start()
        owns.append(own)
    greet(bits)
    copies = {}
    for turn in range(steps + (count - 1) // 2):
        for item in range(count):
            step = turn - item // 2
            if not 0 <= step < steps:
                continue
            order = orders[item % 2]
            here = tuple(
                slice(None) if which in order[:step] else place[which] for which in range(steps)
            )
            target = outs[item].at[here]
            if step == 1:
                owns[item].wait()
            if step > 0:
                copies[item, step - 1].wait_recv()
            copies[item, step] = send(
                bits,
                order[step],
                sources[item] if step == 0 else target,
                target,
                (send_sem.at[item, step], recv_sem.at[item, step]),
            )
    for item in range(count):
        copies[item, steps - 1].wait_recv()
    for copy in copies.values():
        copy.wait_send()


def gather(items, collective_id):
    bits = bit_plan()
    count = len(items)
    sems = pltpu.SemaphoreType.DMA((count, len(bits)))
    outs = pl.pallas_call(
        functools.partial(gather_kernel, bits, count),
        out_shape=[jax.ShapeDtypeStruct((2,) * len(bits) + x.shape, x.dtype) for x in items],
        in_specs=[pl.BlockSpec(memory_space=pltpu.VMEM)] * count,
        out_specs=[pl.BlockSpec(memory_space=pl.ANY)] * count,
        scratch_shapes=[sems, sems, pltpu.SemaphoreType.DMA((count,))],
        compiler_params=pltpu.CompilerParams(collective_id=collective_id, has_side_effects=True),
        name="gather_rows",
    )(*items)
    return [out.reshape((-1,) + x.shape) for out, x in zip(outs, items)]


def scatter_kernel(bits, count, *refs):
    steps = len(bits)
    sources, outs, work = refs[:count], refs[count : 2 * count], refs[2 * count : 3 * count]
    arrivals = refs[3 * count : (3 + steps) * count]
    load_sem, send_sem, recv_sem = refs[(3 + steps) * count :]
    place = coords(bits)
    orders = [list(reversed(order)) for order in bit_orders(bits)]
    loads = []
    for item in range(count):
        load = pltpu.make_async_copy(sources[item], work[item], load_sem.at[item])
        load.start()
        loads.append(load)
    greet(bits)
    copies = {}

    def add(item, step):
        order = orders[item % 2]
        free = [which for which in range(steps) if which not in order[: step + 1]]
        arrived = arrivals[item * steps + step]
        copies[item, step].wait_recv()
        if not free:
            outs[item][...] = work[item][tuple(place)].astype(F32) + arrived[...].astype(F32)
            return

        @pl.loop(0, 1 << len(free))
        def _(block):
            sub = [lax.rem(block // (1 << (len(free) - 1 - i)), 2) for i in range(len(free))]
            here = tuple(
                sub[free.index(which)] if which in free else place[which] for which in range(steps)
            )
            total = work[item][here].astype(F32) + arrived[tuple(sub)].astype(F32)
            work[item][here] = total.astype(work[item].dtype)

    for turn in range(steps + 1 + (count - 1) // 2):
        for item in range(count):
            step = turn - item // 2
            if not 0 <= step <= steps:
                continue
            if step == 0:
                loads[item].wait()
            else:
                add(item, step - 1)
            if step == steps:
                continue
            order = orders[item % 2]
            there = tuple(
                1 - place[which]
                if which == order[step]
                else (place[which] if which in order[:step] else slice(None))
                for which in range(steps)
            )
            copies[item, step] = send(
                bits,
                order[step],
                work[item].at[there],
                arrivals[item * steps + step],
                (send_sem.at[item, step], recv_sem.at[item, step]),
            )
    for copy in copies.values():
        copy.wait_send()


def scatter(items, collective_id):
    bits = bit_plan()
    steps = len(bits)
    count = len(items)
    sems = pltpu.SemaphoreType.DMA((count, steps))
    owners = 1 << steps
    items = [x.reshape((2,) * steps + (x.shape[0] // owners,) + x.shape[1:]) for x in items]
    tails = [x.shape[steps:] for x in items]
    arrivals = [
        pltpu.VMEM((2,) * (steps - 1 - step) + tail, x.dtype)
        for x, tail in zip(items, tails)
        for step in range(steps)
    ]
    return pl.pallas_call(
        functools.partial(scatter_kernel, bits, count),
        out_shape=[jax.ShapeDtypeStruct(tail, F32) for tail in tails],
        in_specs=[pl.BlockSpec(memory_space=pl.ANY)] * count,
        out_specs=[pl.BlockSpec(memory_space=pltpu.VMEM)] * count,
        scratch_shapes=[pltpu.VMEM(x.shape, x.dtype) for x in items]
        + arrivals
        + [pltpu.SemaphoreType.DMA((count,)), sems, sems],
        compiler_params=pltpu.CompilerParams(collective_id=collective_id, has_side_effects=True),
        name="scatter_rows",
    )(*items)


def dot_low(left, right):
    return contract(left, right, 1, 0)


def dot_left(left, right):
    return contract(left, right, 0, 0)


def dot_right(left, right):
    return contract(left, right, 1, 1)


def rms_norm(value, gain):
    return value * lax.rsqrt(jnp.mean(value * value, -1, keepdims=True) + EPSILON) * gain


def norm_back(value, gain, grad):
    return jax.vjp(rms_norm, value, gain)[1](grad)


def gated(gate, upper):
    return jax.nn.gelu(gate, approximate=True) * upper


def pad_rows(rows, dtype):
    return jnp.stack([jnp.pad(row.astype(dtype), (0, 128 - row.shape[0])) for row in rows] + [
        jnp.zeros((128,), dtype)
    ] * (8 - len(rows)))


def on_device(
    hidden_in,
    encoded,
    cotangent,
    buckets,
    self_query,
    self_key,
    self_value,
    self_out,
    cross_query,
    cross_key,
    cross_value,
    cross_out,
    ff_gate,
    ff_up,
    ff_down,
    norm_self,
    norm_cross,
    norm_ff,
    bias_table,
):
    owners = lax.axis_size("seq") * lax.axis_size("shard")
    seq_pos = lax.axis_index("seq")
    seq_row = seq_pos.reshape(1).astype(jnp.int32)
    low_side = seq_pos == 0
    both = ("seq", "shard")
    width = hidden_in.shape[2]
    own_low = hidden_in[0]
    enc_own = encoded[0]
    before_low = lax.ppermute(own_low, "seq", [(0, 1)])
    enc_other = lax.ppermute(enc_own, "seq", [(0, 1), (1, 0)])
    w_gate_up = lax.all_gather(jnp.concatenate([ff_gate, ff_up], 1), both, axis=0, tiled=True)
    w_down = lax.all_gather(ff_down, both, axis=0, tiled=True)

    small = pad_rows([norm_self, norm_cross, norm_ff, bias_table], LOW)
    gathered = gather(
        [small, self_query, self_key, self_value, self_out, cross_query, cross_key, cross_value,
         cross_out],
        1,
    )
    smalls = gathered[0]
    w_query, w_key, w_value, w_sout, w_cquery, w_ckey, w_cvalue, w_cout = [
        x.reshape(-1, width) for x in gathered[1:]
    ]
    gain_one, gain_two, gain_three = [
        smalls[:, i, : norm_self.shape[0]].reshape(-1).astype(F32) for i in range(3)
    ]
    table = smalls[:, 3, : bias_table.shape[0]].reshape(H, BUCKETS)

    hidden = own_low.astype(F32)
    count = hidden.shape[0]
    length = count * lax.axis_size("seq")
    gap, hot = bucket_rows(buckets, length)
    rows = jnp.einsum("hb,bof->hof", table, hot, preferred_element_type=F32)
    rows = jnp.where(gap[None] >= 0, rows, NEGATIVE).reshape(H // PAIR, PAIR, *gap.shape)

    low_half = jnp.where(low_side, own_low, before_low).astype(F32)
    first = rms_norm(hidden, gain_one).astype(LOW)
    first_all = jnp.concatenate([rms_norm(low_half, gain_one).astype(LOW), first], 0)
    enc_all = jnp.concatenate([enc_own, enc_other], 0)

    query = dot_low(first, w_query).astype(LOW)
    key = dot_low(first_all, w_key).astype(LOW)
    value = dot_low(first_all, w_value).astype(LOW)
    self_mixed, self_lse = attend(query, key, value, seq_row, rows)
    after_self = hidden + dot_low(self_mixed, w_sout)
    second = rms_norm(after_self, gain_two).astype(LOW)
    cross_q = dot_low(second, w_cquery).astype(LOW)
    cross_k = dot_low(enc_all, w_ckey).astype(LOW)
    cross_v = dot_low(enc_all, w_cvalue).astype(LOW)
    cross_mixed, cross_lse = attend(cross_q, cross_k, cross_v, None, None)
    after_cross = after_self + dot_low(cross_mixed, w_cout)
    third = rms_norm(after_cross, gain_three).astype(LOW)
    hidden_units = ff_gate.shape[1]
    gate_up = dot_low(third, w_gate_up)
    gate, upper = gate_up[:, :hidden_units], gate_up[:, hidden_units:]
    inner = gated(gate, upper).astype(LOW)
    hidden_out = (after_cross + dot_low(inner, w_down)).astype(LOW)

    grad_top = cotangent[0]
    grad_wdown = dot_left(inner, grad_top).astype(LOW)
    grad_inner = dot_right(grad_top, w_down)
    grad_gate, grad_upper = jax.vjp(gated, gate, upper)[1](grad_inner)
    grads_low = jnp.concatenate([grad_gate.astype(LOW), grad_upper.astype(LOW)], 1)
    grad_wgate_up = dot_left(third, grads_low).astype(LOW)
    sum_gate_up = lax.psum_scatter(grad_wgate_up, both, scatter_dimension=0, tiled=True)
    grad_third = dot_right(grads_low, w_gate_up)
    norm_grad, grad_gain_three = norm_back(after_cross, gain_three, grad_third)
    grad_cross_res = grad_top.astype(F32) + norm_grad
    cross_res_low = grad_cross_res.astype(LOW)
    grad_wcout = dot_left(cross_mixed, cross_res_low).astype(LOW)
    grad_cross_mix = dot_right(cross_res_low, w_cout).astype(LOW)
    grad_cq, grad_ck, grad_cv = attend_back(
        cross_q, cross_k, cross_v, grad_cross_mix, cross_mixed, cross_lse, None, None
    )
    grad_enc = dot_right(grad_ck, w_ckey) + dot_right(grad_cv, w_cvalue)
    enc_back = lax.ppermute(grad_enc[count:].astype(LOW), "seq", [(0, 1), (1, 0)])
    grad_wcquery = dot_left(second, grad_cq).astype(LOW)
    grad_wckey = dot_left(enc_all, grad_ck).astype(LOW)
    grad_wcvalue = dot_left(enc_all, grad_cv).astype(LOW)
    norm_grad, grad_gain_two = norm_back(after_self, gain_two, dot_right(grad_cq, w_cquery))
    grad_self_res = grad_cross_res + norm_grad
    self_res_low = grad_self_res.astype(LOW)
    grad_wsout = dot_left(self_mixed, self_res_low).astype(LOW)
    grad_self_mix = dot_right(self_res_low, w_sout).astype(LOW)
    grad_q, grad_k, grad_v, grad_rows = attend_back(
        query, key, value, grad_self_mix, self_mixed, self_lse, seq_row, rows
    )
    grad_part = dot_right(grad_k, w_key) + dot_right(grad_v, w_value)
    part_back = lax.ppermute(grad_part[:count].astype(LOW), "seq", [(1, 0)])
    grad_wquery = dot_left(first, grad_q).astype(LOW)
    grad_wkey = dot_left(first_all, grad_k).astype(LOW)
    grad_wvalue = dot_left(first_all, grad_v).astype(LOW)
    grad_first = (
        dot_right(grad_q, w_query)
        + grad_part[count:]
        + jnp.where(low_side, grad_part[:count], 0.0)
        + part_back.astype(F32)
    )
    norm_grad, grad_gain_one = norm_back(hidden, gain_one, grad_first)
    grad_hidden = (grad_self_res + norm_grad).astype(LOW)
    grad_encoded = (grad_enc[:count] + enc_back.astype(F32)).astype(LOW)
    table_grad = jnp.einsum(
        "hof,bof->hb", grad_rows.reshape(H, *gap.shape), hot.astype(F32),
        precision=lax.Precision.HIGHEST,
    )
    small_grads = jnp.stack(
        [
            jnp.pad(x.reshape(owners, -1), ((0, 0), (0, 128 - x.size // owners)))
            for x in (grad_gain_one, grad_gain_two, grad_gain_three, table_grad)
        ]
        + [jnp.zeros((owners, 128), F32)] * 4,
        1,
    ).reshape(owners * 8, 128)
    sums = scatter(
        [grad_wdown, grad_wcout, grad_wcquery, grad_wckey, grad_wcvalue, grad_wsout, grad_wquery,
         grad_wkey, grad_wvalue, small_grads],
        2,
    )
    small_sum = sums[9]
    gains = norm_self.shape[0]
    return (
        hidden_out[None],
        grad_hidden[None],
        grad_encoded[None],
        sums[6],
        sums[7],
        sums[8],
        sums[5],
        sums[2],
        sums[3],
        sums[4],
        sums[1],
        sum_gate_up[:, :hidden_units].astype(F32),
        sum_gate_up[:, hidden_units:].astype(F32),
        sums[0],
        small_sum[0, :gains],
        small_sum[1, :gains],
        small_sum[2, :gains],
        small_sum[3, : bias_table.shape[0]],
    )


def solution(mesh):
    rows = P(("seq", "shard"), None)
    flat = P(("seq", "shard"))
    tokens = P("shard", "seq", None)
    return jax.shard_map(
        on_device,
        mesh=mesh,
        in_specs=(tokens,) * 3 + (P(),) + (rows,) * 11 + (flat,) * 4,
        out_specs=(tokens,) * 3 + (rows,) * 11 + (flat,) * 4,
        check_vma=False,
    )
```

```python
import functools
import jax
import jax.numpy as jnp
from jax import lax
from jax.experimental import pallas as pl
from jax.experimental.pallas import tpu as pltpu
from jax.sharding import PartitionSpec as P

H = 12
BUCKETS = 32
NEGATIVE = -1e30
EPSILON = 1e-06
F32 = jnp.float32
LOW = jnp.bfloat16
PAIR = 2
TILE = 256


def contract(left, right, left_dim, right_dim):
    return lax.dot_general(
        left, right, (((left_dim,), (right_dim,)), ((), ())), preferred_element_type=F32
    )


def keep_head(value, head):
    size = value.shape[1] // PAIR
    lane = lax.broadcasted_iota(jnp.int32, value.shape, 1)
    inside = (lane >= head * size) & (lane < (head + 1) * size)
    return jnp.where(inside, value, jnp.zeros_like(value))


def toeplitz(row):
    wide = jnp.broadcast_to(row, (TILE, 2 * TILE))
    return pltpu.roll(wide, 0, 1, stride=1, stride_axis=0)[:, :TILE]


def skew_sum(total_ref):
    group = 8
    width = 2 * TILE
    summed = jnp.zeros((group, width), F32)
    for start in range(0, TILE, group):
        rows = total_ref[start : start + group, :]
        wide = jnp.concatenate([rows, jnp.zeros_like(rows)], 1)
        summed = summed + pltpu.roll(wide, (width - start) % width, 1)
    out = summed[0:1]
    for row in range(1, group):
        out = out + pltpu.roll(summed[row : row + 1], width - row, 1)
    return out


def scores_t(keys, query, tiles, last):
    scores = contract(keys, query, 1, 1)
    if tiles is None:
        return scores
    parts = [
        scores[place * TILE : (place + 1) * TILE] + tiles[last - place] for place in range(last + 1)
    ]
    return jnp.concatenate(parts, 0) if len(parts) > 1 else parts[0]


def attend_block(q_ref, k_ref, v_t, o_ref, lse_ref, tiles_ref, start, last, span):
    query = q_ref[start : start + TILE, :]
    size = query.shape[1] // PAIR
    mixed = []
    for head in range(PAIR):
        tiles = None if tiles_ref is None else tiles_ref.at[head]
        scores = scores_t(k_ref[:span, :], keep_head(query, head), tiles, last)
        summit = jnp.max(scores, 0, keepdims=True)
        exponent = jnp.exp(scores - summit)
        total = jnp.sum(exponent, 0, keepdims=True)
        weighted = contract(
            v_t[head * size : (head + 1) * size, :span], exponent.astype(LOW), 1, 0
        )
        mixed.append(weighted / total)
        lse_ref[0, head : head + 1, start : start + TILE] = summit + jnp.log(total)
    o_ref[start : start + TILE, :] = jnp.concatenate(mixed, 0).T.astype(LOW)


def attend_kernel(causal, *refs):
    if causal:
        seq_ref, q_ref, k_ref, v_ref, z_ref, o_ref, lse_ref, tiles_ref = refs
        make_tiles(z_ref, tiles_ref)
    else:
        q_ref, k_ref, v_ref, o_ref, lse_ref = refs
    v_t = v_ref[...].T
    blocks = q_ref.shape[0] // TILE
    keys = k_ref.shape[0]
    if not causal:
        for block in range(blocks):
            attend_block(q_ref, k_ref, v_t, o_ref, lse_ref, None, block * TILE, None, keys)
        return
    for side in range(keys // q_ref.shape[0]):

        @pl.when(seq_ref[0] == side)
        def _(side=side):
            for block in range(blocks):
                last = side * blocks + block
                attend_block(
                    q_ref, k_ref, v_t, o_ref, lse_ref, tiles_ref, block * TILE, last,
                    (last + 1) * TILE,
                )


def make_tiles(z_ref, tiles_ref):
    for head in range(PAIR):
        for off in range(z_ref.shape[2]):
            tiles_ref[head, off] = toeplitz(z_ref[0, head, off : off + 1, :])


def attend(queries, keys_all, values, seq_pos, rows):
    count, width = queries.shape
    length = keys_all.shape[0]
    pairs = H // PAIR
    lanes = width // pairs
    offs = length // TILE
    causal = rows is not None
    col = lambda size: pl.BlockSpec((size, lanes), lambda pair, *_: (0, pair))
    in_specs = [col(count), col(length), col(length)]
    args = [queries, keys_all, values]
    scratch = []
    if causal:
        in_specs.append(pl.BlockSpec((1, PAIR, offs, 2 * TILE), lambda pair, *_: (pair, 0, 0, 0)))
        args = [seq_pos] + args + [rows]
        scratch = [pltpu.VMEM((PAIR, offs, TILE, TILE), F32)]
    work = H * count * length
    return pl.pallas_call(
        functools.partial(attend_kernel, causal),
        grid_spec=pltpu.PrefetchScalarGridSpec(
            num_scalar_prefetch=1 if causal else 0,
            grid=(pairs,),
            in_specs=in_specs,
            out_specs=[
                col(count),
                pl.BlockSpec((1, PAIR, count), lambda pair, *_: (pair, 0, 0)),
            ],
            scratch_shapes=scratch,
        ),
        out_shape=[
            jax.ShapeDtypeStruct((count, width), LOW),
            jax.ShapeDtypeStruct((pairs, PAIR, count), F32),
        ],
        cost_estimate=pl.CostEstimate(
            flops=work * 256 * 2, bytes_accessed=6 * length * width, transcendentals=work
        ),
        name="attend_causal" if causal else "attend_cross",
    )(*args)


def back_block(refs, k_t, prod_t, start, last, span, first, tiles_ref, total_ref):
    q_ref, k_ref, v_ref, g_ref, lse_ref, dq_ref, dk_acc, dv_acc = refs
    query = q_ref[start : start + TILE, :]
    grad = g_ref[start : start + TILE, :]
    size = query.shape[1] // PAIR
    dq_t = []
    dk = dv = None
    for head in range(PAIR):
        own = keep_head(query, head)
        own_grad = keep_head(grad, head)
        tiles = None if tiles_ref is None else tiles_ref.at[head]
        scores = scores_t(k_ref[:span, :], own, tiles, last)
        probs = jnp.exp(scores - lse_ref[0, head : head + 1, start : start + TILE])
        grad_probs = contract(v_ref[:span, :], own_grad, 1, 1)
        delta = jnp.sum(
            prod_t[head * size : (head + 1) * size, start : start + TILE], 0, keepdims=True
        )
        grad_scores = probs * (grad_probs - delta)
        low = grad_scores.astype(LOW)
        dv_new = contract(probs.astype(LOW), own_grad, 1, 0)
        dk_new = contract(low, own, 1, 0)
        dv = dv_new if dv is None else dv + dv_new
        dk = dk_new if dk is None else dk + dk_new
        dq_t.append(contract(k_t[head * size : (head + 1) * size, :span], low, 1, 0))
        if total_ref is not None:
            for place in range(last + 1):
                off = last - place
                piece = grad_scores[place * TILE : (place + 1) * TILE]
                if first:
                    total_ref[head, off] = piece
                elif off == last:
                    total_ref[head, off] = piece
                else:
                    total_ref[head, off] += piece
    dq_ref[start : start + TILE, :] = jnp.concatenate(dq_t, 0).T.astype(LOW)
    if first:
        dk_acc[:span, :] = dk
        dv_acc[:span, :] = dv
        if span < dk_acc.shape[0]:
            dk_acc[span:, :] = jnp.zeros((dk_acc.shape[0] - span, dk_acc.shape[1]), F32)
            dv_acc[span:, :] = jnp.zeros((dv_acc.shape[0] - span, dv_acc.shape[1]), F32)
    else:
        dk_acc[:span, :] += dk
        dv_acc[:span, :] += dv


def back_kernel(causal, *refs):
    if causal:
        (seq_ref, q_ref, k_ref, v_ref, g_ref, o_ref, lse_ref, z_ref,
         dq_ref, dk_ref, dv_ref, row_ref, dk_acc, dv_acc, tiles_ref, total_ref) = refs
        make_tiles(z_ref, tiles_ref)
    else:
        (q_ref, k_ref, v_ref, g_ref, o_ref, lse_ref,
         dq_ref, dk_ref, dv_ref, dk_acc, dv_acc) = refs
        tiles_ref = total_ref = None
    k_t = k_ref[...].T
    prod_t = (g_ref[...].astype(F32) * o_ref[...].astype(F32)).T
    blocks = q_ref.shape[0] // TILE
    keys = k_ref.shape[0]
    main = (q_ref, k_ref, v_ref, g_ref, lse_ref, dq_ref, dk_acc, dv_acc)
    if not causal:
        for block in range(blocks):
            back_block(main, k_t, prod_t, block * TILE, None, keys, block == 0, None, None)
    else:
        for side in range(keys // q_ref.shape[0]):

            @pl.when(seq_ref[0] == side)
            def _(side=side):
                for block in range(blocks):
                    last = side * blocks + block
                    back_block(
                        main, k_t, prod_t, block * TILE, last, (last + 1) * TILE,
                        block == 0, tiles_ref, total_ref,
                    )
                for head in range(PAIR):
                    for off in range(keys // TILE):
                        if off < (side + 1) * blocks:
                            row_ref[0, head, off : off + 1, :] = skew_sum(total_ref.at[head, off])
                        else:
                            row_ref[0, head, off : off + 1, :] = jnp.zeros((1, 2 * TILE), F32)

    dk_ref[...] = dk_acc[...].astype(LOW)
    dv_ref[...] = dv_acc[...].astype(LOW)


def attend_back(queries, keys_all, values, grad_mixed, mixed, lse, seq_pos, rows):
    count, width = queries.shape
    length = keys_all.shape[0]
    pairs = H // PAIR
    lanes = width // pairs
    offs = length // TILE
    causal = rows is not None
    col = lambda size: pl.BlockSpec((size, lanes), lambda pair, *_: (0, pair))
    in_specs = [col(count), col(length), col(length), col(count), col(count),
                pl.BlockSpec((1, PAIR, count), lambda pair, *_: (pair, 0, 0))]
    out_specs = [col(count), col(length), col(length)]
    out_shape = [
        jax.ShapeDtypeStruct((count, width), LOW),
        jax.ShapeDtypeStruct((length, width), LOW),
        jax.ShapeDtypeStruct((length, width), LOW),
    ]
    args = [queries, keys_all, values, grad_mixed, mixed, lse]
    scratch = [pltpu.VMEM((length, lanes), F32), pltpu.VMEM((length, lanes), F32)]
    if causal:
        row_spec = pl.BlockSpec((1, PAIR, offs, 2 * TILE), lambda pair, *_: (pair, 0, 0, 0))
        in_specs.append(row_spec)
        out_specs.append(row_spec)
        out_shape.append(jax.ShapeDtypeStruct((pairs, PAIR, offs, 2 * TILE), F32))
        args = [seq_pos] + args + [rows]
        scratch += [pltpu.VMEM((PAIR, offs, TILE, TILE), F32)] * 2
    work = H * count * length
    return pl.pallas_call(
        functools.partial(back_kernel, causal),
        grid_spec=pltpu.PrefetchScalarGridSpec(
            num_scalar_prefetch=1 if causal else 0,
            grid=(pairs,),
            in_specs=in_specs,
            out_specs=out_specs,
            scratch_shapes=scratch,
        ),
        out_shape=out_shape,
        cost_estimate=pl.CostEstimate(
            flops=work * 640 * 2, bytes_accessed=12 * length * width, transcendentals=work
        ),
        name="attend_causal_back" if causal else "attend_cross_back",
    )(*args)


def bucket_rows(buckets, length):
    offs = length // TILE
    place = jnp.arange(2 * TILE, dtype=jnp.int32)
    step = jnp.where(place < TILE, place, place - 2 * TILE)
    gap = (jnp.arange(offs, dtype=jnp.int32) * TILE)[:, None] + step[None, :]
    marks = jnp.arange(BUCKETS, dtype=jnp.int32)
    begins = jnp.sum((buckets[None, :] < marks[:, None]).astype(jnp.int32), 1)
    ends = jnp.sum((buckets[None, :] <= marks[:, None]).astype(jnp.int32), 1)
    hot = (gap[None] >= begins[:, None, None]) & (gap[None] < ends[:, None, None])
    return (gap, hot.astype(LOW))


def bit_plan():
    bits = []
    for axis in ("seq", "shard"):
        size = lax.axis_size(axis)
        assert size & (size - 1) == 0
        bits += [(axis, place) for place in reversed(range(size.bit_length() - 1))]
    return bits


def bit_orders(bits):
    ends = [0, len(bits) - 2, len(bits) - 1]
    rest = [place for place in range(len(bits)) if place not in ends]
    flipped = [ends[1], ends[0], ends[2]]
    return (rest + ends, rest + flipped, ends[:2] + rest + ends[2:])


def coords(bits):
    return [lax.rem(lax.axis_index(axis) // (1 << place), 2) for axis, place in bits]


def partner(bits, which):
    axis, place = bits[which]
    index = lax.axis_index(axis)
    mine = lax.rem(index // (1 << place), 2)
    return {axis: index + (1 - 2 * mine) * (1 << place)}


def greet(bits):
    barrier = pltpu.get_barrier_semaphore()
    for which in range(len(bits)):
        pl.semaphore_signal(
            barrier, inc=1, device_id=partner(bits, which), device_id_type=pl.DeviceIdType.MESH
        )
    pl.semaphore_wait(barrier, len(bits))


def remote(bits, which, source, target, sems):
    return pltpu.make_async_remote_copy(
        src_ref=source,
        dst_ref=target,
        send_sem=sems[0],
        recv_sem=sems[1],
        device_id=partner(bits, which),
        device_id_type=pl.DeviceIdType.MESH,
    )


def send(*args):
    copy = remote(*args)
    copy.start()
    return copy


def scatter_kernel(bits, count, *refs):
    steps = len(bits)
    sources, outs, work = refs[:count], refs[count : 2 * count], refs[2 * count : 3 * count]
    arrivals = refs[3 * count : (3 + steps) * count]
    load_sem, send_sem, recv_sem = refs[(3 + steps) * count :]
    place = coords(bits)
    orders = [list(reversed(order)) for order in bit_orders(bits)[:2]]
    loads = []
    for item in range(count):
        load = pltpu.make_async_copy(sources[item], work[item], load_sem.at[item])
        load.start()
        loads.append(load)
    greet(bits)
    copies = {}

    def add(item, step):
        order = orders[item % 2]
        free = [which for which in range(steps) if which not in order[: step + 1]]
        arrived = arrivals[item * steps + step]
        copies[item, step].wait_recv()
        if not free:
            outs[item][...] = work[item][tuple(place)].astype(F32) + arrived[...].astype(F32)
            return

        @pl.loop(0, 1 << len(free))
        def _(block):
            sub = [lax.rem(block // (1 << (len(free) - 1 - i)), 2) for i in range(len(free))]
            here = tuple(
                sub[free.index(which)] if which in free else place[which] for which in range(steps)
            )
            total = work[item][here].astype(F32) + arrived[tuple(sub)].astype(F32)
            work[item][here] = total.astype(work[item].dtype)

    for turn in range(steps + 1 + (count - 1) // 2):
        for item in range(count):
            step = turn - item // 2
            if not 0 <= step <= steps:
                continue
            if step == 0:
                loads[item].wait()
            else:
                add(item, step - 1)
            if step == steps:
                continue
            order = orders[item % 2]
            there = tuple(
                1 - place[which]
                if which == order[step]
                else (place[which] if which in order[:step] else slice(None))
                for which in range(steps)
            )
            copies[item, step] = send(
                bits,
                order[step],
                work[item].at[there],
                arrivals[item * steps + step],
                (send_sem.at[item, step], recv_sem.at[item, step]),
            )
    for copy in copies.values():
        copy.wait_send()


def scatter(items, collective_id):
    bits = bit_plan()
    steps = len(bits)
    count = len(items)
    sems = pltpu.SemaphoreType.DMA((count, steps))
    owners = 1 << steps
    items = [x.reshape((2,) * steps + (x.shape[0] // owners,) + x.shape[1:]) for x in items]
    tails = [x.shape[steps:] for x in items]
    arrivals = [
        pltpu.VMEM((2,) * (steps - 1 - step) + tail, x.dtype)
        for x, tail in zip(items, tails)
        for step in range(steps)
    ]
    return pl.pallas_call(
        functools.partial(scatter_kernel, bits, count),
        out_shape=[jax.ShapeDtypeStruct(tail, F32) for tail in tails],
        in_specs=[pl.BlockSpec(memory_space=pl.ANY)] * count,
        out_specs=[pl.BlockSpec(memory_space=pltpu.VMEM)] * count,
        scratch_shapes=[pltpu.VMEM(x.shape, x.dtype) for x in items]
        + arrivals
        + [pltpu.SemaphoreType.DMA((count,)), sems, sems],
        compiler_params=pltpu.CompilerParams(collective_id=collective_id, has_side_effects=True),
        name="scatter_rows",
    )(*items)


def table_rows(smalls, table_size, row):
    flat = smalls.reshape(-1, smalls.shape[-1])
    count = table_size * flat.shape[0] // 8
    entry = lax.broadcasted_iota(jnp.int32, (count, flat.shape[0]), 0)
    source = lax.broadcasted_iota(jnp.int32, (count, flat.shape[0]), 1)
    begin = (source >> 3) * table_size
    pick = ((source & 7) == row) & (entry >= begin) & (entry < begin + table_size)
    spread = contract(pick.astype(LOW), flat.astype(LOW), 1, 0)
    lane = lax.broadcasted_iota(jnp.int32, spread.shape, 1)
    place = lax.broadcasted_iota(jnp.int32, spread.shape, 0).astype(F32)
    block = jnp.floor((place + 0.5) * (1.0 / table_size))
    return jnp.where(lane.astype(F32) == place - block * table_size, spread, 0.0)


def gain_row(smalls, size, row):
    flat = smalls.reshape(-1, smalls.shape[-1])
    count = size * flat.shape[0] // 8
    source = lax.broadcasted_iota(jnp.int32, (flat.shape[0], count), 0)
    entry = lax.broadcasted_iota(jnp.int32, (flat.shape[0], count), 1)
    begin = (source >> 3) * size
    pick = ((source & 7) == row) & (entry >= begin) & (entry < begin + size)
    spread = contract(flat.astype(LOW), pick.astype(LOW), 0, 0)
    lane = lax.broadcasted_iota(jnp.int32, spread.shape, 0).astype(F32)
    place = lax.broadcasted_iota(jnp.int32, spread.shape, 1).astype(F32)
    block = jnp.floor((place + 0.5) * (1.0 / size))
    return jnp.sum(jnp.where(lane == place - block * size, spread, 0.0), 0, keepdims=True)


def full_weight(ref):
    value = ref[...].astype(F32)
    return value.reshape(-1, value.shape[-1]).astype(LOW)


ARRAYS = 12
INSIDE = 9
ITEMS = 15
PIECES = tuple((array, None, 0) for array in range(INSIDE)) + tuple(
    (array, axis, half) for array, axis in ((9, 1), (10, 1), (11, 0)) for half in range(2)
)
PATHS = ('zZxyc', 'zZyxc', 'xzZyc', 'xzZyc', 'yzZxc', 'yxzZc', 'xzZyc', 'xzZyc', 'xzZyc', 'xyzZc', 'xzZyc', 'zZyxc', 'zZyxc', 'zZxyc', 'yzZxc')
PLAN = (
    (0, 0, 3), (2, 0, 3), (14, 0, 3), (1, 0, 3), (6, 0, 4), (7, 0, 5),
    (13, 0, 5), (0, 1, 6), (3, 0, 6), (15, 0, 6), (2, 1, 7), (0, 2, 9),
    (1, 1, 9), (13, 1, 10), (3, 1, 10), (0, 3, 12), (1, 2, 12), (6, 1, 14),
    (0, 4, 15), (2, 2, 16), (7, 1, 17), (4, 0, 20), (14, 1, 21), (5, 0, 21),
    (2, 3, 22), (3, 2, 24), (1, 3, 25), (4, 1, 25), (6, 2, 29), (12, 0, 29),
    (3, 3, 29), (2, 4, 31), (11, 0, 31), (5, 1, 32), (13, 2, 33), (1, 4, 34),
    (4, 2, 34), (5, 2, 35), (6, 3, 36), (3, 4, 38), (8, 0, 38), (9, 0, 39),
    (4, 3, 40), (7, 2, 41), (8, 1, 42), (13, 3, 43), (6, 4, 45), (5, 3, 46),
    (10, 0, 47), (16, 0, 48), (4, 4, 49), (10, 1, 50), (7, 3, 52), (13, 4, 54),
    (14, 2, 56), (5, 4, 56), (9, 1, 59), (12, 1, 60), (7, 4, 61), (8, 2, 62),
    (9, 2, 63), (12, 2, 64), (14, 3, 66), (8, 3, 69), (11, 1, 70), (10, 2, 73),
    (12, 3, 75), (11, 2, 76), (14, 4, 77), (9, 3, 77), (8, 4, 79), (10, 3, 80),
    (11, 3, 84), (12, 4, 86), (9, 4, 88), (10, 4, 92), (11, 4, 96),
)


T_SMALL, T_QUERY, T_VALUE, T_SELF, T_AFTER, T_CROSS, T_LAST = 27, 38, 42, 45, 68, 78, 97


def path_bits(bits, path):
    count = len(bits)
    rest = list(range(1, count - 2))
    groups = {"x": [0], "y": [count - 2], "c": [count - 1], "z": rest[:-1], "Z": rest[-1:]}
    return [groups[letter] for letter in path]


def open_kernel(bits, sizes, *refs):
    gain_size, table_size = sizes
    sources = refs[:ARRAYS]
    hidden_ref, enc_ref, hot_ref, mask_ref = refs[ARRAYS : ARRAYS + 4]
    outs = refs[ARRAYS + 4 : 2 * ARRAYS + 4]
    (enc_out, first_out, q_out, k_out, v_out, mixed_out, lse_out, after_out, second_out,
     cq_out, ck_out, cv_out, cmixed_out, clse_out, across_out, third_out,
     before_ref, flat_ref, tiles_ref, weight_ref,
     send_sem, recv_sem, own_sem, side_send, side_recv) = refs[2 * ARRAYS + 4 :]
    steps = len(bits)
    place = coords(bits)
    seq_pos = lax.axis_index("seq")
    rows = hidden_ref.shape[0]
    keys = first_out.shape[0]
    lanes = hidden_ref.shape[1] // (H // PAIR)

    def own(array):
        return pltpu.make_async_copy(
            sources[array], outs[array].at[tuple(place)], own_sem.at[array]
        )

    def copy(item, step):
        order = sum(path_bits(bits, PATHS[item]), [])
        array, axis, half = PIECES[item]
        here = tuple(
            slice(None) if which in order[:step] else place[which] for which in range(steps)
        )
        part = ()
        if axis is not None:
            size = sources[array].shape[axis] // 2
            part = (slice(None),) * axis + (pl.ds(half * size, size),)
        target = outs[array].at[here + part]
        source = target
        if step == 0:
            source = sources[array].at[part] if part else sources[array]
        return remote(
            bits,
            order[step],
            source,
            target,
            (send_sem.at[item, step], recv_sem.at[item, step]),
        )

    def arrived(item):
        copy(item, steps - 1).wait_recv()

    def side(which):
        source, target = ((hidden_ref, before_ref), (enc_ref, enc_out.at[rows:]))[which]
        return remote(bits, 0, source, target, (side_send.at[which], side_recv.at[which]))

    todo = list(PLAN)
    seen = set()

    def advance(until):
        while todo and todo[0][2] < until:
            item, step, _ = todo.pop(0)
            if item >= ITEMS:
                side(item - ITEMS).start()
                continue
            groups = path_bits(bits, PATHS[item])
            first = sum(len(group) for group in groups[:step])
            for number in range(first, first + len(groups[step])):
                if number > 0:
                    if PIECES[item][0] not in seen:
                        seen.add(PIECES[item][0])
                        own(PIECES[item][0]).wait()
                    copy(item, number - 1).wait_recv()
                copy(item, number).start()

    for array in range(ARRAYS):
        own(array).start()
    greet(bits)
    advance(20)
    enc_out[:rows, :] = enc_ref[...]
    advance(T_SMALL)
    arrived(0)
    gains = [gain_row(outs[0][...], gain_size, row) for row in range(3)]
    flat_ref[...] = table_rows(outs[0][...], table_size, 3)

    def normed(value, gain):
        scale = lax.rsqrt(jnp.mean(value * value, -1, keepdims=True) + EPSILON)
        return (value * scale * gain).astype(LOW)

    def over_rows(count, body):
        @pl.loop(0, count // TILE)
        def _(block):
            body(lambda base=0: pl.ds(base + pl.multiple_of(block * TILE, TILE), TILE))

    def normed_rows(source, start):
        def body(at):
            first_out[at(start), :] = normed(source[at(), :].astype(F32), gains[0])

        over_rows(rows, body)

    def project(item, source, out, begin, count):
        weight_ref[...] = full_weight(outs[item])

        def body(at):
            out[at(), :] = contract(source[at(begin), :], weight_ref[...], 1, 0).astype(LOW)

        over_rows(count, body)

    normed_rows(hidden_ref, rows)
    advance(T_QUERY)
    arrived(1)
    project(1, first_out, q_out, rows, rows)
    side(0).wait_recv()

    @pl.when(seq_pos == 0)
    def _():
        first_out[:rows, :] = first_out[rows:, :]

    @pl.when(seq_pos != 0)
    def _():
        normed_rows(before_ref, 0)

    arrived(2)
    project(2, first_out, k_out, 0, keys)
    advance(T_VALUE)
    arrived(3)
    project(3, first_out, v_out, 0, keys)

    advance(T_SELF)

    def between(pair, begin, span):
        for done in range(H // PAIR):

            @pl.when(pair == done)
            def _(done=done):
                advance(begin + span * (done + 1) // (H // PAIR))

    @pl.loop(0, H // PAIR)
    def _(pair):
        at = pl.ds(pl.multiple_of(pair * lanes, lanes), lanes)
        q_ref, k_ref, v_ref, o_ref = (ref.at[:, at] for ref in (q_out, k_out, v_out, mixed_out))
        for head in range(PAIR):
            column = jnp.sum(
                flat_ref[pl.ds(pl.multiple_of((pair * PAIR + head) * BUCKETS, BUCKETS), BUCKETS), :],
                1,
                keepdims=True,
            )
            for off in range(keys // TILE):
                row = jnp.sum(column * hot_ref[off].astype(F32), 0, keepdims=True)
                tiles_ref[head, off] = toeplitz(row + mask_ref[off])
        v_t = v_ref[...].T
        blocks = rows // TILE
        for part in range(keys // rows):

            @pl.when(seq_pos == part)
            def _(part=part):
                for block in range(blocks):
                    last = part * blocks + block
                    attend_block(
                        q_ref, k_ref, v_t, o_ref, lse_out.at[pl.ds(pair, 1)], tiles_ref,
                        block * TILE, last, (last + 1) * TILE,
                    )

        between(pair, T_SELF, T_AFTER - T_SELF)

    def residual(item, mixed, base, total, normal, gain):
        weight_ref[...] = full_weight(outs[item])

        def body(at):
            value = base[at(), :].astype(F32) + contract(mixed[at(), :], weight_ref[...], 1, 0)
            total[at(), :] = value
            normal[at(), :] = normed(value, gain)

        over_rows(rows, body)

    arrived(4)
    residual(4, mixed_out, hidden_ref, after_out, second_out, gains[1])
    arrived(5)
    project(5, second_out, cq_out, 0, rows)
    advance(T_CROSS - 4)
    side(1).wait_recv()
    arrived(6)
    project(6, enc_out, ck_out, 0, keys)
    arrived(7)
    project(7, enc_out, cv_out, 0, keys)
    advance(T_CROSS)

    @pl.loop(0, H // PAIR)
    def _(pair):
        at = pl.ds(pl.multiple_of(pair * lanes, lanes), lanes)
        q_ref, k_ref, v_ref, o_ref = (ref.at[:, at] for ref in (cq_out, ck_out, cv_out, cmixed_out))
        v_t = v_ref[...].T
        for block in range(rows // TILE):
            attend_block(
                q_ref, k_ref, v_t, o_ref, clse_out.at[pl.ds(pair, 1)], None, block * TILE, None, keys
            )
        between(pair, T_CROSS, T_LAST - T_CROSS)

    advance(1000)

    arrived(8)
    residual(8, cmixed_out, after_out, across_out, third_out, gains[2])
    for item in range(INSIDE, ITEMS):
        arrived(item)
    for item in range(ITEMS):
        for step in range(steps):
            copy(item, step).wait_send()
    for which in range(2):
        side(which).wait_send()


def open_layer(items, hidden, encoded, hot, mask, sizes, collective_id):
    bits = bit_plan()
    steps = len(bits)
    count, width = hidden.shape
    length = count * lax.axis_size("seq")
    offs = length // TILE
    sems = pltpu.SemaphoreType.DMA((ITEMS, steps))
    inside = pl.BlockSpec(memory_space=pltpu.VMEM)
    outside = pl.BlockSpec(memory_space=pl.ANY)
    few, many = (count, width), (length, width)
    lse = (H // PAIR, PAIR, count)
    shapes = [((2,) * steps + x.shape, x.dtype) for x in items]
    shapes += [(many, LOW), (many, LOW), (few, LOW), (many, LOW), (many, LOW), (few, LOW)]
    shapes += [(lse, F32), (few, F32), (few, LOW), (few, LOW), (many, LOW), (many, LOW)]
    shapes += [(few, LOW), (lse, F32), (few, F32), (few, LOW)]
    outs = pl.pallas_call(
        functools.partial(open_kernel, bits, sizes),
        out_shape=[jax.ShapeDtypeStruct(*x) for x in shapes],
        in_specs=[inside] * (ARRAYS + 4),
        out_specs=[inside] * INSIDE + [outside] * (ARRAYS - INSIDE) + [inside] * 16,
        scratch_shapes=[
            pltpu.VMEM((count, width), LOW),
            pltpu.VMEM((H * BUCKETS, 128), F32),
            pltpu.VMEM((PAIR, offs, TILE, TILE), F32),
            pltpu.VMEM((width, width), LOW),
            sems,
            sems,
            pltpu.SemaphoreType.DMA((ARRAYS,)),
            pltpu.SemaphoreType.DMA((2,)),
            pltpu.SemaphoreType.DMA((2,)),
        ],
        compiler_params=pltpu.CompilerParams(
            collective_id=collective_id, has_side_effects=True, vmem_limit_bytes=66_000_000
        ),
        name="open_layer",
    )(*items, hidden, encoded, hot, mask)
    return [out.reshape((-1,) + x.shape[-2:]) for out, x in zip(outs, items)] + list(outs[ARRAYS:])


def dot_low(left, right):
    return contract(left, right, 1, 0)


def dot_left(left, right):
    return contract(left, right, 0, 0)


def dot_right(left, right):
    return contract(left, right, 1, 1)


def rms_norm(value, gain):
    return value * lax.rsqrt(jnp.mean(value * value, -1, keepdims=True) + EPSILON) * gain


def norm_back(value, gain, grad):
    return jax.vjp(rms_norm, value, gain)[1](grad)


def gated(gate, upper):
    return jax.nn.gelu(gate, approximate=True) * upper


def pad_rows(rows, dtype):
    return jnp.stack([jnp.pad(row.astype(dtype), (0, 128 - row.shape[0])) for row in rows] + [
        jnp.zeros((128,), dtype)
    ] * (8 - len(rows)))


def on_device(
    hidden_in,
    encoded,
    cotangent,
    buckets,
    self_query,
    self_key,
    self_value,
    self_out,
    cross_query,
    cross_key,
    cross_value,
    cross_out,
    ff_gate,
    ff_up,
    ff_down,
    norm_self,
    norm_cross,
    norm_ff,
    bias_table,
):
    owners = lax.axis_size("seq") * lax.axis_size("shard")
    seq_pos = lax.axis_index("seq")
    seq_row = seq_pos.reshape(1).astype(jnp.int32)
    low_side = seq_pos == 0
    both = ("seq", "shard")
    width = hidden_in.shape[2]
    own_low = hidden_in[0]
    enc_own = encoded[0]
    small = pad_rows([norm_self, norm_cross, norm_ff, bias_table], F32)
    hidden = own_low.astype(F32)
    count = hidden.shape[0]
    length = count * lax.axis_size("seq")
    gap, hot = bucket_rows(buckets, length)
    opened = open_layer(
        [small, self_query, self_key, self_value, self_out, cross_query, cross_key, cross_value,
         cross_out, ff_gate, ff_up, ff_down],
        own_low,
        enc_own,
        jnp.swapaxes(hot, 0, 1),
        jnp.where(gap >= 0, 0.0, NEGATIVE)[:, None, :],
        (norm_self.shape[0], bias_table.shape[0]),
        1,
    )
    smalls = opened[0]
    (w_query, w_key, w_value, w_sout, w_cquery, w_ckey, w_cvalue, w_cout, w_gate, w_up, w_down) = [
        x.reshape(-1, x.shape[-1]) for x in opened[1:12]
    ]
    (enc_all, first_all, query, key, value, self_mixed, self_lse, after_self, second,
     cross_q, cross_k, cross_v, cross_mixed, cross_lse, after_cross, third) = opened[12:]
    gain_one, gain_two, gain_three = [
        smalls[:, i, : norm_self.shape[0]].reshape(-1) for i in range(3)
    ]
    table = smalls[:, 3, : bias_table.shape[0]].reshape(H, BUCKETS)
    rows = jnp.einsum("hb,bof->hof", table.astype(LOW), hot, preferred_element_type=F32)
    rows = jnp.where(gap[None] >= 0, rows, NEGATIVE).reshape(H // PAIR, PAIR, *gap.shape)
    first = first_all[count:]

    hidden_units = ff_gate.shape[1]
    gate = dot_low(third, w_gate)
    upper = dot_low(third, w_up)
    inner = gated(gate, upper).astype(LOW)
    hidden_out = (after_cross + dot_low(inner, w_down)).astype(LOW)

    grad_top = cotangent[0]
    grad_wdown = dot_left(inner, grad_top).astype(LOW)
    grad_inner = dot_right(grad_top, w_down)
    grad_gate, grad_upper = jax.vjp(gated, gate, upper)[1](grad_inner)
    gate_low = grad_gate.astype(LOW)
    upper_low = grad_upper.astype(LOW)
    grad_wgate_up = jnp.concatenate([dot_left(third, gate_low), dot_left(third, upper_low)], 1)
    sum_gate_up = lax.psum_scatter(
        grad_wgate_up.astype(LOW), both, scatter_dimension=0, tiled=True
    )
    grad_third = dot_right(gate_low, w_gate) + dot_right(upper_low, w_up)
    norm_grad, grad_gain_three = norm_back(after_cross, gain_three, grad_third)
    grad_cross_res = grad_top.astype(F32) + norm_grad
    cross_res_low = grad_cross_res.astype(LOW)
    grad_wcout = dot_left(cross_mixed, cross_res_low).astype(LOW)
    grad_cross_mix = dot_right(cross_res_low, w_cout).astype(LOW)
    grad_cq, grad_ck, grad_cv = attend_back(
        cross_q, cross_k, cross_v, grad_cross_mix, cross_mixed, cross_lse, None, None
    )
    grad_enc = dot_right(grad_ck, w_ckey) + dot_right(grad_cv, w_cvalue)
    enc_back = lax.ppermute(grad_enc[count:].astype(LOW), "seq", [(0, 1), (1, 0)])
    grad_wcquery = dot_left(second, grad_cq).astype(LOW)
    grad_wckey = dot_left(enc_all, grad_ck).astype(LOW)
    grad_wcvalue = dot_left(enc_all, grad_cv).astype(LOW)
    norm_grad, grad_gain_two = norm_back(after_self, gain_two, dot_right(grad_cq, w_cquery))
    grad_self_res = grad_cross_res + norm_grad
    self_res_low = grad_self_res.astype(LOW)
    grad_wsout = dot_left(self_mixed, self_res_low).astype(LOW)
    grad_self_mix = dot_right(self_res_low, w_sout).astype(LOW)
    grad_q, grad_k, grad_v, grad_rows = attend_back(
        query, key, value, grad_self_mix, self_mixed, self_lse, seq_row, rows
    )
    grad_part = dot_right(grad_k, w_key) + dot_right(grad_v, w_value)
    part_back = lax.ppermute(grad_part[:count].astype(LOW), "seq", [(1, 0)])
    grad_wquery = dot_left(first, grad_q).astype(LOW)
    grad_wkey = dot_left(first_all, grad_k).astype(LOW)
    grad_wvalue = dot_left(first_all, grad_v).astype(LOW)
    grad_first = (
        dot_right(grad_q, w_query)
        + grad_part[count:]
        + jnp.where(low_side, grad_part[:count], 0.0)
        + part_back.astype(F32)
    )
    norm_grad, grad_gain_one = norm_back(hidden, gain_one, grad_first)
    grad_hidden = (grad_self_res + norm_grad).astype(LOW)
    grad_encoded = (grad_enc[:count] + enc_back.astype(F32)).astype(LOW)
    table_grad = jnp.einsum(
        "hof,bof->hb", grad_rows.reshape(H, *gap.shape), hot.astype(F32),
        precision=lax.Precision.HIGHEST,
    )
    small_grads = jnp.stack(
        [
            jnp.pad(x.reshape(owners, -1), ((0, 0), (0, 128 - x.size // owners)))
            for x in (grad_gain_one, grad_gain_two, grad_gain_three, table_grad)
        ]
        + [jnp.zeros((owners, 128), F32)] * 4,
        1,
    ).reshape(owners * 8, 128)
    sums = scatter(
        [grad_wdown, grad_wcout, grad_wcquery, grad_wckey, grad_wcvalue, grad_wsout, grad_wquery,
         grad_wkey, grad_wvalue, small_grads],
        2,
    )
    small_sum = sums[9]
    gains = norm_self.shape[0]
    return (
        hidden_out[None],
        grad_hidden[None],
        grad_encoded[None],
        sums[6],
        sums[7],
        sums[8],
        sums[5],
        sums[2],
        sums[3],
        sums[4],
        sums[1],
        sum_gate_up[:, :hidden_units].astype(F32),
        sum_gate_up[:, hidden_units:].astype(F32),
        sums[0],
        small_sum[0, :gains],
        small_sum[1, :gains],
        small_sum[2, :gains],
        small_sum[3, : bias_table.shape[0]],
    )


def solution(mesh):
    rows = P(("seq", "shard"), None)
    flat = P(("seq", "shard"))
    tokens = P("shard", "seq", None)
    return jax.shard_map(
        on_device,
        mesh=mesh,
        in_specs=(tokens,) * 3 + (P(),) + (rows,) * 11 + (flat,) * 4,
        out_specs=(tokens,) * 3 + (rows,) * 11 + (flat,) * 4,
        check_vma=False,
    )
```

```python
import functools
import jax
import jax.numpy as jnp
from jax import lax
from jax.experimental import pallas as pl
from jax.experimental.pallas import tpu as pltpu
from jax.sharding import PartitionSpec as P

H = 12
BUCKETS = 32
NEGATIVE = -1e30
EPSILON = 1e-06
F32 = jnp.float32
LOW = jnp.bfloat16
PAIR = 2
TILE = 256


def contract(left, right, left_dim, right_dim):
    return lax.dot_general(
        left, right, (((left_dim,), (right_dim,)), ((), ())), preferred_element_type=F32
    )


def keep_head(value, head):
    size = value.shape[1] // PAIR
    lane = lax.broadcasted_iota(jnp.int32, value.shape, 1)
    inside = (lane >= head * size) & (lane < (head + 1) * size)
    return jnp.where(inside, value, jnp.zeros_like(value))


def toeplitz(row):
    wide = jnp.broadcast_to(row, (TILE, 2 * TILE))
    return pltpu.roll(wide, 0, 1, stride=1, stride_axis=0)[:, :TILE]


def skew_sum(total_ref):
    group = 8
    width = 2 * TILE
    summed = jnp.zeros((group, width), F32)
    for start in range(0, TILE, group):
        rows = total_ref[start : start + group, :]
        wide = jnp.concatenate([rows, jnp.zeros_like(rows)], 1)
        summed = summed + pltpu.roll(wide, (width - start) % width, 1)
    out = summed[0:1]
    for row in range(1, group):
        out = out + pltpu.roll(summed[row : row + 1], width - row, 1)
    return out


def scores_t(keys, query, tiles, last):
    scores = contract(keys, query, 1, 1)
    if tiles is None:
        return scores
    parts = [
        scores[place * TILE : (place + 1) * TILE] + tiles[last - place] for place in range(last + 1)
    ]
    return jnp.concatenate(parts, 0) if len(parts) > 1 else parts[0]


def attend_block(q_ref, k_ref, v_t, o_ref, lse_ref, tiles_ref, start, last, span):
    query = q_ref[start : start + TILE, :]
    size = query.shape[1] // PAIR
    mixed = []
    for head in range(PAIR):
        tiles = None if tiles_ref is None else tiles_ref.at[head]
        scores = scores_t(k_ref[:span, :], keep_head(query, head), tiles, last)
        summit = jnp.max(scores, 0, keepdims=True)
        exponent = jnp.exp(scores - summit)
        total = jnp.sum(exponent, 0, keepdims=True)
        weighted = contract(
            v_t[head * size : (head + 1) * size, :span], exponent.astype(LOW), 1, 0
        )
        mixed.append(weighted / total)
        lse_ref[0, head : head + 1, start : start + TILE] = summit + jnp.log(total)
    o_ref[start : start + TILE, :] = jnp.concatenate(mixed, 0).T.astype(LOW)


def attend_kernel(causal, *refs):
    if causal:
        seq_ref, q_ref, k_ref, v_ref, z_ref, o_ref, lse_ref, tiles_ref = refs
        make_tiles(z_ref, tiles_ref)
    else:
        q_ref, k_ref, v_ref, o_ref, lse_ref = refs
    v_t = v_ref[...].T
    blocks = q_ref.shape[0] // TILE
    keys = k_ref.shape[0]
    if not causal:
        for block in range(blocks):
            attend_block(q_ref, k_ref, v_t, o_ref, lse_ref, None, block * TILE, None, keys)
        return
    for side in range(keys // q_ref.shape[0]):

        @pl.when(seq_ref[0] == side)
        def _(side=side):
            for block in range(blocks):
                last = side * blocks + block
                attend_block(
                    q_ref, k_ref, v_t, o_ref, lse_ref, tiles_ref, block * TILE, last,
                    (last + 1) * TILE,
                )


def make_tiles(z_ref, tiles_ref):
    for head in range(PAIR):
        for off in range(z_ref.shape[2]):
            tiles_ref[head, off] = toeplitz(z_ref[0, head, off : off + 1, :])


def attend(queries, keys_all, values, seq_pos, rows):
    count, width = queries.shape
    length = keys_all.shape[0]
    pairs = H // PAIR
    lanes = width // pairs
    offs = length // TILE
    causal = rows is not None
    col = lambda size: pl.BlockSpec((size, lanes), lambda pair, *_: (0, pair))
    in_specs = [col(count), col(length), col(length)]
    args = [queries, keys_all, values]
    scratch = []
    if causal:
        in_specs.append(pl.BlockSpec((1, PAIR, offs, 2 * TILE), lambda pair, *_: (pair, 0, 0, 0)))
        args = [seq_pos] + args + [rows]
        scratch = [pltpu.VMEM((PAIR, offs, TILE, TILE), F32)]
    work = H * count * length
    return pl.pallas_call(
        functools.partial(attend_kernel, causal),
        grid_spec=pltpu.PrefetchScalarGridSpec(
            num_scalar_prefetch=1 if causal else 0,
            grid=(pairs,),
            in_specs=in_specs,
            out_specs=[
                col(count),
                pl.BlockSpec((1, PAIR, count), lambda pair, *_: (pair, 0, 0)),
            ],
            scratch_shapes=scratch,
        ),
        out_shape=[
            jax.ShapeDtypeStruct((count, width), LOW),
            jax.ShapeDtypeStruct((pairs, PAIR, count), F32),
        ],
        cost_estimate=pl.CostEstimate(
            flops=work * 256 * 2, bytes_accessed=6 * length * width, transcendentals=work
        ),
        name="attend_causal" if causal else "attend_cross",
    )(*args)


def back_block(refs, k_t, prod_t, start, last, span, first, tiles_ref, total_ref):
    q_ref, k_ref, v_ref, g_ref, lse_ref, dq_ref, dk_acc, dv_acc = refs
    query = q_ref[start : start + TILE, :]
    grad = g_ref[start : start + TILE, :]
    size = query.shape[1] // PAIR
    dq_t = []
    dk = dv = None
    for head in range(PAIR):
        own = keep_head(query, head)
        own_grad = keep_head(grad, head)
        tiles = None if tiles_ref is None else tiles_ref.at[head]
        scores = scores_t(k_ref[:span, :], own, tiles, last)
        probs = jnp.exp(scores - lse_ref[0, head : head + 1, start : start + TILE])
        grad_probs = contract(v_ref[:span, :], own_grad, 1, 1)
        delta = jnp.sum(
            prod_t[head * size : (head + 1) * size, start : start + TILE], 0, keepdims=True
        )
        grad_scores = probs * (grad_probs - delta)
        low = grad_scores.astype(LOW)
        dv_new = contract(probs.astype(LOW), own_grad, 1, 0)
        dk_new = contract(low, own, 1, 0)
        dv = dv_new if dv is None else dv + dv_new
        dk = dk_new if dk is None else dk + dk_new
        dq_t.append(contract(k_t[head * size : (head + 1) * size, :span], low, 1, 0))
        if total_ref is not None:
            for place in range(last + 1):
                off = last - place
                piece = grad_scores[place * TILE : (place + 1) * TILE]
                if first:
                    total_ref[head, off] = piece
                elif off == last:
                    total_ref[head, off] = piece
                else:
                    total_ref[head, off] += piece
    dq_ref[start : start + TILE, :] = jnp.concatenate(dq_t, 0).T.astype(LOW)
    if first:
        dk_acc[:span, :] = dk
        dv_acc[:span, :] = dv
        if span < dk_acc.shape[0]:
            dk_acc[span:, :] = jnp.zeros((dk_acc.shape[0] - span, dk_acc.shape[1]), F32)
            dv_acc[span:, :] = jnp.zeros((dv_acc.shape[0] - span, dv_acc.shape[1]), F32)
    else:
        dk_acc[:span, :] += dk
        dv_acc[:span, :] += dv


def back_kernel(causal, *refs):
    if causal:
        (seq_ref, q_ref, k_ref, v_ref, g_ref, o_ref, lse_ref, z_ref,
         dq_ref, dk_ref, dv_ref, row_ref, dk_acc, dv_acc, tiles_ref, total_ref) = refs
        make_tiles(z_ref, tiles_ref)
    else:
        (q_ref, k_ref, v_ref, g_ref, o_ref, lse_ref,
         dq_ref, dk_ref, dv_ref, dk_acc, dv_acc) = refs
        tiles_ref = total_ref = None
    k_t = k_ref[...].T
    prod_t = (g_ref[...].astype(F32) * o_ref[...].astype(F32)).T
    blocks = q_ref.shape[0] // TILE
    keys = k_ref.shape[0]
    main = (q_ref, k_ref, v_ref, g_ref, lse_ref, dq_ref, dk_acc, dv_acc)
    if not causal:
        for block in range(blocks):
            back_block(main, k_t, prod_t, block * TILE, None, keys, block == 0, None, None)
    else:
        for side in range(keys // q_ref.shape[0]):

            @pl.when(seq_ref[0] == side)
            def _(side=side):
                for block in range(blocks):
                    last = side * blocks + block
                    back_block(
                        main, k_t, prod_t, block * TILE, last, (last + 1) * TILE,
                        block == 0, tiles_ref, total_ref,
                    )
                for head in range(PAIR):
                    for off in range(keys // TILE):
                        if off < (side + 1) * blocks:
                            row_ref[0, head, off : off + 1, :] = skew_sum(total_ref.at[head, off])
                        else:
                            row_ref[0, head, off : off + 1, :] = jnp.zeros((1, 2 * TILE), F32)

    dk_ref[...] = dk_acc[...].astype(LOW)
    dv_ref[...] = dv_acc[...].astype(LOW)


def attend_back(queries, keys_all, values, grad_mixed, mixed, lse, seq_pos, rows):
    count, width = queries.shape
    length = keys_all.shape[0]
    pairs = H // PAIR
    lanes = width // pairs
    offs = length // TILE
    causal = rows is not None
    col = lambda size: pl.BlockSpec((size, lanes), lambda pair, *_: (0, pair))
    in_specs = [col(count), col(length), col(length), col(count), col(count),
                pl.BlockSpec((1, PAIR, count), lambda pair, *_: (pair, 0, 0))]
    out_specs = [col(count), col(length), col(length)]
    out_shape = [
        jax.ShapeDtypeStruct((count, width), LOW),
        jax.ShapeDtypeStruct((length, width), LOW),
        jax.ShapeDtypeStruct((length, width), LOW),
    ]
    args = [queries, keys_all, values, grad_mixed, mixed, lse]
    scratch = [pltpu.VMEM((length, lanes), F32), pltpu.VMEM((length, lanes), F32)]
    if causal:
        row_spec = pl.BlockSpec((1, PAIR, offs, 2 * TILE), lambda pair, *_: (pair, 0, 0, 0))
        in_specs.append(row_spec)
        out_specs.append(row_spec)
        out_shape.append(jax.ShapeDtypeStruct((pairs, PAIR, offs, 2 * TILE), F32))
        args = [seq_pos] + args + [rows]
        scratch += [pltpu.VMEM((PAIR, offs, TILE, TILE), F32)] * 2
    work = H * count * length
    return pl.pallas_call(
        functools.partial(back_kernel, causal),
        grid_spec=pltpu.PrefetchScalarGridSpec(
            num_scalar_prefetch=1 if causal else 0,
            grid=(pairs,),
            in_specs=in_specs,
            out_specs=out_specs,
            scratch_shapes=scratch,
        ),
        out_shape=out_shape,
        cost_estimate=pl.CostEstimate(
            flops=work * 640 * 2, bytes_accessed=12 * length * width, transcendentals=work
        ),
        name="attend_causal_back" if causal else "attend_cross_back",
    )(*args)


def bucket_rows(buckets, length):
    offs = length // TILE
    place = jnp.arange(2 * TILE, dtype=jnp.int32)
    step = jnp.where(place < TILE, place, place - 2 * TILE)
    gap = (jnp.arange(offs, dtype=jnp.int32) * TILE)[:, None] + step[None, :]
    marks = jnp.arange(BUCKETS, dtype=jnp.int32)
    begins = jnp.sum((buckets[None, :] < marks[:, None]).astype(jnp.int32), 1)
    ends = jnp.sum((buckets[None, :] <= marks[:, None]).astype(jnp.int32), 1)
    hot = (gap[None] >= begins[:, None, None]) & (gap[None] < ends[:, None, None])
    return (gap, hot.astype(LOW))


def bit_plan():
    bits = []
    for axis in ("seq", "shard"):
        size = lax.axis_size(axis)
        assert size & (size - 1) == 0
        bits += [(axis, place) for place in reversed(range(size.bit_length() - 1))]
    return bits


def bit_orders(bits):
    ends = [0, len(bits) - 2, len(bits) - 1]
    rest = [place for place in range(len(bits)) if place not in ends]
    flipped = [ends[1], ends[0], ends[2]]
    return (rest + ends, rest + flipped, ends[:2] + rest + ends[2:])


def coords(bits):
    return [lax.rem(lax.axis_index(axis) // (1 << place), 2) for axis, place in bits]


def partner(bits, which):
    axis, place = bits[which]
    index = lax.axis_index(axis)
    mine = lax.rem(index // (1 << place), 2)
    return {axis: index + (1 - 2 * mine) * (1 << place)}


def greet(bits):
    barrier = pltpu.get_barrier_semaphore()
    for which in range(len(bits)):
        pl.semaphore_signal(
            barrier, inc=1, device_id=partner(bits, which), device_id_type=pl.DeviceIdType.MESH
        )
    pl.semaphore_wait(barrier, len(bits))


def remote(bits, which, source, target, sems):
    return pltpu.make_async_remote_copy(
        src_ref=source,
        dst_ref=target,
        send_sem=sems[0],
        recv_sem=sems[1],
        device_id=partner(bits, which),
        device_id_type=pl.DeviceIdType.MESH,
    )


def send(*args):
    copy = remote(*args)
    copy.start()
    return copy


def scatter_kernel(bits, count, *refs):
    steps = len(bits)
    sources, outs, work = refs[:count], refs[count : 2 * count], refs[2 * count : 3 * count]
    arrivals = refs[3 * count : (3 + steps) * count]
    load_sem, send_sem, recv_sem = refs[(3 + steps) * count :]
    place = coords(bits)
    orders = [list(reversed(order)) for order in bit_orders(bits)[:2]]
    loads = []
    for item in range(count):
        load = pltpu.make_async_copy(sources[item], work[item], load_sem.at[item])
        load.start()
        loads.append(load)
    greet(bits)
    copies = {}

    def add(item, step):
        order = orders[item % 2]
        free = [which for which in range(steps) if which not in order[: step + 1]]
        arrived = arrivals[item * steps + step]
        copies[item, step].wait_recv()
        if not free:
            outs[item][...] = work[item][tuple(place)].astype(F32) + arrived[...].astype(F32)
            return

        @pl.loop(0, 1 << len(free))
        def _(block):
            sub = [lax.rem(block // (1 << (len(free) - 1 - i)), 2) for i in range(len(free))]
            here = tuple(
                sub[free.index(which)] if which in free else place[which] for which in range(steps)
            )
            total = work[item][here].astype(F32) + arrived[tuple(sub)].astype(F32)
            work[item][here] = total.astype(work[item].dtype)

    for turn in range(steps + 1 + (count - 1) // 2):
        for item in range(count):
            step = turn - item // 2
            if not 0 <= step <= steps:
                continue
            if step == 0:
                loads[item].wait()
            else:
                add(item, step - 1)
            if step == steps:
                continue
            order = orders[item % 2]
            there = tuple(
                1 - place[which]
                if which == order[step]
                else (place[which] if which in order[:step] else slice(None))
                for which in range(steps)
            )
            copies[item, step] = send(
                bits,
                order[step],
                work[item].at[there],
                arrivals[item * steps + step],
                (send_sem.at[item, step], recv_sem.at[item, step]),
            )
    for copy in copies.values():
        copy.wait_send()


def scatter(items, collective_id):
    bits = bit_plan()
    steps = len(bits)
    count = len(items)
    sems = pltpu.SemaphoreType.DMA((count, steps))
    owners = 1 << steps
    items = [x.reshape((2,) * steps + (x.shape[0] // owners,) + x.shape[1:]) for x in items]
    tails = [x.shape[steps:] for x in items]
    arrivals = [
        pltpu.VMEM((2,) * (steps - 1 - step) + tail, x.dtype)
        for x, tail in zip(items, tails)
        for step in range(steps)
    ]
    return pl.pallas_call(
        functools.partial(scatter_kernel, bits, count),
        out_shape=[jax.ShapeDtypeStruct(tail, F32) for tail in tails],
        in_specs=[pl.BlockSpec(memory_space=pl.ANY)] * count,
        out_specs=[pl.BlockSpec(memory_space=pltpu.VMEM)] * count,
        scratch_shapes=[pltpu.VMEM(x.shape, x.dtype) for x in items]
        + arrivals
        + [pltpu.SemaphoreType.DMA((count,)), sems, sems],
        compiler_params=pltpu.CompilerParams(collective_id=collective_id, has_side_effects=True),
        name="scatter_rows",
    )(*items)


def table_rows(smalls, table_size, row):
    flat = smalls.reshape(-1, smalls.shape[-1])
    count = table_size * flat.shape[0] // 8
    entry = lax.broadcasted_iota(jnp.int32, (count, flat.shape[0]), 0)
    source = lax.broadcasted_iota(jnp.int32, (count, flat.shape[0]), 1)
    begin = (source >> 3) * table_size
    pick = ((source & 7) == row) & (entry >= begin) & (entry < begin + table_size)
    spread = contract(pick.astype(LOW), flat.astype(LOW), 1, 0)
    lane = lax.broadcasted_iota(jnp.int32, spread.shape, 1)
    place = lax.broadcasted_iota(jnp.int32, spread.shape, 0).astype(F32)
    block = jnp.floor((place + 0.5) * (1.0 / table_size))
    return jnp.where(lane.astype(F32) == place - block * table_size, spread, 0.0)


def gain_row(smalls, size, row):
    flat = smalls.reshape(-1, smalls.shape[-1])
    count = size * flat.shape[0] // 8
    source = lax.broadcasted_iota(jnp.int32, (flat.shape[0], count), 0)
    entry = lax.broadcasted_iota(jnp.int32, (flat.shape[0], count), 1)
    begin = (source >> 3) * size
    pick = ((source & 7) == row) & (entry >= begin) & (entry < begin + size)
    spread = contract(flat.astype(LOW), pick.astype(LOW), 0, 0)
    lane = lax.broadcasted_iota(jnp.int32, spread.shape, 0).astype(F32)
    place = lax.broadcasted_iota(jnp.int32, spread.shape, 1).astype(F32)
    block = jnp.floor((place + 0.5) * (1.0 / size))
    return jnp.sum(jnp.where(lane == place - block * size, spread, 0.0), 0, keepdims=True)


def full_weight(ref):
    value = ref[...].astype(F32)
    return value.reshape(-1, value.shape[-1]).astype(LOW)


ARRAYS = 12
INSIDE = 9
ITEMS = 15
PIECES = tuple((array, None, 0) for array in range(INSIDE)) + tuple(
    (array, axis, half) for array, axis in ((9, 1), (10, 1), (11, 0)) for half in range(2)
)
PATHS = ('zZxyc', 'zZyxc', 'xzZyc', 'xzZyc', 'yzZxc', 'yxzZc', 'xzZyc', 'xzZyc', 'xzZyc', 'xyzZc', 'xzZyc', 'zZyxc', 'zZyxc', 'zZxyc', 'yzZxc')
PLAN = (
    (0, 0, 3), (2, 0, 3), (14, 0, 3), (1, 0, 3), (6, 0, 4), (7, 0, 5),
    (13, 0, 5), (0, 1, 6), (3, 0, 6), (15, 0, 6), (2, 1, 7), (0, 2, 9),
    (1, 1, 9), (13, 1, 10), (3, 1, 10), (0, 3, 12), (1, 2, 12), (6, 1, 14),
    (0, 4, 15), (2, 2, 16), (7, 1, 17), (4, 0, 20), (14, 1, 21), (5, 0, 21),
    (2, 3, 22), (3, 2, 24), (1, 3, 25), (4, 1, 25), (6, 2, 29), (12, 0, 29),
    (3, 3, 29), (2, 4, 31), (11, 0, 31), (5, 1, 32), (13, 2, 33), (1, 4, 34),
    (4, 2, 34), (5, 2, 35), (6, 3, 36), (3, 4, 38), (8, 0, 38), (9, 0, 39),
    (4, 3, 40), (7, 2, 41), (8, 1, 42), (13, 3, 43), (6, 4, 45), (5, 3, 46),
    (10, 0, 47), (16, 0, 48), (4, 4, 49), (10, 1, 50), (7, 3, 52), (13, 4, 54),
    (14, 2, 56), (5, 4, 56), (9, 1, 59), (12, 1, 60), (7, 4, 61), (8, 2, 62),
    (9, 2, 63), (12, 2, 64), (14, 3, 66), (8, 3, 69), (11, 1, 70), (10, 2, 73),
    (12, 3, 75), (11, 2, 76), (14, 4, 77), (9, 3, 77), (8, 4, 79), (10, 3, 80),
    (11, 3, 84), (12, 4, 86), (9, 4, 88), (10, 4, 92), (11, 4, 96),
)


T_SMALL, T_QUERY, T_VALUE, T_SELF, T_AFTER, T_CROSS, T_LAST = 27, 38, 42, 45, 68, 78, 97


def path_bits(bits, path):
    count = len(bits)
    rest = list(range(1, count - 2))
    groups = {"x": [0], "y": [count - 2], "c": [count - 1], "z": rest[:-1], "Z": rest[-1:]}
    return [groups[letter] for letter in path]


def open_kernel(bits, sizes, *refs):
    gain_size, table_size = sizes
    sources = refs[:ARRAYS]
    hidden_ref, enc_ref, hot_ref, mask_ref = refs[ARRAYS : ARRAYS + 4]
    outs = refs[ARRAYS + 4 : 2 * ARRAYS + 4]
    (enc_out, first_out, q_out, k_out, v_out, mixed_out, lse_out, after_out, second_out,
     cq_out, ck_out, cv_out, cmixed_out, clse_out, across_out, third_out,
     before_ref, flat_ref, tiles_ref, weight_ref,
     send_sem, recv_sem, own_sem, side_send, side_recv) = refs[2 * ARRAYS + 4 :]
    steps = len(bits)
    place = coords(bits)
    seq_pos = lax.axis_index("seq")
    rows = hidden_ref.shape[0]
    keys = first_out.shape[0]
    lanes = hidden_ref.shape[1] // (H // PAIR)

    def own(array):
        return pltpu.make_async_copy(
            sources[array], outs[array].at[tuple(place)], own_sem.at[array]
        )

    def copy(item, step):
        order = sum(path_bits(bits, PATHS[item]), [])
        array, axis, half = PIECES[item]
        here = tuple(
            slice(None) if which in order[:step] else place[which] for which in range(steps)
        )
        part = ()
        if axis is not None:
            size = sources[array].shape[axis] // 2
            part = (slice(None),) * axis + (pl.ds(half * size, size),)
        target = outs[array].at[here + part]
        source = target
        if step == 0:
            source = sources[array].at[part] if part else sources[array]
        return remote(
            bits,
            order[step],
            source,
            target,
            (send_sem.at[item, step], recv_sem.at[item, step]),
        )

    def arrived(item):
        copy(item, steps - 1).wait_recv()

    def side(which):
        source, target = ((hidden_ref, before_ref), (enc_ref, enc_out.at[rows:]))[which]
        return remote(bits, 0, source, target, (side_send.at[which], side_recv.at[which]))

    todo = list(PLAN)
    seen = set()

    def advance(until):
        while todo and todo[0][2] < until:
            item, step, _ = todo.pop(0)
            if item >= ITEMS:
                side(item - ITEMS).start()
                continue
            groups = path_bits(bits, PATHS[item])
            first = sum(len(group) for group in groups[:step])
            for number in range(first, first + len(groups[step])):
                if number > 0:
                    if PIECES[item][0] not in seen:
                        seen.add(PIECES[item][0])
                        own(PIECES[item][0]).wait()
                    copy(item, number - 1).wait_recv()
                copy(item, number).start()

    for array in range(ARRAYS):
        own(array).start()
    greet(bits)
    advance(20)
    enc_out[:rows, :] = enc_ref[...]
    advance(T_SMALL)
    arrived(0)
    gains = [gain_row(outs[0][...], gain_size, row) for row in range(3)]
    flat_ref[...] = table_rows(outs[0][...], table_size, 3)

    def normed(value, gain):
        scale = lax.rsqrt(jnp.mean(value * value, -1, keepdims=True) + EPSILON)
        return (value * scale * gain).astype(LOW)

    def over_rows(count, body):
        @pl.loop(0, count // TILE)
        def _(block):
            body(lambda base=0: pl.ds(base + pl.multiple_of(block * TILE, TILE), TILE))

    def normed_rows(source, start):
        def body(at):
            first_out[at(start), :] = normed(source[at(), :].astype(F32), gains[0])

        over_rows(rows, body)

    def project(item, source, out, begin, count):
        weight_ref[...] = full_weight(outs[item])

        def body(at):
            out[at(), :] = contract(source[at(begin), :], weight_ref[...], 1, 0).astype(LOW)

        over_rows(count, body)

    normed_rows(hidden_ref, rows)
    advance(T_QUERY)
    arrived(1)
    project(1, first_out, q_out, rows, rows)
    side(0).wait_recv()

    @pl.when(seq_pos == 0)
    def _():
        first_out[:rows, :] = first_out[rows:, :]

    @pl.when(seq_pos != 0)
    def _():
        normed_rows(before_ref, 0)

    arrived(2)
    project(2, first_out, k_out, 0, keys)
    advance(T_VALUE)
    arrived(3)
    project(3, first_out, v_out, 0, keys)

    advance(T_SELF)

    def between(pair, begin, span):
        for done in range(H // PAIR):

            @pl.when(pair == done)
            def _(done=done):
                advance(begin + span * (done + 1) // (H // PAIR))

    @pl.loop(0, H // PAIR)
    def _(pair):
        at = pl.ds(pl.multiple_of(pair * lanes, lanes), lanes)
        q_ref, k_ref, v_ref, o_ref = (ref.at[:, at] for ref in (q_out, k_out, v_out, mixed_out))
        for head in range(PAIR):
            column = jnp.sum(
                flat_ref[pl.ds(pl.multiple_of((pair * PAIR + head) * BUCKETS, BUCKETS), BUCKETS), :],
                1,
                keepdims=True,
            )
            for off in range(keys // TILE):
                row = jnp.sum(column * hot_ref[off].astype(F32), 0, keepdims=True)
                tiles_ref[head, off] = toeplitz(row + mask_ref[off])
        v_t = v_ref[...].T
        blocks = rows // TILE
        for part in range(keys // rows):

            @pl.when(seq_pos == part)
            def _(part=part):
                for block in range(blocks):
                    last = part * blocks + block
                    attend_block(
                        q_ref, k_ref, v_t, o_ref, lse_out.at[pl.ds(pair, 1)], tiles_ref,
                        block * TILE, last, (last + 1) * TILE,
                    )

        between(pair, T_SELF, T_AFTER - T_SELF)

    def residual(item, mixed, base, total, normal, gain):
        weight_ref[...] = full_weight(outs[item])

        def body(at):
            value = base[at(), :].astype(F32) + contract(mixed[at(), :], weight_ref[...], 1, 0)
            total[at(), :] = value
            normal[at(), :] = normed(value, gain)

        over_rows(rows, body)

    arrived(4)
    residual(4, mixed_out, hidden_ref, after_out, second_out, gains[1])
    arrived(5)
    project(5, second_out, cq_out, 0, rows)
    advance(T_CROSS - 4)
    side(1).wait_recv()
    arrived(6)
    project(6, enc_out, ck_out, 0, keys)
    arrived(7)
    project(7, enc_out, cv_out, 0, keys)
    advance(T_CROSS)

    @pl.loop(0, H // PAIR)
    def _(pair):
        at = pl.ds(pl.multiple_of(pair * lanes, lanes), lanes)
        q_ref, k_ref, v_ref, o_ref = (ref.at[:, at] for ref in (cq_out, ck_out, cv_out, cmixed_out))
        v_t = v_ref[...].T
        for block in range(rows // TILE):
            attend_block(
                q_ref, k_ref, v_t, o_ref, clse_out.at[pl.ds(pair, 1)], None, block * TILE, None, keys
            )
        between(pair, T_CROSS, T_LAST - T_CROSS)

    advance(1000)

    arrived(8)
    residual(8, cmixed_out, after_out, across_out, third_out, gains[2])
    for item in range(INSIDE, ITEMS):
        arrived(item)
    for item in range(ITEMS):
        for step in range(steps):
            copy(item, step).wait_send()
    for which in range(2):
        side(which).wait_send()


def open_layer(items, hidden, encoded, hot, mask, sizes, collective_id):
    bits = bit_plan()
    steps = len(bits)
    count, width = hidden.shape
    length = count * lax.axis_size("seq")
    offs = length // TILE
    sems = pltpu.SemaphoreType.DMA((ITEMS, steps))
    inside = pl.BlockSpec(memory_space=pltpu.VMEM)
    outside = pl.BlockSpec(memory_space=pl.ANY)
    few, many = (count, width), (length, width)
    lse = (H // PAIR, PAIR, count)
    shapes = [((2,) * steps + x.shape, x.dtype) for x in items]
    shapes += [(many, LOW), (many, LOW), (few, LOW), (many, LOW), (many, LOW), (few, LOW)]
    shapes += [(lse, F32), (few, F32), (few, LOW), (few, LOW), (many, LOW), (many, LOW)]
    shapes += [(few, LOW), (lse, F32), (few, F32), (few, LOW)]
    outs = pl.pallas_call(
        functools.partial(open_kernel, bits, sizes),
        out_shape=[jax.ShapeDtypeStruct(*x) for x in shapes],
        in_specs=[inside] * (ARRAYS + 4),
        out_specs=[inside] * INSIDE + [outside] * (ARRAYS - INSIDE) + [inside] * 16,
        scratch_shapes=[
            pltpu.VMEM((count, width), LOW),
            pltpu.VMEM((H * BUCKETS, 128), F32),
            pltpu.VMEM((PAIR, offs, TILE, TILE), F32),
            pltpu.VMEM((width, width), LOW),
            sems,
            sems,
            pltpu.SemaphoreType.DMA((ARRAYS,)),
            pltpu.SemaphoreType.DMA((2,)),
            pltpu.SemaphoreType.DMA((2,)),
        ],
        compiler_params=pltpu.CompilerParams(
            collective_id=collective_id, has_side_effects=True, vmem_limit_bytes=66_000_000
        ),
        name="open_layer",
    )(*items, hidden, encoded, hot, mask)
    return [out.reshape((-1,) + x.shape[-2:]) for out, x in zip(outs, items)] + list(outs[ARRAYS:])


def reversed_bits(bits, path):
    return list(reversed(sum(path_bits(bits, path), [])))


def close_kernel(bits, sizes, *refs):
    gain_size, table_size = sizes
    (ff_refs, weights, cross_refs, self_refs, (cres_ref, gain3_ref, smalls_ref, hot_ref, mask_ref),
     (after_buf, hidden_buf), (hidden_out, enc_out), outs, (small_out,)) = take(
        refs, (3, 8, 7, 6, 5, 2, 2, 11, 1)
    )
    rest = refs[45:]
    arrivals = rest[: CLOSE_ITEMS * len(bits)]
    (work_ref, load_ref, small_ref, q_buf, k_buf, v_buf, mixed_buf, keys_in_buf,
     query_in_buf, grad_buf, res_buf, weight_buf, enc_own, send_buf, recv_buf, dk_acc, dv_acc,
     tiles_ref, total_ref, rows_ref, flat_ref, send_sem, recv_sem, side_send, side_recv, load_sem,
     fetch_sem) = rest[CLOSE_ITEMS * len(bits) :]
    steps = len(bits)
    place = coords(bits)
    seq_pos = lax.axis_index("seq")
    rows = cres_ref.shape[0]
    keys = k_buf.shape[0]
    lanes = cres_ref.shape[1] // (H // PAIR)

    def pick(names, which, side):
        return tuple(side if name == which else slice(None) for name in names)

    def order_of(item):
        return reversed_bits(bits, CLOSE_PATHS[item])

    def part_of(item):
        if item >= 6:
            return ()
        if item < 4:
            size = ff_refs[item // 2].shape[-1] // 2
            return (slice(None), pl.ds(item % 2 * size, size))
        size = ff_refs[2].shape[-2] // 2
        return (pl.ds(item % 2 * size, size),)

    def base(item):
        if item == SMALL:
            return small_ref
        return ff_refs[item // 2] if item < 6 else work_ref.at[item % SLOTS]

    def arrival(item, step):
        return arrivals[item * steps + step]

    def names_at(item, step):
        order = order_of(item)
        return [which for which in range(steps) if which not in order[:step]]

    def copy(item, step):
        which = order_of(item)[step]
        names = names_at(item, step)
        there = pick(names, which, 1 - place[which])
        if step == 0:
            source = base(item).at[there + part_of(item)]
        else:
            source = arrival(item, step - 1).at[there]
        return remote(
            bits, which, source, arrival(item, step), (send_sem.at[item, step], recv_sem.at[item, step])
        )

    def own_load(item):
        which = order_of(item)[0]
        here = pick(names_at(item, 0), which, place[which])
        block = arrival(item, 0).shape
        target = load_ref.at[
            (item % 2,) + (slice(None),) * (steps - 1) + (pl.ds(0, block[-2]), pl.ds(0, block[-1]))
        ]
        return pltpu.make_async_copy(
            base(item).at[here + part_of(item)], target, load_sem.at[item % 2]
        )

    def add(item, step):
        which = order_of(item)[step]
        names = names_at(item, step)
        free = [name for name in names if name != which]
        target = arrival(item, step)
        block = tuple(slice(0, size) for size in target.shape[-2:])
        copy(item, step).wait_recv()
        if step == 0 and item < 6:
            own_load(item).wait()

        def one(sub):
            here = tuple(place[which] if name == which else sub[free.index(name)] for name in names)
            if step > 0:
                mine = arrival(item, step - 1)[here]
            elif item < 6:
                mine = load_ref[(item % 2,) + tuple(sub) + block]
            elif item == SMALL:
                mine = small_ref[here]
            else:
                mine = work_ref[(item % SLOTS,) + here]
            return mine.astype(F32) + target[tuple(sub)].astype(F32)

        if not free:
            if item == SMALL:
                small_out[...] = one(())
            elif item < 6:
                outs[item // 2][part_of(item)] = one(())
            else:
                outs[item - 3][...] = one(())
            return

        @pl.loop(0, 1 << len(free))
        def _(index):
            sub = [lax.rem(index // (1 << (len(free) - 1 - i)), 2) for i in range(len(free))]
            target[tuple(sub)] = one(sub).astype(target.dtype)

        if step == 0 and item < 4:
            own_load(item + 2).start()

    def side(which):
        return remote(
            bits, 0, send_buf.at[which], recv_buf.at[which], (side_send.at[which], side_recv.at[which])
        )

    todo = list(CLOSE_PLAN)
    ready = set(range(6))
    drained = set()

    def take_next():
        item, step, _ = todo.pop(0)
        groups = list(reversed(path_bits(bits, CLOSE_PATHS[item]))) + [[None]]
        first = sum(len(group) for group in groups[:step])
        for number in range(first, first + len(groups[step])):
            if number > 0:
                add(item, number - 1)
            if number < steps:
                copy(item, number).start()

    def advance(until):
        while todo and todo[0][2] < until and (todo[0][1] > 0 or todo[0][0] in ready):
            take_next()

    def free_slot(item):
        while any(entry[:2] == (item, 1) for entry in todo):
            assert todo[0][1] > 0 or todo[0][0] in ready
            take_next()
        copy(item, 0).wait_send()
        drained.add((item, 0))

    def fetch(source, target, sem):
        return pltpu.make_async_copy(source, target, fetch_sem.at[sem])

    def weight(number):
        return fetch(weights[number], weight_buf.at[number % 2], number % 2)

    def over_rows(count, body):
        @pl.loop(0, count // TILE)
        def _(block):
            body(lambda start=0: pl.ds(start + pl.multiple_of(block * TILE, TILE), TILE))

    def weight_grad(item, left, right):
        if item - SLOTS >= 6:
            free_slot(item - SLOTS)
        half = left.shape[1] // 2
        for side_index in range(2):
            value = contract(left[:, side_index * half : (side_index + 1) * half], right[...], 0, 0)
            shape = work_ref.shape[2:]
            work_ref[item % SLOTS, side_index] = value.reshape(shape).astype(LOW)
        ready.add(item)

    def pairs_back(lse_ref, tiles, begin, span):
        @pl.loop(0, H // PAIR)
        def _(pair):
            at = pl.ds(pl.multiple_of(pair * lanes, lanes), lanes)
            q_ref, k_ref, v_ref, g_ref, o_ref = (
                ref.at[:, at] for ref in (q_buf, k_buf, v_buf, grad_buf, mixed_buf)
            )
            if tiles:
                for head in range(PAIR):
                    start = pl.multiple_of((pair * PAIR + head) * BUCKETS, BUCKETS)
                    column = jnp.sum(flat_ref[pl.ds(start, BUCKETS), :], 1, keepdims=True)
                    for off in range(keys // TILE):
                        row = jnp.sum(column * hot_ref[off].astype(F32), 0, keepdims=True)
                        tiles_ref[head, off] = toeplitz(row + mask_ref[off])
            k_t = k_ref[...].T
            prod_t = (g_ref[...].astype(F32) * o_ref[...].astype(F32)).T
            main = (q_ref, k_ref, v_ref, g_ref, lse_ref.at[pl.ds(pair, 1)], q_ref, dk_acc, dv_acc)
            blocks = rows // TILE
            if not tiles:
                for block in range(blocks):
                    back_block(main, k_t, prod_t, block * TILE, None, keys, block == 0, None, None)
            else:
                for part in range(keys // rows):

                    @pl.when(seq_pos == part)
                    def _(part=part):
                        for block in range(blocks):
                            last = part * blocks + block
                            back_block(
                                main, k_t, prod_t, block * TILE, last, (last + 1) * TILE,
                                block == 0, tiles_ref, total_ref,
                            )
                        for head in range(PAIR):
                            column = jnp.zeros((BUCKETS, 1), F32)
                            for off in range((part + 1) * blocks):
                                row = skew_sum(total_ref.at[head, off])
                                column = column + jnp.sum(
                                    hot_ref[off].astype(F32) * row, 1, keepdims=True
                                )
                            start = pl.multiple_of((pair * PAIR + head) * BUCKETS, BUCKETS)
                            rows_ref[pl.ds(start, BUCKETS), :] = jnp.broadcast_to(
                                column, (BUCKETS, rows_ref.shape[1])
                            )

            k_ref[...] = dk_acc[...].astype(LOW)
            v_ref[...] = dv_acc[...].astype(LOW)
            for done in range(H // PAIR):

                @pl.when(pair == done)
                def _(done=done):
                    advance(begin + span * (done + 1) // (H // PAIR))

    def norm_back_rows(value, gain, grad):
        scale = lax.rsqrt(jnp.mean(value * value, -1, keepdims=True) + EPSILON)
        scaled = gain * grad
        inner = jnp.mean(value * scaled, -1, keepdims=True)
        back = scale * scaled - value * (scale * scale * scale) * inner
        return back, jnp.sum(grad * value * scale, 0, keepdims=True)

    cq_in, ck_in, cv_in, cmixed_in, enc_in, second_in, clse_ref = cross_refs
    q_in, k_in, v_in, mixed_in, first_in, lse_ref = self_refs[:6]
    fetches = [
        fetch(cmixed_in, mixed_buf, 2), fetch(cq_in, q_buf, 3), fetch(ck_in, k_buf, 4),
        fetch(cv_in, v_buf, 5), fetch(enc_in, keys_in_buf, 6), fetch(second_in, query_in_buf, 7),
    ]
    weight(0).start()
    weight(1).start()
    own_load(0).start()
    own_load(1).start()
    for one in fetches:
        one.start()
    greet(bits)
    advance(1)
    flat_ref[...] = table_rows(smalls_ref[...], table_size, 3)
    gain_one = gain_row(smalls_ref[...], gain_size, 0)
    gain_two = gain_row(smalls_ref[...], gain_size, 1)

    def to_mixed(number, source):
        weight(number).wait()

        def body(at):
            grad_buf[at(), :] = contract(
                source[at(), :].astype(LOW), weight_buf[number % 2], 1, 1
            ).astype(LOW)

        over_rows(rows, body)
        weight(number + 2).start()

    to_mixed(0, cres_ref)
    fetches[0].wait()

    def low_rows(source, target):
        def body(at):
            target[at(), :] = source[at(), :].astype(LOW)

        over_rows(rows, body)

    low_rows(cres_ref, send_buf.at[0])
    weight_grad(6, mixed_buf, send_buf.at[0])
    advance(5)
    for one in fetches[1:4]:
        one.wait()
    pairs_back(clse_ref, False, 5, 20)
    fetch(mixed_in, mixed_buf, 2).start()

    def both_back(numbers, keep, count):
        def body_other(at):
            total = contract(k_buf[at(count), :], weight_buf[numbers[0] % 2], 1, 1)
            total = total + contract(v_buf[at(count), :], weight_buf[numbers[1] % 2], 1, 1)
            send_buf[keep[0], at(), :] = total.astype(LOW)

        def body_own(at):
            begin = 0 if count else rows
            total = contract(k_buf[at(begin), :], weight_buf[numbers[0] % 2], 1, 1)
            total = total + contract(v_buf[at(begin), :], weight_buf[numbers[1] % 2], 1, 1)
            keep[1][at(), :] = total

        over_rows(rows, body_other)
        return body_own

    weight(1).wait()
    weight(2).wait()
    own_part = both_back((1, 2), (0, enc_own), rows)
    side(0).start()
    for one in fetches[4:]:
        one.wait()
    weight_grad(7, keys_in_buf, k_buf)
    advance(30)
    weight_grad(8, keys_in_buf, v_buf)
    advance(32)
    over_rows(rows, own_part)
    fetch(k_in, k_buf, 4).start()
    fetch(v_in, v_buf, 5).start()
    fetch(first_in, keys_in_buf, 6).start()
    weight(3).start()
    weight(4).start()
    weight_grad(9, query_in_buf, q_buf)
    advance(35)
    weight(3).wait()
    sums = [jnp.zeros((1, cres_ref.shape[1]), F32)] * 2
    for block in range(rows // TILE):
        at = slice(block * TILE, (block + 1) * TILE)
        grad = contract(q_buf[at, :], weight_buf[1], 1, 1)
        back, total = norm_back_rows(after_buf[at, :], gain_two, grad)
        sums[1] = sums[1] + total
        res_buf[at, :] = cres_ref[at, :] + back
    fetch(q_in, q_buf, 3).start()
    weight(5).start()
    weight(4).wait()

    def body(at):
        grad_buf[at(), :] = contract(res_buf[at(), :].astype(LOW), weight_buf[0], 1, 1).astype(LOW)

    over_rows(rows, body)
    weight(6).start()
    fetch(mixed_in, mixed_buf, 2).wait()
    low_rows(res_buf, query_in_buf)
    weight_grad(10, mixed_buf, query_in_buf)
    advance(40)
    fetch(q_in, q_buf, 3).wait()
    fetch(k_in, k_buf, 4).wait()
    fetch(v_in, v_buf, 5).wait()
    pairs_back(lse_ref, True, 40, 24)
    side(0).wait_recv()

    def body(at):
        enc_out[at(), :] = (enc_own[at(), :] + recv_buf[0, at(), :].astype(F32)).astype(LOW)

    over_rows(rows, body)
    weight(5).wait()
    weight(6).wait()
    own_part = both_back((5, 6), (1, enc_own), 0)

    @pl.when(seq_pos != 0)
    def _():
        side(1).start()

    over_rows(rows, own_part)
    weight(7).start()
    fetch(first_in, keys_in_buf, 6).wait()
    weight_grad(11, keys_in_buf, v_buf)
    advance(70)
    weight_grad(12, keys_in_buf, k_buf)
    advance(73)
    weight_grad(13, keys_in_buf.at[rows:], q_buf)
    advance(76)
    weight(7).wait()

    @pl.when(seq_pos == 0)
    def _():
        side(1).wait_recv()

    @pl.when(seq_pos != 0)
    def _():
        side(1).wait_send()

    own_low = (seq_pos == 0).astype(F32)
    for block in range(rows // TILE):
        at = slice(block * TILE, (block + 1) * TILE)
        grad = contract(q_buf[at, :], weight_buf[1], 1, 1) + enc_own[at, :]
        low = send_buf[1, at, :].astype(F32) + jnp.where(
            seq_pos == 0, recv_buf[1, at, :].astype(F32), 0.0
        )
        grad = grad + own_low * low
        back, total = norm_back_rows(hidden_buf[at, :].astype(F32), gain_one, grad)
        sums[0] = sums[0] + total
        hidden_out[at, :] = (res_buf[at, :] + back).astype(LOW)
    small_ref[...] = small_rows(
        sums[0], sums[1], gain3_ref[...], rows_ref[...], gain_size, table_size, small_ref.shape
    )
    ready.add(SMALL)
    advance(1000)
    assert not todo
    for item in range(CLOSE_ITEMS):
        for step in range(steps):
            if (item, step) not in drained:
                copy(item, step).wait_send()
    side(0).wait_send()


def take(refs, counts):
    out = []
    begin = 0
    for count in counts:
        out.append(refs[begin : begin + count])
        begin += count
    return out


def small_rows(one, two, three, table, gain_size, table_size, shape):
    owners = one.shape[1] // gain_size

    def spread(source, size, row):
        count = owners * size
        target = lax.broadcasted_iota(jnp.int32, (owners * 8, count), 0)
        entry = lax.broadcasted_iota(jnp.int32, (owners * 8, count), 1)
        begin = (target >> 3) * size
        hot = ((target & 7) == row) & (entry >= begin) & (entry < begin + size)
        return lax.dot_general(
            hot.astype(F32), source, (((1,), (0 if row == 3 else 1,)), ((), ())),
            precision=lax.Precision.HIGHEST, preferred_element_type=F32,
        )

    def wheel(shape, axis, size):
        entry = lax.broadcasted_iota(jnp.int32, shape, axis).astype(F32)
        lane = lax.broadcasted_iota(jnp.int32, shape, 1 - axis).astype(F32)
        return lane == entry - size * jnp.floor((entry + 0.5) * (1.0 / size))

    total = jnp.zeros((owners * 8, 128), F32)
    for row, value in enumerate((one, two, three)):
        grid = (128, value.shape[1])
        total = total + spread(
            jnp.where(wheel(grid, 1, gain_size), jnp.broadcast_to(value, grid), 0.0), gain_size, row
        )
    total = total + spread(jnp.where(wheel(table.shape, 0, table_size), table, 0.0), table_size, 3)
    return total.reshape(shape)


SLOTS = 2
SMALL = 14
CLOSE_ITEMS = 15
CLOSE_PATHS = ('xzZyc', 'xyzZc', 'yzZxc', 'xzZyc', 'zZyxc', 'zZyxc', 'zZxyc', 'zZxyc', 'xyzZc', 'xzZyc', 'zZxyc', 'xzZyc', 'zZxyc', 'xyzZc', 'zZxyc')
CLOSE_PLAN = (
    (0, 0, 3), (1, 0, 5), (2, 0, 7), (0, 1, 8), (3, 0, 10), (1, 1, 10),
    (4, 0, 12), (2, 1, 12), (5, 0, 14), (6, 0, 16), (3, 1, 17), (0, 2, 20),
    (5, 1, 21), (1, 2, 22), (6, 1, 26), (2, 2, 29), (7, 0, 29), (4, 1, 30),
    (0, 3, 31), (8, 0, 31), (7, 1, 33), (9, 0, 35), (8, 1, 36), (2, 3, 36),
    (10, 0, 39), (0, 4, 40), (5, 2, 40), (0, 5, 43), (4, 2, 45), (3, 2, 45),
    (8, 2, 45), (2, 4, 49), (1, 3, 50), (3, 3, 52), (9, 1, 53), (2, 5, 53),
    (5, 3, 55), (4, 3, 57), (7, 2, 59), (10, 1, 59), (5, 4, 60), (4, 4, 62),
    (1, 4, 62), (9, 2, 63), (6, 2, 64), (5, 5, 65), (1, 5, 66), (8, 3, 66),
    (7, 3, 67), (3, 4, 67), (4, 5, 68), (9, 3, 69), (11, 0, 70), (3, 5, 70),
    (6, 3, 71), (12, 0, 73), (7, 4, 73), (11, 1, 74), (13, 0, 75), (6, 4, 76),
    (7, 5, 78), (13, 1, 79), (6, 5, 80), (12, 1, 81), (14, 0, 81), (11, 2, 86),
    (9, 4, 86), (10, 2, 87), (14, 1, 88), (13, 2, 89), (9, 5, 90), (12, 2, 91),
    (10, 3, 93), (14, 2, 94), (8, 4, 94), (11, 3, 96), (14, 3, 97), (8, 5, 97),
    (12, 3, 98), (10, 4, 99), (13, 3, 99), (14, 4, 101), (12, 4, 102), (11, 4, 103),
    (13, 4, 104), (10, 5, 104), (14, 5, 104), (11, 5, 106), (12, 5, 107), (13, 5, 107),
)


def close_layer(ff_grads, weights, cross, own, cres, after, hidden, gain3, smalls, hot, mask, sizes,
                collective_id):
    bits = bit_plan()
    steps = len(bits)
    owners = 1 << steps
    count, width = cres.shape
    length = cross[1].shape[0]
    offs = length // TILE
    lanes = width // (H // PAIR)
    split_rows = lambda x: x.reshape((2,) * steps + (x.shape[0] // owners,) + x.shape[1:])
    ff_grads = [split_rows(x) for x in ff_grads]
    gate, down = ff_grads[0].shape[steps:], ff_grads[2].shape[steps:]
    square = (width // owners, width)
    blocks = [(gate[0], gate[1] // 2)] * 4 + [(down[0] // 2, down[1])] * 2 + [square] * 8
    kinds = [LOW] * 14 + [F32]
    blocks.append((8, 128))
    arrivals = [
        pltpu.VMEM((2,) * (steps - 1 - step) + block, kind)
        for block, kind in zip(blocks, kinds)
        for step in range(steps)
    ]
    load_block = (max(gate[0], down[0] // 2), max(gate[1] // 2, down[1]))
    inside = pl.BlockSpec(memory_space=pltpu.VMEM)
    outside = pl.BlockSpec(memory_space=pl.ANY)
    few, many = (count, width), (length, width)
    vm = pltpu.VMEM
    sems = pltpu.SemaphoreType.DMA((CLOSE_ITEMS, steps))
    pair_sem = pltpu.SemaphoreType.DMA((2,))
    return pl.pallas_call(
        functools.partial(close_kernel, bits, sizes),
        out_shape=[jax.ShapeDtypeStruct(few, LOW)] * 2
        + [jax.ShapeDtypeStruct(block, F32) for block in (gate, gate, down)]
        + [jax.ShapeDtypeStruct(square, F32)] * 8
        + [jax.ShapeDtypeStruct((8, 128), F32)],
        in_specs=[outside] * (3 + 8) + [outside] * 6 + [inside] + [outside] * 5 + [inside]
        + [inside] * 5 + [inside] * 2,
        out_specs=[inside] * 14,
        scratch_shapes=arrivals
        + [
            vm((SLOTS,) + (2,) * steps + square, LOW),
            vm((2,) + (2,) * (steps - 1) + load_block, LOW),
            vm((2,) * steps + (8, 128), F32),
            vm(few, LOW), vm(many, LOW), vm(many, LOW), vm(few, LOW), vm(many, LOW),
            vm(few, LOW), vm(few, LOW), vm(few, F32),
            vm((2, width, width), LOW), vm(few, F32), vm((2,) + few, LOW), vm((2,) + few, LOW),
            vm((length, lanes), F32), vm((length, lanes), F32),
            vm((PAIR, offs, TILE, TILE), F32), vm((PAIR, offs, TILE, TILE), F32),
            vm((H * BUCKETS, 128), F32), vm((H * BUCKETS, 128), F32),
            sems, sems, pair_sem, pair_sem, pair_sem, pltpu.SemaphoreType.DMA((8,)),
        ],
        compiler_params=pltpu.CompilerParams(
            collective_id=collective_id, has_side_effects=True, vmem_limit_bytes=67_000_000
        ),
        name="close_layer",
    )(*ff_grads, *weights, *cross, *own, cres, gain3, smalls, hot, mask, after, hidden)


def dot_low(left, right):
    return contract(left, right, 1, 0)


def dot_left(left, right):
    return contract(left, right, 0, 0)


def dot_right(left, right):
    return contract(left, right, 1, 1)


def rms_norm(value, gain):
    return value * lax.rsqrt(jnp.mean(value * value, -1, keepdims=True) + EPSILON) * gain


def norm_back(value, gain, grad):
    return jax.vjp(rms_norm, value, gain)[1](grad)


def gated(gate, upper):
    return jax.nn.gelu(gate, approximate=True) * upper


def pad_rows(rows, dtype):
    return jnp.stack([jnp.pad(row.astype(dtype), (0, 128 - row.shape[0])) for row in rows] + [
        jnp.zeros((128,), dtype)
    ] * (8 - len(rows)))


def on_device(
    hidden_in,
    encoded,
    cotangent,
    buckets,
    self_query,
    self_key,
    self_value,
    self_out,
    cross_query,
    cross_key,
    cross_value,
    cross_out,
    ff_gate,
    ff_up,
    ff_down,
    norm_self,
    norm_cross,
    norm_ff,
    bias_table,
):
    owners = lax.axis_size("seq") * lax.axis_size("shard")
    seq_pos = lax.axis_index("seq")
    seq_row = seq_pos.reshape(1).astype(jnp.int32)
    low_side = seq_pos == 0
    both = ("seq", "shard")
    width = hidden_in.shape[2]
    own_low = hidden_in[0]
    enc_own = encoded[0]
    small = pad_rows([norm_self, norm_cross, norm_ff, bias_table], F32)
    hidden = own_low.astype(F32)
    count = hidden.shape[0]
    length = count * lax.axis_size("seq")
    gap, hot = bucket_rows(buckets, length)
    hot_rows = jnp.swapaxes(hot, 0, 1)
    hot_mask = jnp.where(gap >= 0, 0.0, NEGATIVE)[:, None, :]
    opened = open_layer(
        [small, self_query, self_key, self_value, self_out, cross_query, cross_key, cross_value,
         cross_out, ff_gate, ff_up, ff_down],
        own_low,
        enc_own,
        hot_rows,
        hot_mask,
        (norm_self.shape[0], bias_table.shape[0]),
        1,
    )
    smalls = opened[0]
    (w_query, w_key, w_value, w_sout, w_cquery, w_ckey, w_cvalue, w_cout, w_gate, w_up, w_down) = [
        x.reshape(-1, x.shape[-1]) for x in opened[1:12]
    ]
    (enc_all, first_all, query, key, value, self_mixed, self_lse, after_self, second,
     cross_q, cross_k, cross_v, cross_mixed, cross_lse, after_cross, third) = opened[12:]
    gain_one, gain_two, gain_three = [
        smalls[:, i, : norm_self.shape[0]].reshape(-1) for i in range(3)
    ]
    table = smalls[:, 3, : bias_table.shape[0]].reshape(H, BUCKETS)
    rows = jnp.einsum("hb,bof->hof", table.astype(LOW), hot, preferred_element_type=F32)
    rows = jnp.where(gap[None] >= 0, rows, NEGATIVE).reshape(H // PAIR, PAIR, *gap.shape)
    first = first_all[count:]

    gate = dot_low(third, w_gate)
    upper = dot_low(third, w_up)
    inner = gated(gate, upper).astype(LOW)
    hidden_out = (after_cross + dot_low(inner, w_down)).astype(LOW)

    grad_top = cotangent[0]
    grad_wdown = dot_left(inner, grad_top).astype(LOW)
    grad_inner = dot_right(grad_top, w_down)
    grad_gate, grad_upper = jax.vjp(gated, gate, upper)[1](grad_inner)
    gate_low = grad_gate.astype(LOW)
    upper_low = grad_upper.astype(LOW)
    grad_wgate = dot_left(third, gate_low).astype(LOW)
    grad_wup = dot_left(third, upper_low).astype(LOW)
    grad_third = dot_right(gate_low, w_gate) + dot_right(upper_low, w_up)
    norm_grad, grad_gain_three = norm_back(after_cross, gain_three, grad_third)
    grad_cross_res = grad_top.astype(F32) + norm_grad
    gains = norm_self.shape[0]
    if width // owners >= 16:
        grad_hidden, grad_encoded, *sums, small_sum = close_layer(
            [grad_wgate, grad_wup, grad_wdown],
            [w_cout, w_ckey, w_cvalue, w_cquery, w_sout, w_key, w_value, w_query],
            [cross_q, cross_k, cross_v, cross_mixed, enc_all, second, cross_lse],
            [query, key, value, self_mixed, first_all, self_lse],
            grad_cross_res,
            after_self,
            own_low,
            grad_gain_three.reshape(1, -1),
            smalls,
            hot_rows,
            hot_mask,
            (gains, bias_table.shape[0]),
            2,
        )
        return (
            hidden_out[None],
            grad_hidden[None],
            grad_encoded[None],
            sums[10],
            sums[9],
            sums[8],
            sums[7],
            sums[6],
            sums[4],
            sums[5],
            sums[3],
            sums[0],
            sums[1],
            sums[2],
            small_sum[0, :gains],
            small_sum[1, :gains],
            small_sum[2, :gains],
            small_sum[3, : bias_table.shape[0]],
        )
    sum_gate, sum_up = [
        lax.psum_scatter(x, both, scatter_dimension=0, tiled=True).astype(F32)
        for x in (grad_wgate, grad_wup)
    ]
    cross_res_low = grad_cross_res.astype(LOW)
    grad_wcout = dot_left(cross_mixed, cross_res_low).astype(LOW)
    grad_cross_mix = dot_right(cross_res_low, w_cout).astype(LOW)
    grad_cq, grad_ck, grad_cv = attend_back(
        cross_q, cross_k, cross_v, grad_cross_mix, cross_mixed, cross_lse, None, None
    )
    grad_enc = dot_right(grad_ck, w_ckey) + dot_right(grad_cv, w_cvalue)
    enc_back = lax.ppermute(grad_enc[count:].astype(LOW), "seq", [(0, 1), (1, 0)])
    grad_wcquery = dot_left(second, grad_cq).astype(LOW)
    grad_wckey = dot_left(enc_all, grad_ck).astype(LOW)
    grad_wcvalue = dot_left(enc_all, grad_cv).astype(LOW)
    norm_grad, grad_gain_two = norm_back(after_self, gain_two, dot_right(grad_cq, w_cquery))
    grad_self_res = grad_cross_res + norm_grad
    self_res_low = grad_self_res.astype(LOW)
    grad_wsout = dot_left(self_mixed, self_res_low).astype(LOW)
    grad_self_mix = dot_right(self_res_low, w_sout).astype(LOW)
    grad_q, grad_k, grad_v, grad_rows = attend_back(
        query, key, value, grad_self_mix, self_mixed, self_lse, seq_row, rows
    )
    grad_part = dot_right(grad_k, w_key) + dot_right(grad_v, w_value)
    part_back = lax.ppermute(grad_part[:count].astype(LOW), "seq", [(1, 0)])
    grad_wquery = dot_left(first, grad_q).astype(LOW)
    grad_wkey = dot_left(first_all, grad_k).astype(LOW)
    grad_wvalue = dot_left(first_all, grad_v).astype(LOW)
    grad_first = (
        dot_right(grad_q, w_query)
        + grad_part[count:]
        + jnp.where(low_side, grad_part[:count], 0.0)
        + part_back.astype(F32)
    )
    norm_grad, grad_gain_one = norm_back(hidden, gain_one, grad_first)
    grad_hidden = (grad_self_res + norm_grad).astype(LOW)
    grad_encoded = (grad_enc[:count] + enc_back.astype(F32)).astype(LOW)
    table_grad = jnp.einsum(
        "hof,bof->hb", grad_rows.reshape(H, *gap.shape), hot.astype(F32),
        precision=lax.Precision.HIGHEST,
    )
    small_grads = jnp.stack(
        [
            jnp.pad(x.reshape(owners, -1), ((0, 0), (0, 128 - x.size // owners)))
            for x in (grad_gain_one, grad_gain_two, grad_gain_three, table_grad)
        ]
        + [jnp.zeros((owners, 128), F32)] * 4,
        1,
    ).reshape(owners * 8, 128)
    sums = scatter(
        [grad_wdown, grad_wcout, grad_wcquery, grad_wckey, grad_wcvalue, grad_wsout, grad_wquery,
         grad_wkey, grad_wvalue, small_grads],
        2,
    )
    small_sum = sums[9]
    return (
        hidden_out[None],
        grad_hidden[None],
        grad_encoded[None],
        sums[6],
        sums[7],
        sums[8],
        sums[5],
        sums[2],
        sums[3],
        sums[4],
        sums[1],
        sum_gate,
        sum_up,
        sums[0],
        small_sum[0, :gains],
        small_sum[1, :gains],
        small_sum[2, :gains],
        small_sum[3, : bias_table.shape[0]],
    )


def solution(mesh):
    rows = P(("seq", "shard"), None)
    flat = P(("seq", "shard"))
    tokens = P("shard", "seq", None)
    return jax.shard_map(
        on_device,
        mesh=mesh,
        in_specs=(tokens,) * 3 + (P(),) + (rows,) * 11 + (flat,) * 4,
        out_specs=(tokens,) * 3 + (rows,) * 11 + (flat,) * 4,
        check_vma=False,
    )
```

```python
import functools
import jax
import jax.numpy as jnp
from jax import lax
from jax.experimental import pallas as pl
from jax.experimental.pallas import tpu as pltpu
from jax.sharding import PartitionSpec as P

H = 12
BUCKETS = 32
NEGATIVE = -1e30
EPSILON = 1e-06
F32 = jnp.float32
LOW = jnp.bfloat16
PAIR = 2
TILE = 256


def contract(left, right, left_dim, right_dim):
    return lax.dot_general(
        left, right, (((left_dim,), (right_dim,)), ((), ())), preferred_element_type=F32
    )


def keep_head(value, head):
    size = value.shape[1] // PAIR
    lane = lax.broadcasted_iota(jnp.int32, value.shape, 1)
    inside = (lane >= head * size) & (lane < (head + 1) * size)
    return jnp.where(inside, value, jnp.zeros_like(value))


def toeplitz(row):
    wide = jnp.broadcast_to(row, (TILE, 2 * TILE))
    return pltpu.roll(wide, 0, 1, stride=1, stride_axis=0)[:, :TILE]


def skew_sum(total_ref):
    group = 8
    width = 2 * TILE
    summed = jnp.zeros((group, width), F32)
    for start in range(0, TILE, group):
        rows = total_ref[start : start + group, :]
        wide = jnp.concatenate([rows, jnp.zeros_like(rows)], 1)
        summed = summed + pltpu.roll(wide, (width - start) % width, 1)
    out = summed[0:1]
    for row in range(1, group):
        out = out + pltpu.roll(summed[row : row + 1], width - row, 1)
    return out


def scores_t(keys, query, tiles, last):
    scores = contract(keys, query, 1, 1)
    if tiles is None:
        return scores
    parts = [
        scores[place * TILE : (place + 1) * TILE] + tiles[last - place] for place in range(last + 1)
    ]
    return jnp.concatenate(parts, 0) if len(parts) > 1 else parts[0]


def attend_block(q_ref, k_ref, v_t, o_ref, lse_ref, tiles_ref, start, last, span):
    query = q_ref[start : start + TILE, :]
    size = query.shape[1] // PAIR
    mixed = []
    for head in range(PAIR):
        tiles = None if tiles_ref is None else tiles_ref.at[head]
        scores = scores_t(k_ref[:span, :], keep_head(query, head), tiles, last)
        summit = jnp.max(scores, 0, keepdims=True)
        exponent = jnp.exp(scores - summit)
        total = jnp.sum(exponent, 0, keepdims=True)
        weighted = contract(
            v_t[head * size : (head + 1) * size, :span], exponent.astype(LOW), 1, 0
        )
        mixed.append(weighted / total)
        lse_ref[0, head : head + 1, start : start + TILE] = summit + jnp.log(total)
    o_ref[start : start + TILE, :] = jnp.concatenate(mixed, 0).T.astype(LOW)


def attend_kernel(causal, *refs):
    if causal:
        seq_ref, q_ref, k_ref, v_ref, z_ref, o_ref, lse_ref, tiles_ref = refs
        make_tiles(z_ref, tiles_ref)
    else:
        q_ref, k_ref, v_ref, o_ref, lse_ref = refs
    v_t = v_ref[...].T
    blocks = q_ref.shape[0] // TILE
    keys = k_ref.shape[0]
    if not causal:
        for block in range(blocks):
            attend_block(q_ref, k_ref, v_t, o_ref, lse_ref, None, block * TILE, None, keys)
        return
    for side in range(keys // q_ref.shape[0]):

        @pl.when(seq_ref[0] == side)
        def _(side=side):
            for block in range(blocks):
                last = side * blocks + block
                attend_block(
                    q_ref, k_ref, v_t, o_ref, lse_ref, tiles_ref, block * TILE, last,
                    (last + 1) * TILE,
                )


def make_tiles(z_ref, tiles_ref):
    for head in range(PAIR):
        for off in range(z_ref.shape[2]):
            tiles_ref[head, off] = toeplitz(z_ref[0, head, off : off + 1, :])


def attend(queries, keys_all, values, seq_pos, rows):
    count, width = queries.shape
    length = keys_all.shape[0]
    pairs = H // PAIR
    lanes = width // pairs
    offs = length // TILE
    causal = rows is not None
    col = lambda size: pl.BlockSpec((size, lanes), lambda pair, *_: (0, pair))
    in_specs = [col(count), col(length), col(length)]
    args = [queries, keys_all, values]
    scratch = []
    if causal:
        in_specs.append(pl.BlockSpec((1, PAIR, offs, 2 * TILE), lambda pair, *_: (pair, 0, 0, 0)))
        args = [seq_pos] + args + [rows]
        scratch = [pltpu.VMEM((PAIR, offs, TILE, TILE), F32)]
    work = H * count * length
    return pl.pallas_call(
        functools.partial(attend_kernel, causal),
        grid_spec=pltpu.PrefetchScalarGridSpec(
            num_scalar_prefetch=1 if causal else 0,
            grid=(pairs,),
            in_specs=in_specs,
            out_specs=[
                col(count),
                pl.BlockSpec((1, PAIR, count), lambda pair, *_: (pair, 0, 0)),
            ],
            scratch_shapes=scratch,
        ),
        out_shape=[
            jax.ShapeDtypeStruct((count, width), LOW),
            jax.ShapeDtypeStruct((pairs, PAIR, count), F32),
        ],
        cost_estimate=pl.CostEstimate(
            flops=work * 256 * 2, bytes_accessed=6 * length * width, transcendentals=work
        ),
        name="attend_causal" if causal else "attend_cross",
    )(*args)


def back_block(refs, k_t, prod_t, start, last, span, first, tiles_ref, total_ref):
    q_ref, k_ref, v_ref, g_ref, lse_ref, dq_ref, dk_acc, dv_acc = refs
    query = q_ref[start : start + TILE, :]
    grad = g_ref[start : start + TILE, :]
    size = query.shape[1] // PAIR
    dq_t = []
    dk = dv = None
    for head in range(PAIR):
        own = keep_head(query, head)
        own_grad = keep_head(grad, head)
        tiles = None if tiles_ref is None else tiles_ref.at[head]
        scores = scores_t(k_ref[:span, :], own, tiles, last)
        probs = jnp.exp(scores - lse_ref[0, head : head + 1, start : start + TILE])
        grad_probs = contract(v_ref[:span, :], own_grad, 1, 1)
        delta = jnp.sum(
            prod_t[head * size : (head + 1) * size, start : start + TILE], 0, keepdims=True
        )
        grad_scores = probs * (grad_probs - delta)
        low = grad_scores.astype(LOW)
        dv_new = contract(probs.astype(LOW), own_grad, 1, 0)
        dk_new = contract(low, own, 1, 0)
        dv = dv_new if dv is None else dv + dv_new
        dk = dk_new if dk is None else dk + dk_new
        dq_t.append(contract(k_t[head * size : (head + 1) * size, :span], low, 1, 0))
        if total_ref is not None:
            for place in range(last + 1):
                off = last - place
                piece = grad_scores[place * TILE : (place + 1) * TILE]
                if first:
                    total_ref[head, off] = piece
                elif off == last:
                    total_ref[head, off] = piece
                else:
                    total_ref[head, off] += piece
    dq_ref[start : start + TILE, :] = jnp.concatenate(dq_t, 0).T.astype(LOW)
    if first:
        dk_acc[:span, :] = dk
        dv_acc[:span, :] = dv
        if span < dk_acc.shape[0]:
            dk_acc[span:, :] = jnp.zeros((dk_acc.shape[0] - span, dk_acc.shape[1]), F32)
            dv_acc[span:, :] = jnp.zeros((dv_acc.shape[0] - span, dv_acc.shape[1]), F32)
    else:
        dk_acc[:span, :] += dk
        dv_acc[:span, :] += dv


def back_kernel(causal, *refs):
    if causal:
        (seq_ref, q_ref, k_ref, v_ref, g_ref, o_ref, lse_ref, z_ref,
         dq_ref, dk_ref, dv_ref, row_ref, dk_acc, dv_acc, tiles_ref, total_ref) = refs
        make_tiles(z_ref, tiles_ref)
    else:
        (q_ref, k_ref, v_ref, g_ref, o_ref, lse_ref,
         dq_ref, dk_ref, dv_ref, dk_acc, dv_acc) = refs
        tiles_ref = total_ref = None
    k_t = k_ref[...].T
    prod_t = (g_ref[...].astype(F32) * o_ref[...].astype(F32)).T
    blocks = q_ref.shape[0] // TILE
    keys = k_ref.shape[0]
    main = (q_ref, k_ref, v_ref, g_ref, lse_ref, dq_ref, dk_acc, dv_acc)
    if not causal:
        for block in range(blocks):
            back_block(main, k_t, prod_t, block * TILE, None, keys, block == 0, None, None)
    else:
        for side in range(keys // q_ref.shape[0]):

            @pl.when(seq_ref[0] == side)
            def _(side=side):
                for block in range(blocks):
                    last = side * blocks + block
                    back_block(
                        main, k_t, prod_t, block * TILE, last, (last + 1) * TILE,
                        block == 0, tiles_ref, total_ref,
                    )
                for head in range(PAIR):
                    for off in range(keys // TILE):
                        if off < (side + 1) * blocks:
                            row_ref[0, head, off : off + 1, :] = skew_sum(total_ref.at[head, off])
                        else:
                            row_ref[0, head, off : off + 1, :] = jnp.zeros((1, 2 * TILE), F32)

    dk_ref[...] = dk_acc[...].astype(LOW)
    dv_ref[...] = dv_acc[...].astype(LOW)


def attend_back(queries, keys_all, values, grad_mixed, mixed, lse, seq_pos, rows):
    count, width = queries.shape
    length = keys_all.shape[0]
    pairs = H // PAIR
    lanes = width // pairs
    offs = length // TILE
    causal = rows is not None
    col = lambda size: pl.BlockSpec((size, lanes), lambda pair, *_: (0, pair))
    in_specs = [col(count), col(length), col(length), col(count), col(count),
                pl.BlockSpec((1, PAIR, count), lambda pair, *_: (pair, 0, 0))]
    out_specs = [col(count), col(length), col(length)]
    out_shape = [
        jax.ShapeDtypeStruct((count, width), LOW),
        jax.ShapeDtypeStruct((length, width), LOW),
        jax.ShapeDtypeStruct((length, width), LOW),
    ]
    args = [queries, keys_all, values, grad_mixed, mixed, lse]
    scratch = [pltpu.VMEM((length, lanes), F32), pltpu.VMEM((length, lanes), F32)]
    if causal:
        row_spec = pl.BlockSpec((1, PAIR, offs, 2 * TILE), lambda pair, *_: (pair, 0, 0, 0))
        in_specs.append(row_spec)
        out_specs.append(row_spec)
        out_shape.append(jax.ShapeDtypeStruct((pairs, PAIR, offs, 2 * TILE), F32))
        args = [seq_pos] + args + [rows]
        scratch += [pltpu.VMEM((PAIR, offs, TILE, TILE), F32)] * 2
    work = H * count * length
    return pl.pallas_call(
        functools.partial(back_kernel, causal),
        grid_spec=pltpu.PrefetchScalarGridSpec(
            num_scalar_prefetch=1 if causal else 0,
            grid=(pairs,),
            in_specs=in_specs,
            out_specs=out_specs,
            scratch_shapes=scratch,
        ),
        out_shape=out_shape,
        cost_estimate=pl.CostEstimate(
            flops=work * 640 * 2, bytes_accessed=12 * length * width, transcendentals=work
        ),
        name="attend_causal_back" if causal else "attend_cross_back",
    )(*args)


def bucket_rows(buckets, length):
    offs = length // TILE
    place = jnp.arange(2 * TILE, dtype=jnp.int32)
    step = jnp.where(place < TILE, place, place - 2 * TILE)
    gap = (jnp.arange(offs, dtype=jnp.int32) * TILE)[:, None] + step[None, :]
    marks = jnp.arange(BUCKETS, dtype=jnp.int32)
    begins = jnp.sum((buckets[None, :] < marks[:, None]).astype(jnp.int32), 1)
    ends = jnp.sum((buckets[None, :] <= marks[:, None]).astype(jnp.int32), 1)
    hot = (gap[None] >= begins[:, None, None]) & (gap[None] < ends[:, None, None])
    return (gap, hot.astype(LOW))


def bit_plan():
    bits = []
    for axis in ("seq", "shard"):
        size = lax.axis_size(axis)
        assert size & (size - 1) == 0
        bits += [(axis, place) for place in reversed(range(size.bit_length() - 1))]
    return bits


def bit_orders(bits):
    ends = [0, len(bits) - 2, len(bits) - 1]
    rest = [place for place in range(len(bits)) if place not in ends]
    flipped = [ends[1], ends[0], ends[2]]
    return (rest + ends, rest + flipped, ends[:2] + rest + ends[2:])


def coords(bits):
    return [lax.rem(lax.axis_index(axis) // (1 << place), 2) for axis, place in bits]


def partner(bits, which):
    axis, place = bits[which]
    index = lax.axis_index(axis)
    mine = lax.rem(index // (1 << place), 2)
    return {axis: index + (1 - 2 * mine) * (1 << place)}


def greet(bits):
    barrier = pltpu.get_barrier_semaphore()
    for which in range(len(bits)):
        pl.semaphore_signal(
            barrier, inc=1, device_id=partner(bits, which), device_id_type=pl.DeviceIdType.MESH
        )
    pl.semaphore_wait(barrier, len(bits))


def remote(bits, which, source, target, sems):
    return pltpu.make_async_remote_copy(
        src_ref=source,
        dst_ref=target,
        send_sem=sems[0],
        recv_sem=sems[1],
        device_id=partner(bits, which),
        device_id_type=pl.DeviceIdType.MESH,
    )


def send(*args):
    copy = remote(*args)
    copy.start()
    return copy


def scatter_kernel(bits, count, *refs):
    steps = len(bits)
    sources, outs, work = refs[:count], refs[count : 2 * count], refs[2 * count : 3 * count]
    arrivals = refs[3 * count : (3 + steps) * count]
    load_sem, send_sem, recv_sem = refs[(3 + steps) * count :]
    place = coords(bits)
    orders = [list(reversed(order)) for order in bit_orders(bits)[:2]]
    loads = []
    for item in range(count):
        load = pltpu.make_async_copy(sources[item], work[item], load_sem.at[item])
        load.start()
        loads.append(load)
    greet(bits)
    copies = {}

    def add(item, step):
        order = orders[item % 2]
        free = [which for which in range(steps) if which not in order[: step + 1]]
        arrived = arrivals[item * steps + step]
        copies[item, step].wait_recv()
        if not free:
            outs[item][...] = work[item][tuple(place)].astype(F32) + arrived[...].astype(F32)
            return

        @pl.loop(0, 1 << len(free))
        def _(block):
            sub = [lax.rem(block // (1 << (len(free) - 1 - i)), 2) for i in range(len(free))]
            here = tuple(
                sub[free.index(which)] if which in free else place[which] for which in range(steps)
            )
            total = work[item][here].astype(F32) + arrived[tuple(sub)].astype(F32)
            work[item][here] = total.astype(work[item].dtype)

    for turn in range(steps + 1 + (count - 1) // 2):
        for item in range(count):
            step = turn - item // 2
            if not 0 <= step <= steps:
                continue
            if step == 0:
                loads[item].wait()
            else:
                add(item, step - 1)
            if step == steps:
                continue
            order = orders[item % 2]
            there = tuple(
                1 - place[which]
                if which == order[step]
                else (place[which] if which in order[:step] else slice(None))
                for which in range(steps)
            )
            copies[item, step] = send(
                bits,
                order[step],
                work[item].at[there],
                arrivals[item * steps + step],
                (send_sem.at[item, step], recv_sem.at[item, step]),
            )
    for copy in copies.values():
        copy.wait_send()


def scatter(items, collective_id):
    bits = bit_plan()
    steps = len(bits)
    count = len(items)
    sems = pltpu.SemaphoreType.DMA((count, steps))
    owners = 1 << steps
    items = [x.reshape((2,) * steps + (x.shape[0] // owners,) + x.shape[1:]) for x in items]
    tails = [x.shape[steps:] for x in items]
    arrivals = [
        pltpu.VMEM((2,) * (steps - 1 - step) + tail, x.dtype)
        for x, tail in zip(items, tails)
        for step in range(steps)
    ]
    return pl.pallas_call(
        functools.partial(scatter_kernel, bits, count),
        out_shape=[jax.ShapeDtypeStruct(tail, F32) for tail in tails],
        in_specs=[pl.BlockSpec(memory_space=pl.ANY)] * count,
        out_specs=[pl.BlockSpec(memory_space=pltpu.VMEM)] * count,
        scratch_shapes=[pltpu.VMEM(x.shape, x.dtype) for x in items]
        + arrivals
        + [pltpu.SemaphoreType.DMA((count,)), sems, sems],
        compiler_params=pltpu.CompilerParams(collective_id=collective_id, has_side_effects=True),
        name="scatter_rows",
    )(*items)


def table_rows(smalls, table_size, row):
    flat = smalls.reshape(-1, smalls.shape[-1])
    count = table_size * flat.shape[0] // 8
    entry = lax.broadcasted_iota(jnp.int32, (count, flat.shape[0]), 0)
    source = lax.broadcasted_iota(jnp.int32, (count, flat.shape[0]), 1)
    begin = (source >> 3) * table_size
    pick = ((source & 7) == row) & (entry >= begin) & (entry < begin + table_size)
    spread = contract(pick.astype(LOW), flat.astype(LOW), 1, 0)
    lane = lax.broadcasted_iota(jnp.int32, spread.shape, 1)
    place = lax.broadcasted_iota(jnp.int32, spread.shape, 0).astype(F32)
    block = jnp.floor((place + 0.5) * (1.0 / table_size))
    return jnp.where(lane.astype(F32) == place - block * table_size, spread, 0.0)


def gain_row(smalls, size, row):
    flat = smalls.reshape(-1, smalls.shape[-1])
    count = size * flat.shape[0] // 8
    source = lax.broadcasted_iota(jnp.int32, (flat.shape[0], count), 0)
    entry = lax.broadcasted_iota(jnp.int32, (flat.shape[0], count), 1)
    begin = (source >> 3) * size
    pick = ((source & 7) == row) & (entry >= begin) & (entry < begin + size)
    spread = contract(flat.astype(LOW), pick.astype(LOW), 0, 0)
    lane = lax.broadcasted_iota(jnp.int32, spread.shape, 0).astype(F32)
    place = lax.broadcasted_iota(jnp.int32, spread.shape, 1).astype(F32)
    block = jnp.floor((place + 0.5) * (1.0 / size))
    return jnp.sum(jnp.where(lane == place - block * size, spread, 0.0), 0, keepdims=True)


def full_weight(ref):
    value = ref[...].astype(F32)
    return value.reshape(-1, value.shape[-1]).astype(LOW)


ARRAYS = 12
INSIDE = 9
ITEMS = 15
PIECES = tuple((array, None, 0) for array in range(INSIDE)) + tuple(
    (array, axis, half) for array, axis in ((9, 1), (10, 1), (11, 0)) for half in range(2)
)
PATHS = ('xzZyc', 'xzZyc', 'zZxyc', 'zZyxc', 'yxzZc', 'xzZyc', 'zZxyc', 'zZxyc', 'xyzZc', 'zZyxc', 'zZyxc', 'xzZyc', 'yzZxc', 'xzZyc', 'xyzZc')
PLAN = (
    (1, 0, 0), (3, 0, 0), (2, 0, 0), (0, 0, 0), (14, 0, 0), (15, 0, 0),
    (1, 1, 0), (3, 1, 0), (0, 1, 0), (2, 1, 0), (7, 0, 0), (6, 0, 0),
    (1, 2, 0), (3, 2, 0), (9, 0, 0), (10, 0, 0), (11, 0, 0), (2, 2, 0),
    (7, 1, 0), (4, 0, 0), (0, 2, 0), (5, 0, 0), (12, 0, 0), (9, 1, 0),
    (1, 3, 0), (12, 1, 0), (10, 1, 0), (13, 0, 0), (6, 1, 0), (0, 3, 0),
    (8, 0, 0), (4, 1, 0), (11, 1, 0), (3, 3, 0), (14, 1, 0), (1, 4, 0),
    (2, 3, 0), (0, 4, 0), (5, 1, 0), (12, 2, 0), (6, 2, 0), (8, 1, 0),
    (4, 2, 0), (7, 2, 0), (5, 2, 1), (9, 2, 1), (11, 2, 1), (10, 2, 1),
    (13, 1, 1), (2, 4, 1), (14, 2, 2), (16, 0, 2), (12, 3, 2), (3, 4, 2),
    (6, 3, 3), (4, 3, 6), (5, 3, 6), (13, 2, 7), (8, 2, 7), (10, 3, 7),
    (6, 4, 7), (7, 3, 8), (11, 3, 8), (9, 3, 8), (14, 3, 8), (4, 4, 9),
    (5, 4, 9), (8, 3, 11), (13, 3, 11), (7, 4, 11), (12, 4, 14), (11, 4, 16),
    (14, 4, 17), (10, 4, 17), (8, 4, 18), (13, 4, 18), (9, 4, 19),
)
(STAGE_GAIN, STAGE_QUERY, STAGE_KEY, STAGE_VALUE, STAGE_SELF, STAGE_OUT, STAGE_CQUERY, STAGE_CKEY,
 STAGE_CVALUE, STAGE_CROSS, STAGE_COUT, STAGE_END) = (0, 1, 2, 3, 4, 10, 11, 12, 13, 14, 20, 21)


def path_bits(bits, path):
    count = len(bits)
    rest = list(range(1, count - 2))
    groups = {"x": [0], "y": [count - 2], "c": [count - 1], "z": rest[:-1], "Z": rest[-1:]}
    return [groups[letter] for letter in path]


def open_kernel(bits, sizes, *refs):
    gain_size, table_size = sizes
    sources = refs[:ARRAYS]
    hidden_ref, enc_ref, hot_ref, mask_ref = refs[ARRAYS : ARRAYS + 4]
    outs = refs[ARRAYS + 4 : 2 * ARRAYS + 4]
    (enc_out, first_out, q_out, k_out, v_out, mixed_out, lse_out, after_out, second_out,
     cq_out, ck_out, cv_out, cmixed_out, clse_out, across_out, third_out,
     before_ref, flat_ref, tiles_ref, weight_ref,
     send_sem, recv_sem, own_sem, side_send, side_recv) = refs[2 * ARRAYS + 4 :]
    steps = len(bits)
    place = coords(bits)
    seq_pos = lax.axis_index("seq")
    rows = hidden_ref.shape[0]
    keys = first_out.shape[0]
    lanes = hidden_ref.shape[1] // (H // PAIR)

    def own(array):
        return pltpu.make_async_copy(
            sources[array], outs[array].at[tuple(place)], own_sem.at[array]
        )

    def copy(item, step):
        order = sum(path_bits(bits, PATHS[item]), [])
        array, axis, half = PIECES[item]
        here = tuple(
            slice(None) if which in order[:step] else place[which] for which in range(steps)
        )
        part = ()
        if axis is not None:
            size = sources[array].shape[axis] // 2
            part = (slice(None),) * axis + (pl.ds(half * size, size),)
        target = outs[array].at[here + part]
        source = target
        if step == 0:
            source = sources[array].at[part] if part else sources[array]
        return remote(
            bits,
            order[step],
            source,
            target,
            (send_sem.at[item, step], recv_sem.at[item, step]),
        )

    def arrived(item):
        copy(item, steps - 1).wait_recv()

    def side(which):
        source, target = ((hidden_ref, before_ref), (enc_ref, enc_out.at[rows:]))[which]
        return remote(bits, 0, source, target, (side_send.at[which], side_recv.at[which]))

    todo = list(PLAN)
    seen = set()

    def advance(until):
        while todo and todo[0][2] <= until:
            item, step, _ = todo.pop(0)
            if item >= ITEMS:
                side(item - ITEMS).start()
                continue
            groups = path_bits(bits, PATHS[item])
            first = sum(len(group) for group in groups[:step])
            for number in range(first, first + len(groups[step])):
                if number > 0:
                    if PIECES[item][0] not in seen:
                        seen.add(PIECES[item][0])
                        own(PIECES[item][0]).wait()
                    copy(item, number - 1).wait_recv()
                copy(item, number).start()

    for array in range(ARRAYS):
        own(array).start()
    greet(bits)
    enc_out[:rows, :] = enc_ref[...]
    advance(STAGE_GAIN)
    arrived(0)
    gains = [gain_row(outs[0][...], gain_size, row) for row in range(3)]
    flat_ref[...] = table_rows(outs[0][...], table_size, 3)

    def normed(value, gain):
        scale = lax.rsqrt(jnp.mean(value * value, -1, keepdims=True) + EPSILON)
        return (value * scale * gain).astype(LOW)

    def over_rows(count, body):
        @pl.loop(0, count // TILE)
        def _(block):
            body(lambda base=0: pl.ds(base + pl.multiple_of(block * TILE, TILE), TILE))

    def normed_rows(source, start):
        def body(at):
            first_out[at(start), :] = normed(source[at(), :].astype(F32), gains[0])

        over_rows(rows, body)

    def project(item, source, out, begin, count):
        weight_ref[...] = full_weight(outs[item])

        def body(at):
            out[at(), :] = contract(source[at(begin), :], weight_ref[...], 1, 0).astype(LOW)

        over_rows(count, body)

    normed_rows(hidden_ref, rows)
    advance(STAGE_QUERY)
    arrived(1)
    project(1, first_out, q_out, rows, rows)
    advance(STAGE_KEY)
    side(0).wait_recv()

    @pl.when(seq_pos == 0)
    def _():
        first_out[:rows, :] = first_out[rows:, :]

    @pl.when(seq_pos != 0)
    def _():
        normed_rows(before_ref, 0)

    arrived(2)
    project(2, first_out, k_out, 0, keys)
    advance(STAGE_VALUE)
    arrived(3)
    project(3, first_out, v_out, 0, keys)

    advance(STAGE_SELF)

    def between(pair, begin):
        for done in range(H // PAIR - 1):

            @pl.when(pair == done)
            def _(done=done):
                advance(begin + done + 1)

    @pl.loop(0, H // PAIR)
    def _(pair):
        at = pl.ds(pl.multiple_of(pair * lanes, lanes), lanes)
        q_ref, k_ref, v_ref, o_ref = (ref.at[:, at] for ref in (q_out, k_out, v_out, mixed_out))
        for head in range(PAIR):
            column = jnp.sum(
                flat_ref[pl.ds(pl.multiple_of((pair * PAIR + head) * BUCKETS, BUCKETS), BUCKETS), :],
                1,
                keepdims=True,
            )
            for off in range(keys // TILE):
                row = jnp.sum(column * hot_ref[off].astype(F32), 0, keepdims=True)
                tiles_ref[head, off] = toeplitz(row + mask_ref[off])
        v_t = v_ref[...].T
        blocks = rows // TILE
        for part in range(keys // rows):

            @pl.when(seq_pos == part)
            def _(part=part):
                for block in range(blocks):
                    last = part * blocks + block
                    attend_block(
                        q_ref, k_ref, v_t, o_ref, lse_out.at[pl.ds(pair, 1)], tiles_ref,
                        block * TILE, last, (last + 1) * TILE,
                    )

        between(pair, STAGE_SELF)

    def residual(item, mixed, base, total, normal, gain):
        weight_ref[...] = full_weight(outs[item])

        def body(at):
            value = base[at(), :].astype(F32) + contract(mixed[at(), :], weight_ref[...], 1, 0)
            total[at(), :] = value
            normal[at(), :] = normed(value, gain)

        over_rows(rows, body)

    advance(STAGE_OUT)
    arrived(4)
    residual(4, mixed_out, hidden_ref, after_out, second_out, gains[1])
    advance(STAGE_CQUERY)
    arrived(5)
    project(5, second_out, cq_out, 0, rows)
    advance(STAGE_CKEY)
    side(1).wait_recv()
    arrived(6)
    project(6, enc_out, ck_out, 0, keys)
    advance(STAGE_CVALUE)
    arrived(7)
    project(7, enc_out, cv_out, 0, keys)
    advance(STAGE_CROSS)

    @pl.loop(0, H // PAIR)
    def _(pair):
        at = pl.ds(pl.multiple_of(pair * lanes, lanes), lanes)
        q_ref, k_ref, v_ref, o_ref = (ref.at[:, at] for ref in (cq_out, ck_out, cv_out, cmixed_out))
        v_t = v_ref[...].T
        for block in range(rows // TILE):
            attend_block(
                q_ref, k_ref, v_t, o_ref, clse_out.at[pl.ds(pair, 1)], None, block * TILE, None, keys
            )
        between(pair, STAGE_CROSS)

    advance(1000)

    arrived(8)
    residual(8, cmixed_out, after_out, across_out, third_out, gains[2])
    for item in range(INSIDE, ITEMS):
        arrived(item)
    for item in range(ITEMS):
        for step in range(steps):
            copy(item, step).wait_send()
    for which in range(2):
        side(which).wait_send()


def open_layer(items, hidden, encoded, hot, mask, sizes, collective_id):
    bits = bit_plan()
    steps = len(bits)
    count, width = hidden.shape
    length = count * lax.axis_size("seq")
    offs = length // TILE
    sems = pltpu.SemaphoreType.DMA((ITEMS, steps))
    inside = pl.BlockSpec(memory_space=pltpu.VMEM)
    outside = pl.BlockSpec(memory_space=pl.ANY)
    few, many = (count, width), (length, width)
    lse = (H // PAIR, PAIR, count)
    shapes = [((2,) * steps + x.shape, x.dtype) for x in items]
    shapes += [(many, LOW), (many, LOW), (few, LOW), (many, LOW), (many, LOW), (few, LOW)]
    shapes += [(lse, F32), (few, F32), (few, LOW), (few, LOW), (many, LOW), (many, LOW)]
    shapes += [(few, LOW), (lse, F32), (few, F32), (few, LOW)]
    outs = pl.pallas_call(
        functools.partial(open_kernel, bits, sizes),
        out_shape=[jax.ShapeDtypeStruct(*x) for x in shapes],
        in_specs=[inside] * (ARRAYS + 4),
        out_specs=[inside] * INSIDE + [outside] * (ARRAYS - INSIDE) + [inside] * 16,
        scratch_shapes=[
            pltpu.VMEM((count, width), LOW),
            pltpu.VMEM((H * BUCKETS, 128), F32),
            pltpu.VMEM((PAIR, offs, TILE, TILE), F32),
            pltpu.VMEM((width, width), LOW),
            sems,
            sems,
            pltpu.SemaphoreType.DMA((ARRAYS,)),
            pltpu.SemaphoreType.DMA((2,)),
            pltpu.SemaphoreType.DMA((2,)),
        ],
        compiler_params=pltpu.CompilerParams(
            collective_id=collective_id, has_side_effects=True, vmem_limit_bytes=66_000_000
        ),
        name="open_layer",
    )(*items, hidden, encoded, hot, mask)
    return [out.reshape((-1,) + x.shape[-2:]) for out, x in zip(outs, items)] + list(outs[ARRAYS:])


def reversed_bits(bits, path):
    return list(reversed(sum(path_bits(bits, path), [])))


def close_kernel(bits, sizes, *refs):
    gain_size, table_size = sizes
    (ff_refs, weights, cross_refs, self_refs, (cres_ref, gain3_ref, smalls_ref, hot_ref, mask_ref),
     (after_buf, hidden_buf), (hidden_out, enc_out), outs, (small_out,)) = take(
        refs, (3, 8, 7, 6, 5, 2, 2, 11, 1)
    )
    rest = refs[45:]
    arrivals = rest[: CLOSE_ITEMS * len(bits)]
    (work_ref, load_ref, small_ref, q_buf, k_buf, v_buf, mixed_buf, keys_in_buf,
     query_in_buf, grad_buf, res_buf, weight_buf, enc_own, send_buf, recv_buf, dk_acc, dv_acc,
     tiles_ref, total_ref, rows_ref, flat_ref, send_sem, recv_sem, side_send, side_recv, load_sem,
     fetch_sem) = rest[CLOSE_ITEMS * len(bits) :]
    steps = len(bits)
    place = coords(bits)
    seq_pos = lax.axis_index("seq")
    rows = cres_ref.shape[0]
    keys = k_buf.shape[0]
    lanes = cres_ref.shape[1] // (H // PAIR)

    def pick(names, which, side):
        return tuple(side if name == which else slice(None) for name in names)

    def order_of(item):
        return reversed_bits(bits, CLOSE_PATHS[item])

    def part_of(item):
        if item >= 6:
            return ()
        if item < 4:
            size = ff_refs[item // 2].shape[-1] // 2
            return (slice(None), pl.ds(item % 2 * size, size))
        size = ff_refs[2].shape[-2] // 2
        return (pl.ds(item % 2 * size, size),)

    def base(item):
        if item == SMALL:
            return small_ref
        return ff_refs[item // 2] if item < 6 else work_ref.at[item % SLOTS]

    def arrival(item, step):
        return arrivals[item * steps + step]

    def names_at(item, step):
        order = order_of(item)
        return [which for which in range(steps) if which not in order[:step]]

    def copy(item, step):
        which = order_of(item)[step]
        names = names_at(item, step)
        there = pick(names, which, 1 - place[which])
        if step == 0:
            source = base(item).at[there + part_of(item)]
        else:
            source = arrival(item, step - 1).at[there]
        return remote(
            bits, which, source, arrival(item, step), (send_sem.at[item, step], recv_sem.at[item, step])
        )

    def own_load(item):
        which = order_of(item)[0]
        here = pick(names_at(item, 0), which, place[which])
        block = arrival(item, 0).shape
        target = load_ref.at[
            (item % 2,) + (slice(None),) * (steps - 1) + (pl.ds(0, block[-2]), pl.ds(0, block[-1]))
        ]
        return pltpu.make_async_copy(
            base(item).at[here + part_of(item)], target, load_sem.at[item % 2]
        )

    def add(item, step):
        which = order_of(item)[step]
        names = names_at(item, step)
        free = [name for name in names if name != which]
        target = arrival(item, step)
        block = tuple(slice(0, size) for size in target.shape[-2:])
        copy(item, step).wait_recv()
        if step == 0 and item < 6:
            own_load(item).wait()

        def one(sub):
            here = tuple(place[which] if name == which else sub[free.index(name)] for name in names)
            if step > 0:
                mine = arrival(item, step - 1)[here]
            elif item < 6:
                mine = load_ref[(item % 2,) + tuple(sub) + block]
            elif item == SMALL:
                mine = small_ref[here]
            else:
                mine = work_ref[(item % SLOTS,) + here]
            return mine.astype(F32) + target[tuple(sub)].astype(F32)

        if not free:
            if item == SMALL:
                small_out[...] = one(())
            elif item < 6:
                outs[item // 2][part_of(item)] = one(())
            else:
                outs[item - 3][...] = one(())
            return

        @pl.loop(0, 1 << len(free))
        def _(index):
            sub = [lax.rem(index // (1 << (len(free) - 1 - i)), 2) for i in range(len(free))]
            target[tuple(sub)] = one(sub).astype(target.dtype)

        if step == 0 and item < 4:
            own_load(item + 2).start()

    def side(which):
        return remote(
            bits, 0, send_buf.at[which], recv_buf.at[which], (side_send.at[which], side_recv.at[which])
        )

    todo = list(CLOSE_PLAN)
    ready = set(range(6)) | {CLOSE_ITEMS, CLOSE_ITEMS + 1}
    drained = set()

    def take_next():
        item, step, _ = todo.pop(0)
        if item == CLOSE_ITEMS:
            side(0).start()
            return
        if item > CLOSE_ITEMS:

            @pl.when(seq_pos != 0)
            def _():
                side(1).start()

            return
        groups = list(reversed(path_bits(bits, CLOSE_PATHS[item]))) + [[None]]
        first = sum(len(group) for group in groups[:step])
        for number in range(first, first + len(groups[step])):
            if number > 0:
                add(item, number - 1)
            if number < steps:
                copy(item, number).start()

    def advance(until):
        while todo and todo[0][2] <= until:
            assert todo[0][1] > 0 or todo[0][0] in ready
            take_next()

    def free_slot(item):
        while any(entry[:2] == (item, 1) for entry in todo):
            take_next()
        copy(item, 0).wait_send()
        drained.add((item, 0))

    def fetch(source, target, sem):
        return pltpu.make_async_copy(source, target, fetch_sem.at[sem])

    def weight(number):
        return fetch(weights[number], weight_buf.at[number % 2], number % 2)

    def over_rows(count, body):
        @pl.loop(0, count // TILE)
        def _(block):
            body(lambda start=0: pl.ds(start + pl.multiple_of(block * TILE, TILE), TILE))

    def weight_grad(item, left, right):
        if item - SLOTS >= 6:
            free_slot(item - SLOTS)
        half = left.shape[1] // 2
        for side_index in range(2):
            value = contract(left[:, side_index * half : (side_index + 1) * half], right[...], 0, 0)
            shape = work_ref.shape[2:]
            work_ref[item % SLOTS, side_index] = value.reshape(shape).astype(LOW)
        ready.add(item)

    def pairs_back(lse_ref, tiles, begin):
        @pl.loop(0, H // PAIR)
        def _(pair):
            at = pl.ds(pl.multiple_of(pair * lanes, lanes), lanes)
            q_ref, k_ref, v_ref, g_ref, o_ref = (
                ref.at[:, at] for ref in (q_buf, k_buf, v_buf, grad_buf, mixed_buf)
            )
            if tiles:
                for head in range(PAIR):
                    start = pl.multiple_of((pair * PAIR + head) * BUCKETS, BUCKETS)
                    column = jnp.sum(flat_ref[pl.ds(start, BUCKETS), :], 1, keepdims=True)
                    for off in range(keys // TILE):
                        row = jnp.sum(column * hot_ref[off].astype(F32), 0, keepdims=True)
                        tiles_ref[head, off] = toeplitz(row + mask_ref[off])
            k_t = k_ref[...].T
            prod_t = (g_ref[...].astype(F32) * o_ref[...].astype(F32)).T
            main = (q_ref, k_ref, v_ref, g_ref, lse_ref.at[pl.ds(pair, 1)], q_ref, dk_acc, dv_acc)
            blocks = rows // TILE
            if not tiles:
                for block in range(blocks):
                    back_block(main, k_t, prod_t, block * TILE, None, keys, block == 0, None, None)
            else:
                for part in range(keys // rows):

                    @pl.when(seq_pos == part)
                    def _(part=part):
                        for block in range(blocks):
                            last = part * blocks + block
                            back_block(
                                main, k_t, prod_t, block * TILE, last, (last + 1) * TILE,
                                block == 0, tiles_ref, total_ref,
                            )
                        for head in range(PAIR):
                            column = jnp.zeros((BUCKETS, 1), F32)
                            for off in range((part + 1) * blocks):
                                row = skew_sum(total_ref.at[head, off])
                                column = column + jnp.sum(
                                    hot_ref[off].astype(F32) * row, 1, keepdims=True
                                )
                            start = pl.multiple_of((pair * PAIR + head) * BUCKETS, BUCKETS)
                            rows_ref[pl.ds(start, BUCKETS), :] = jnp.broadcast_to(
                                column, (BUCKETS, rows_ref.shape[1])
                            )

            k_ref[...] = dk_acc[...].astype(LOW)
            v_ref[...] = dv_acc[...].astype(LOW)
            for done in range(H // PAIR - 1):

                @pl.when(pair == done)
                def _(done=done):
                    advance(begin + done + 1)

    def norm_back_rows(value, gain, grad):
        scale = lax.rsqrt(jnp.mean(value * value, -1, keepdims=True) + EPSILON)
        scaled = gain * grad
        inner = jnp.mean(value * scaled, -1, keepdims=True)
        back = scale * scaled - value * (scale * scale * scale) * inner
        return back, jnp.sum(grad * value * scale, 0, keepdims=True)

    cq_in, ck_in, cv_in, cmixed_in, enc_in, second_in, clse_ref = cross_refs
    q_in, k_in, v_in, mixed_in, first_in, lse_ref = self_refs[:6]
    fetches = [
        fetch(cmixed_in, mixed_buf, 2), fetch(cq_in, q_buf, 3), fetch(ck_in, k_buf, 4),
        fetch(cv_in, v_buf, 5), fetch(enc_in, keys_in_buf, 6), fetch(second_in, query_in_buf, 7),
    ]
    weight(0).start()
    weight(1).start()
    own_load(0).start()
    own_load(1).start()
    for one in fetches:
        one.start()
    greet(bits)
    advance(1)
    flat_ref[...] = table_rows(smalls_ref[...], table_size, 3)
    gain_one = gain_row(smalls_ref[...], gain_size, 0)
    gain_two = gain_row(smalls_ref[...], gain_size, 1)

    def to_mixed(number, source):
        weight(number).wait()

        def body(at):
            grad_buf[at(), :] = contract(
                source[at(), :].astype(LOW), weight_buf[number % 2], 1, 1
            ).astype(LOW)

        over_rows(rows, body)
        weight(number + 2).start()

    advance(2)
    to_mixed(0, cres_ref)
    fetches[0].wait()

    def low_rows(source, target):
        def body(at):
            target[at(), :] = source[at(), :].astype(LOW)

        over_rows(rows, body)

    low_rows(cres_ref, send_buf.at[0])
    weight_grad(6, mixed_buf, send_buf.at[0])
    advance(3)
    for one in fetches[1:4]:
        one.wait()
    pairs_back(clse_ref, False, 3)
    fetch(mixed_in, mixed_buf, 2).start()
    advance(9)

    def both_back(numbers, keep, count):
        def body_other(at):
            total = contract(k_buf[at(count), :], weight_buf[numbers[0] % 2], 1, 1)
            total = total + contract(v_buf[at(count), :], weight_buf[numbers[1] % 2], 1, 1)
            send_buf[keep[0], at(), :] = total.astype(LOW)

        def body_own(at):
            begin = 0 if count else rows
            total = contract(k_buf[at(begin), :], weight_buf[numbers[0] % 2], 1, 1)
            total = total + contract(v_buf[at(begin), :], weight_buf[numbers[1] % 2], 1, 1)
            keep[1][at(), :] = total

        over_rows(rows, body_other)
        return body_own

    weight(1).wait()
    weight(2).wait()
    own_part = both_back((1, 2), (0, enc_own), rows)
    for one in fetches[4:]:
        one.wait()
    advance(10)
    weight_grad(7, keys_in_buf, k_buf)
    advance(11)
    weight_grad(8, keys_in_buf, v_buf)
    advance(12)
    over_rows(rows, own_part)
    fetch(k_in, k_buf, 4).start()
    fetch(v_in, v_buf, 5).start()
    fetch(first_in, keys_in_buf, 6).start()
    weight(3).start()
    weight(4).start()
    advance(13)
    weight_grad(9, query_in_buf, q_buf)
    advance(14)
    weight(3).wait()
    sums = [jnp.zeros((1, cres_ref.shape[1]), F32)] * 2
    for block in range(rows // TILE):
        at = slice(block * TILE, (block + 1) * TILE)
        grad = contract(q_buf[at, :], weight_buf[1], 1, 1)
        back, total = norm_back_rows(after_buf[at, :], gain_two, grad)
        sums[1] = sums[1] + total
        res_buf[at, :] = cres_ref[at, :] + back
    fetch(q_in, q_buf, 3).start()
    weight(5).start()
    weight(4).wait()

    def body(at):
        grad_buf[at(), :] = contract(res_buf[at(), :].astype(LOW), weight_buf[0], 1, 1).astype(LOW)

    over_rows(rows, body)
    weight(6).start()
    fetch(mixed_in, mixed_buf, 2).wait()
    low_rows(res_buf, query_in_buf)
    weight_grad(10, mixed_buf, query_in_buf)
    advance(15)
    fetch(q_in, q_buf, 3).wait()
    fetch(k_in, k_buf, 4).wait()
    fetch(v_in, v_buf, 5).wait()
    pairs_back(lse_ref, True, 15)
    advance(21)
    side(0).wait_recv()

    def body(at):
        enc_out[at(), :] = (enc_own[at(), :] + recv_buf[0, at(), :].astype(F32)).astype(LOW)

    over_rows(rows, body)
    weight(5).wait()
    weight(6).wait()
    own_part = both_back((5, 6), (1, enc_own), 0)

    fetch(first_in, keys_in_buf, 6).wait()
    advance(22)
    weight_grad(11, keys_in_buf, v_buf)
    advance(23)
    weight_grad(12, keys_in_buf, k_buf)
    advance(24)
    weight_grad(13, keys_in_buf.at[rows:], q_buf)
    advance(25)
    over_rows(rows, own_part)
    weight(7).start()
    advance(26)
    weight(7).wait()

    @pl.when(seq_pos == 0)
    def _():
        side(1).wait_recv()

    @pl.when(seq_pos != 0)
    def _():
        side(1).wait_send()

    own_low = (seq_pos == 0).astype(F32)
    for block in range(rows // TILE):
        at = slice(block * TILE, (block + 1) * TILE)
        grad = contract(q_buf[at, :], weight_buf[1], 1, 1) + enc_own[at, :]
        low = send_buf[1, at, :].astype(F32) + jnp.where(
            seq_pos == 0, recv_buf[1, at, :].astype(F32), 0.0
        )
        grad = grad + own_low * low
        back, total = norm_back_rows(hidden_buf[at, :].astype(F32), gain_one, grad)
        sums[0] = sums[0] + total
        hidden_out[at, :] = (res_buf[at, :] + back).astype(LOW)
    small_ref[...] = small_rows(
        sums[0], sums[1], gain3_ref[...], rows_ref[...], gain_size, table_size, small_ref.shape
    )
    ready.add(SMALL)
    advance(27)
    assert not todo
    for item in range(CLOSE_ITEMS):
        for step in range(steps):
            if (item, step) not in drained:
                copy(item, step).wait_send()
    side(0).wait_send()


def take(refs, counts):
    out = []
    begin = 0
    for count in counts:
        out.append(refs[begin : begin + count])
        begin += count
    return out


def small_rows(one, two, three, table, gain_size, table_size, shape):
    owners = one.shape[1] // gain_size

    def spread(source, size, row):
        count = owners * size
        target = lax.broadcasted_iota(jnp.int32, (owners * 8, count), 0)
        entry = lax.broadcasted_iota(jnp.int32, (owners * 8, count), 1)
        begin = (target >> 3) * size
        hot = ((target & 7) == row) & (entry >= begin) & (entry < begin + size)
        return lax.dot_general(
            hot.astype(F32), source, (((1,), (0 if row == 3 else 1,)), ((), ())),
            precision=lax.Precision.HIGHEST, preferred_element_type=F32,
        )

    def wheel(shape, axis, size):
        entry = lax.broadcasted_iota(jnp.int32, shape, axis).astype(F32)
        lane = lax.broadcasted_iota(jnp.int32, shape, 1 - axis).astype(F32)
        return lane == entry - size * jnp.floor((entry + 0.5) * (1.0 / size))

    total = jnp.zeros((owners * 8, 128), F32)
    for row, value in enumerate((one, two, three)):
        grid = (128, value.shape[1])
        total = total + spread(
            jnp.where(wheel(grid, 1, gain_size), jnp.broadcast_to(value, grid), 0.0), gain_size, row
        )
    total = total + spread(jnp.where(wheel(table.shape, 0, table_size), table, 0.0), table_size, 3)
    return total.reshape(shape)


SLOTS = 2
SMALL = 14
CLOSE_ITEMS = 15
CLOSE_PATHS = ('xyzZc', 'xyzZc', 'zZyxc', 'xzZyc', 'xyzZc', 'zZxyc', 'zZyxc', 'xzZyc', 'xzZyc', 'xzZyc', 'zZyxc', 'xyzZc', 'zZxyc', 'zZxyc', 'xzZyc')
CLOSE_PLAN = (
    (1, 0, 1), (3, 0, 2), (1, 1, 3), (0, 0, 3), (3, 1, 3), (6, 0, 3),
    (5, 0, 3), (2, 0, 3), (0, 1, 6), (2, 1, 6), (4, 0, 6), (6, 1, 10),
    (5, 1, 10), (15, 0, 11), (4, 1, 11), (7, 0, 11), (8, 0, 12), (7, 1, 13),
    (1, 2, 14), (8, 1, 14), (3, 2, 14), (0, 2, 14), (9, 0, 15), (10, 0, 16),
    (9, 1, 16), (7, 2, 17), (5, 2, 17), (10, 1, 17), (4, 2, 18), (6, 2, 20),
    (9, 2, 20), (5, 3, 20), (0, 3, 21), (8, 2, 21), (16, 0, 22), (2, 2, 22),
    (9, 3, 22), (10, 2, 22), (7, 3, 22), (12, 0, 24), (6, 3, 24), (11, 0, 24),
    (3, 3, 24), (12, 1, 24), (11, 1, 24), (5, 4, 24), (6, 4, 25), (13, 0, 25),
    (8, 3, 25), (13, 1, 25), (2, 3, 25), (7, 4, 25), (12, 2, 26), (4, 3, 26),
    (11, 2, 26), (1, 3, 26), (9, 4, 26), (13, 2, 27), (14, 0, 27), (3, 4, 27),
    (8, 4, 27), (12, 3, 27), (14, 1, 27), (0, 4, 27), (6, 5, 27), (2, 4, 27),
    (10, 3, 27), (4, 4, 27), (11, 3, 27), (14, 2, 27), (13, 3, 27), (12, 4, 27),
    (2, 5, 27), (14, 3, 27), (10, 4, 27), (11, 4, 27), (8, 5, 27), (1, 4, 27),
    (13, 4, 27), (3, 5, 27), (12, 5, 27), (9, 5, 27), (5, 5, 27), (0, 5, 27),
    (14, 4, 27), (1, 5, 27), (10, 5, 27), (4, 5, 27), (7, 5, 27), (11, 5, 27),
    (14, 5, 27), (13, 5, 27),
)


def close_layer(ff_grads, weights, cross, own, cres, after, hidden, gain3, smalls, hot, mask, sizes,
                collective_id):
    bits = bit_plan()
    steps = len(bits)
    owners = 1 << steps
    count, width = cres.shape
    length = cross[1].shape[0]
    offs = length // TILE
    lanes = width // (H // PAIR)
    split_rows = lambda x: x.reshape((2,) * steps + (x.shape[0] // owners,) + x.shape[1:])
    ff_grads = [split_rows(x) for x in ff_grads]
    gate, down = ff_grads[0].shape[steps:], ff_grads[2].shape[steps:]
    square = (width // owners, width)
    blocks = [(gate[0], gate[1] // 2)] * 4 + [(down[0] // 2, down[1])] * 2 + [square] * 8
    kinds = [LOW] * 14 + [F32]
    blocks.append((8, 128))
    arrivals = [
        pltpu.VMEM((2,) * (steps - 1 - step) + block, kind)
        for block, kind in zip(blocks, kinds)
        for step in range(steps)
    ]
    load_block = (max(gate[0], down[0] // 2), max(gate[1] // 2, down[1]))
    inside = pl.BlockSpec(memory_space=pltpu.VMEM)
    outside = pl.BlockSpec(memory_space=pl.ANY)
    few, many = (count, width), (length, width)
    vm = pltpu.VMEM
    sems = pltpu.SemaphoreType.DMA((CLOSE_ITEMS, steps))
    pair_sem = pltpu.SemaphoreType.DMA((2,))
    return pl.pallas_call(
        functools.partial(close_kernel, bits, sizes),
        out_shape=[jax.ShapeDtypeStruct(few, LOW)] * 2
        + [jax.ShapeDtypeStruct(block, F32) for block in (gate, gate, down)]
        + [jax.ShapeDtypeStruct(square, F32)] * 8
        + [jax.ShapeDtypeStruct((8, 128), F32)],
        in_specs=[outside] * (3 + 8) + [outside] * 6 + [inside] + [outside] * 5 + [inside]
        + [inside] * 5 + [inside] * 2,
        out_specs=[inside] * 14,
        scratch_shapes=arrivals
        + [
            vm((SLOTS,) + (2,) * steps + square, LOW),
            vm((2,) + (2,) * (steps - 1) + load_block, LOW),
            vm((2,) * steps + (8, 128), F32),
            vm(few, LOW), vm(many, LOW), vm(many, LOW), vm(few, LOW), vm(many, LOW),
            vm(few, LOW), vm(few, LOW), vm(few, F32),
            vm((2, width, width), LOW), vm(few, F32), vm((2,) + few, LOW), vm((2,) + few, LOW),
            vm((length, lanes), F32), vm((length, lanes), F32),
            vm((PAIR, offs, TILE, TILE), F32), vm((PAIR, offs, TILE, TILE), F32),
            vm((H * BUCKETS, 128), F32), vm((H * BUCKETS, 128), F32),
            sems, sems, pair_sem, pair_sem, pair_sem, pltpu.SemaphoreType.DMA((8,)),
        ],
        compiler_params=pltpu.CompilerParams(
            collective_id=collective_id, has_side_effects=True, vmem_limit_bytes=67_000_000
        ),
        name="close_layer",
    )(*ff_grads, *weights, *cross, *own, cres, gain3, smalls, hot, mask, after, hidden)


def finish_kernel(*refs):
    count = (len(refs) - 5) // 2
    for source, target in zip(refs[: count], refs[count + 1 :]):
        target[...] = source[...]
    small = refs[count]
    for row, target in enumerate(refs[2 * count + 1 :]):
        target[...] = small[row, : target.shape[0]]


def finish(arrays, small, sizes):
    count = len(arrays)
    inside = pl.BlockSpec(memory_space=pltpu.VMEM)
    return pl.pallas_call(
        finish_kernel,
        out_shape=[jax.ShapeDtypeStruct(x.shape, x.dtype) for x in arrays]
        + [jax.ShapeDtypeStruct((size,), F32) for size in sizes],
        in_specs=[inside] * (count + 1),
        out_specs=[inside] * (count + 4),
        name="finish",
    )(*arrays, small)


def dot_low(left, right):
    return contract(left, right, 1, 0)


def dot_left(left, right):
    return contract(left, right, 0, 0)


def dot_right(left, right):
    return contract(left, right, 1, 1)


def rms_norm(value, gain):
    return value * lax.rsqrt(jnp.mean(value * value, -1, keepdims=True) + EPSILON) * gain


def norm_back(value, gain, grad):
    return jax.vjp(rms_norm, value, gain)[1](grad)


def gated(gate, upper):
    return jax.nn.gelu(gate, approximate=True) * upper


def pad_rows(rows, dtype):
    return jnp.stack([jnp.pad(row.astype(dtype), (0, 128 - row.shape[0])) for row in rows] + [
        jnp.zeros((128,), dtype)
    ] * (8 - len(rows)))


def on_device(
    hidden_in,
    encoded,
    cotangent,
    buckets,
    self_query,
    self_key,
    self_value,
    self_out,
    cross_query,
    cross_key,
    cross_value,
    cross_out,
    ff_gate,
    ff_up,
    ff_down,
    norm_self,
    norm_cross,
    norm_ff,
    bias_table,
):
    owners = lax.axis_size("seq") * lax.axis_size("shard")
    seq_pos = lax.axis_index("seq")
    seq_row = seq_pos.reshape(1).astype(jnp.int32)
    low_side = seq_pos == 0
    both = ("seq", "shard")
    width = hidden_in.shape[2]
    own_low = hidden_in[0]
    enc_own = encoded[0]
    small = pad_rows([norm_self, norm_cross, norm_ff, bias_table], F32)
    hidden = own_low.astype(F32)
    count = hidden.shape[0]
    length = count * lax.axis_size("seq")
    gap, hot = bucket_rows(buckets, length)
    hot_rows = jnp.swapaxes(hot, 0, 1)
    hot_mask = jnp.where(gap >= 0, 0.0, NEGATIVE)[:, None, :]
    opened = open_layer(
        [small, self_query, self_key, self_value, self_out, cross_query, cross_key, cross_value,
         cross_out, ff_gate, ff_up, ff_down],
        own_low,
        enc_own,
        hot_rows,
        hot_mask,
        (norm_self.shape[0], bias_table.shape[0]),
        1,
    )
    smalls = opened[0]
    (w_query, w_key, w_value, w_sout, w_cquery, w_ckey, w_cvalue, w_cout, w_gate, w_up, w_down) = [
        x.reshape(-1, x.shape[-1]) for x in opened[1:12]
    ]
    (enc_all, first_all, query, key, value, self_mixed, self_lse, after_self, second,
     cross_q, cross_k, cross_v, cross_mixed, cross_lse, after_cross, third) = opened[12:]
    gain_one, gain_two, gain_three = [
        smalls[:, i, : norm_self.shape[0]].reshape(-1) for i in range(3)
    ]
    table = smalls[:, 3, : bias_table.shape[0]].reshape(H, BUCKETS)
    rows = jnp.einsum("hb,bof->hof", table.astype(LOW), hot, preferred_element_type=F32)
    rows = jnp.where(gap[None] >= 0, rows, NEGATIVE).reshape(H // PAIR, PAIR, *gap.shape)
    first = first_all[count:]

    gate = dot_low(third, w_gate)
    upper = dot_low(third, w_up)
    inner = gated(gate, upper).astype(LOW)
    hidden_out = (after_cross + dot_low(inner, w_down)).astype(LOW)

    grad_top = cotangent[0]
    grad_wdown = dot_left(inner, grad_top).astype(LOW)
    grad_inner = dot_right(grad_top, w_down)
    grad_gate, grad_upper = jax.vjp(gated, gate, upper)[1](grad_inner)
    gate_low = grad_gate.astype(LOW)
    upper_low = grad_upper.astype(LOW)
    grad_wgate = dot_left(third, gate_low).astype(LOW)
    grad_wup = dot_left(third, upper_low).astype(LOW)
    grad_third = dot_right(gate_low, w_gate) + dot_right(upper_low, w_up)
    norm_grad, grad_gain_three = norm_back(after_cross, gain_three, grad_third)
    grad_cross_res = grad_top.astype(F32) + norm_grad
    gains = norm_self.shape[0]
    if width // owners >= 16:
        grad_hidden, grad_encoded, *sums, small_sum = close_layer(
            [grad_wgate, grad_wup, grad_wdown],
            [w_cout, w_ckey, w_cvalue, w_cquery, w_sout, w_key, w_value, w_query],
            [cross_q, cross_k, cross_v, cross_mixed, enc_all, second, cross_lse],
            [query, key, value, self_mixed, first_all, self_lse],
            grad_cross_res,
            after_self,
            own_low,
            grad_gain_three.reshape(1, -1),
            smalls,
            hot_rows,
            hot_mask,
            (gains, bias_table.shape[0]),
            2,
        )
        *arrays, one, two, three, four = finish(
            [grad_hidden, grad_encoded] + sums, small_sum, (gains,) * 3 + bias_table.shape
        )
        grad_hidden, grad_encoded, *sums = arrays
        return (
            hidden_out[None],
            grad_hidden[None],
            grad_encoded[None],
            sums[10],
            sums[9],
            sums[8],
            sums[7],
            sums[6],
            sums[4],
            sums[5],
            sums[3],
            sums[0],
            sums[1],
            sums[2],
            one,
            two,
            three,
            four,
        )
    sum_gate, sum_up = [
        lax.psum_scatter(x, both, scatter_dimension=0, tiled=True).astype(F32)
        for x in (grad_wgate, grad_wup)
    ]
    cross_res_low = grad_cross_res.astype(LOW)
    grad_wcout = dot_left(cross_mixed, cross_res_low).astype(LOW)
    grad_cross_mix = dot_right(cross_res_low, w_cout).astype(LOW)
    grad_cq, grad_ck, grad_cv = attend_back(
        cross_q, cross_k, cross_v, grad_cross_mix, cross_mixed, cross_lse, None, None
    )
    grad_enc = dot_right(grad_ck, w_ckey) + dot_right(grad_cv, w_cvalue)
    enc_back = lax.ppermute(grad_enc[count:].astype(LOW), "seq", [(0, 1), (1, 0)])
    grad_wcquery = dot_left(second, grad_cq).astype(LOW)
    grad_wckey = dot_left(enc_all, grad_ck).astype(LOW)
    grad_wcvalue = dot_left(enc_all, grad_cv).astype(LOW)
    norm_grad, grad_gain_two = norm_back(after_self, gain_two, dot_right(grad_cq, w_cquery))
    grad_self_res = grad_cross_res + norm_grad
    self_res_low = grad_self_res.astype(LOW)
    grad_wsout = dot_left(self_mixed, self_res_low).astype(LOW)
    grad_self_mix = dot_right(self_res_low, w_sout).astype(LOW)
    grad_q, grad_k, grad_v, grad_rows = attend_back(
        query, key, value, grad_self_mix, self_mixed, self_lse, seq_row, rows
    )
    grad_part = dot_right(grad_k, w_key) + dot_right(grad_v, w_value)
    part_back = lax.ppermute(grad_part[:count].astype(LOW), "seq", [(1, 0)])
    grad_wquery = dot_left(first, grad_q).astype(LOW)
    grad_wkey = dot_left(first_all, grad_k).astype(LOW)
    grad_wvalue = dot_left(first_all, grad_v).astype(LOW)
    grad_first = (
        dot_right(grad_q, w_query)
        + grad_part[count:]
        + jnp.where(low_side, grad_part[:count], 0.0)
        + part_back.astype(F32)
    )
    norm_grad, grad_gain_one = norm_back(hidden, gain_one, grad_first)
    grad_hidden = (grad_self_res + norm_grad).astype(LOW)
    grad_encoded = (grad_enc[:count] + enc_back.astype(F32)).astype(LOW)
    table_grad = jnp.einsum(
        "hof,bof->hb", grad_rows.reshape(H, *gap.shape), hot.astype(F32),
        precision=lax.Precision.HIGHEST,
    )
    small_grads = jnp.stack(
        [
            jnp.pad(x.reshape(owners, -1), ((0, 0), (0, 128 - x.size // owners)))
            for x in (grad_gain_one, grad_gain_two, grad_gain_three, table_grad)
        ]
        + [jnp.zeros((owners, 128), F32)] * 4,
        1,
    ).reshape(owners * 8, 128)
    sums = scatter(
        [grad_wdown, grad_wcout, grad_wcquery, grad_wckey, grad_wcvalue, grad_wsout, grad_wquery,
         grad_wkey, grad_wvalue, small_grads],
        2,
    )
    small_sum = sums[9]
    return (
        hidden_out[None],
        grad_hidden[None],
        grad_encoded[None],
        sums[6],
        sums[7],
        sums[8],
        sums[5],
        sums[2],
        sums[3],
        sums[4],
        sums[1],
        sum_gate,
        sum_up,
        sums[0],
        small_sum[0, :gains],
        small_sum[1, :gains],
        small_sum[2, :gains],
        small_sum[3, : bias_table.shape[0]],
    )


def solution(mesh):
    rows = P(("seq", "shard"), None)
    flat = P(("seq", "shard"))
    tokens = P("shard", "seq", None)
    return jax.shard_map(
        on_device,
        mesh=mesh,
        in_specs=(tokens,) * 3 + (P(),) + (rows,) * 11 + (flat,) * 4,
        out_specs=(tokens,) * 3 + (rows,) * 11 + (flat,) * 4,
        check_vma=False,
    )
```

```python
import functools
import jax
import jax.numpy as jnp
from jax import lax
from jax.experimental import pallas as pl
from jax.experimental.pallas import tpu as pltpu
from jax.sharding import PartitionSpec as P

H = 12
BUCKETS = 32
NEGATIVE = -1e30
EPSILON = 1e-06
F32 = jnp.float32
LOW = jnp.bfloat16
PAIR = 2
TILE = 256


def contract(left, right, left_dim, right_dim):
    return lax.dot_general(
        left, right, (((left_dim,), (right_dim,)), ((), ())), preferred_element_type=F32
    )


def keep_head(value, head):
    size = value.shape[1] // PAIR
    lane = lax.broadcasted_iota(jnp.int32, value.shape, 1)
    inside = (lane >= head * size) & (lane < (head + 1) * size)
    return jnp.where(inside, value, jnp.zeros_like(value))


def toeplitz(row):
    wide = jnp.broadcast_to(row, (TILE, 2 * TILE))
    return pltpu.roll(wide, 0, 1, stride=1, stride_axis=0)[:, :TILE]


def skew_sum(total_ref):
    group = 8
    width = 2 * TILE
    summed = jnp.zeros((group, width), F32)
    for start in range(0, TILE, group):
        rows = total_ref[start : start + group, :]
        wide = jnp.concatenate([rows, jnp.zeros_like(rows)], 1)
        summed = summed + pltpu.roll(wide, (width - start) % width, 1)
    out = summed[0:1]
    for row in range(1, group):
        out = out + pltpu.roll(summed[row : row + 1], width - row, 1)
    return out


def scores_t(keys, query, tiles, last):
    scores = contract(keys, query, 1, 1)
    if tiles is None:
        return scores
    parts = [
        scores[place * TILE : (place + 1) * TILE] + tiles[last - place] for place in range(last + 1)
    ]
    return jnp.concatenate(parts, 0) if len(parts) > 1 else parts[0]


def attend_block(q_ref, k_ref, v_t, o_ref, lse_ref, tiles_ref, start, last, span):
    query = q_ref[start : start + TILE, :]
    size = query.shape[1] // PAIR
    mixed = []
    for head in range(PAIR):
        tiles = None if tiles_ref is None else tiles_ref.at[head]
        scores = scores_t(k_ref[:span, :], keep_head(query, head), tiles, last)
        summit = jnp.max(scores, 0, keepdims=True)
        exponent = jnp.exp(scores - summit)
        total = jnp.sum(exponent, 0, keepdims=True)
        weighted = contract(
            v_t[head * size : (head + 1) * size, :span], exponent.astype(LOW), 1, 0
        )
        mixed.append(weighted / total)
        lse_ref[0, head : head + 1, start : start + TILE] = summit + jnp.log(total)
    o_ref[start : start + TILE, :] = jnp.concatenate(mixed, 0).T.astype(LOW)


def attend_kernel(causal, *refs):
    if causal:
        seq_ref, q_ref, k_ref, v_ref, z_ref, o_ref, lse_ref, tiles_ref = refs
        make_tiles(z_ref, tiles_ref)
    else:
        q_ref, k_ref, v_ref, o_ref, lse_ref = refs
    v_t = v_ref[...].T
    blocks = q_ref.shape[0] // TILE
    keys = k_ref.shape[0]
    if not causal:
        for block in range(blocks):
            attend_block(q_ref, k_ref, v_t, o_ref, lse_ref, None, block * TILE, None, keys)
        return
    for side in range(keys // q_ref.shape[0]):

        @pl.when(seq_ref[0] == side)
        def _(side=side):
            for block in range(blocks):
                last = side * blocks + block
                attend_block(
                    q_ref, k_ref, v_t, o_ref, lse_ref, tiles_ref, block * TILE, last,
                    (last + 1) * TILE,
                )


def make_tiles(z_ref, tiles_ref):
    for head in range(PAIR):
        for off in range(z_ref.shape[2]):
            tiles_ref[head, off] = toeplitz(z_ref[0, head, off : off + 1, :])


def attend(queries, keys_all, values, seq_pos, rows):
    count, width = queries.shape
    length = keys_all.shape[0]
    pairs = H // PAIR
    lanes = width // pairs
    offs = length // TILE
    causal = rows is not None
    col = lambda size: pl.BlockSpec((size, lanes), lambda pair, *_: (0, pair))
    in_specs = [col(count), col(length), col(length)]
    args = [queries, keys_all, values]
    scratch = []
    if causal:
        in_specs.append(pl.BlockSpec((1, PAIR, offs, 2 * TILE), lambda pair, *_: (pair, 0, 0, 0)))
        args = [seq_pos] + args + [rows]
        scratch = [pltpu.VMEM((PAIR, offs, TILE, TILE), F32)]
    work = H * count * length
    return pl.pallas_call(
        functools.partial(attend_kernel, causal),
        grid_spec=pltpu.PrefetchScalarGridSpec(
            num_scalar_prefetch=1 if causal else 0,
            grid=(pairs,),
            in_specs=in_specs,
            out_specs=[
                col(count),
                pl.BlockSpec((1, PAIR, count), lambda pair, *_: (pair, 0, 0)),
            ],
            scratch_shapes=scratch,
        ),
        out_shape=[
            jax.ShapeDtypeStruct((count, width), LOW),
            jax.ShapeDtypeStruct((pairs, PAIR, count), F32),
        ],
        cost_estimate=pl.CostEstimate(
            flops=work * 256 * 2, bytes_accessed=6 * length * width, transcendentals=work
        ),
        name="attend_causal" if causal else "attend_cross",
    )(*args)


def back_block(refs, k_t, prod_t, start, last, span, first, tiles_ref, total_ref):
    q_ref, k_ref, v_ref, g_ref, lse_ref, dq_ref, dk_acc, dv_acc = refs
    query = q_ref[start : start + TILE, :]
    grad = g_ref[start : start + TILE, :]
    size = query.shape[1] // PAIR
    dq_t = []
    dk = dv = None
    for head in range(PAIR):
        own = keep_head(query, head)
        own_grad = keep_head(grad, head)
        tiles = None if tiles_ref is None else tiles_ref.at[head]
        scores = scores_t(k_ref[:span, :], own, tiles, last)
        probs = jnp.exp(scores - lse_ref[0, head : head + 1, start : start + TILE])
        grad_probs = contract(v_ref[:span, :], own_grad, 1, 1)
        delta = jnp.sum(
            prod_t[head * size : (head + 1) * size, start : start + TILE], 0, keepdims=True
        )
        grad_scores = probs * (grad_probs - delta)
        low = grad_scores.astype(LOW)
        dv_new = contract(probs.astype(LOW), own_grad, 1, 0)
        dk_new = contract(low, own, 1, 0)
        dv = dv_new if dv is None else dv + dv_new
        dk = dk_new if dk is None else dk + dk_new
        dq_t.append(contract(k_t[head * size : (head + 1) * size, :span], low, 1, 0))
        if total_ref is not None:
            for place in range(last + 1):
                off = last - place
                piece = grad_scores[place * TILE : (place + 1) * TILE]
                if first:
                    total_ref[head, off] = piece
                elif off == last:
                    total_ref[head, off] = piece
                else:
                    total_ref[head, off] += piece
    dq_ref[start : start + TILE, :] = jnp.concatenate(dq_t, 0).T.astype(LOW)
    if first:
        dk_acc[:span, :] = dk
        dv_acc[:span, :] = dv
        if span < dk_acc.shape[0]:
            dk_acc[span:, :] = jnp.zeros((dk_acc.shape[0] - span, dk_acc.shape[1]), F32)
            dv_acc[span:, :] = jnp.zeros((dv_acc.shape[0] - span, dv_acc.shape[1]), F32)
    else:
        dk_acc[:span, :] += dk
        dv_acc[:span, :] += dv


def back_kernel(causal, *refs):
    if causal:
        (seq_ref, q_ref, k_ref, v_ref, g_ref, o_ref, lse_ref, z_ref,
         dq_ref, dk_ref, dv_ref, row_ref, dk_acc, dv_acc, tiles_ref, total_ref) = refs
        make_tiles(z_ref, tiles_ref)
    else:
        (q_ref, k_ref, v_ref, g_ref, o_ref, lse_ref,
         dq_ref, dk_ref, dv_ref, dk_acc, dv_acc) = refs
        tiles_ref = total_ref = None
    k_t = k_ref[...].T
    prod_t = (g_ref[...].astype(F32) * o_ref[...].astype(F32)).T
    blocks = q_ref.shape[0] // TILE
    keys = k_ref.shape[0]
    main = (q_ref, k_ref, v_ref, g_ref, lse_ref, dq_ref, dk_acc, dv_acc)
    if not causal:
        for block in range(blocks):
            back_block(main, k_t, prod_t, block * TILE, None, keys, block == 0, None, None)
    else:
        for side in range(keys // q_ref.shape[0]):

            @pl.when(seq_ref[0] == side)
            def _(side=side):
                for block in range(blocks):
                    last = side * blocks + block
                    back_block(
                        main, k_t, prod_t, block * TILE, last, (last + 1) * TILE,
                        block == 0, tiles_ref, total_ref,
                    )
                for head in range(PAIR):
                    for off in range(keys // TILE):
                        if off < (side + 1) * blocks:
                            row_ref[0, head, off : off + 1, :] = skew_sum(total_ref.at[head, off])
                        else:
                            row_ref[0, head, off : off + 1, :] = jnp.zeros((1, 2 * TILE), F32)

    dk_ref[...] = dk_acc[...].astype(LOW)
    dv_ref[...] = dv_acc[...].astype(LOW)


def attend_back(queries, keys_all, values, grad_mixed, mixed, lse, seq_pos, rows):
    count, width = queries.shape
    length = keys_all.shape[0]
    pairs = H // PAIR
    lanes = width // pairs
    offs = length // TILE
    causal = rows is not None
    col = lambda size: pl.BlockSpec((size, lanes), lambda pair, *_: (0, pair))
    in_specs = [col(count), col(length), col(length), col(count), col(count),
                pl.BlockSpec((1, PAIR, count), lambda pair, *_: (pair, 0, 0))]
    out_specs = [col(count), col(length), col(length)]
    out_shape = [
        jax.ShapeDtypeStruct((count, width), LOW),
        jax.ShapeDtypeStruct((length, width), LOW),
        jax.ShapeDtypeStruct((length, width), LOW),
    ]
    args = [queries, keys_all, values, grad_mixed, mixed, lse]
    scratch = [pltpu.VMEM((length, lanes), F32), pltpu.VMEM((length, lanes), F32)]
    if causal:
        row_spec = pl.BlockSpec((1, PAIR, offs, 2 * TILE), lambda pair, *_: (pair, 0, 0, 0))
        in_specs.append(row_spec)
        out_specs.append(row_spec)
        out_shape.append(jax.ShapeDtypeStruct((pairs, PAIR, offs, 2 * TILE), F32))
        args = [seq_pos] + args + [rows]
        scratch += [pltpu.VMEM((PAIR, offs, TILE, TILE), F32)] * 2
    work = H * count * length
    return pl.pallas_call(
        functools.partial(back_kernel, causal),
        grid_spec=pltpu.PrefetchScalarGridSpec(
            num_scalar_prefetch=1 if causal else 0,
            grid=(pairs,),
            in_specs=in_specs,
            out_specs=out_specs,
            scratch_shapes=scratch,
        ),
        out_shape=out_shape,
        cost_estimate=pl.CostEstimate(
            flops=work * 640 * 2, bytes_accessed=12 * length * width, transcendentals=work
        ),
        name="attend_causal_back" if causal else "attend_cross_back",
    )(*args)


def bucket_rows(buckets, length):
    offs = length // TILE
    place = jnp.arange(2 * TILE, dtype=jnp.int32)
    step = jnp.where(place < TILE, place, place - 2 * TILE)
    gap = (jnp.arange(offs, dtype=jnp.int32) * TILE)[:, None] + step[None, :]
    marks = jnp.arange(BUCKETS, dtype=jnp.int32)
    begins = jnp.sum((buckets[None, :] < marks[:, None]).astype(jnp.int32), 1)
    ends = jnp.sum((buckets[None, :] <= marks[:, None]).astype(jnp.int32), 1)
    hot = (gap[None] >= begins[:, None, None]) & (gap[None] < ends[:, None, None])
    return (gap, hot.astype(LOW))


def bit_plan():
    bits = []
    for axis in ("seq", "shard"):
        size = lax.axis_size(axis)
        assert size & (size - 1) == 0
        bits += [(axis, place) for place in reversed(range(size.bit_length() - 1))]
    return bits


def bit_orders(bits):
    ends = [0, len(bits) - 2, len(bits) - 1]
    rest = [place for place in range(len(bits)) if place not in ends]
    flipped = [ends[1], ends[0], ends[2]]
    return (rest + ends, rest + flipped, ends[:2] + rest + ends[2:])


def coords(bits):
    return [lax.rem(lax.axis_index(axis) // (1 << place), 2) for axis, place in bits]


def partner(bits, which):
    axis, place = bits[which]
    index = lax.axis_index(axis)
    mine = lax.rem(index // (1 << place), 2)
    return {axis: index + (1 - 2 * mine) * (1 << place)}


def greet(bits):
    barrier = pltpu.get_barrier_semaphore()
    for which in range(len(bits)):
        pl.semaphore_signal(
            barrier, inc=1, device_id=partner(bits, which), device_id_type=pl.DeviceIdType.MESH
        )
    pl.semaphore_wait(barrier, len(bits))


def remote(bits, which, source, target, sems):
    return pltpu.make_async_remote_copy(
        src_ref=source,
        dst_ref=target,
        send_sem=sems[0],
        recv_sem=sems[1],
        device_id=partner(bits, which),
        device_id_type=pl.DeviceIdType.MESH,
    )


def send(*args):
    copy = remote(*args)
    copy.start()
    return copy


def scatter_kernel(bits, count, *refs):
    steps = len(bits)
    sources, outs, work = refs[:count], refs[count : 2 * count], refs[2 * count : 3 * count]
    arrivals = refs[3 * count : (3 + steps) * count]
    load_sem, send_sem, recv_sem = refs[(3 + steps) * count :]
    place = coords(bits)
    orders = [list(reversed(order)) for order in bit_orders(bits)[:2]]
    loads = []
    for item in range(count):
        load = pltpu.make_async_copy(sources[item], work[item], load_sem.at[item])
        load.start()
        loads.append(load)
    greet(bits)
    copies = {}

    def add(item, step):
        order = orders[item % 2]
        free = [which for which in range(steps) if which not in order[: step + 1]]
        arrived = arrivals[item * steps + step]
        copies[item, step].wait_recv()
        if not free:
            outs[item][...] = work[item][tuple(place)].astype(F32) + arrived[...].astype(F32)
            return

        @pl.loop(0, 1 << len(free))
        def _(block):
            sub = [lax.rem(block // (1 << (len(free) - 1 - i)), 2) for i in range(len(free))]
            here = tuple(
                sub[free.index(which)] if which in free else place[which] for which in range(steps)
            )
            total = work[item][here].astype(F32) + arrived[tuple(sub)].astype(F32)
            work[item][here] = total.astype(work[item].dtype)

    for turn in range(steps + 1 + (count - 1) // 2):
        for item in range(count):
            step = turn - item // 2
            if not 0 <= step <= steps:
                continue
            if step == 0:
                loads[item].wait()
            else:
                add(item, step - 1)
            if step == steps:
                continue
            order = orders[item % 2]
            there = tuple(
                1 - place[which]
                if which == order[step]
                else (place[which] if which in order[:step] else slice(None))
                for which in range(steps)
            )
            copies[item, step] = send(
                bits,
                order[step],
                work[item].at[there],
                arrivals[item * steps + step],
                (send_sem.at[item, step], recv_sem.at[item, step]),
            )
    for copy in copies.values():
        copy.wait_send()


def scatter(items, collective_id):
    bits = bit_plan()
    steps = len(bits)
    count = len(items)
    sems = pltpu.SemaphoreType.DMA((count, steps))
    owners = 1 << steps
    items = [x.reshape((2,) * steps + (x.shape[0] // owners,) + x.shape[1:]) for x in items]
    tails = [x.shape[steps:] for x in items]
    arrivals = [
        pltpu.VMEM((2,) * (steps - 1 - step) + tail, x.dtype)
        for x, tail in zip(items, tails)
        for step in range(steps)
    ]
    return pl.pallas_call(
        functools.partial(scatter_kernel, bits, count),
        out_shape=[jax.ShapeDtypeStruct(tail, F32) for tail in tails],
        in_specs=[pl.BlockSpec(memory_space=pl.ANY)] * count,
        out_specs=[pl.BlockSpec(memory_space=pltpu.VMEM)] * count,
        scratch_shapes=[pltpu.VMEM(x.shape, x.dtype) for x in items]
        + arrivals
        + [pltpu.SemaphoreType.DMA((count,)), sems, sems],
        compiler_params=pltpu.CompilerParams(collective_id=collective_id, has_side_effects=True),
        name="scatter_rows",
    )(*items)


def table_rows(smalls, table_size, row):
    flat = smalls.reshape(-1, smalls.shape[-1])
    count = table_size * flat.shape[0] // 8
    entry = lax.broadcasted_iota(jnp.int32, (count, flat.shape[0]), 0)
    source = lax.broadcasted_iota(jnp.int32, (count, flat.shape[0]), 1)
    begin = (source >> 3) * table_size
    pick = ((source & 7) == row) & (entry >= begin) & (entry < begin + table_size)
    spread = contract(pick.astype(LOW), flat.astype(LOW), 1, 0)
    lane = lax.broadcasted_iota(jnp.int32, spread.shape, 1)
    place = lax.broadcasted_iota(jnp.int32, spread.shape, 0).astype(F32)
    block = jnp.floor((place + 0.5) * (1.0 / table_size))
    return jnp.where(lane.astype(F32) == place - block * table_size, spread, 0.0)


def gain_row(smalls, size, row):
    flat = smalls.reshape(-1, smalls.shape[-1])
    count = size * flat.shape[0] // 8
    source = lax.broadcasted_iota(jnp.int32, (flat.shape[0], count), 0)
    entry = lax.broadcasted_iota(jnp.int32, (flat.shape[0], count), 1)
    begin = (source >> 3) * size
    pick = ((source & 7) == row) & (entry >= begin) & (entry < begin + size)
    spread = contract(flat.astype(LOW), pick.astype(LOW), 0, 0)
    lane = lax.broadcasted_iota(jnp.int32, spread.shape, 0).astype(F32)
    place = lax.broadcasted_iota(jnp.int32, spread.shape, 1).astype(F32)
    block = jnp.floor((place + 0.5) * (1.0 / size))
    return jnp.sum(jnp.where(lane == place - block * size, spread, 0.0), 0, keepdims=True)


def full_weight(ref):
    value = ref[...].astype(F32)
    return value.reshape(-1, value.shape[-1]).astype(LOW)


ARRAYS = 12
INSIDE = 9
ITEMS = 15
PIECES = tuple((array, None, 0) for array in range(INSIDE)) + tuple(
    (array, axis, half) for array, axis in ((9, 1), (10, 1), (11, 0)) for half in range(2)
)
PATHS = ('xzZyc', 'xzZyc', 'zZxyc', 'zZyxc', 'yxzZc', 'xzZyc', 'zZxyc', 'zZxyc', 'xyzZc', 'zZyxc', 'zZyxc', 'xzZyc', 'yzZxc', 'xzZyc', 'xyzZc')
PLAN = (
    (1, 0, 0), (3, 0, 0), (2, 0, 0), (0, 0, 0), (14, 0, 0), (15, 0, 0),
    (1, 1, 0), (3, 1, 0), (0, 1, 0), (2, 1, 0), (7, 0, 0), (6, 0, 0),
    (1, 2, 0), (3, 2, 0), (9, 0, 0), (10, 0, 0), (11, 0, 0), (2, 2, 0),
    (7, 1, 0), (4, 0, 0), (0, 2, 0), (5, 0, 0), (12, 0, 0), (9, 1, 0),
    (1, 3, 0), (12, 1, 0), (10, 1, 0), (13, 0, 0), (6, 1, 0), (0, 3, 0),
    (8, 0, 0), (4, 1, 0), (11, 1, 0), (3, 3, 0), (14, 1, 0), (1, 4, 0),
    (2, 3, 0), (0, 4, 0), (5, 1, 0), (12, 2, 0), (6, 2, 0), (8, 1, 0),
    (4, 2, 0), (7, 2, 0), (5, 2, 1), (9, 2, 1), (11, 2, 1), (10, 2, 1),
    (13, 1, 1), (2, 4, 1), (14, 2, 2), (16, 0, 2), (12, 3, 2), (3, 4, 2),
    (6, 3, 3), (4, 3, 6), (5, 3, 6), (13, 2, 7), (8, 2, 7), (10, 3, 7),
    (6, 4, 7), (7, 3, 8), (11, 3, 8), (9, 3, 8), (14, 3, 8), (4, 4, 9),
    (5, 4, 9), (8, 3, 11), (13, 3, 11), (7, 4, 11), (12, 4, 14), (11, 4, 16),
    (14, 4, 17), (10, 4, 17), (8, 4, 18), (13, 4, 18), (9, 4, 19),
)
(STAGE_GAIN, STAGE_QUERY, STAGE_KEY, STAGE_VALUE, STAGE_SELF, STAGE_OUT, STAGE_CQUERY, STAGE_CKEY,
 STAGE_CVALUE, STAGE_CROSS, STAGE_COUT, STAGE_END) = (0, 1, 2, 3, 4, 10, 11, 12, 13, 14, 20, 21)


def path_bits(bits, path):
    count = len(bits)
    rest = list(range(1, count - 2))
    groups = {"x": [0], "y": [count - 2], "c": [count - 1], "z": rest[:-1], "Z": rest[-1:]}
    return [groups[letter] for letter in path]


def open_kernel(bits, sizes, *refs):
    gain_size, table_size = sizes
    sources = refs[:ARRAYS]
    hidden_ref, enc_ref, hot_ref, mask_ref = refs[ARRAYS : ARRAYS + 4]
    outs = refs[ARRAYS + 4 : 2 * ARRAYS + 4]
    (enc_out, first_out, q_out, k_out, v_out, mixed_out, lse_out, after_out, second_out,
     cq_out, ck_out, cv_out, cmixed_out, clse_out, across_out, third_out,
     before_ref, flat_ref, tiles_ref, weight_ref,
     send_sem, recv_sem, own_sem, side_send, side_recv) = refs[2 * ARRAYS + 4 :]
    steps = len(bits)
    place = coords(bits)
    seq_pos = lax.axis_index("seq")
    rows = hidden_ref.shape[0]
    keys = first_out.shape[0]
    lanes = hidden_ref.shape[1] // (H // PAIR)

    def own(array):
        return pltpu.make_async_copy(
            sources[array], outs[array].at[tuple(place)], own_sem.at[array]
        )

    def copy(item, step):
        order = sum(path_bits(bits, PATHS[item]), [])
        array, axis, half = PIECES[item]
        here = tuple(
            slice(None) if which in order[:step] else place[which] for which in range(steps)
        )
        part = ()
        if axis is not None:
            size = sources[array].shape[axis] // 2
            part = (slice(None),) * axis + (pl.ds(half * size, size),)
        target = outs[array].at[here + part]
        source = target
        if step == 0:
            source = sources[array].at[part] if part else sources[array]
        return remote(
            bits,
            order[step],
            source,
            target,
            (send_sem.at[item, step], recv_sem.at[item, step]),
        )

    def arrived(item):
        copy(item, steps - 1).wait_recv()

    def side(which):
        source, target = ((hidden_ref, before_ref), (enc_ref, enc_out.at[rows:]))[which]
        return remote(bits, 0, source, target, (side_send.at[which], side_recv.at[which]))

    todo = list(PLAN)
    seen = set()

    def advance(until):
        while todo and todo[0][2] <= until:
            item, step, _ = todo.pop(0)
            if item >= ITEMS:
                side(item - ITEMS).start()
                continue
            groups = path_bits(bits, PATHS[item])
            first = sum(len(group) for group in groups[:step])
            for number in range(first, first + len(groups[step])):
                if number > 0:
                    if PIECES[item][0] not in seen:
                        seen.add(PIECES[item][0])
                        own(PIECES[item][0]).wait()
                    copy(item, number - 1).wait_recv()
                copy(item, number).start()

    for array in range(ARRAYS):
        own(array).start()
    greet(bits)
    enc_out[:rows, :] = enc_ref[...]
    advance(STAGE_GAIN)
    arrived(0)
    gains = [gain_row(outs[0][...], gain_size, row) for row in range(3)]
    flat_ref[...] = table_rows(outs[0][...], table_size, 3)

    def normed(value, gain):
        scale = lax.rsqrt(jnp.mean(value * value, -1, keepdims=True) + EPSILON)
        return (value * scale * gain).astype(LOW)

    def over_rows(count, body):
        @pl.loop(0, count // TILE)
        def _(block):
            body(lambda base=0: pl.ds(base + pl.multiple_of(block * TILE, TILE), TILE))

    def normed_rows(source, start):
        def body(at):
            first_out[at(start), :] = normed(source[at(), :].astype(F32), gains[0])

        over_rows(rows, body)

    def project(item, source, out, begin, count):
        weight_ref[...] = full_weight(outs[item])

        def body(at):
            out[at(), :] = contract(source[at(begin), :], weight_ref[...], 1, 0).astype(LOW)

        over_rows(count, body)

    normed_rows(hidden_ref, rows)
    advance(STAGE_QUERY)
    arrived(1)
    project(1, first_out, q_out, rows, rows)
    advance(STAGE_KEY)
    side(0).wait_recv()

    @pl.when(seq_pos == 0)
    def _():
        first_out[:rows, :] = first_out[rows:, :]

    @pl.when(seq_pos != 0)
    def _():
        normed_rows(before_ref, 0)

    arrived(2)
    project(2, first_out, k_out, 0, keys)
    advance(STAGE_VALUE)
    arrived(3)
    project(3, first_out, v_out, 0, keys)

    advance(STAGE_SELF)

    def between(pair, begin):
        for done in range(H // PAIR - 1):

            @pl.when(pair == done)
            def _(done=done):
                advance(begin + done + 1)

    @pl.loop(0, H // PAIR)
    def _(pair):
        at = pl.ds(pl.multiple_of(pair * lanes, lanes), lanes)
        q_ref, k_ref, v_ref, o_ref = (ref.at[:, at] for ref in (q_out, k_out, v_out, mixed_out))
        for head in range(PAIR):
            column = jnp.sum(
                flat_ref[pl.ds(pl.multiple_of((pair * PAIR + head) * BUCKETS, BUCKETS), BUCKETS), :],
                1,
                keepdims=True,
            )
            for off in range(keys // TILE):
                row = jnp.sum(column * hot_ref[off].astype(F32), 0, keepdims=True)
                tiles_ref[head, off] = toeplitz(row + mask_ref[off])
        v_t = v_ref[...].T
        blocks = rows // TILE
        for part in range(keys // rows):

            @pl.when(seq_pos == part)
            def _(part=part):
                for block in range(blocks):
                    last = part * blocks + block
                    attend_block(
                        q_ref, k_ref, v_t, o_ref, lse_out.at[pl.ds(pair, 1)], tiles_ref,
                        block * TILE, last, (last + 1) * TILE,
                    )

        between(pair, STAGE_SELF)

    def residual(item, mixed, base, total, normal, gain):
        weight_ref[...] = full_weight(outs[item])

        def body(at):
            value = base[at(), :].astype(F32) + contract(mixed[at(), :], weight_ref[...], 1, 0)
            total[at(), :] = value
            normal[at(), :] = normed(value, gain)

        over_rows(rows, body)

    advance(STAGE_OUT)
    arrived(4)
    residual(4, mixed_out, hidden_ref, after_out, second_out, gains[1])
    advance(STAGE_CQUERY)
    arrived(5)
    project(5, second_out, cq_out, 0, rows)
    advance(STAGE_CKEY)
    side(1).wait_recv()
    arrived(6)
    project(6, enc_out, ck_out, 0, keys)
    advance(STAGE_CVALUE)
    arrived(7)
    project(7, enc_out, cv_out, 0, keys)
    advance(STAGE_CROSS)

    @pl.loop(0, H // PAIR)
    def _(pair):
        at = pl.ds(pl.multiple_of(pair * lanes, lanes), lanes)
        q_ref, k_ref, v_ref, o_ref = (ref.at[:, at] for ref in (cq_out, ck_out, cv_out, cmixed_out))
        v_t = v_ref[...].T
        for block in range(rows // TILE):
            attend_block(
                q_ref, k_ref, v_t, o_ref, clse_out.at[pl.ds(pair, 1)], None, block * TILE, None, keys
            )
        between(pair, STAGE_CROSS)

    advance(1000)

    arrived(8)
    residual(8, cmixed_out, after_out, across_out, third_out, gains[2])
    for item in range(INSIDE, ITEMS):
        arrived(item)
    for item in range(ITEMS):
        for step in range(steps):
            copy(item, step).wait_send()
    for which in range(2):
        side(which).wait_send()


def open_layer(items, hidden, encoded, hot, mask, sizes, collective_id):
    bits = bit_plan()
    steps = len(bits)
    count, width = hidden.shape
    length = count * lax.axis_size("seq")
    offs = length // TILE
    sems = pltpu.SemaphoreType.DMA((ITEMS, steps))
    inside = pl.BlockSpec(memory_space=pltpu.VMEM)
    outside = pl.BlockSpec(memory_space=pl.ANY)
    few, many = (count, width), (length, width)
    lse = (H // PAIR, PAIR, count)
    shapes = [((2,) * steps + x.shape, x.dtype) for x in items]
    shapes += [(many, LOW), (many, LOW), (few, LOW), (many, LOW), (many, LOW), (few, LOW)]
    shapes += [(lse, F32), (few, F32), (few, LOW), (few, LOW), (many, LOW), (many, LOW)]
    shapes += [(few, LOW), (lse, F32), (few, F32), (few, LOW)]
    outs = pl.pallas_call(
        functools.partial(open_kernel, bits, sizes),
        out_shape=[jax.ShapeDtypeStruct(*x) for x in shapes],
        in_specs=[inside] * (ARRAYS + 4),
        out_specs=[inside] * INSIDE + [outside] * (ARRAYS - INSIDE) + [inside] * 16,
        scratch_shapes=[
            pltpu.VMEM((count, width), LOW),
            pltpu.VMEM((H * BUCKETS, 128), F32),
            pltpu.VMEM((PAIR, offs, TILE, TILE), F32),
            pltpu.VMEM((width, width), LOW),
            sems,
            sems,
            pltpu.SemaphoreType.DMA((ARRAYS,)),
            pltpu.SemaphoreType.DMA((2,)),
            pltpu.SemaphoreType.DMA((2,)),
        ],
        compiler_params=pltpu.CompilerParams(
            collective_id=collective_id, has_side_effects=True, vmem_limit_bytes=66_000_000
        ),
        name="open_layer",
    )(*items, hidden, encoded, hot, mask)
    return [out.reshape((-1,) + x.shape[-2:]) for out, x in zip(outs, items)] + list(outs[ARRAYS:])


def reversed_bits(bits, path):
    return list(reversed(sum(path_bits(bits, path), [])))


def close_kernel(bits, sizes, *refs):
    gain_size, table_size = sizes
    (ff_refs, weights, cross_refs, self_refs, (smalls_ref, hot_ref, mask_ref, hidden_in),
     (layer_out, hidden_out, enc_out), outs, (small_out,)) = take(refs, (7, 8, 7, 6, 4, 3, 11, 1))
    rest = refs[47:]
    arrivals = rest[: CLOSE_ITEMS * len(bits)]
    (work_ref, ff_work, down_work, small_ref, q_buf, k_buf, pair_buf, rows_buf, grad_buf,
     res_buf, after_buf, weight_buf, enc_own, send_buf, recv_buf, dk_acc, dv_acc,
     tiles_ref, total_ref, rows_ref, flat_ref, gain_sums, send_sem, recv_sem, side_send, side_recv,
     fetch_sem) = rest[CLOSE_ITEMS * len(bits) :]
    steps = len(bits)
    place = coords(bits)
    seq_pos = lax.axis_index("seq")
    rows = res_buf.shape[0]
    keys = k_buf.shape[0]
    lanes = res_buf.shape[1] // (H // PAIR)
    v_buf, keys_in_buf = pair_buf.at[0], pair_buf.at[1]
    mixed_buf, query_in_buf = rows_buf.at[0], rows_buf.at[1]

    def pick(names, which, side):
        return tuple(side if name == which else slice(None) for name in names)

    def order_of(item):
        return reversed_bits(bits, CLOSE_PATHS[item])

    def part_of(item):
        if item not in (DOWN, DOWN + 1):
            return ()
        size = outs[2].shape[0] // 2
        return (pl.ds((item - DOWN) * size, size),)

    def base(item):
        if item == SMALL:
            return small_ref
        if item < DOWN:
            return ff_work.at[item % 4]
        return down_work if item < SQUARES else work_ref.at[item % SLOTS]

    def arrival(item, step):
        return arrivals[item * steps + step]

    def names_at(item, step):
        order = order_of(item)
        return [which for which in range(steps) if which not in order[:step]]

    def copy(item, step):
        which = order_of(item)[step]
        names = names_at(item, step)
        there = pick(names, which, 1 - place[which])
        if step == 0:
            source = base(item).at[there + part_of(item)]
        else:
            source = arrival(item, step - 1).at[there]
        return remote(
            bits, which, source, arrival(item, step), (send_sem.at[item, step], recv_sem.at[item, step])
        )

    def add(item, step):
        which = order_of(item)[step]
        names = names_at(item, step)
        free = [name for name in names if name != which]
        target = arrival(item, step)
        copy(item, step).wait_recv()

        def one(sub):
            here = tuple(place[which] if name == which else sub[free.index(name)] for name in names)
            if step > 0:
                mine = arrival(item, step - 1)[here]
            else:
                mine = base(item)[here + part_of(item)]
            return mine.astype(F32) + target[tuple(sub)].astype(F32)

        if not free:
            if item == SMALL:
                small_out[...] = one(())
            elif item < DOWN:
                size = outs[0].shape[1] // FF_BLOCKS
                outs[item % 2][:, item // 2 * size : (item // 2 + 1) * size] = one(())
            elif item < SQUARES:
                outs[2][part_of(item)] = one(())
            else:
                outs[item - SQUARES + 3][...] = one(())
            return

        @pl.loop(0, 1 << len(free))
        def _(index):
            sub = [lax.rem(index // (1 << (len(free) - 1 - i)), 2) for i in range(len(free))]
            target[tuple(sub)] = one(sub).astype(target.dtype)

    def side(which):
        return remote(
            bits, 0, send_buf.at[which], recv_buf.at[which], (side_send.at[which], side_recv.at[which])
        )

    slots = {entry[:2]: entry[2] for entry in CLOSE_PLAN}
    done_slots = set()
    drained = set()

    def act(item, step):
        if item == CLOSE_ITEMS:
            side(0).start()
            return
        if item > CLOSE_ITEMS:

            @pl.when(seq_pos != 0)
            def _():
                side(1).start()

            return
        groups = list(reversed(path_bits(bits, CLOSE_PATHS[item]))) + [[None]]
        first = sum(len(group) for group in groups[:step])
        for number in range(first, first + len(groups[step])):
            if number > 0:
                add(item, number - 1)
            if number < steps:
                copy(item, number).start()

    def advance(slot):
        assert slot not in done_slots
        done_slots.add(slot)
        for item, step, planned in CLOSE_PLAN:
            if planned == slot:
                act(item, step)

    def drain(item, slot):
        assert slots[item, 1] <= slot
        copy(item, 0).wait_send()
        drained.add((item, 0))

    def fetch(source, target, sem):
        return pltpu.make_async_copy(source, target, fetch_sem.at[sem])

    def weight(number):
        return fetch(weights[number], weight_buf.at[number % 2], number % 2)

    def over_rows(count, body):
        @pl.loop(0, count // TILE)
        def _(block):
            body(lambda start=0: pl.ds(start + pl.multiple_of(block * TILE, TILE), TILE))

    def weight_grad(item, left, right):
        if item - SLOTS >= SQUARES:
            drain(item - SLOTS, max(done_slots))
        owner_grad(work_ref.at[item % SLOTS], left, right)

    def owner_grad(target, left, right):
        half = left.shape[1] // 2

        @pl.loop(0, 2)
        def _(top):
            at = pl.ds(pl.multiple_of(top * half, half), half)
            value = contract(left[:, at], right[...], 0, 0)
            target[top] = value.reshape(target.shape[1:]).astype(LOW)

    def pairs_back(lse_ref, tiles, begin):
        @pl.loop(0, H // PAIR)
        def _(pair):
            at = pl.ds(pl.multiple_of(pair * lanes, lanes), lanes)
            q_ref, k_ref, v_ref, g_ref, o_ref = (
                ref.at[:, at] for ref in (q_buf, k_buf, v_buf, grad_buf, mixed_buf)
            )
            if tiles:
                for head in range(PAIR):
                    start = pl.multiple_of((pair * PAIR + head) * BUCKETS, BUCKETS)
                    column = jnp.sum(flat_ref[pl.ds(start, BUCKETS), :], 1, keepdims=True)
                    for off in range(keys // TILE):
                        row = jnp.sum(column * hot_ref[off].astype(F32), 0, keepdims=True)
                        tiles_ref[head, off] = toeplitz(row + mask_ref[off])
            k_t = k_ref[...].T
            prod_t = (g_ref[...].astype(F32) * o_ref[...].astype(F32)).T
            main = (q_ref, k_ref, v_ref, g_ref, lse_ref.at[pl.ds(pair, 1)], q_ref, dk_acc, dv_acc)
            blocks = rows // TILE
            if not tiles:
                for block in range(blocks):
                    back_block(main, k_t, prod_t, block * TILE, None, keys, block == 0, None, None)
            else:
                for part in range(keys // rows):

                    @pl.when(seq_pos == part)
                    def _(part=part):
                        for block in range(blocks):
                            last = part * blocks + block
                            back_block(
                                main, k_t, prod_t, block * TILE, last, (last + 1) * TILE,
                                block == 0, tiles_ref, total_ref,
                            )
                        for head in range(PAIR):
                            column = jnp.zeros((BUCKETS, 1), F32)
                            for off in range((part + 1) * blocks):
                                row = skew_sum(total_ref.at[head, off])
                                column = column + jnp.sum(
                                    hot_ref[off].astype(F32) * row, 1, keepdims=True
                                )
                            start = pl.multiple_of((pair * PAIR + head) * BUCKETS, BUCKETS)
                            rows_ref[pl.ds(start, BUCKETS), :] = jnp.broadcast_to(
                                column, (BUCKETS, rows_ref.shape[1])
                            )

            k_ref[...] = dk_acc[...].astype(LOW)
            v_ref[...] = dv_acc[...].astype(LOW)
            for done in range(H // PAIR - 1):

                @pl.when(pair == done)
                def _(done=done):
                    advance(begin + done + 1)

    cq_in, ck_in, cv_in, cmixed_in, enc_in, second_in, clse_ref = cross_refs
    q_in, k_in, v_in, mixed_in, first_in, lse_ref = self_refs[:6]
    fetches = [
        fetch(cmixed_in, mixed_buf, 2), fetch(cq_in, q_buf, 3), fetch(ck_in, k_buf, 4),
        fetch(cv_in, v_buf, 5), fetch(enc_in, keys_in_buf, 6), fetch(second_in, query_in_buf, 7),
    ]
    third_in, grad_in, across_in, gate_in, up_in, down_in, after_in = ff_refs
    width = gate_in.shape[1] // FF_BLOCKS
    third_ref, grad_ref = k_buf.at[:rows], k_buf.at[rows:]
    loads = [fetch(third_in, third_ref, 2), fetch(grad_in, grad_ref, 3), fetch(across_in, after_buf, 4)]

    def ff_loads(block, slot):
        at = pl.ds(pl.multiple_of(block * width, width), width)
        return (
            fetch(gate_in.at[:, at], weight_buf.at[slot, :, pl.ds(0, width)], 8 + slot),
            fetch(up_in.at[:, at], pair_buf.at[slot, pl.ds(0, weight_buf.shape[1]), pl.ds(0, width)],
                  10 + slot),
            fetch(down_in.at[at], rows_buf.at[slot, pl.ds(0, width)], 12 + slot),
        )

    for one in ff_loads(0, 0):
        one.start()
    for one in loads:
        one.start()
    greet(bits)
    flat_ref[...] = table_rows(smalls_ref[...], table_size, 3)
    gain_one, gain_two, gain_three = [gain_row(smalls_ref[...], gain_size, row) for row in range(3)]
    for one in loads:
        one.wait()
    res_buf[...] = jnp.zeros_like(res_buf)
    enc_own[...] = jnp.zeros_like(enc_own)

    def ff_rows(slot, at):
        w_gate = weight_buf[slot, :, 0:width]
        w_up = pair_buf[slot, 0 : weight_buf.shape[1], 0:width]
        w_down = rows_buf[slot, 0:width, :]
        gate = contract(third_ref[at, :], w_gate, 1, 0)
        upper = contract(third_ref[at, :], w_up, 1, 0)
        grad = contract(grad_ref[at, :], w_down, 1, 1)
        square = gate * gate
        bend = jnp.tanh(GELU_SCALE * gate * (1.0 + 0.044715 * square))
        open_part = 0.5 * (1.0 + bend)
        active = gate * open_part
        slope = open_part + 0.5 * gate * (1.0 - bend * bend) * (
            GELU_SCALE * (1.0 + 3.0 * 0.044715 * square)
        )
        inner = (active * upper).astype(LOW)
        gate_grad = (grad * upper * slope).astype(LOW)
        upper_grad = (grad * active).astype(LOW)
        q_buf[at, 0:width] = inner
        grad_buf[at, 0:width] = gate_grad
        send_buf[0, at, 0:width] = upper_grad
        res_buf[at, :] += contract(inner, w_down, 1, 0)
        enc_own[at, :] += contract(gate_grad, w_gate, 1, 1) + contract(upper_grad, w_up, 1, 1)

    @pl.loop(0, FF_BLOCKS)
    def _(block):
        slot = lax.rem(block, 2)
        for one in ff_loads(block, slot):
            one.wait()

        @pl.when(block < FF_BLOCKS - 1)
        def _():
            for one in ff_loads(block + 1, 1 - slot):
                one.start()

        @pl.loop(0, rows // TILE)
        def _(part):
            ff_rows(slot, pl.ds(pl.multiple_of(part * TILE, TILE), TILE))

        for now in range(FF_BLOCKS):

            @pl.when(block == now)
            def _(now=now):
                advance(2 + 2 * now)
                if now >= 2:
                    drain(2 * now - 4, 2 + 2 * now)
                    drain(2 * now - 3, 2 + 2 * now)

        owner_grad(ff_work.at[2 * slot], third_ref, grad_buf.at[:, 0:width])
        owner_grad(ff_work.at[2 * slot + 1], third_ref, send_buf.at[0, :, 0:width])
        value = contract(q_buf[:, 0:width], grad_ref[...], 0, 0)
        down_work[lax.div(block, 2), slot] = value.reshape(down_work.shape[2:]).astype(LOW)
        for now in range(FF_BLOCKS):

            @pl.when(block == now)
            def _(now=now):
                advance(3 + 2 * now)

    weight(0).start()
    weight(1).start()
    for one in (fetches[0], fetches[1], fetches[3], fetches[4], fetches[5]):
        one.start()

    def norm_back_rows(value, gain, grad):
        scale = lax.rsqrt(jnp.mean(value * value, -1, keepdims=True) + EPSILON)
        scaled = gain * grad
        inner = jnp.mean(value * scaled, -1, keepdims=True)
        back = scale * scaled - value * (scale * scale * scale) * inner
        return back, jnp.sum(grad * value * scale, 0, keepdims=True)

    gain_sums[...] = jnp.zeros_like(gain_sums)

    def body(at):
        value = after_buf[at(), :]
        send_buf[1, at(), :] = (value + res_buf[at(), :]).astype(LOW)
        back, total = norm_back_rows(value, gain_three, enc_own[at(), :])
        gain_sums[2:3, :] += total
        res_buf[at(), :] = grad_ref[at(), :].astype(F32) + back

    over_rows(rows, body)
    layer_copy = fetch(send_buf.at[1], layer_out, 15)
    layer_copy.start()
    fetch(after_in, after_buf, 14).start()
    fetches[2].start()

    def to_mixed(number, source):
        weight(number).wait()

        def body(at):
            grad_buf[at(), :] = contract(
                source[at(), :].astype(LOW), weight_buf[number % 2], 1, 1
            ).astype(LOW)

        over_rows(rows, body)
        weight(number + 2).start()

    advance(10)
    to_mixed(0, res_buf)
    fetches[0].wait()

    def low_rows(source, target):
        def body(at):
            target[at(), :] = source[at(), :].astype(LOW)

        over_rows(rows, body)

    low_rows(res_buf, send_buf.at[0])
    weight_grad(SQUARES, mixed_buf, send_buf.at[0])
    advance(11)
    for one in fetches[1:4]:
        one.wait()
    pairs_back(clse_ref, False, 11)
    fetch(mixed_in, mixed_buf, 2).start()
    advance(17)

    def both_back(numbers, keep, count):
        def body_other(at):
            total = contract(k_buf[at(count), :], weight_buf[numbers[0] % 2], 1, 1)
            total = total + contract(v_buf[at(count), :], weight_buf[numbers[1] % 2], 1, 1)
            send_buf[keep[0], at(), :] = total.astype(LOW)
            if not count:
                gain_sums[3:4, :] += jnp.sum(
                    total * keys_in_buf[at(), :].astype(F32), 0, keepdims=True
                )

        def body_own(at):
            begin = 0 if count else rows
            total = contract(k_buf[at(begin), :], weight_buf[numbers[0] % 2], 1, 1)
            total = total + contract(v_buf[at(begin), :], weight_buf[numbers[1] % 2], 1, 1)
            keep[1][at(), :] = total

        over_rows(rows, body_other)
        return body_own

    weight(1).wait()
    weight(2).wait()
    own_part = both_back((1, 2), (0, enc_own), rows)
    for one in fetches[4:]:
        one.wait()
    advance(18)
    weight_grad(SQUARES + 1, keys_in_buf, k_buf)
    advance(19)
    weight_grad(SQUARES + 2, keys_in_buf, v_buf)
    advance(20)
    over_rows(rows, own_part)
    fetch(k_in, k_buf, 4).start()
    fetch(v_in, v_buf, 5).start()
    fetch(first_in, keys_in_buf, 6).start()
    weight(3).start()
    weight(4).start()
    advance(21)
    weight_grad(SQUARES + 3, query_in_buf, q_buf)
    advance(22)
    weight(3).wait()
    fetch(after_in, after_buf, 14).wait()

    def body(at):
        grad = contract(q_buf[at(), :], weight_buf[1], 1, 1)
        back, total = norm_back_rows(after_buf[at(), :], gain_two, grad)
        gain_sums[1:2, :] += total
        res_buf[at(), :] += back

    over_rows(rows, body)
    fetch(q_in, q_buf, 3).start()
    weight(5).start()
    weight(4).wait()

    def body(at):
        grad_buf[at(), :] = contract(res_buf[at(), :].astype(LOW), weight_buf[0], 1, 1).astype(LOW)

    over_rows(rows, body)
    weight(6).start()
    fetch(mixed_in, mixed_buf, 2).wait()
    low_rows(res_buf, query_in_buf)
    weight_grad(SQUARES + 4, mixed_buf, query_in_buf)
    advance(23)
    fetch(q_in, q_buf, 3).wait()
    fetch(k_in, k_buf, 4).wait()
    fetch(v_in, v_buf, 5).wait()
    pairs_back(lse_ref, True, 23)
    advance(29)
    side(0).wait_recv()
    side(0).wait_send()

    def body(at):
        send_buf[0, at(), :] = (enc_own[at(), :] + recv_buf[0, at(), :].astype(F32)).astype(LOW)

    over_rows(rows, body)
    enc_copy = fetch(send_buf.at[0], enc_out, 8)
    enc_copy.start()
    fetch(hidden_in, grad_buf, 9).start()
    layer_copy.wait()
    weight(5).wait()
    weight(6).wait()
    fetch(first_in, keys_in_buf, 6).wait()
    own_part = both_back((5, 6), (1, enc_own), 0)

    advance(30)
    weight_grad(SQUARES + 5, keys_in_buf, v_buf)
    advance(31)
    weight_grad(SQUARES + 6, keys_in_buf, k_buf)
    advance(32)
    weight_grad(SQUARES + 7, keys_in_buf.at[rows:], q_buf)
    advance(33)
    over_rows(rows, own_part)
    weight(7).start()
    own_low = (seq_pos == 0).astype(F32)
    fetch(hidden_in, grad_buf, 9).wait()
    weight(7).wait()

    def body(at):
        grad = contract(q_buf[at(), :], weight_buf[1], 1, 1) + enc_own[at(), :]
        grad = grad + own_low * send_buf[1, at(), :].astype(F32)
        enc_own[at(), :] = grad
        value = grad_buf[at(), :].astype(F32)
        scale = lax.rsqrt(jnp.mean(value * value, -1, keepdims=True) + EPSILON)
        gain_sums[0:1, :] += jnp.sum(grad * value * scale, 0, keepdims=True)

    over_rows(rows, body)
    gain_sums[0:1, :] += (1.0 - own_low) * gain_sums[3:4, :] / gain_one
    small_ref[...] = small_rows(
        gain_sums[0:1, :], gain_sums[1:2, :], gain_sums[2:3, :], rows_ref[...], gain_size,
        table_size, small_ref.shape
    )
    advance(34)

    @pl.when(seq_pos == 0)
    def _():
        side(1).wait_recv()

    @pl.when(seq_pos != 0)
    def _():
        side(1).wait_send()

    def body(at):
        grad = enc_own[at(), :] + jnp.where(
            seq_pos == 0, recv_buf[1, at(), :].astype(F32), 0.0
        )
        back, _ = norm_back_rows(grad_buf[at(), :].astype(F32), gain_one, grad)
        hidden_out[at(), :] = (res_buf[at(), :] + back).astype(LOW)

    over_rows(rows, body)
    advance(35)
    assert all(entry[2] in done_slots for entry in CLOSE_PLAN)
    for item in range(CLOSE_ITEMS):
        for step in range(steps):
            if (item, step) not in drained:
                copy(item, step).wait_send()
    enc_copy.wait()


def take(refs, counts):
    out = []
    begin = 0
    for count in counts:
        out.append(refs[begin : begin + count])
        begin += count
    return out


def small_rows(one, two, three, table, gain_size, table_size, shape):
    owners = one.shape[1] // gain_size

    def spread(source, size, row):
        count = owners * size
        target = lax.broadcasted_iota(jnp.int32, (owners * 8, count), 0)
        entry = lax.broadcasted_iota(jnp.int32, (owners * 8, count), 1)
        begin = (target >> 3) * size
        hot = ((target & 7) == row) & (entry >= begin) & (entry < begin + size)
        return lax.dot_general(
            hot.astype(F32), source, (((1,), (0 if row == 3 else 1,)), ((), ())),
            precision=lax.Precision.HIGHEST, preferred_element_type=F32,
        )

    def wheel(shape, axis, size):
        entry = lax.broadcasted_iota(jnp.int32, shape, axis).astype(F32)
        lane = lax.broadcasted_iota(jnp.int32, shape, 1 - axis).astype(F32)
        return lane == entry - size * jnp.floor((entry + 0.5) * (1.0 / size))

    total = jnp.zeros((owners * 8, 128), F32)
    for row, value in enumerate((one, two, three)):
        grid = (128, value.shape[1])
        total = total + spread(
            jnp.where(wheel(grid, 1, gain_size), jnp.broadcast_to(value, grid), 0.0), gain_size, row
        )
    total = total + spread(jnp.where(wheel(table.shape, 0, table_size), table, 0.0), table_size, 3)
    return total.reshape(shape)


SLOTS = 2
FF_BLOCKS = 4
DOWN = 2 * FF_BLOCKS
SQUARES = DOWN + 2
SMALL = SQUARES + 8
CLOSE_ITEMS = SMALL + 1
GELU_SCALE = 0.7978845608028654
CLOSE_PATHS = ('xzZyc', 'xyzZc', 'yzZxc', 'yxzZc', 'xzZyc', 'yzZxc', 'xzZyc', 'yxzZc', 'yzZxc', 'xzZyc', 'zZyxc', 'xyzZc', 'xzZyc', 'xzZyc', 'zZyxc', 'zZxyc', 'xyzZc', 'zZxyc', 'xyzZc')
CLOSE_PLAN = (
    (1, 0, 3), (0, 0, 3), (0, 1, 4), (1, 1, 5), (3, 0, 5), (2, 0, 5),
    (3, 1, 6), (2, 1, 6), (1, 2, 9), (6, 0, 9), (9, 0, 9), (7, 0, 9),
    (8, 0, 10), (5, 0, 10), (0, 2, 11), (9, 1, 11), (6, 1, 11), (10, 0, 11),
    (4, 0, 12), (8, 1, 12), (7, 1, 12), (3, 2, 13), (2, 2, 13), (10, 1, 15),
    (9, 2, 15), (5, 1, 16), (19, 0, 19), (11, 0, 19), (8, 2, 19), (6, 2, 19),
    (4, 1, 20), (10, 2, 20), (12, 0, 20), (3, 3, 20), (11, 1, 21), (7, 2, 21),
    (0, 3, 22), (9, 3, 22), (12, 1, 22), (5, 2, 23), (14, 0, 23), (8, 3, 24),
    (13, 0, 24), (14, 1, 26), (7, 3, 26), (10, 3, 27), (12, 2, 27), (13, 1, 27),
    (4, 2, 27), (11, 2, 27), (6, 3, 27), (20, 0, 30), (14, 2, 30), (2, 3, 31),
    (15, 0, 31), (7, 4, 31), (13, 2, 31), (16, 0, 32), (1, 3, 32), (15, 1, 32),
    (5, 3, 32), (17, 0, 33), (16, 1, 33), (4, 3, 33), (12, 3, 33), (13, 3, 33),
    (17, 1, 33), (10, 4, 33), (11, 3, 34), (7, 5, 34), (18, 0, 34), (8, 4, 34),
    (15, 2, 34), (18, 1, 34), (16, 2, 34), (17, 2, 34), (1, 4, 34), (12, 4, 34),
    (2, 4, 34), (14, 3, 34), (15, 3, 34), (5, 4, 34), (11, 4, 34), (6, 4, 34),
    (18, 2, 34), (3, 4, 34), (9, 4, 34), (8, 5, 34), (17, 3, 34), (14, 4, 34),
    (16, 3, 34), (2, 5, 34), (5, 5, 34), (3, 5, 34), (0, 4, 34), (15, 4, 34),
    (10, 5, 34), (11, 5, 34), (18, 3, 34), (13, 4, 34), (1, 5, 34), (17, 4, 34),
    (4, 4, 34), (6, 5, 34), (9, 5, 34), (16, 4, 34), (18, 4, 34), (13, 5, 35),
    (4, 5, 35), (12, 5, 35), (14, 5, 35), (15, 5, 35), (18, 5, 35), (16, 5, 35),
    (0, 5, 35), (17, 5, 35),
)


def close_layer(forward, weights, cross, own, smalls, hot, mask, hidden, sizes, collective_id):
    bits = bit_plan()
    steps = len(bits)
    owners = 1 << steps
    count, width = hidden.shape
    units = forward[3].shape[1]
    length = cross[1].shape[0]
    offs = length // TILE
    lanes = width // (H // PAIR)
    gate, down = (width // owners, units), (units // owners, width)
    square = (width // owners, width)
    blocks = [(gate[0], units // FF_BLOCKS)] * DOWN + [(down[0] // 2, width)] * 2 + [square] * 8
    kinds = [LOW] * SMALL + [F32]
    blocks.append((8, 128))
    arrivals = [
        pltpu.VMEM((2,) * (steps - 1 - step) + block, kind)
        for block, kind in zip(blocks, kinds)
        for step in range(steps)
    ]
    inside = pl.BlockSpec(memory_space=pltpu.VMEM)
    outside = pl.BlockSpec(memory_space=pl.ANY)
    few, many = (count, width), (length, width)
    vm = pltpu.VMEM
    sems = pltpu.SemaphoreType.DMA((CLOSE_ITEMS, steps))
    pair_sem = pltpu.SemaphoreType.DMA((2,))
    return pl.pallas_call(
        functools.partial(close_kernel, bits, sizes),
        out_shape=[jax.ShapeDtypeStruct(few, LOW)] * 3
        + [jax.ShapeDtypeStruct(block, F32) for block in (gate, gate, down)]
        + [jax.ShapeDtypeStruct(square, F32)] * 8
        + [jax.ShapeDtypeStruct((8, 128), F32)],
        in_specs=[outside] * (7 + 8) + [outside] * 6 + [inside] + [outside] * 5 + [inside]
        + [inside] * 3 + [outside],
        out_specs=[outside, inside, outside] + [inside] * 12,
        scratch_shapes=arrivals
        + [
            vm((SLOTS,) + (2,) * steps + square, LOW),
            vm((4,) + (2,) * steps + (gate[0], units // FF_BLOCKS), LOW),
            vm((2,) * steps + down, LOW),
            vm((2,) * steps + (8, 128), F32),
            vm(few, LOW), vm(many, LOW), vm((2,) + many, LOW), vm((2,) + few, LOW),
            vm(few, LOW), vm(few, F32), vm(few, F32),
            vm((2, width, width), LOW), vm(few, F32), vm((2,) + few, LOW), vm((2,) + few, LOW),
            vm((length, lanes), F32), vm((length, lanes), F32),
            vm((PAIR, offs, TILE, TILE), F32), vm((PAIR, offs, TILE, TILE), F32),
            vm((H * BUCKETS, 128), F32), vm((H * BUCKETS, 128), F32), vm((8, width), F32),
            sems, sems, pair_sem, pair_sem, pltpu.SemaphoreType.DMA((16,)),
        ],
        compiler_params=pltpu.CompilerParams(
            collective_id=collective_id, has_side_effects=True, vmem_limit_bytes=67_000_000
        ),
        name="close_layer",
    )(*forward, *weights, *cross, *own, smalls, hot, mask, hidden)


def finish_kernel(*refs):
    count = (len(refs) - 5) // 2
    for source, target in zip(refs[: count], refs[count + 1 :]):
        target[...] = source[...]
    small = refs[count]
    for row, target in enumerate(refs[2 * count + 1 :]):
        target[...] = small[row, : target.shape[0]]


def finish(arrays, small, sizes):
    count = len(arrays)
    inside = pl.BlockSpec(memory_space=pltpu.VMEM)
    return pl.pallas_call(
        finish_kernel,
        out_shape=[jax.ShapeDtypeStruct(x.shape, x.dtype) for x in arrays]
        + [jax.ShapeDtypeStruct((size,), F32) for size in sizes],
        in_specs=[inside] * (count + 1),
        out_specs=[inside] * (count + 4),
        name="finish",
    )(*arrays, small)


def dot_low(left, right):
    return contract(left, right, 1, 0)


def dot_left(left, right):
    return contract(left, right, 0, 0)


def dot_right(left, right):
    return contract(left, right, 1, 1)


def rms_norm(value, gain):
    return value * lax.rsqrt(jnp.mean(value * value, -1, keepdims=True) + EPSILON) * gain


def norm_back(value, gain, grad):
    return jax.vjp(rms_norm, value, gain)[1](grad)


def gated(gate, upper):
    return jax.nn.gelu(gate, approximate=True) * upper


def pad_rows(rows, dtype):
    return jnp.stack([jnp.pad(row.astype(dtype), (0, 128 - row.shape[0])) for row in rows] + [
        jnp.zeros((128,), dtype)
    ] * (8 - len(rows)))


def on_device(
    hidden_in,
    encoded,
    cotangent,
    buckets,
    self_query,
    self_key,
    self_value,
    self_out,
    cross_query,
    cross_key,
    cross_value,
    cross_out,
    ff_gate,
    ff_up,
    ff_down,
    norm_self,
    norm_cross,
    norm_ff,
    bias_table,
):
    owners = lax.axis_size("seq") * lax.axis_size("shard")
    seq_pos = lax.axis_index("seq")
    seq_row = seq_pos.reshape(1).astype(jnp.int32)
    low_side = seq_pos == 0
    both = ("seq", "shard")
    width = hidden_in.shape[2]
    own_low = hidden_in[0]
    enc_own = encoded[0]
    small = pad_rows([norm_self, norm_cross, norm_ff, bias_table], F32)
    hidden = own_low.astype(F32)
    count = hidden.shape[0]
    length = count * lax.axis_size("seq")
    gap, hot = bucket_rows(buckets, length)
    hot_rows = jnp.swapaxes(hot, 0, 1)
    hot_mask = jnp.where(gap >= 0, 0.0, NEGATIVE)[:, None, :]
    opened = open_layer(
        [small, self_query, self_key, self_value, self_out, cross_query, cross_key, cross_value,
         cross_out, ff_gate, ff_up, ff_down],
        own_low,
        enc_own,
        hot_rows,
        hot_mask,
        (norm_self.shape[0], bias_table.shape[0]),
        1,
    )
    smalls = opened[0]
    (w_query, w_key, w_value, w_sout, w_cquery, w_ckey, w_cvalue, w_cout, w_gate, w_up, w_down) = [
        x.reshape(-1, x.shape[-1]) for x in opened[1:12]
    ]
    (enc_all, first_all, query, key, value, self_mixed, self_lse, after_self, second,
     cross_q, cross_k, cross_v, cross_mixed, cross_lse, after_cross, third) = opened[12:]
    gain_one, gain_two, gain_three = [
        smalls[:, i, : norm_self.shape[0]].reshape(-1) for i in range(3)
    ]
    table = smalls[:, 3, : bias_table.shape[0]].reshape(H, BUCKETS)
    rows = jnp.einsum("hb,bof->hof", table.astype(LOW), hot, preferred_element_type=F32)
    rows = jnp.where(gap[None] >= 0, rows, NEGATIVE).reshape(H // PAIR, PAIR, *gap.shape)
    first = first_all[count:]

    gains = norm_self.shape[0]
    if width // owners >= 16:
        *arrays, small_sum = close_layer(
            [third, cotangent[0], after_cross, w_gate, w_up, w_down, after_self],
            [w_cout, w_ckey, w_cvalue, w_cquery, w_sout, w_key, w_value, w_query],
            [cross_q, cross_k, cross_v, cross_mixed, enc_all, second, cross_lse],
            [query, key, value, self_mixed, first_all, self_lse],
            smalls,
            hot_rows,
            hot_mask,
            own_low,
            (gains, bias_table.shape[0]),
            2,
        )
        *arrays, one, two, three, four = finish(
            arrays, small_sum, (gains,) * 3 + bias_table.shape
        )
        hidden_out, grad_hidden, grad_encoded, *sums = arrays
        return (
            hidden_out[None],
            grad_hidden[None],
            grad_encoded[None],
            sums[10],
            sums[9],
            sums[8],
            sums[7],
            sums[6],
            sums[4],
            sums[5],
            sums[3],
            sums[0],
            sums[1],
            sums[2],
            one,
            two,
            three,
            four,
        )
    gate = dot_low(third, w_gate)
    upper = dot_low(third, w_up)
    inner = gated(gate, upper).astype(LOW)
    hidden_out = (after_cross + dot_low(inner, w_down)).astype(LOW)

    grad_top = cotangent[0]
    grad_wdown = dot_left(inner, grad_top).astype(LOW)
    grad_inner = dot_right(grad_top, w_down)
    grad_gate, grad_upper = jax.vjp(gated, gate, upper)[1](grad_inner)
    gate_low = grad_gate.astype(LOW)
    upper_low = grad_upper.astype(LOW)
    grad_wgate = dot_left(third, gate_low).astype(LOW)
    grad_wup = dot_left(third, upper_low).astype(LOW)
    grad_third = dot_right(gate_low, w_gate) + dot_right(upper_low, w_up)
    norm_grad, grad_gain_three = norm_back(after_cross, gain_three, grad_third)
    grad_cross_res = grad_top.astype(F32) + norm_grad
    sum_gate, sum_up = [
        lax.psum_scatter(x, both, scatter_dimension=0, tiled=True).astype(F32)
        for x in (grad_wgate, grad_wup)
    ]
    cross_res_low = grad_cross_res.astype(LOW)
    grad_wcout = dot_left(cross_mixed, cross_res_low).astype(LOW)
    grad_cross_mix = dot_right(cross_res_low, w_cout).astype(LOW)
    grad_cq, grad_ck, grad_cv = attend_back(
        cross_q, cross_k, cross_v, grad_cross_mix, cross_mixed, cross_lse, None, None
    )
    grad_enc = dot_right(grad_ck, w_ckey) + dot_right(grad_cv, w_cvalue)
    enc_back = lax.ppermute(grad_enc[count:].astype(LOW), "seq", [(0, 1), (1, 0)])
    grad_wcquery = dot_left(second, grad_cq).astype(LOW)
    grad_wckey = dot_left(enc_all, grad_ck).astype(LOW)
    grad_wcvalue = dot_left(enc_all, grad_cv).astype(LOW)
    norm_grad, grad_gain_two = norm_back(after_self, gain_two, dot_right(grad_cq, w_cquery))
    grad_self_res = grad_cross_res + norm_grad
    self_res_low = grad_self_res.astype(LOW)
    grad_wsout = dot_left(self_mixed, self_res_low).astype(LOW)
    grad_self_mix = dot_right(self_res_low, w_sout).astype(LOW)
    grad_q, grad_k, grad_v, grad_rows = attend_back(
        query, key, value, grad_self_mix, self_mixed, self_lse, seq_row, rows
    )
    grad_part = dot_right(grad_k, w_key) + dot_right(grad_v, w_value)
    part_back = lax.ppermute(grad_part[:count].astype(LOW), "seq", [(1, 0)])
    grad_wquery = dot_left(first, grad_q).astype(LOW)
    grad_wkey = dot_left(first_all, grad_k).astype(LOW)
    grad_wvalue = dot_left(first_all, grad_v).astype(LOW)
    grad_first = (
        dot_right(grad_q, w_query)
        + grad_part[count:]
        + jnp.where(low_side, grad_part[:count], 0.0)
        + part_back.astype(F32)
    )
    norm_grad, grad_gain_one = norm_back(hidden, gain_one, grad_first)
    grad_hidden = (grad_self_res + norm_grad).astype(LOW)
    grad_encoded = (grad_enc[:count] + enc_back.astype(F32)).astype(LOW)
    table_grad = jnp.einsum(
        "hof,bof->hb", grad_rows.reshape(H, *gap.shape), hot.astype(F32),
        precision=lax.Precision.HIGHEST,
    )
    small_grads = jnp.stack(
        [
            jnp.pad(x.reshape(owners, -1), ((0, 0), (0, 128 - x.size // owners)))
            for x in (grad_gain_one, grad_gain_two, grad_gain_three, table_grad)
        ]
        + [jnp.zeros((owners, 128), F32)] * 4,
        1,
    ).reshape(owners * 8, 128)
    sums = scatter(
        [grad_wdown, grad_wcout, grad_wcquery, grad_wckey, grad_wcvalue, grad_wsout, grad_wquery,
         grad_wkey, grad_wvalue, small_grads],
        2,
    )
    small_sum = sums[9]
    return (
        hidden_out[None],
        grad_hidden[None],
        grad_encoded[None],
        sums[6],
        sums[7],
        sums[8],
        sums[5],
        sums[2],
        sums[3],
        sums[4],
        sums[1],
        sum_gate,
        sum_up,
        sums[0],
        small_sum[0, :gains],
        small_sum[1, :gains],
        small_sum[2, :gains],
        small_sum[3, : bias_table.shape[0]],
    )


def solution(mesh):
    rows = P(("seq", "shard"), None)
    flat = P(("seq", "shard"))
    tokens = P("shard", "seq", None)
    return jax.shard_map(
        on_device,
        mesh=mesh,
        in_specs=(tokens,) * 3 + (P(),) + (rows,) * 11 + (flat,) * 4,
        out_specs=(tokens,) * 3 + (rows,) * 11 + (flat,) * 4,
        check_vma=False,
    )
```

```python
import functools
import jax
import jax.numpy as jnp
from jax import lax
from jax.experimental import pallas as pl
from jax.experimental.pallas import tpu as pltpu
from jax.sharding import PartitionSpec as P

H = 12
BUCKETS = 32
NEGATIVE = -1e30
EPSILON = 1e-06
F32 = jnp.float32
LOW = jnp.bfloat16
PAIR = 2
TILE = 256


def contract(left, right, left_dim, right_dim):
    return lax.dot_general(
        left, right, (((left_dim,), (right_dim,)), ((), ())), preferred_element_type=F32
    )


def keep_head(value, head):
    size = value.shape[1] // PAIR
    lane = lax.broadcasted_iota(jnp.int32, value.shape, 1)
    inside = (lane >= head * size) & (lane < (head + 1) * size)
    return jnp.where(inside, value, jnp.zeros_like(value))


def toeplitz(row):
    wide = jnp.broadcast_to(row, (TILE, 2 * TILE))
    return pltpu.roll(wide, 0, 1, stride=1, stride_axis=0)[:, :TILE]


def skew_sum(total_ref):
    group = 8
    width = 2 * TILE
    summed = jnp.zeros((group, width), F32)
    for start in range(0, TILE, group):
        rows = total_ref[start : start + group, :]
        wide = jnp.concatenate([rows, jnp.zeros_like(rows)], 1)
        summed = summed + pltpu.roll(wide, (width - start) % width, 1)
    out = summed[0:1]
    for row in range(1, group):
        out = out + pltpu.roll(summed[row : row + 1], width - row, 1)
    return out


def scores_t(keys, query, tiles, last):
    scores = contract(keys, query, 1, 1)
    if tiles is None:
        return scores
    parts = [
        scores[place * TILE : (place + 1) * TILE] + tiles[last - place] for place in range(last + 1)
    ]
    return jnp.concatenate(parts, 0) if len(parts) > 1 else parts[0]


def attend_block(q_ref, k_ref, v_t, o_ref, lse_ref, tiles_ref, start, last, span):
    query = q_ref[start : start + TILE, :]
    size = query.shape[1] // PAIR
    mixed = []
    for head in range(PAIR):
        tiles = None if tiles_ref is None else tiles_ref.at[head]
        scores = scores_t(k_ref[:span, :], keep_head(query, head), tiles, last)
        summit = jnp.max(scores, 0, keepdims=True)
        exponent = jnp.exp(scores - summit)
        total = jnp.sum(exponent, 0, keepdims=True)
        weighted = contract(
            v_t[head * size : (head + 1) * size, :span], exponent.astype(LOW), 1, 0
        )
        mixed.append(weighted / total)
        lse_ref[0, head : head + 1, start : start + TILE] = summit + jnp.log(total)
    o_ref[start : start + TILE, :] = jnp.concatenate(mixed, 0).T.astype(LOW)


def attend_kernel(causal, *refs):
    if causal:
        seq_ref, q_ref, k_ref, v_ref, z_ref, o_ref, lse_ref, tiles_ref = refs
        make_tiles(z_ref, tiles_ref)
    else:
        q_ref, k_ref, v_ref, o_ref, lse_ref = refs
    v_t = v_ref[...].T
    blocks = q_ref.shape[0] // TILE
    keys = k_ref.shape[0]
    if not causal:
        for block in range(blocks):
            attend_block(q_ref, k_ref, v_t, o_ref, lse_ref, None, block * TILE, None, keys)
        return
    for side in range(keys // q_ref.shape[0]):

        @pl.when(seq_ref[0] == side)
        def _(side=side):
            for block in range(blocks):
                last = side * blocks + block
                attend_block(
                    q_ref, k_ref, v_t, o_ref, lse_ref, tiles_ref, block * TILE, last,
                    (last + 1) * TILE,
                )


def make_tiles(z_ref, tiles_ref):
    for head in range(PAIR):
        for off in range(z_ref.shape[2]):
            tiles_ref[head, off] = toeplitz(z_ref[0, head, off : off + 1, :])


def attend(queries, keys_all, values, seq_pos, rows):
    count, width = queries.shape
    length = keys_all.shape[0]
    pairs = H // PAIR
    lanes = width // pairs
    offs = length // TILE
    causal = rows is not None
    col = lambda size: pl.BlockSpec((size, lanes), lambda pair, *_: (0, pair))
    in_specs = [col(count), col(length), col(length)]
    args = [queries, keys_all, values]
    scratch = []
    if causal:
        in_specs.append(pl.BlockSpec((1, PAIR, offs, 2 * TILE), lambda pair, *_: (pair, 0, 0, 0)))
        args = [seq_pos] + args + [rows]
        scratch = [pltpu.VMEM((PAIR, offs, TILE, TILE), F32)]
    work = H * count * length
    return pl.pallas_call(
        functools.partial(attend_kernel, causal),
        grid_spec=pltpu.PrefetchScalarGridSpec(
            num_scalar_prefetch=1 if causal else 0,
            grid=(pairs,),
            in_specs=in_specs,
            out_specs=[
                col(count),
                pl.BlockSpec((1, PAIR, count), lambda pair, *_: (pair, 0, 0)),
            ],
            scratch_shapes=scratch,
        ),
        out_shape=[
            jax.ShapeDtypeStruct((count, width), LOW),
            jax.ShapeDtypeStruct((pairs, PAIR, count), F32),
        ],
        cost_estimate=pl.CostEstimate(
            flops=work * 256 * 2, bytes_accessed=6 * length * width, transcendentals=work
        ),
        name="attend_causal" if causal else "attend_cross",
    )(*args)


def back_block(refs, k_t, prod_t, start, last, span, first, tiles_ref, total_ref):
    q_ref, k_ref, v_ref, g_ref, lse_ref, dq_ref, dk_acc, dv_acc = refs
    query = q_ref[start : start + TILE, :]
    grad = g_ref[start : start + TILE, :]
    size = query.shape[1] // PAIR
    dq_t = []
    dk = dv = None
    for head in range(PAIR):
        own = keep_head(query, head)
        own_grad = keep_head(grad, head)
        tiles = None if tiles_ref is None else tiles_ref.at[head]
        scores = scores_t(k_ref[:span, :], own, tiles, last)
        probs = jnp.exp(scores - lse_ref[0, head : head + 1, start : start + TILE])
        grad_probs = contract(v_ref[:span, :], own_grad, 1, 1)
        delta = jnp.sum(
            prod_t[head * size : (head + 1) * size, start : start + TILE], 0, keepdims=True
        )
        grad_scores = probs * (grad_probs - delta)
        low = grad_scores.astype(LOW)
        dv_new = contract(probs.astype(LOW), own_grad, 1, 0)
        dk_new = contract(low, own, 1, 0)
        dv = dv_new if dv is None else dv + dv_new
        dk = dk_new if dk is None else dk + dk_new
        dq_t.append(contract(k_t[head * size : (head + 1) * size, :span], low, 1, 0))
        if total_ref is not None:
            for place in range(last + 1):
                off = last - place
                piece = grad_scores[place * TILE : (place + 1) * TILE]
                if first:
                    total_ref[head, off] = piece
                elif off == last:
                    total_ref[head, off] = piece
                else:
                    total_ref[head, off] += piece
    dq_ref[start : start + TILE, :] = jnp.concatenate(dq_t, 0).T.astype(LOW)
    if first:
        dk_acc[:span, :] = dk
        dv_acc[:span, :] = dv
        if span < dk_acc.shape[0]:
            dk_acc[span:, :] = jnp.zeros((dk_acc.shape[0] - span, dk_acc.shape[1]), F32)
            dv_acc[span:, :] = jnp.zeros((dv_acc.shape[0] - span, dv_acc.shape[1]), F32)
    else:
        dk_acc[:span, :] += dk
        dv_acc[:span, :] += dv


def back_kernel(causal, *refs):
    if causal:
        (seq_ref, q_ref, k_ref, v_ref, g_ref, o_ref, lse_ref, z_ref,
         dq_ref, dk_ref, dv_ref, row_ref, dk_acc, dv_acc, tiles_ref, total_ref) = refs
        make_tiles(z_ref, tiles_ref)
    else:
        (q_ref, k_ref, v_ref, g_ref, o_ref, lse_ref,
         dq_ref, dk_ref, dv_ref, dk_acc, dv_acc) = refs
        tiles_ref = total_ref = None
    k_t = k_ref[...].T
    prod_t = (g_ref[...].astype(F32) * o_ref[...].astype(F32)).T
    blocks = q_ref.shape[0] // TILE
    keys = k_ref.shape[0]
    main = (q_ref, k_ref, v_ref, g_ref, lse_ref, dq_ref, dk_acc, dv_acc)
    if not causal:
        for block in range(blocks):
            back_block(main, k_t, prod_t, block * TILE, None, keys, block == 0, None, None)
    else:
        for side in range(keys // q_ref.shape[0]):

            @pl.when(seq_ref[0] == side)
            def _(side=side):
                for block in range(blocks):
                    last = side * blocks + block
                    back_block(
                        main, k_t, prod_t, block * TILE, last, (last + 1) * TILE,
                        block == 0, tiles_ref, total_ref,
                    )
                for head in range(PAIR):
                    for off in range(keys // TILE):
                        if off < (side + 1) * blocks:
                            row_ref[0, head, off : off + 1, :] = skew_sum(total_ref.at[head, off])
                        else:
                            row_ref[0, head, off : off + 1, :] = jnp.zeros((1, 2 * TILE), F32)

    dk_ref[...] = dk_acc[...].astype(LOW)
    dv_ref[...] = dv_acc[...].astype(LOW)


def attend_back(queries, keys_all, values, grad_mixed, mixed, lse, seq_pos, rows):
    count, width = queries.shape
    length = keys_all.shape[0]
    pairs = H // PAIR
    lanes = width // pairs
    offs = length // TILE
    causal = rows is not None
    col = lambda size: pl.BlockSpec((size, lanes), lambda pair, *_: (0, pair))
    in_specs = [col(count), col(length), col(length), col(count), col(count),
                pl.BlockSpec((1, PAIR, count), lambda pair, *_: (pair, 0, 0))]
    out_specs = [col(count), col(length), col(length)]
    out_shape = [
        jax.ShapeDtypeStruct((count, width), LOW),
        jax.ShapeDtypeStruct((length, width), LOW),
        jax.ShapeDtypeStruct((length, width), LOW),
    ]
    args = [queries, keys_all, values, grad_mixed, mixed, lse]
    scratch = [pltpu.VMEM((length, lanes), F32), pltpu.VMEM((length, lanes), F32)]
    if causal:
        row_spec = pl.BlockSpec((1, PAIR, offs, 2 * TILE), lambda pair, *_: (pair, 0, 0, 0))
        in_specs.append(row_spec)
        out_specs.append(row_spec)
        out_shape.append(jax.ShapeDtypeStruct((pairs, PAIR, offs, 2 * TILE), F32))
        args = [seq_pos] + args + [rows]
        scratch += [pltpu.VMEM((PAIR, offs, TILE, TILE), F32)] * 2
    work = H * count * length
    return pl.pallas_call(
        functools.partial(back_kernel, causal),
        grid_spec=pltpu.PrefetchScalarGridSpec(
            num_scalar_prefetch=1 if causal else 0,
            grid=(pairs,),
            in_specs=in_specs,
            out_specs=out_specs,
            scratch_shapes=scratch,
        ),
        out_shape=out_shape,
        cost_estimate=pl.CostEstimate(
            flops=work * 640 * 2, bytes_accessed=12 * length * width, transcendentals=work
        ),
        name="attend_causal_back" if causal else "attend_cross_back",
    )(*args)


def bucket_rows(buckets, length):
    offs = length // TILE
    place = jnp.arange(2 * TILE, dtype=jnp.int32)
    step = jnp.where(place < TILE, place, place - 2 * TILE)
    gap = (jnp.arange(offs, dtype=jnp.int32) * TILE)[:, None] + step[None, :]
    marks = jnp.arange(BUCKETS, dtype=jnp.int32)
    begins = jnp.sum((buckets[None, :] < marks[:, None]).astype(jnp.int32), 1)
    ends = jnp.sum((buckets[None, :] <= marks[:, None]).astype(jnp.int32), 1)
    hot = (gap[None] >= begins[:, None, None]) & (gap[None] < ends[:, None, None])
    return (gap, hot.astype(LOW))


def bit_plan():
    bits = []
    for axis in ("seq", "shard"):
        size = lax.axis_size(axis)
        assert size & (size - 1) == 0
        bits += [(axis, place) for place in reversed(range(size.bit_length() - 1))]
    return bits


def bit_orders(bits):
    ends = [0, len(bits) - 2, len(bits) - 1]
    rest = [place for place in range(len(bits)) if place not in ends]
    flipped = [ends[1], ends[0], ends[2]]
    return (rest + ends, rest + flipped, ends[:2] + rest + ends[2:])


def coords(bits):
    return [lax.rem(lax.axis_index(axis) // (1 << place), 2) for axis, place in bits]


def partner(bits, which):
    axis, place = bits[which]
    index = lax.axis_index(axis)
    mine = lax.rem(index // (1 << place), 2)
    return {axis: index + (1 - 2 * mine) * (1 << place)}


def greet(bits):
    barrier = pltpu.get_barrier_semaphore()
    for which in range(len(bits)):
        pl.semaphore_signal(
            barrier, inc=1, device_id=partner(bits, which), device_id_type=pl.DeviceIdType.MESH
        )
    pl.semaphore_wait(barrier, len(bits))


def remote(bits, which, source, target, sems):
    return pltpu.make_async_remote_copy(
        src_ref=source,
        dst_ref=target,
        send_sem=sems[0],
        recv_sem=sems[1],
        device_id=partner(bits, which),
        device_id_type=pl.DeviceIdType.MESH,
    )


def send(*args):
    copy = remote(*args)
    copy.start()
    return copy


def scatter_kernel(bits, count, *refs):
    steps = len(bits)
    sources, outs, work = refs[:count], refs[count : 2 * count], refs[2 * count : 3 * count]
    arrivals = refs[3 * count : (3 + steps) * count]
    load_sem, send_sem, recv_sem = refs[(3 + steps) * count :]
    place = coords(bits)
    orders = [list(reversed(order)) for order in bit_orders(bits)[:2]]
    loads = []
    for item in range(count):
        load = pltpu.make_async_copy(sources[item], work[item], load_sem.at[item])
        load.start()
        loads.append(load)
    greet(bits)
    copies = {}

    def add(item, step):
        order = orders[item % 2]
        free = [which for which in range(steps) if which not in order[: step + 1]]
        arrived = arrivals[item * steps + step]
        copies[item, step].wait_recv()
        if not free:
            outs[item][...] = work[item][tuple(place)].astype(F32) + arrived[...].astype(F32)
            return

        @pl.loop(0, 1 << len(free))
        def _(block):
            sub = [lax.rem(block // (1 << (len(free) - 1 - i)), 2) for i in range(len(free))]
            here = tuple(
                sub[free.index(which)] if which in free else place[which] for which in range(steps)
            )
            total = work[item][here].astype(F32) + arrived[tuple(sub)].astype(F32)
            work[item][here] = total.astype(work[item].dtype)

    for turn in range(steps + 1 + (count - 1) // 2):
        for item in range(count):
            step = turn - item // 2
            if not 0 <= step <= steps:
                continue
            if step == 0:
                loads[item].wait()
            else:
                add(item, step - 1)
            if step == steps:
                continue
            order = orders[item % 2]
            there = tuple(
                1 - place[which]
                if which == order[step]
                else (place[which] if which in order[:step] else slice(None))
                for which in range(steps)
            )
            copies[item, step] = send(
                bits,
                order[step],
                work[item].at[there],
                arrivals[item * steps + step],
                (send_sem.at[item, step], recv_sem.at[item, step]),
            )
    for copy in copies.values():
        copy.wait_send()


def scatter(items, collective_id):
    bits = bit_plan()
    steps = len(bits)
    count = len(items)
    sems = pltpu.SemaphoreType.DMA((count, steps))
    owners = 1 << steps
    items = [x.reshape((2,) * steps + (x.shape[0] // owners,) + x.shape[1:]) for x in items]
    tails = [x.shape[steps:] for x in items]
    arrivals = [
        pltpu.VMEM((2,) * (steps - 1 - step) + tail, x.dtype)
        for x, tail in zip(items, tails)
        for step in range(steps)
    ]
    return pl.pallas_call(
        functools.partial(scatter_kernel, bits, count),
        out_shape=[jax.ShapeDtypeStruct(tail, F32) for tail in tails],
        in_specs=[pl.BlockSpec(memory_space=pl.ANY)] * count,
        out_specs=[pl.BlockSpec(memory_space=pltpu.VMEM)] * count,
        scratch_shapes=[pltpu.VMEM(x.shape, x.dtype) for x in items]
        + arrivals
        + [pltpu.SemaphoreType.DMA((count,)), sems, sems],
        compiler_params=pltpu.CompilerParams(collective_id=collective_id, has_side_effects=True),
        name="scatter_rows",
    )(*items)


def table_rows(smalls, table_size, row):
    flat = smalls.reshape(-1, smalls.shape[-1])
    count = table_size * flat.shape[0] // 8
    entry = lax.broadcasted_iota(jnp.int32, (count, flat.shape[0]), 0)
    source = lax.broadcasted_iota(jnp.int32, (count, flat.shape[0]), 1)
    begin = (source >> 3) * table_size
    pick = ((source & 7) == row) & (entry >= begin) & (entry < begin + table_size)
    spread = contract(pick.astype(LOW), flat.astype(LOW), 1, 0)
    lane = lax.broadcasted_iota(jnp.int32, spread.shape, 1)
    place = lax.broadcasted_iota(jnp.int32, spread.shape, 0).astype(F32)
    block = jnp.floor((place + 0.5) * (1.0 / table_size))
    return jnp.where(lane.astype(F32) == place - block * table_size, spread, 0.0)


def gain_row(smalls, size, row):
    flat = smalls.reshape(-1, smalls.shape[-1])
    count = size * flat.shape[0] // 8
    source = lax.broadcasted_iota(jnp.int32, (flat.shape[0], count), 0)
    entry = lax.broadcasted_iota(jnp.int32, (flat.shape[0], count), 1)
    begin = (source >> 3) * size
    pick = ((source & 7) == row) & (entry >= begin) & (entry < begin + size)
    spread = contract(flat.astype(LOW), pick.astype(LOW), 0, 0)
    lane = lax.broadcasted_iota(jnp.int32, spread.shape, 0).astype(F32)
    place = lax.broadcasted_iota(jnp.int32, spread.shape, 1).astype(F32)
    block = jnp.floor((place + 0.5) * (1.0 / size))
    return jnp.sum(jnp.where(lane == place - block * size, spread, 0.0), 0, keepdims=True)


def full_weight(ref):
    value = ref[...].astype(F32)
    return value.reshape(-1, value.shape[-1]).astype(LOW)


ARRAYS = 12
INSIDE = 9
ITEMS = 15
PIECES = tuple((array, None, 0) for array in range(INSIDE)) + tuple(
    (array, axis, half) for array, axis in ((9, 1), (10, 1), (11, 0)) for half in range(2)
)
PATHS = ('xzZyc', 'xzZyc', 'zZxyc', 'zZyxc', 'yxzZc', 'xzZyc', 'zZxyc', 'zZxyc', 'xyzZc', 'zZyxc', 'zZyxc', 'xzZyc', 'yzZxc', 'xzZyc', 'xyzZc')
PLAN = (
    (1, 0, 0), (3, 0, 0), (2, 0, 0), (0, 0, 0), (14, 0, 0), (15, 0, 0),
    (1, 1, 0), (3, 1, 0), (0, 1, 0), (2, 1, 0), (7, 0, 0), (6, 0, 0),
    (1, 2, 0), (3, 2, 0), (9, 0, 0), (10, 0, 0), (11, 0, 0), (2, 2, 0),
    (7, 1, 0), (4, 0, 0), (0, 2, 0), (5, 0, 0), (12, 0, 0), (9, 1, 0),
    (1, 3, 0), (12, 1, 0), (10, 1, 0), (13, 0, 0), (6, 1, 0), (0, 3, 0),
    (8, 0, 0), (4, 1, 0), (11, 1, 0), (3, 3, 0), (14, 1, 0), (1, 4, 0),
    (2, 3, 0), (0, 4, 0), (5, 1, 0), (12, 2, 0), (6, 2, 0), (8, 1, 0),
    (4, 2, 0), (7, 2, 0), (5, 2, 1), (9, 2, 1), (11, 2, 1), (10, 2, 1),
    (13, 1, 1), (2, 4, 1), (14, 2, 2), (16, 0, 2), (12, 3, 2), (3, 4, 2),
    (6, 3, 3), (4, 3, 6), (5, 3, 6), (13, 2, 7), (8, 2, 7), (10, 3, 7),
    (6, 4, 7), (7, 3, 8), (11, 3, 8), (9, 3, 8), (14, 3, 8), (4, 4, 9),
    (5, 4, 9), (8, 3, 11), (13, 3, 11), (7, 4, 11), (12, 4, 14), (11, 4, 16),
    (14, 4, 17), (10, 4, 17), (8, 4, 18), (13, 4, 18), (9, 4, 19),
)
(STAGE_GAIN, STAGE_QUERY, STAGE_KEY, STAGE_VALUE, STAGE_SELF, STAGE_OUT, STAGE_CQUERY, STAGE_CKEY,
 STAGE_CVALUE, STAGE_CROSS, STAGE_COUT, STAGE_END) = (0, 1, 2, 3, 4, 10, 11, 12, 13, 14, 20, 21)


def path_bits(bits, path):
    count = len(bits)
    rest = list(range(1, count - 2))
    groups = {"x": [0], "y": [count - 2], "c": [count - 1], "z": rest[:-1], "Z": rest[-1:]}
    return [groups[letter] for letter in path]


def open_kernel(bits, sizes, *refs):
    gain_size, table_size = sizes
    sources = refs[:ARRAYS]
    hidden_ref, enc_ref, buckets_ref = refs[ARRAYS : ARRAYS + 3]
    finals = refs[ARRAYS + 3 : 2 * ARRAYS + 19]
    kept = refs[2 * ARRAYS + 19 : 2 * ARRAYS + 35 + INSIDE]
    outs = kept[:INSIDE] + finals[INSIDE:ARRAYS]
    (enc_out, first_out, q_out, k_out, v_out, mixed_out, lse_out, after_out, second_out,
     cq_out, ck_out, cv_out, cmixed_out, clse_out, across_out, third_out) = kept[INSIDE:]
    (before_ref, flat_ref, hot_ref, mask_ref, tiles_ref, weight_ref,
     send_sem, recv_sem, own_sem, side_send, side_recv, keep_sem) = refs[2 * ARRAYS + 35 + INSIDE :]
    steps = len(bits)
    place = coords(bits)
    seq_pos = lax.axis_index("seq")
    rows = hidden_ref.shape[0]
    keys = first_out.shape[0]
    lanes = hidden_ref.shape[1] // (H // PAIR)

    def kept_copy(number):
        final = finals[number] if number < INSIDE else finals[number - INSIDE + ARRAYS]
        return pltpu.make_async_copy(kept[number], final, keep_sem.at[number])

    def keep(*numbers):
        for number in numbers:
            kept_copy(number).start()

    def keep_act(*numbers):
        keep(*(number + INSIDE for number in numbers))

    def own(array):
        return pltpu.make_async_copy(
            sources[array], outs[array].at[tuple(place)], own_sem.at[array]
        )

    def copy(item, step):
        order = sum(path_bits(bits, PATHS[item]), [])
        array, axis, half = PIECES[item]
        here = tuple(
            slice(None) if which in order[:step] else place[which] for which in range(steps)
        )
        part = ()
        if axis is not None:
            size = sources[array].shape[axis] // 2
            part = (slice(None),) * axis + (pl.ds(half * size, size),)
        target = outs[array].at[here + part]
        source = target
        if step == 0:
            source = sources[array].at[part] if part else sources[array]
        return remote(
            bits,
            order[step],
            source,
            target,
            (send_sem.at[item, step], recv_sem.at[item, step]),
        )

    def arrived(item):
        copy(item, steps - 1).wait_recv()
        if item < INSIDE:
            keep(item)

    def side(which):
        source, target = ((hidden_ref, before_ref), (enc_ref, enc_out.at[rows:]))[which]
        return remote(bits, 0, source, target, (side_send.at[which], side_recv.at[which]))

    todo = list(PLAN)
    seen = set()

    def advance(until):
        while todo and todo[0][2] <= until:
            item, step, _ = todo.pop(0)
            if item >= ITEMS:
                side(item - ITEMS).start()
                continue
            groups = path_bits(bits, PATHS[item])
            first = sum(len(group) for group in groups[:step])
            for number in range(first, first + len(groups[step])):
                if number > 0:
                    if PIECES[item][0] not in seen:
                        seen.add(PIECES[item][0])
                        own(PIECES[item][0]).wait()
                    copy(item, number - 1).wait_recv()
                copy(item, number).start()

    for array in range(ARRAYS):
        own(array).start()
    greet(bits)
    enc_out[:rows, :] = enc_ref[...]
    make_hot(buckets_ref, hot_ref, mask_ref)
    advance(STAGE_GAIN)
    arrived(0)
    gains = [gain_row(outs[0][...], gain_size, row) for row in range(3)]
    flat_ref[...] = table_rows(outs[0][...], table_size, 3)

    def normed(value, gain):
        scale = lax.rsqrt(jnp.mean(value * value, -1, keepdims=True) + EPSILON)
        return (value * scale * gain).astype(LOW)

    def over_rows(count, body):
        @pl.loop(0, count // TILE)
        def _(block):
            body(lambda base=0: pl.ds(base + pl.multiple_of(block * TILE, TILE), TILE))

    def normed_rows(source, start):
        def body(at):
            first_out[at(start), :] = normed(source[at(), :].astype(F32), gains[0])

        over_rows(rows, body)

    def project(item, source, out, begin, count):
        weight_ref[...] = full_weight(outs[item])

        def body(at):
            out[at(), :] = contract(source[at(begin), :], weight_ref[...], 1, 0).astype(LOW)

        over_rows(count, body)

    normed_rows(hidden_ref, rows)
    advance(STAGE_QUERY)
    arrived(1)
    project(1, first_out, q_out, rows, rows)
    keep_act(2)
    advance(STAGE_KEY)
    side(0).wait_recv()

    @pl.when(seq_pos == 0)
    def _():
        first_out[:rows, :] = first_out[rows:, :]

    @pl.when(seq_pos != 0)
    def _():
        normed_rows(before_ref, 0)

    arrived(2)
    project(2, first_out, k_out, 0, keys)
    keep_act(1, 3)
    advance(STAGE_VALUE)
    arrived(3)
    project(3, first_out, v_out, 0, keys)
    keep_act(4)

    advance(STAGE_SELF)

    def between(pair, begin):
        for done in range(H // PAIR - 1):

            @pl.when(pair == done)
            def _(done=done):
                advance(begin + done + 1)

    @pl.loop(0, H // PAIR)
    def _(pair):
        at = pl.ds(pl.multiple_of(pair * lanes, lanes), lanes)
        q_ref, k_ref, v_ref, o_ref = (ref.at[:, at] for ref in (q_out, k_out, v_out, mixed_out))
        for head in range(PAIR):
            column = jnp.sum(
                flat_ref[pl.ds(pl.multiple_of((pair * PAIR + head) * BUCKETS, BUCKETS), BUCKETS), :],
                1,
                keepdims=True,
            )
            for off in range(keys // TILE):
                row = jnp.sum(column * hot_ref[off].astype(F32), 0, keepdims=True)
                tiles_ref[head, off] = toeplitz(row + mask_ref[off])
        v_t = v_ref[...].T
        blocks = rows // TILE
        for part in range(keys // rows):

            @pl.when(seq_pos == part)
            def _(part=part):
                for block in range(blocks):
                    last = part * blocks + block
                    attend_block(
                        q_ref, k_ref, v_t, o_ref, lse_out.at[pl.ds(pair, 1)], tiles_ref,
                        block * TILE, last, (last + 1) * TILE,
                    )

        between(pair, STAGE_SELF)

    def residual(item, mixed, base, total, normal, gain):
        weight_ref[...] = full_weight(outs[item])

        def body(at):
            value = base[at(), :].astype(F32) + contract(mixed[at(), :], weight_ref[...], 1, 0)
            total[at(), :] = value
            normal[at(), :] = normed(value, gain)

        over_rows(rows, body)

    keep_act(5, 6)
    advance(STAGE_OUT)
    arrived(4)
    residual(4, mixed_out, hidden_ref, after_out, second_out, gains[1])
    keep_act(7, 8)
    advance(STAGE_CQUERY)
    arrived(5)
    project(5, second_out, cq_out, 0, rows)
    keep_act(9)
    advance(STAGE_CKEY)
    side(1).wait_recv()
    arrived(6)
    project(6, enc_out, ck_out, 0, keys)
    keep_act(0, 10)
    advance(STAGE_CVALUE)
    arrived(7)
    project(7, enc_out, cv_out, 0, keys)
    keep_act(11)
    advance(STAGE_CROSS)

    @pl.loop(0, H // PAIR)
    def _(pair):
        at = pl.ds(pl.multiple_of(pair * lanes, lanes), lanes)
        q_ref, k_ref, v_ref, o_ref = (ref.at[:, at] for ref in (cq_out, ck_out, cv_out, cmixed_out))
        v_t = v_ref[...].T
        for block in range(rows // TILE):
            attend_block(
                q_ref, k_ref, v_t, o_ref, clse_out.at[pl.ds(pair, 1)], None, block * TILE, None, keys
            )
        between(pair, STAGE_CROSS)

    keep_act(12, 13)
    advance(STAGE_COUT)
    arrived(8)
    residual(8, cmixed_out, after_out, across_out, third_out, gains[2])
    keep_act(14, 15)
    advance(STAGE_END)
    assert not todo
    for item in range(INSIDE, ITEMS):
        arrived(item)
    for item in range(ITEMS):
        for step in range(steps):
            copy(item, step).wait_send()
    for which in range(2):
        side(which).wait_send()
    for number in range(len(kept)):
        kept_copy(number).wait()


def make_hot(buckets_ref, hot_ref, mask_ref):
    offs, marks, width = hot_ref.shape
    bucket = buckets_ref[...].astype(F32)
    mark = lax.broadcasted_iota(jnp.int32, (marks, bucket.shape[1]), 0).astype(F32)
    begin = jnp.sum((bucket < mark).astype(F32), 1, keepdims=True)
    end = jnp.sum((bucket <= mark).astype(F32), 1, keepdims=True)
    place = lax.broadcasted_iota(jnp.int32, (marks, width), 1).astype(F32)
    step = jnp.where(place < TILE, place, place - width)
    for off in range(offs):
        gap = step + off * TILE
        hot_ref[off] = ((gap >= begin) & (gap < end)).astype(F32).astype(LOW)
        mask_ref[off] = jnp.where(gap[:1] >= 0, 0.0, NEGATIVE)


def open_layer(items, hidden, encoded, buckets, sizes, collective_id):
    bits = bit_plan()
    steps = len(bits)
    count, width = hidden.shape
    length = count * lax.axis_size("seq")
    offs = length // TILE
    sems = pltpu.SemaphoreType.DMA((ITEMS, steps))
    inside = pl.BlockSpec(memory_space=pltpu.VMEM)
    outside = pl.BlockSpec(memory_space=pl.ANY)
    few, many = (count, width), (length, width)
    lse = (H // PAIR, PAIR, count)
    shapes = [((2,) * steps + x.shape, x.dtype) for x in items]
    shapes += [(many, LOW), (many, LOW), (few, LOW), (many, LOW), (many, LOW), (few, LOW)]
    shapes += [(lse, F32), (few, F32), (few, LOW), (few, LOW), (many, LOW), (many, LOW)]
    shapes += [(few, LOW), (lse, F32), (few, F32), (few, LOW)]
    outs = pl.pallas_call(
        functools.partial(open_kernel, bits, sizes),
        out_shape=[jax.ShapeDtypeStruct(*x) for x in shapes],
        in_specs=[inside] * (ARRAYS + 3),
        out_specs=[outside] * (ARRAYS + 16),
        scratch_shapes=[pltpu.VMEM(*x) for x in shapes[:INSIDE] + shapes[ARRAYS:]]
        + [
            pltpu.VMEM((count, width), LOW),
            pltpu.VMEM((H * BUCKETS, 128), F32),
            pltpu.VMEM((offs, BUCKETS, 2 * TILE), LOW),
            pltpu.VMEM((offs, 1, 2 * TILE), F32),
            pltpu.VMEM((PAIR, offs, TILE, TILE), F32),
            pltpu.VMEM((width, width), LOW),
            sems,
            sems,
            pltpu.SemaphoreType.DMA((ARRAYS,)),
            pltpu.SemaphoreType.DMA((2,)),
            pltpu.SemaphoreType.DMA((2,)),
            pltpu.SemaphoreType.DMA((INSIDE + 16,)),
        ],
        compiler_params=pltpu.CompilerParams(
            collective_id=collective_id, has_side_effects=True, vmem_limit_bytes=66_000_000
        ),
        name="open_layer",
    )(*items, hidden, encoded, buckets)
    return [out.reshape((-1,) + x.shape[-2:]) for out, x in zip(outs, items)] + list(outs[ARRAYS:])


def reversed_bits(bits, path):
    return list(reversed(sum(path_bits(bits, path), [])))


def close_kernel(bits, sizes, *refs):
    gain_size, table_size = sizes
    (ff_refs, weights, cross_refs, self_refs, (smalls_ref, buckets_ref, hidden_in),
     (layer_out, hidden_out, enc_out), outs, (small_out,)) = take(refs, (7, 8, 7, 6, 3, 3, 11, 1))
    rest = refs[46:]
    arrivals = rest[: CLOSE_ITEMS * len(bits)]
    (work_ref, ff_work, down_work, small_ref, q_buf, k_buf, pair_buf, rows_buf, grad_buf,
     res_buf, after_buf, weight_buf, enc_own, send_buf, recv_buf, dk_acc, dv_acc,
     tiles_ref, total_ref, rows_ref, flat_ref, gain_sums, hot_ref,
     mask_ref, send_sem, recv_sem, side_send, side_recv,
     fetch_sem) = rest[CLOSE_ITEMS * len(bits) :]
    steps = len(bits)
    place = coords(bits)
    seq_pos = lax.axis_index("seq")
    rows = res_buf.shape[0]
    keys = k_buf.shape[0]
    lanes = res_buf.shape[1] // (H // PAIR)
    v_buf, keys_in_buf = pair_buf.at[0], pair_buf.at[1]
    mixed_buf, query_in_buf = rows_buf.at[0], rows_buf.at[1]

    def pick(names, which, side):
        return tuple(side if name == which else slice(None) for name in names)

    def order_of(item):
        return reversed_bits(bits, CLOSE_PATHS[item])

    def part_of(item):
        if item not in (DOWN, DOWN + 1):
            return ()
        size = outs[2].shape[0] // 2
        return (pl.ds((item - DOWN) * size, size),)

    def base(item):
        if item == SMALL:
            return small_ref
        if item < DOWN:
            return ff_work.at[item % 4]
        return down_work if item < SQUARES else work_ref.at[item % SLOTS]

    def arrival(item, step):
        return arrivals[item * steps + step]

    def names_at(item, step):
        order = order_of(item)
        return [which for which in range(steps) if which not in order[:step]]

    def copy(item, step):
        which = order_of(item)[step]
        names = names_at(item, step)
        there = pick(names, which, 1 - place[which])
        if step == 0:
            source = base(item).at[there + part_of(item)]
        else:
            source = arrival(item, step - 1).at[there]
        return remote(
            bits, which, source, arrival(item, step), (send_sem.at[item, step], recv_sem.at[item, step])
        )

    def add(item, step):
        which = order_of(item)[step]
        names = names_at(item, step)
        free = [name for name in names if name != which]
        target = arrival(item, step)
        copy(item, step).wait_recv()

        def one(sub):
            here = tuple(place[which] if name == which else sub[free.index(name)] for name in names)
            if step > 0:
                mine = arrival(item, step - 1)[here]
            else:
                mine = base(item)[here + part_of(item)]
            return mine.astype(F32) + target[tuple(sub)].astype(F32)

        if not free:
            if item == SMALL:
                small_out[...] = one(())
            elif item < DOWN:
                size = outs[0].shape[1] // FF_BLOCKS
                outs[item % 2][:, item // 2 * size : (item // 2 + 1) * size] = one(())
            elif item < SQUARES:
                outs[2][part_of(item)] = one(())
            else:
                outs[item - SQUARES + 3][...] = one(())
            return

        @pl.loop(0, 1 << len(free))
        def _(index):
            sub = [lax.rem(index // (1 << (len(free) - 1 - i)), 2) for i in range(len(free))]
            target[tuple(sub)] = one(sub).astype(target.dtype)

    def side(which):
        return remote(
            bits, 0, send_buf.at[which], recv_buf.at[which], (side_send.at[which], side_recv.at[which])
        )

    slots = {entry[:2]: entry[2] for entry in CLOSE_PLAN}
    done_slots = set()
    drained = set()

    def act(item, step):
        if item == CLOSE_ITEMS:
            side(0).start()
            return
        if item > CLOSE_ITEMS:

            @pl.when(seq_pos != 0)
            def _():
                side(1).start()

            return
        groups = list(reversed(path_bits(bits, CLOSE_PATHS[item]))) + [[None]]
        first = sum(len(group) for group in groups[:step])
        for number in range(first, first + len(groups[step])):
            if number > 0:
                add(item, number - 1)
            if number < steps:
                copy(item, number).start()

    def advance(slot):
        assert slot not in done_slots
        done_slots.add(slot)
        for item, step, planned in CLOSE_PLAN:
            if planned == slot:
                act(item, step)

    def drain(item, slot):
        assert slots[item, 1] <= slot
        copy(item, 0).wait_send()
        drained.add((item, 0))

    def fetch(source, target, sem):
        return pltpu.make_async_copy(source, target, fetch_sem.at[sem])

    def weight(number):
        return fetch(weights[number], weight_buf.at[number % 2], number % 2)

    def over_rows(count, body):
        @pl.loop(0, count // TILE)
        def _(block):
            body(lambda start=0: pl.ds(start + pl.multiple_of(block * TILE, TILE), TILE))

    def weight_grad(item, left, right):
        if item - SLOTS >= SQUARES:
            drain(item - SLOTS, max(done_slots))
        owner_grad(work_ref.at[item % SLOTS], left, right)

    def owner_grad(target, left, right):
        half = left.shape[1] // 2

        @pl.loop(0, 2)
        def _(top):
            at = pl.ds(pl.multiple_of(top * half, half), half)
            value = contract(left[:, at], right[...], 0, 0)
            target[top] = value.reshape(target.shape[1:]).astype(LOW)

    def pairs_back(lse_ref, tiles, begin):
        @pl.loop(0, H // PAIR)
        def _(pair):
            at = pl.ds(pl.multiple_of(pair * lanes, lanes), lanes)
            q_ref, k_ref, v_ref, g_ref, o_ref = (
                ref.at[:, at] for ref in (q_buf, k_buf, v_buf, grad_buf, mixed_buf)
            )
            if tiles:
                for head in range(PAIR):
                    start = pl.multiple_of((pair * PAIR + head) * BUCKETS, BUCKETS)
                    column = jnp.sum(flat_ref[pl.ds(start, BUCKETS), :], 1, keepdims=True)
                    for off in range(keys // TILE):
                        row = jnp.sum(column * hot_ref[off].astype(F32), 0, keepdims=True)
                        tiles_ref[head, off] = toeplitz(row + mask_ref[off])
            k_t = k_ref[...].T
            prod_t = (g_ref[...].astype(F32) * o_ref[...].astype(F32)).T
            main = (q_ref, k_ref, v_ref, g_ref, lse_ref.at[pl.ds(pair, 1)], q_ref, dk_acc, dv_acc)
            blocks = rows // TILE
            if not tiles:
                for block in range(blocks):
                    back_block(main, k_t, prod_t, block * TILE, None, keys, block == 0, None, None)
            else:
                for part in range(keys // rows):

                    @pl.when(seq_pos == part)
                    def _(part=part):
                        for block in range(blocks):
                            last = part * blocks + block
                            back_block(
                                main, k_t, prod_t, block * TILE, last, (last + 1) * TILE,
                                block == 0, tiles_ref, total_ref,
                            )
                        for head in range(PAIR):
                            column = jnp.zeros((BUCKETS, 1), F32)
                            for off in range((part + 1) * blocks):
                                row = skew_sum(total_ref.at[head, off])
                                column = column + jnp.sum(
                                    hot_ref[off].astype(F32) * row, 1, keepdims=True
                                )
                            start = pl.multiple_of((pair * PAIR + head) * BUCKETS, BUCKETS)
                            rows_ref[pl.ds(start, BUCKETS), :] = jnp.broadcast_to(
                                column, (BUCKETS, rows_ref.shape[1])
                            )

            k_ref[...] = dk_acc[...].astype(LOW)
            v_ref[...] = dv_acc[...].astype(LOW)
            for done in range(H // PAIR - 1):

                @pl.when(pair == done)
                def _(done=done):
                    advance(begin + done + 1)

    cq_in, ck_in, cv_in, cmixed_in, enc_in, second_in, clse_ref = cross_refs
    q_in, k_in, v_in, mixed_in, first_in, lse_ref = self_refs[:6]
    fetches = [
        fetch(cmixed_in, mixed_buf, 2), fetch(cq_in, q_buf, 3), fetch(ck_in, k_buf, 4),
        fetch(cv_in, v_buf, 5), fetch(enc_in, keys_in_buf, 6), fetch(second_in, query_in_buf, 7),
    ]
    third_in, grad_in, across_in, gate_in, up_in, down_in, after_in = ff_refs
    width = gate_in.shape[1] // FF_BLOCKS
    third_ref, grad_ref = k_buf.at[:rows], k_buf.at[rows:]
    loads = [fetch(third_in, third_ref, 2), fetch(grad_in, grad_ref, 3), fetch(across_in, after_buf, 4)]

    def ff_loads(block, slot):
        at = pl.ds(pl.multiple_of(block * width, width), width)
        return (
            fetch(gate_in.at[:, at], weight_buf.at[slot, :, pl.ds(0, width)], 8 + slot),
            fetch(up_in.at[:, at], pair_buf.at[slot, pl.ds(0, weight_buf.shape[1]), pl.ds(0, width)],
                  10 + slot),
            fetch(down_in.at[at], rows_buf.at[slot, pl.ds(0, width)], 12 + slot),
        )

    for one in ff_loads(0, 0):
        one.start()
    for one in loads:
        one.start()
    make_hot(buckets_ref, hot_ref, mask_ref)
    greet(bits)
    flat_ref[...] = table_rows(smalls_ref[...], table_size, 3)
    gain_one, gain_two, gain_three = [gain_row(smalls_ref[...], gain_size, row) for row in range(3)]
    for one in loads:
        one.wait()
    res_buf[...] = jnp.zeros_like(res_buf)
    enc_own[...] = jnp.zeros_like(enc_own)

    def ff_rows(slot, at):
        w_gate = weight_buf[slot, :, 0:width]
        w_up = pair_buf[slot, 0 : weight_buf.shape[1], 0:width]
        w_down = rows_buf[slot, 0:width, :]
        gate = contract(third_ref[at, :], w_gate, 1, 0)
        upper = contract(third_ref[at, :], w_up, 1, 0)
        grad = contract(grad_ref[at, :], w_down, 1, 1)
        square = gate * gate
        bend = jnp.tanh(GELU_SCALE * gate * (1.0 + 0.044715 * square))
        open_part = 0.5 * (1.0 + bend)
        active = gate * open_part
        slope = open_part + 0.5 * gate * (1.0 - bend * bend) * (
            GELU_SCALE * (1.0 + 3.0 * 0.044715 * square)
        )
        inner = (active * upper).astype(LOW)
        gate_grad = (grad * upper * slope).astype(LOW)
        upper_grad = (grad * active).astype(LOW)
        q_buf[at, 0:width] = inner
        grad_buf[at, 0:width] = gate_grad
        send_buf[0, at, 0:width] = upper_grad
        res_buf[at, :] += contract(inner, w_down, 1, 0)
        enc_own[at, :] += contract(gate_grad, w_gate, 1, 1) + contract(upper_grad, w_up, 1, 1)

    @pl.loop(0, FF_BLOCKS)
    def _(block):
        slot = lax.rem(block, 2)
        for one in ff_loads(block, slot):
            one.wait()

        @pl.when(block < FF_BLOCKS - 1)
        def _():
            for one in ff_loads(block + 1, 1 - slot):
                one.start()

        @pl.loop(0, rows // TILE)
        def _(part):
            ff_rows(slot, pl.ds(pl.multiple_of(part * TILE, TILE), TILE))

        for now in range(FF_BLOCKS):

            @pl.when(block == now)
            def _(now=now):
                advance(2 + 2 * now)
                if now >= 2:
                    drain(2 * now - 4, 2 + 2 * now)
                    drain(2 * now - 3, 2 + 2 * now)

        owner_grad(ff_work.at[2 * slot], third_ref, grad_buf.at[:, 0:width])
        owner_grad(ff_work.at[2 * slot + 1], third_ref, send_buf.at[0, :, 0:width])
        value = contract(q_buf[:, 0:width], grad_ref[...], 0, 0)
        down_work[lax.div(block, 2), slot] = value.reshape(down_work.shape[2:]).astype(LOW)
        for now in range(FF_BLOCKS):

            @pl.when(block == now)
            def _(now=now):
                advance(3 + 2 * now)

    weight(0).start()
    weight(1).start()
    for one in (fetches[0], fetches[1], fetches[3], fetches[4], fetches[5]):
        one.start()

    def norm_back_rows(value, gain, grad):
        scale = lax.rsqrt(jnp.mean(value * value, -1, keepdims=True) + EPSILON)
        scaled = gain * grad
        inner = jnp.mean(value * scaled, -1, keepdims=True)
        back = scale * scaled - value * (scale * scale * scale) * inner
        return back, jnp.sum(grad * value * scale, 0, keepdims=True)

    gain_sums[...] = jnp.zeros_like(gain_sums)

    def body(at):
        value = after_buf[at(), :]
        send_buf[1, at(), :] = (value + res_buf[at(), :]).astype(LOW)
        back, total = norm_back_rows(value, gain_three, enc_own[at(), :])
        gain_sums[2:3, :] += total
        res_buf[at(), :] = grad_ref[at(), :].astype(F32) + back

    over_rows(rows, body)
    layer_copy = fetch(send_buf.at[1], layer_out, 15)
    layer_copy.start()
    fetch(after_in, after_buf, 14).start()
    fetches[2].start()

    def to_mixed(number, source):
        weight(number).wait()

        def body(at):
            grad_buf[at(), :] = contract(
                source[at(), :].astype(LOW), weight_buf[number % 2], 1, 1
            ).astype(LOW)

        over_rows(rows, body)
        weight(number + 2).start()

    advance(10)
    to_mixed(0, res_buf)
    fetches[0].wait()

    def low_rows(source, target):
        def body(at):
            target[at(), :] = source[at(), :].astype(LOW)

        over_rows(rows, body)

    low_rows(res_buf, send_buf.at[0])
    weight_grad(SQUARES, mixed_buf, send_buf.at[0])
    advance(11)
    for one in fetches[1:4]:
        one.wait()
    pairs_back(clse_ref, False, 11)
    fetch(mixed_in, mixed_buf, 2).start()
    advance(17)

    def both_back(numbers, keep, count):
        def body_other(at):
            total = contract(k_buf[at(count), :], weight_buf[numbers[0] % 2], 1, 1)
            total = total + contract(v_buf[at(count), :], weight_buf[numbers[1] % 2], 1, 1)
            send_buf[keep[0], at(), :] = total.astype(LOW)
            if not count:
                gain_sums[3:4, :] += jnp.sum(
                    total * keys_in_buf[at(), :].astype(F32), 0, keepdims=True
                )

        def body_own(at):
            begin = 0 if count else rows
            total = contract(k_buf[at(begin), :], weight_buf[numbers[0] % 2], 1, 1)
            total = total + contract(v_buf[at(begin), :], weight_buf[numbers[1] % 2], 1, 1)
            keep[1][at(), :] = total

        over_rows(rows, body_other)
        return body_own

    weight(1).wait()
    weight(2).wait()
    own_part = both_back((1, 2), (0, enc_own), rows)
    for one in fetches[4:]:
        one.wait()
    advance(18)
    weight_grad(SQUARES + 1, keys_in_buf, k_buf)
    advance(19)
    weight_grad(SQUARES + 2, keys_in_buf, v_buf)
    advance(20)
    over_rows(rows, own_part)
    fetch(k_in, k_buf, 4).start()
    fetch(v_in, v_buf, 5).start()
    fetch(first_in, keys_in_buf, 6).start()
    weight(3).start()
    weight(4).start()
    advance(21)
    weight_grad(SQUARES + 3, query_in_buf, q_buf)
    advance(22)
    weight(3).wait()
    fetch(after_in, after_buf, 14).wait()

    def body(at):
        grad = contract(q_buf[at(), :], weight_buf[1], 1, 1)
        back, total = norm_back_rows(after_buf[at(), :], gain_two, grad)
        gain_sums[1:2, :] += total
        res_buf[at(), :] += back

    over_rows(rows, body)
    fetch(q_in, q_buf, 3).start()
    weight(5).start()
    weight(4).wait()

    def body(at):
        grad_buf[at(), :] = contract(res_buf[at(), :].astype(LOW), weight_buf[0], 1, 1).astype(LOW)

    over_rows(rows, body)
    weight(6).start()
    fetch(mixed_in, mixed_buf, 2).wait()
    low_rows(res_buf, query_in_buf)
    weight_grad(SQUARES + 4, mixed_buf, query_in_buf)
    advance(23)
    fetch(q_in, q_buf, 3).wait()
    fetch(k_in, k_buf, 4).wait()
    fetch(v_in, v_buf, 5).wait()
    pairs_back(lse_ref, True, 23)
    advance(29)
    side(0).wait_recv()
    side(0).wait_send()

    def body(at):
        send_buf[0, at(), :] = (enc_own[at(), :] + recv_buf[0, at(), :].astype(F32)).astype(LOW)

    over_rows(rows, body)
    enc_copy = fetch(send_buf.at[0], enc_out, 8)
    enc_copy.start()
    fetch(hidden_in, grad_buf, 9).start()
    layer_copy.wait()
    weight(5).wait()
    weight(6).wait()
    fetch(first_in, keys_in_buf, 6).wait()
    own_part = both_back((5, 6), (1, enc_own), 0)

    advance(30)
    weight_grad(SQUARES + 5, keys_in_buf, v_buf)
    advance(31)
    weight_grad(SQUARES + 6, keys_in_buf, k_buf)
    advance(32)
    weight_grad(SQUARES + 7, keys_in_buf.at[rows:], q_buf)
    advance(33)
    over_rows(rows, own_part)
    weight(7).start()
    own_low = (seq_pos == 0).astype(F32)
    fetch(hidden_in, grad_buf, 9).wait()
    weight(7).wait()

    def body(at):
        grad = contract(q_buf[at(), :], weight_buf[1], 1, 1) + enc_own[at(), :]
        grad = grad + own_low * send_buf[1, at(), :].astype(F32)
        enc_own[at(), :] = grad
        value = grad_buf[at(), :].astype(F32)
        scale = lax.rsqrt(jnp.mean(value * value, -1, keepdims=True) + EPSILON)
        gain_sums[0:1, :] += jnp.sum(grad * value * scale, 0, keepdims=True)

    over_rows(rows, body)
    gain_sums[0:1, :] += (1.0 - own_low) * gain_sums[3:4, :] / gain_one
    small_ref[...] = small_rows(
        gain_sums[0:1, :], gain_sums[1:2, :], gain_sums[2:3, :], rows_ref[...], gain_size,
        table_size, small_ref.shape
    )
    advance(34)

    @pl.when(seq_pos == 0)
    def _():
        side(1).wait_recv()

    @pl.when(seq_pos != 0)
    def _():
        side(1).wait_send()

    def body(at):
        grad = enc_own[at(), :] + jnp.where(
            seq_pos == 0, recv_buf[1, at(), :].astype(F32), 0.0
        )
        back, _ = norm_back_rows(grad_buf[at(), :].astype(F32), gain_one, grad)
        hidden_out[at(), :] = (res_buf[at(), :] + back).astype(LOW)

    over_rows(rows, body)
    advance(35)
    assert all(entry[2] in done_slots for entry in CLOSE_PLAN)
    for item in range(CLOSE_ITEMS):
        for step in range(steps):
            if (item, step) not in drained:
                copy(item, step).wait_send()
    enc_copy.wait()


def take(refs, counts):
    out = []
    begin = 0
    for count in counts:
        out.append(refs[begin : begin + count])
        begin += count
    return out


def small_rows(one, two, three, table, gain_size, table_size, shape):
    owners = one.shape[1] // gain_size

    def spread(source, size, row):
        count = owners * size
        target = lax.broadcasted_iota(jnp.int32, (owners * 8, count), 0)
        entry = lax.broadcasted_iota(jnp.int32, (owners * 8, count), 1)
        begin = (target >> 3) * size
        hot = ((target & 7) == row) & (entry >= begin) & (entry < begin + size)
        return lax.dot_general(
            hot.astype(F32), source, (((1,), (0 if row == 3 else 1,)), ((), ())),
            precision=lax.Precision.HIGHEST, preferred_element_type=F32,
        )

    def wheel(shape, axis, size):
        entry = lax.broadcasted_iota(jnp.int32, shape, axis).astype(F32)
        lane = lax.broadcasted_iota(jnp.int32, shape, 1 - axis).astype(F32)
        return lane == entry - size * jnp.floor((entry + 0.5) * (1.0 / size))

    total = jnp.zeros((owners * 8, 128), F32)
    for row, value in enumerate((one, two, three)):
        grid = (128, value.shape[1])
        total = total + spread(
            jnp.where(wheel(grid, 1, gain_size), jnp.broadcast_to(value, grid), 0.0), gain_size, row
        )
    total = total + spread(jnp.where(wheel(table.shape, 0, table_size), table, 0.0), table_size, 3)
    return total.reshape(shape)


SLOTS = 2
FF_BLOCKS = 4
DOWN = 2 * FF_BLOCKS
SQUARES = DOWN + 2
SMALL = SQUARES + 8
CLOSE_ITEMS = SMALL + 1
GELU_SCALE = 0.7978845608028654
CLOSE_PATHS = ('xzZyc', 'xyzZc', 'yzZxc', 'yxzZc', 'xzZyc', 'yzZxc', 'xzZyc', 'yxzZc', 'yzZxc', 'xzZyc', 'zZyxc', 'xyzZc', 'xzZyc', 'xzZyc', 'zZyxc', 'zZxyc', 'xyzZc', 'zZxyc', 'xyzZc')
CLOSE_PLAN = (
    (1, 0, 3), (0, 0, 3), (0, 1, 4), (1, 1, 5), (3, 0, 5), (2, 0, 5),
    (3, 1, 6), (2, 1, 6), (1, 2, 9), (6, 0, 9), (9, 0, 9), (7, 0, 9),
    (8, 0, 10), (5, 0, 10), (0, 2, 11), (9, 1, 11), (6, 1, 11), (10, 0, 11),
    (4, 0, 12), (8, 1, 12), (7, 1, 12), (3, 2, 13), (2, 2, 13), (10, 1, 15),
    (9, 2, 15), (5, 1, 16), (19, 0, 19), (11, 0, 19), (8, 2, 19), (6, 2, 19),
    (4, 1, 20), (10, 2, 20), (12, 0, 20), (3, 3, 20), (11, 1, 21), (7, 2, 21),
    (0, 3, 22), (9, 3, 22), (12, 1, 22), (5, 2, 23), (14, 0, 23), (8, 3, 24),
    (13, 0, 24), (14, 1, 26), (7, 3, 26), (10, 3, 27), (12, 2, 27), (13, 1, 27),
    (4, 2, 27), (11, 2, 27), (6, 3, 27), (20, 0, 30), (14, 2, 30), (2, 3, 31),
    (15, 0, 31), (7, 4, 31), (13, 2, 31), (16, 0, 32), (1, 3, 32), (15, 1, 32),
    (5, 3, 32), (17, 0, 33), (16, 1, 33), (4, 3, 33), (12, 3, 33), (13, 3, 33),
    (17, 1, 33), (10, 4, 33), (11, 3, 34), (7, 5, 34), (18, 0, 34), (8, 4, 34),
    (15, 2, 34), (18, 1, 34), (16, 2, 34), (17, 2, 34), (1, 4, 34), (12, 4, 34),
    (2, 4, 34), (14, 3, 34), (15, 3, 34), (5, 4, 34), (11, 4, 34), (6, 4, 34),
    (18, 2, 34), (3, 4, 34), (9, 4, 34), (8, 5, 34), (17, 3, 34), (14, 4, 34),
    (16, 3, 34), (2, 5, 34), (5, 5, 34), (3, 5, 34), (0, 4, 34), (15, 4, 34),
    (10, 5, 34), (11, 5, 34), (18, 3, 34), (13, 4, 34), (1, 5, 34), (17, 4, 34),
    (4, 4, 34), (6, 5, 34), (9, 5, 34), (16, 4, 34), (18, 4, 34), (13, 5, 35),
    (4, 5, 35), (12, 5, 35), (14, 5, 35), (15, 5, 35), (18, 5, 35), (16, 5, 35),
    (0, 5, 35), (17, 5, 35),
)


def close_layer(forward, weights, cross, own, smalls, buckets, hidden, sizes, collective_id):
    bits = bit_plan()
    steps = len(bits)
    owners = 1 << steps
    count, width = hidden.shape
    units = forward[3].shape[1]
    length = cross[1].shape[0]
    offs = length // TILE
    lanes = width // (H // PAIR)
    gate, down = (width // owners, units), (units // owners, width)
    square = (width // owners, width)
    blocks = [(gate[0], units // FF_BLOCKS)] * DOWN + [(down[0] // 2, width)] * 2 + [square] * 8
    kinds = [LOW] * SMALL + [F32]
    blocks.append((8, 128))
    arrivals = [
        pltpu.VMEM((2,) * (steps - 1 - step) + block, kind)
        for block, kind in zip(blocks, kinds)
        for step in range(steps)
    ]
    inside = pl.BlockSpec(memory_space=pltpu.VMEM)
    outside = pl.BlockSpec(memory_space=pl.ANY)
    few, many = (count, width), (length, width)
    vm = pltpu.VMEM
    sems = pltpu.SemaphoreType.DMA((CLOSE_ITEMS, steps))
    pair_sem = pltpu.SemaphoreType.DMA((2,))
    return pl.pallas_call(
        functools.partial(close_kernel, bits, sizes),
        out_shape=[jax.ShapeDtypeStruct(few, LOW)] * 3
        + [jax.ShapeDtypeStruct(block, F32) for block in (gate, gate, down)]
        + [jax.ShapeDtypeStruct(square, F32)] * 8
        + [jax.ShapeDtypeStruct((8, 128), F32)],
        in_specs=[outside] * (7 + 8) + [outside] * 6 + [inside] + [outside] * 5 + [inside]
        + [inside] * 2 + [outside],
        out_specs=[outside, inside, outside] + [inside] * 12,
        scratch_shapes=arrivals
        + [
            vm((SLOTS,) + (2,) * steps + square, LOW),
            vm((4,) + (2,) * steps + (gate[0], units // FF_BLOCKS), LOW),
            vm((2,) * steps + down, LOW),
            vm((2,) * steps + (8, 128), F32),
            vm(few, LOW), vm(many, LOW), vm((2,) + many, LOW), vm((2,) + few, LOW),
            vm(few, LOW), vm(few, F32), vm(few, F32),
            vm((2, width, width), LOW), vm(few, F32), vm((2,) + few, LOW), vm((2,) + few, LOW),
            vm((length, lanes), F32), vm((length, lanes), F32),
            vm((PAIR, offs, TILE, TILE), F32), vm((PAIR, offs, TILE, TILE), F32),
            vm((H * BUCKETS, 128), F32), vm((H * BUCKETS, 128), F32), vm((8, width), F32),
            vm((offs, BUCKETS, 2 * TILE), LOW), vm((offs, 1, 2 * TILE), F32),
            sems, sems, pair_sem, pair_sem, pltpu.SemaphoreType.DMA((16,)),
        ],
        compiler_params=pltpu.CompilerParams(
            collective_id=collective_id, has_side_effects=True, vmem_limit_bytes=67_000_000
        ),
        name="close_layer",
    )(*forward, *weights, *cross, *own, smalls, buckets, hidden)


def finish_kernel(*refs):
    count = (len(refs) - 5) // 2
    for source, target in zip(refs[: count], refs[count + 1 :]):
        target[...] = source[...]
    small = refs[count]
    for row, target in enumerate(refs[2 * count + 1 :]):
        target[...] = small[row, : target.shape[0]]


def finish(arrays, small, sizes):
    count = len(arrays)
    inside = pl.BlockSpec(memory_space=pltpu.VMEM)
    return pl.pallas_call(
        finish_kernel,
        out_shape=[jax.ShapeDtypeStruct(x.shape, x.dtype) for x in arrays]
        + [jax.ShapeDtypeStruct((size,), F32) for size in sizes],
        in_specs=[inside] * (count + 1),
        out_specs=[inside] * (count + 4),
        name="finish",
    )(*arrays, small)


def dot_low(left, right):
    return contract(left, right, 1, 0)


def dot_left(left, right):
    return contract(left, right, 0, 0)


def dot_right(left, right):
    return contract(left, right, 1, 1)


def rms_norm(value, gain):
    return value * lax.rsqrt(jnp.mean(value * value, -1, keepdims=True) + EPSILON) * gain


def norm_back(value, gain, grad):
    return jax.vjp(rms_norm, value, gain)[1](grad)


def gated(gate, upper):
    return jax.nn.gelu(gate, approximate=True) * upper


def pad_rows(rows):
    return sum(
        jnp.pad(row.astype(F32)[None], ((place, 7 - place), (0, 128 - row.shape[0])))
        for place, row in enumerate(rows)
    )


def on_device(
    hidden_in,
    encoded,
    cotangent,
    buckets,
    self_query,
    self_key,
    self_value,
    self_out,
    cross_query,
    cross_key,
    cross_value,
    cross_out,
    ff_gate,
    ff_up,
    ff_down,
    norm_self,
    norm_cross,
    norm_ff,
    bias_table,
):
    owners = lax.axis_size("seq") * lax.axis_size("shard")
    seq_pos = lax.axis_index("seq")
    seq_row = seq_pos.reshape(1).astype(jnp.int32)
    low_side = seq_pos == 0
    both = ("seq", "shard")
    width = hidden_in.shape[2]
    own_low = hidden_in[0]
    enc_own = encoded[0]
    small = pad_rows([norm_self, norm_cross, norm_ff, bias_table])
    hidden = own_low.astype(F32)
    count = hidden.shape[0]
    length = count * lax.axis_size("seq")
    gap, hot = bucket_rows(buckets, length)
    opened = open_layer(
        [small, self_query, self_key, self_value, self_out, cross_query, cross_key, cross_value,
         cross_out, ff_gate, ff_up, ff_down],
        own_low,
        enc_own,
        buckets.reshape(1, -1),
        (norm_self.shape[0], bias_table.shape[0]),
        1,
    )
    smalls = opened[0]
    (w_query, w_key, w_value, w_sout, w_cquery, w_ckey, w_cvalue, w_cout, w_gate, w_up, w_down) = [
        x.reshape(-1, x.shape[-1]) for x in opened[1:12]
    ]
    (enc_all, first_all, query, key, value, self_mixed, self_lse, after_self, second,
     cross_q, cross_k, cross_v, cross_mixed, cross_lse, after_cross, third) = opened[12:]
    gain_one, gain_two, gain_three = [
        smalls[:, i, : norm_self.shape[0]].reshape(-1) for i in range(3)
    ]
    table = smalls[:, 3, : bias_table.shape[0]].reshape(H, BUCKETS)
    rows = jnp.einsum("hb,bof->hof", table.astype(LOW), hot, preferred_element_type=F32)
    rows = jnp.where(gap[None] >= 0, rows, NEGATIVE).reshape(H // PAIR, PAIR, *gap.shape)
    first = first_all[count:]

    gains = norm_self.shape[0]
    if width // owners >= 16:
        *arrays, small_sum = close_layer(
            [third, cotangent[0], after_cross, w_gate, w_up, w_down, after_self],
            [w_cout, w_ckey, w_cvalue, w_cquery, w_sout, w_key, w_value, w_query],
            [cross_q, cross_k, cross_v, cross_mixed, enc_all, second, cross_lse],
            [query, key, value, self_mixed, first_all, self_lse],
            smalls,
            buckets.reshape(1, -1),
            own_low,
            (gains, bias_table.shape[0]),
            2,
        )
        *arrays, one, two, three, four = finish(
            arrays, small_sum, (gains,) * 3 + bias_table.shape
        )
        hidden_out, grad_hidden, grad_encoded, *sums = arrays
        return (
            hidden_out[None],
            grad_hidden[None],
            grad_encoded[None],
            sums[10],
            sums[9],
            sums[8],
            sums[7],
            sums[6],
            sums[4],
            sums[5],
            sums[3],
            sums[0],
            sums[1],
            sums[2],
            one,
            two,
            three,
            four,
        )
    gate = dot_low(third, w_gate)
    upper = dot_low(third, w_up)
    inner = gated(gate, upper).astype(LOW)
    hidden_out = (after_cross + dot_low(inner, w_down)).astype(LOW)

    grad_top = cotangent[0]
    grad_wdown = dot_left(inner, grad_top).astype(LOW)
    grad_inner = dot_right(grad_top, w_down)
    grad_gate, grad_upper = jax.vjp(gated, gate, upper)[1](grad_inner)
    gate_low = grad_gate.astype(LOW)
    upper_low = grad_upper.astype(LOW)
    grad_wgate = dot_left(third, gate_low).astype(LOW)
    grad_wup = dot_left(third, upper_low).astype(LOW)
    grad_third = dot_right(gate_low, w_gate) + dot_right(upper_low, w_up)
    norm_grad, grad_gain_three = norm_back(after_cross, gain_three, grad_third)
    grad_cross_res = grad_top.astype(F32) + norm_grad
    sum_gate, sum_up = [
        lax.psum_scatter(x, both, scatter_dimension=0, tiled=True).astype(F32)
        for x in (grad_wgate, grad_wup)
    ]
    cross_res_low = grad_cross_res.astype(LOW)
    grad_wcout = dot_left(cross_mixed, cross_res_low).astype(LOW)
    grad_cross_mix = dot_right(cross_res_low, w_cout).astype(LOW)
    grad_cq, grad_ck, grad_cv = attend_back(
        cross_q, cross_k, cross_v, grad_cross_mix, cross_mixed, cross_lse, None, None
    )
    grad_enc = dot_right(grad_ck, w_ckey) + dot_right(grad_cv, w_cvalue)
    enc_back = lax.ppermute(grad_enc[count:].astype(LOW), "seq", [(0, 1), (1, 0)])
    grad_wcquery = dot_left(second, grad_cq).astype(LOW)
    grad_wckey = dot_left(enc_all, grad_ck).astype(LOW)
    grad_wcvalue = dot_left(enc_all, grad_cv).astype(LOW)
    norm_grad, grad_gain_two = norm_back(after_self, gain_two, dot_right(grad_cq, w_cquery))
    grad_self_res = grad_cross_res + norm_grad
    self_res_low = grad_self_res.astype(LOW)
    grad_wsout = dot_left(self_mixed, self_res_low).astype(LOW)
    grad_self_mix = dot_right(self_res_low, w_sout).astype(LOW)
    grad_q, grad_k, grad_v, grad_rows = attend_back(
        query, key, value, grad_self_mix, self_mixed, self_lse, seq_row, rows
    )
    grad_part = dot_right(grad_k, w_key) + dot_right(grad_v, w_value)
    part_back = lax.ppermute(grad_part[:count].astype(LOW), "seq", [(1, 0)])
    grad_wquery = dot_left(first, grad_q).astype(LOW)
    grad_wkey = dot_left(first_all, grad_k).astype(LOW)
    grad_wvalue = dot_left(first_all, grad_v).astype(LOW)
    grad_first = (
        dot_right(grad_q, w_query)
        + grad_part[count:]
        + jnp.where(low_side, grad_part[:count], 0.0)
        + part_back.astype(F32)
    )
    norm_grad, grad_gain_one = norm_back(hidden, gain_one, grad_first)
    grad_hidden = (grad_self_res + norm_grad).astype(LOW)
    grad_encoded = (grad_enc[:count] + enc_back.astype(F32)).astype(LOW)
    table_grad = jnp.einsum(
        "hof,bof->hb", grad_rows.reshape(H, *gap.shape), hot.astype(F32),
        precision=lax.Precision.HIGHEST,
    )
    small_grads = jnp.stack(
        [
            jnp.pad(x.reshape(owners, -1), ((0, 0), (0, 128 - x.size // owners)))
            for x in (grad_gain_one, grad_gain_two, grad_gain_three, table_grad)
        ]
        + [jnp.zeros((owners, 128), F32)] * 4,
        1,
    ).reshape(owners * 8, 128)
    sums = scatter(
        [grad_wdown, grad_wcout, grad_wcquery, grad_wckey, grad_wcvalue, grad_wsout, grad_wquery,
         grad_wkey, grad_wvalue, small_grads],
        2,
    )
    small_sum = sums[9]
    return (
        hidden_out[None],
        grad_hidden[None],
        grad_encoded[None],
        sums[6],
        sums[7],
        sums[8],
        sums[5],
        sums[2],
        sums[3],
        sums[4],
        sums[1],
        sum_gate,
        sum_up,
        sums[0],
        small_sum[0, :gains],
        small_sum[1, :gains],
        small_sum[2, :gains],
        small_sum[3, : bias_table.shape[0]],
    )


def solution(mesh):
    rows = P(("seq", "shard"), None)
    flat = P(("seq", "shard"))
    tokens = P("shard", "seq", None)
    return jax.shard_map(
        on_device,
        mesh=mesh,
        in_specs=(tokens,) * 3 + (P(),) + (rows,) * 11 + (flat,) * 4,
        out_specs=(tokens,) * 3 + (rows,) * 11 + (flat,) * 4,
        check_vma=False,
    )
```

```python
import functools
import jax
import jax.numpy as jnp
from jax import lax
from jax.experimental import pallas as pl
from jax.experimental.pallas import tpu as pltpu
from jax.sharding import PartitionSpec as P

H = 12
BUCKETS = 32
NEGATIVE = -1e30
EPSILON = 1e-06
F32 = jnp.float32
LOW = jnp.bfloat16
PAIR = 2
TILE = 256


def contract(left, right, left_dim, right_dim):
    return lax.dot_general(
        left, right, (((left_dim,), (right_dim,)), ((), ())), preferred_element_type=F32
    )


def keep_head(value, head):
    size = value.shape[1] // PAIR
    lane = lax.broadcasted_iota(jnp.int32, value.shape, 1)
    inside = (lane >= head * size) & (lane < (head + 1) * size)
    return jnp.where(inside, value, jnp.zeros_like(value))


def toeplitz(row):
    wide = jnp.broadcast_to(row, (TILE, 2 * TILE))
    return pltpu.roll(wide, 0, 1, stride=1, stride_axis=0)[:, :TILE]


def skew_sum(total_ref):
    group = 8
    width = 2 * TILE
    summed = jnp.zeros((group, width), F32)
    for start in range(0, TILE, group):
        rows = total_ref[start : start + group, :]
        wide = jnp.concatenate([rows, jnp.zeros_like(rows)], 1)
        summed = summed + pltpu.roll(wide, (width - start) % width, 1)
    out = summed[0:1]
    for row in range(1, group):
        out = out + pltpu.roll(summed[row : row + 1], width - row, 1)
    return out


def scores_t(keys, query, tiles, last):
    scores = contract(keys, query, 1, 1)
    if tiles is None:
        return scores
    parts = [
        scores[place * TILE : (place + 1) * TILE] + tiles[last - place] for place in range(last + 1)
    ]
    return jnp.concatenate(parts, 0) if len(parts) > 1 else parts[0]


def attend_block(q_ref, k_ref, v_t, o_ref, lse_ref, tiles_ref, start, last, span):
    query = q_ref[start : start + TILE, :]
    size = query.shape[1] // PAIR
    mixed = []
    for head in range(PAIR):
        tiles = None if tiles_ref is None else tiles_ref.at[head]
        scores = scores_t(k_ref[:span, :], keep_head(query, head), tiles, last)
        summit = jnp.max(scores, 0, keepdims=True)
        exponent = jnp.exp(scores - summit)
        total = jnp.sum(exponent, 0, keepdims=True)
        weighted = contract(
            v_t[head * size : (head + 1) * size, :span], exponent.astype(LOW), 1, 0
        )
        mixed.append(weighted / total)
        lse_ref[0, head : head + 1, start : start + TILE] = summit + jnp.log(total)
    o_ref[start : start + TILE, :] = jnp.concatenate(mixed, 0).T.astype(LOW)


def attend_kernel(causal, *refs):
    if causal:
        seq_ref, q_ref, k_ref, v_ref, z_ref, o_ref, lse_ref, tiles_ref = refs
        make_tiles(z_ref, tiles_ref)
    else:
        q_ref, k_ref, v_ref, o_ref, lse_ref = refs
    v_t = v_ref[...].T
    blocks = q_ref.shape[0] // TILE
    keys = k_ref.shape[0]
    if not causal:
        for block in range(blocks):
            attend_block(q_ref, k_ref, v_t, o_ref, lse_ref, None, block * TILE, None, keys)
        return
    for side in range(keys // q_ref.shape[0]):

        @pl.when(seq_ref[0] == side)
        def _(side=side):
            for block in range(blocks):
                last = side * blocks + block
                attend_block(
                    q_ref, k_ref, v_t, o_ref, lse_ref, tiles_ref, block * TILE, last,
                    (last + 1) * TILE,
                )


def make_tiles(z_ref, tiles_ref):
    for head in range(PAIR):
        for off in range(z_ref.shape[2]):
            tiles_ref[head, off] = toeplitz(z_ref[0, head, off : off + 1, :])


def attend(queries, keys_all, values, seq_pos, rows):
    count, width = queries.shape
    length = keys_all.shape[0]
    pairs = H // PAIR
    lanes = width // pairs
    offs = length // TILE
    causal = rows is not None
    col = lambda size: pl.BlockSpec((size, lanes), lambda pair, *_: (0, pair))
    in_specs = [col(count), col(length), col(length)]
    args = [queries, keys_all, values]
    scratch = []
    if causal:
        in_specs.append(pl.BlockSpec((1, PAIR, offs, 2 * TILE), lambda pair, *_: (pair, 0, 0, 0)))
        args = [seq_pos] + args + [rows]
        scratch = [pltpu.VMEM((PAIR, offs, TILE, TILE), F32)]
    work = H * count * length
    return pl.pallas_call(
        functools.partial(attend_kernel, causal),
        grid_spec=pltpu.PrefetchScalarGridSpec(
            num_scalar_prefetch=1 if causal else 0,
            grid=(pairs,),
            in_specs=in_specs,
            out_specs=[
                col(count),
                pl.BlockSpec((1, PAIR, count), lambda pair, *_: (pair, 0, 0)),
            ],
            scratch_shapes=scratch,
        ),
        out_shape=[
            jax.ShapeDtypeStruct((count, width), LOW),
            jax.ShapeDtypeStruct((pairs, PAIR, count), F32),
        ],
        cost_estimate=pl.CostEstimate(
            flops=work * 256 * 2, bytes_accessed=6 * length * width, transcendentals=work
        ),
        name="attend_causal" if causal else "attend_cross",
    )(*args)


def back_block(refs, k_t, prod_t, start, last, span, first, tiles_ref, total_ref):
    q_ref, k_ref, v_ref, g_ref, lse_ref, dq_ref, dk_acc, dv_acc = refs
    query = q_ref[start : start + TILE, :]
    grad = g_ref[start : start + TILE, :]
    size = query.shape[1] // PAIR
    dq_t = []
    dk = dv = None
    for head in range(PAIR):
        own = keep_head(query, head)
        own_grad = keep_head(grad, head)
        tiles = None if tiles_ref is None else tiles_ref.at[head]
        scores = scores_t(k_ref[:span, :], own, tiles, last)
        probs = jnp.exp(scores - lse_ref[0, head : head + 1, start : start + TILE])
        grad_probs = contract(v_ref[:span, :], own_grad, 1, 1)
        delta = jnp.sum(
            prod_t[head * size : (head + 1) * size, start : start + TILE], 0, keepdims=True
        )
        grad_scores = probs * (grad_probs - delta)
        low = grad_scores.astype(LOW)
        dv_new = contract(probs.astype(LOW), own_grad, 1, 0)
        dk_new = contract(low, own, 1, 0)
        dv = dv_new if dv is None else dv + dv_new
        dk = dk_new if dk is None else dk + dk_new
        dq_t.append(contract(k_t[head * size : (head + 1) * size, :span], low, 1, 0))
        if total_ref is not None:
            for place in range(last + 1):
                off = last - place
                piece = grad_scores[place * TILE : (place + 1) * TILE]
                if first:
                    total_ref[head, off] = piece
                elif off == last:
                    total_ref[head, off] = piece
                else:
                    total_ref[head, off] += piece
    dq_ref[start : start + TILE, :] = jnp.concatenate(dq_t, 0).T.astype(LOW)
    if first:
        dk_acc[:span, :] = dk
        dv_acc[:span, :] = dv
        if span < dk_acc.shape[0]:
            dk_acc[span:, :] = jnp.zeros((dk_acc.shape[0] - span, dk_acc.shape[1]), F32)
            dv_acc[span:, :] = jnp.zeros((dv_acc.shape[0] - span, dv_acc.shape[1]), F32)
    else:
        dk_acc[:span, :] += dk
        dv_acc[:span, :] += dv


def back_kernel(causal, *refs):
    if causal:
        (seq_ref, q_ref, k_ref, v_ref, g_ref, o_ref, lse_ref, z_ref,
         dq_ref, dk_ref, dv_ref, row_ref, dk_acc, dv_acc, tiles_ref, total_ref) = refs
        make_tiles(z_ref, tiles_ref)
    else:
        (q_ref, k_ref, v_ref, g_ref, o_ref, lse_ref,
         dq_ref, dk_ref, dv_ref, dk_acc, dv_acc) = refs
        tiles_ref = total_ref = None
    k_t = k_ref[...].T
    prod_t = (g_ref[...].astype(F32) * o_ref[...].astype(F32)).T
    blocks = q_ref.shape[0] // TILE
    keys = k_ref.shape[0]
    main = (q_ref, k_ref, v_ref, g_ref, lse_ref, dq_ref, dk_acc, dv_acc)
    if not causal:
        for block in range(blocks):
            back_block(main, k_t, prod_t, block * TILE, None, keys, block == 0, None, None)
    else:
        for side in range(keys // q_ref.shape[0]):

            @pl.when(seq_ref[0] == side)
            def _(side=side):
                for block in range(blocks):
                    last = side * blocks + block
                    back_block(
                        main, k_t, prod_t, block * TILE, last, (last + 1) * TILE,
                        block == 0, tiles_ref, total_ref,
                    )
                for head in range(PAIR):
                    for off in range(keys // TILE):
                        if off < (side + 1) * blocks:
                            row_ref[0, head, off : off + 1, :] = skew_sum(total_ref.at[head, off])
                        else:
                            row_ref[0, head, off : off + 1, :] = jnp.zeros((1, 2 * TILE), F32)

    dk_ref[...] = dk_acc[...].astype(LOW)
    dv_ref[...] = dv_acc[...].astype(LOW)


def attend_back(queries, keys_all, values, grad_mixed, mixed, lse, seq_pos, rows):
    count, width = queries.shape
    length = keys_all.shape[0]
    pairs = H // PAIR
    lanes = width // pairs
    offs = length // TILE
    causal = rows is not None
    col = lambda size: pl.BlockSpec((size, lanes), lambda pair, *_: (0, pair))
    in_specs = [col(count), col(length), col(length), col(count), col(count),
                pl.BlockSpec((1, PAIR, count), lambda pair, *_: (pair, 0, 0))]
    out_specs = [col(count), col(length), col(length)]
    out_shape = [
        jax.ShapeDtypeStruct((count, width), LOW),
        jax.ShapeDtypeStruct((length, width), LOW),
        jax.ShapeDtypeStruct((length, width), LOW),
    ]
    args = [queries, keys_all, values, grad_mixed, mixed, lse]
    scratch = [pltpu.VMEM((length, lanes), F32), pltpu.VMEM((length, lanes), F32)]
    if causal:
        row_spec = pl.BlockSpec((1, PAIR, offs, 2 * TILE), lambda pair, *_: (pair, 0, 0, 0))
        in_specs.append(row_spec)
        out_specs.append(row_spec)
        out_shape.append(jax.ShapeDtypeStruct((pairs, PAIR, offs, 2 * TILE), F32))
        args = [seq_pos] + args + [rows]
        scratch += [pltpu.VMEM((PAIR, offs, TILE, TILE), F32)] * 2
    work = H * count * length
    return pl.pallas_call(
        functools.partial(back_kernel, causal),
        grid_spec=pltpu.PrefetchScalarGridSpec(
            num_scalar_prefetch=1 if causal else 0,
            grid=(pairs,),
            in_specs=in_specs,
            out_specs=out_specs,
            scratch_shapes=scratch,
        ),
        out_shape=out_shape,
        cost_estimate=pl.CostEstimate(
            flops=work * 640 * 2, bytes_accessed=12 * length * width, transcendentals=work
        ),
        name="attend_causal_back" if causal else "attend_cross_back",
    )(*args)


def bucket_rows(buckets, length):
    offs = length // TILE
    place = jnp.arange(2 * TILE, dtype=jnp.int32)
    step = jnp.where(place < TILE, place, place - 2 * TILE)
    gap = (jnp.arange(offs, dtype=jnp.int32) * TILE)[:, None] + step[None, :]
    marks = jnp.arange(BUCKETS, dtype=jnp.int32)
    begins = jnp.sum((buckets[None, :] < marks[:, None]).astype(jnp.int32), 1)
    ends = jnp.sum((buckets[None, :] <= marks[:, None]).astype(jnp.int32), 1)
    hot = (gap[None] >= begins[:, None, None]) & (gap[None] < ends[:, None, None])
    return (gap, hot.astype(LOW))


def bit_plan():
    bits = []
    for axis in ("seq", "shard"):
        size = lax.axis_size(axis)
        assert size & (size - 1) == 0
        bits += [(axis, place) for place in reversed(range(size.bit_length() - 1))]
    return bits


def bit_orders(bits):
    ends = [0, len(bits) - 2, len(bits) - 1]
    rest = [place for place in range(len(bits)) if place not in ends]
    flipped = [ends[1], ends[0], ends[2]]
    return (rest + ends, rest + flipped, ends[:2] + rest + ends[2:])


def coords(bits):
    return [lax.rem(lax.axis_index(axis) // (1 << place), 2) for axis, place in bits]


def partner(bits, which):
    axis, place = bits[which]
    index = lax.axis_index(axis)
    mine = lax.rem(index // (1 << place), 2)
    return {axis: index + (1 - 2 * mine) * (1 << place)}


def greet(bits):
    barrier = pltpu.get_barrier_semaphore()
    for which in range(len(bits)):
        pl.semaphore_signal(
            barrier, inc=1, device_id=partner(bits, which), device_id_type=pl.DeviceIdType.MESH
        )
    pl.semaphore_wait(barrier, len(bits))


def remote(bits, which, source, target, sems):
    return pltpu.make_async_remote_copy(
        src_ref=source,
        dst_ref=target,
        send_sem=sems[0],
        recv_sem=sems[1],
        device_id=partner(bits, which),
        device_id_type=pl.DeviceIdType.MESH,
    )


def send(*args):
    copy = remote(*args)
    copy.start()
    return copy


def scatter_kernel(bits, count, *refs):
    steps = len(bits)
    sources, outs, work = refs[:count], refs[count : 2 * count], refs[2 * count : 3 * count]
    arrivals = refs[3 * count : (3 + steps) * count]
    load_sem, send_sem, recv_sem = refs[(3 + steps) * count :]
    place = coords(bits)
    orders = [list(reversed(order)) for order in bit_orders(bits)[:2]]
    loads = []
    for item in range(count):
        load = pltpu.make_async_copy(sources[item], work[item], load_sem.at[item])
        load.start()
        loads.append(load)
    greet(bits)
    copies = {}

    def add(item, step):
        order = orders[item % 2]
        free = [which for which in range(steps) if which not in order[: step + 1]]
        arrived = arrivals[item * steps + step]
        copies[item, step].wait_recv()
        if not free:
            outs[item][...] = work[item][tuple(place)].astype(F32) + arrived[...].astype(F32)
            return

        @pl.loop(0, 1 << len(free))
        def _(block):
            sub = [lax.rem(block // (1 << (len(free) - 1 - i)), 2) for i in range(len(free))]
            here = tuple(
                sub[free.index(which)] if which in free else place[which] for which in range(steps)
            )
            total = work[item][here].astype(F32) + arrived[tuple(sub)].astype(F32)
            work[item][here] = total.astype(work[item].dtype)

    for turn in range(steps + 1 + (count - 1) // 2):
        for item in range(count):
            step = turn - item // 2
            if not 0 <= step <= steps:
                continue
            if step == 0:
                loads[item].wait()
            else:
                add(item, step - 1)
            if step == steps:
                continue
            order = orders[item % 2]
            there = tuple(
                1 - place[which]
                if which == order[step]
                else (place[which] if which in order[:step] else slice(None))
                for which in range(steps)
            )
            copies[item, step] = send(
                bits,
                order[step],
                work[item].at[there],
                arrivals[item * steps + step],
                (send_sem.at[item, step], recv_sem.at[item, step]),
            )
    for copy in copies.values():
        copy.wait_send()


def scatter(items, collective_id):
    bits = bit_plan()
    steps = len(bits)
    count = len(items)
    sems = pltpu.SemaphoreType.DMA((count, steps))
    owners = 1 << steps
    items = [x.reshape((2,) * steps + (x.shape[0] // owners,) + x.shape[1:]) for x in items]
    tails = [x.shape[steps:] for x in items]
    arrivals = [
        pltpu.VMEM((2,) * (steps - 1 - step) + tail, x.dtype)
        for x, tail in zip(items, tails)
        for step in range(steps)
    ]
    return pl.pallas_call(
        functools.partial(scatter_kernel, bits, count),
        out_shape=[jax.ShapeDtypeStruct(tail, F32) for tail in tails],
        in_specs=[pl.BlockSpec(memory_space=pl.ANY)] * count,
        out_specs=[pl.BlockSpec(memory_space=pltpu.VMEM)] * count,
        scratch_shapes=[pltpu.VMEM(x.shape, x.dtype) for x in items]
        + arrivals
        + [pltpu.SemaphoreType.DMA((count,)), sems, sems],
        compiler_params=pltpu.CompilerParams(collective_id=collective_id, has_side_effects=True),
        name="scatter_rows",
    )(*items)


def table_rows(smalls, table_size, row):
    flat = smalls.reshape(-1, smalls.shape[-1])
    count = table_size * flat.shape[0] // 8
    entry = lax.broadcasted_iota(jnp.int32, (count, flat.shape[0]), 0)
    source = lax.broadcasted_iota(jnp.int32, (count, flat.shape[0]), 1)
    begin = (source >> 3) * table_size
    pick = ((source & 7) == row) & (entry >= begin) & (entry < begin + table_size)
    spread = contract(pick.astype(LOW), flat.astype(LOW), 1, 0)
    lane = lax.broadcasted_iota(jnp.int32, spread.shape, 1)
    place = lax.broadcasted_iota(jnp.int32, spread.shape, 0).astype(F32)
    block = jnp.floor((place + 0.5) * (1.0 / table_size))
    return jnp.where(lane.astype(F32) == place - block * table_size, spread, 0.0)


def gain_row(smalls, size, row):
    flat = smalls.reshape(-1, smalls.shape[-1])
    count = size * flat.shape[0] // 8
    source = lax.broadcasted_iota(jnp.int32, (flat.shape[0], count), 0)
    entry = lax.broadcasted_iota(jnp.int32, (flat.shape[0], count), 1)
    begin = (source >> 3) * size
    pick = ((source & 7) == row) & (entry >= begin) & (entry < begin + size)
    spread = contract(flat.astype(LOW), pick.astype(LOW), 0, 0)
    lane = lax.broadcasted_iota(jnp.int32, spread.shape, 0).astype(F32)
    place = lax.broadcasted_iota(jnp.int32, spread.shape, 1).astype(F32)
    block = jnp.floor((place + 0.5) * (1.0 / size))
    return jnp.sum(jnp.where(lane == place - block * size, spread, 0.0), 0, keepdims=True)


def full_weight(ref):
    value = ref[...].astype(F32)
    return value.reshape(-1, value.shape[-1]).astype(LOW)


ARRAYS = 12
INSIDE = 9
ITEMS = 15
PIECES = tuple((array, None, 0) for array in range(INSIDE)) + tuple(
    (array, axis, half) for array, axis in ((9, 1), (10, 1), (11, 0)) for half in range(2)
)
PATHS = ('xzZyc', 'xzZyc', 'zZxyc', 'zZyxc', 'yxzZc', 'xzZyc', 'zZxyc', 'zZxyc', 'xyzZc', 'zZyxc', 'zZyxc', 'xzZyc', 'yzZxc', 'xzZyc', 'xyzZc')
PLAN = (
    (1, 0, 0), (3, 0, 0), (2, 0, 0), (0, 0, 0), (14, 0, 0), (15, 0, 0),
    (1, 1, 0), (3, 1, 0), (0, 1, 0), (2, 1, 0), (7, 0, 0), (6, 0, 0),
    (1, 2, 0), (3, 2, 0), (9, 0, 0), (10, 0, 0), (11, 0, 0), (2, 2, 0),
    (7, 1, 0), (4, 0, 0), (0, 2, 0), (5, 0, 0), (12, 0, 0), (9, 1, 0),
    (1, 3, 0), (12, 1, 0), (10, 1, 0), (13, 0, 0), (6, 1, 0), (0, 3, 0),
    (8, 0, 0), (4, 1, 0), (11, 1, 0), (3, 3, 0), (14, 1, 0), (1, 4, 0),
    (2, 3, 0), (0, 4, 0), (5, 1, 0), (12, 2, 0), (6, 2, 0), (8, 1, 0),
    (4, 2, 0), (7, 2, 0), (5, 2, 1), (9, 2, 1), (11, 2, 1), (10, 2, 1),
    (13, 1, 1), (2, 4, 1), (14, 2, 2), (16, 0, 2), (12, 3, 2), (3, 4, 2),
    (6, 3, 3), (4, 3, 6), (5, 3, 6), (13, 2, 7), (8, 2, 7), (10, 3, 7),
    (6, 4, 7), (7, 3, 8), (11, 3, 8), (9, 3, 8), (14, 3, 8), (4, 4, 9),
    (5, 4, 9), (8, 3, 11), (13, 3, 11), (7, 4, 11), (12, 4, 14), (11, 4, 16),
    (14, 4, 17), (10, 4, 17), (8, 4, 18), (13, 4, 18), (9, 4, 19),
)
(STAGE_GAIN, STAGE_QUERY, STAGE_KEY, STAGE_VALUE, STAGE_SELF, STAGE_OUT, STAGE_CQUERY, STAGE_CKEY,
 STAGE_CVALUE, STAGE_CROSS, STAGE_COUT, STAGE_END) = (0, 1, 2, 3, 4, 10, 11, 12, 13, 14, 20, 21)


def path_bits(bits, path):
    count = len(bits)
    rest = list(range(1, count - 2))
    groups = {"x": [0], "y": [count - 2], "c": [count - 1], "z": rest[:-1], "Z": rest[-1:]}
    return [groups[letter] for letter in path]


def open_kernel(bits, sizes, *refs):
    gain_size, table_size = sizes
    sources = refs[:ARRAYS]
    hidden_ref, enc_ref, buckets_ref = refs[ARRAYS : ARRAYS + 3]
    finals = refs[ARRAYS + 3 : 2 * ARRAYS + 19]
    kept = refs[2 * ARRAYS + 19 : 2 * ARRAYS + 35 + INSIDE]
    outs = kept[:INSIDE] + finals[INSIDE:ARRAYS]
    (enc_out, first_out, q_out, k_out, v_out, mixed_out, lse_out, after_out, second_out,
     cq_out, ck_out, cv_out, cmixed_out, clse_out, across_out, third_out) = kept[INSIDE:]
    (before_ref, flat_ref, hot_ref, mask_ref, tiles_ref, weight_ref,
     send_sem, recv_sem, own_sem, side_send, side_recv, keep_sem) = refs[2 * ARRAYS + 35 + INSIDE :]
    steps = len(bits)
    place = coords(bits)
    seq_pos = lax.axis_index("seq")
    rows = hidden_ref.shape[0]
    keys = first_out.shape[0]
    lanes = hidden_ref.shape[1] // (H // PAIR)

    def kept_copy(number):
        final = finals[number] if number < INSIDE else finals[number - INSIDE + ARRAYS]
        return pltpu.make_async_copy(kept[number], final, keep_sem.at[number])

    def keep(*numbers):
        for number in numbers:
            kept_copy(number).start()

    def keep_act(*numbers):
        keep(*(number + INSIDE for number in numbers))

    def own(array):
        return pltpu.make_async_copy(
            sources[array], outs[array].at[tuple(place)], own_sem.at[array]
        )

    def copy(item, step):
        order = sum(path_bits(bits, PATHS[item]), [])
        array, axis, half = PIECES[item]
        here = tuple(
            slice(None) if which in order[:step] else place[which] for which in range(steps)
        )
        part = ()
        if axis is not None:
            size = sources[array].shape[axis] // 2
            part = (slice(None),) * axis + (pl.ds(half * size, size),)
        target = outs[array].at[here + part]
        source = target
        if step == 0:
            source = sources[array].at[part] if part else sources[array]
        return remote(
            bits,
            order[step],
            source,
            target,
            (send_sem.at[item, step], recv_sem.at[item, step]),
        )

    def arrived(item):
        copy(item, steps - 1).wait_recv()
        if item < INSIDE:
            keep(item)

    def side(which):
        source, target = ((hidden_ref, before_ref), (enc_ref, enc_out.at[rows:]))[which]
        return remote(bits, 0, source, target, (side_send.at[which], side_recv.at[which]))

    todo = list(PLAN)
    seen = set()

    def advance(until):
        while todo and todo[0][2] <= until:
            item, step, _ = todo.pop(0)
            if item >= ITEMS:
                side(item - ITEMS).start()
                continue
            groups = path_bits(bits, PATHS[item])
            first = sum(len(group) for group in groups[:step])
            for number in range(first, first + len(groups[step])):
                if number > 0:
                    if PIECES[item][0] not in seen:
                        seen.add(PIECES[item][0])
                        own(PIECES[item][0]).wait()
                    copy(item, number - 1).wait_recv()
                copy(item, number).start()

    for array in range(ARRAYS):
        own(array).start()
    greet(bits)
    enc_out[:rows, :] = enc_ref[...]
    make_hot(buckets_ref, hot_ref, mask_ref)
    advance(STAGE_GAIN)
    arrived(0)
    gains = [gain_row(outs[0][...], gain_size, row) for row in range(3)]
    flat_ref[...] = table_rows(outs[0][...], table_size, 3)

    def normed(value, gain):
        scale = lax.rsqrt(jnp.mean(value * value, -1, keepdims=True) + EPSILON)
        return (value * scale * gain).astype(LOW)

    def over_rows(count, body):
        @pl.loop(0, count // TILE)
        def _(block):
            body(lambda base=0: pl.ds(base + pl.multiple_of(block * TILE, TILE), TILE))

    def normed_rows(source, start):
        def body(at):
            first_out[at(start), :] = normed(source[at(), :].astype(F32), gains[0])

        over_rows(rows, body)

    def project(item, source, out, begin, count):
        weight_ref[...] = full_weight(outs[item])

        def body(at):
            out[at(), :] = contract(source[at(begin), :], weight_ref[...], 1, 0).astype(LOW)

        over_rows(count, body)

    normed_rows(hidden_ref, rows)
    advance(STAGE_QUERY)
    arrived(1)
    project(1, first_out, q_out, rows, rows)
    keep_act(2)
    advance(STAGE_KEY)
    side(0).wait_recv()

    @pl.when(seq_pos == 0)
    def _():
        first_out[:rows, :] = first_out[rows:, :]

    @pl.when(seq_pos != 0)
    def _():
        normed_rows(before_ref, 0)

    arrived(2)
    project(2, first_out, k_out, 0, keys)
    keep_act(1, 3)
    advance(STAGE_VALUE)
    arrived(3)
    project(3, first_out, v_out, 0, keys)
    keep_act(4)

    advance(STAGE_SELF)

    def between(pair, begin):
        for done in range(H // PAIR - 1):

            @pl.when(pair == done)
            def _(done=done):
                advance(begin + done + 1)

    @pl.loop(0, H // PAIR)
    def _(pair):
        at = pl.ds(pl.multiple_of(pair * lanes, lanes), lanes)
        q_ref, k_ref, v_ref, o_ref = (ref.at[:, at] for ref in (q_out, k_out, v_out, mixed_out))
        for head in range(PAIR):
            column = jnp.sum(
                flat_ref[pl.ds(pl.multiple_of((pair * PAIR + head) * BUCKETS, BUCKETS), BUCKETS), :],
                1,
                keepdims=True,
            )
            for off in range(keys // TILE):
                row = jnp.sum(column * hot_ref[off].astype(F32), 0, keepdims=True)
                tiles_ref[head, off] = toeplitz(row + mask_ref[off])
        v_t = v_ref[...].T
        blocks = rows // TILE
        for part in range(keys // rows):

            @pl.when(seq_pos == part)
            def _(part=part):
                for block in range(blocks):
                    last = part * blocks + block
                    attend_block(
                        q_ref, k_ref, v_t, o_ref, lse_out.at[pl.ds(pair, 1)], tiles_ref,
                        block * TILE, last, (last + 1) * TILE,
                    )

        between(pair, STAGE_SELF)

    def residual(item, mixed, base, total, normal, gain):
        weight_ref[...] = full_weight(outs[item])

        def body(at):
            value = base[at(), :].astype(F32) + contract(mixed[at(), :], weight_ref[...], 1, 0)
            total[at(), :] = value
            normal[at(), :] = normed(value, gain)

        over_rows(rows, body)

    keep_act(5, 6)
    advance(STAGE_OUT)
    arrived(4)
    residual(4, mixed_out, hidden_ref, after_out, second_out, gains[1])
    keep_act(7, 8)
    advance(STAGE_CQUERY)
    arrived(5)
    project(5, second_out, cq_out, 0, rows)
    keep_act(9)
    advance(STAGE_CKEY)
    side(1).wait_recv()
    arrived(6)
    project(6, enc_out, ck_out, 0, keys)
    keep_act(0, 10)
    advance(STAGE_CVALUE)
    arrived(7)
    project(7, enc_out, cv_out, 0, keys)
    keep_act(11)
    advance(STAGE_CROSS)

    @pl.loop(0, H // PAIR)
    def _(pair):
        at = pl.ds(pl.multiple_of(pair * lanes, lanes), lanes)
        q_ref, k_ref, v_ref, o_ref = (ref.at[:, at] for ref in (cq_out, ck_out, cv_out, cmixed_out))
        v_t = v_ref[...].T
        for block in range(rows // TILE):
            attend_block(
                q_ref, k_ref, v_t, o_ref, clse_out.at[pl.ds(pair, 1)], None, block * TILE, None, keys
            )
        between(pair, STAGE_CROSS)

    keep_act(12, 13)
    advance(STAGE_COUT)
    arrived(8)
    residual(8, cmixed_out, after_out, across_out, third_out, gains[2])
    keep_act(14, 15)
    advance(STAGE_END)
    assert not todo
    for item in range(INSIDE, ITEMS):
        arrived(item)
    for item in range(ITEMS):
        for step in range(steps):
            copy(item, step).wait_send()
    for which in range(2):
        side(which).wait_send()
    for number in range(len(kept)):
        kept_copy(number).wait()


def make_hot(buckets_ref, hot_ref, mask_ref):
    offs, marks, width = hot_ref.shape
    bucket = buckets_ref[...].astype(F32)
    mark = lax.broadcasted_iota(jnp.int32, (marks, bucket.shape[1]), 0).astype(F32)
    begin = jnp.sum((bucket < mark).astype(F32), 1, keepdims=True)
    end = jnp.sum((bucket <= mark).astype(F32), 1, keepdims=True)
    place = lax.broadcasted_iota(jnp.int32, (marks, width), 1).astype(F32)
    step = jnp.where(place < TILE, place, place - width)
    for off in range(offs):
        gap = step + off * TILE
        hot_ref[off] = ((gap >= begin) & (gap < end)).astype(F32).astype(LOW)
        mask_ref[off] = jnp.where(gap[:1] >= 0, 0.0, NEGATIVE)


def open_layer(items, hidden, encoded, buckets, sizes, collective_id):
    bits = bit_plan()
    steps = len(bits)
    count, width = hidden.shape
    length = count * lax.axis_size("seq")
    offs = length // TILE
    sems = pltpu.SemaphoreType.DMA((ITEMS, steps))
    inside = pl.BlockSpec(memory_space=pltpu.VMEM)
    outside = pl.BlockSpec(memory_space=pl.ANY)
    few, many = (count, width), (length, width)
    lse = (H // PAIR, PAIR, count)
    shapes = [((2,) * steps + x.shape, x.dtype) for x in items]
    shapes += [(many, LOW), (many, LOW), (few, LOW), (many, LOW), (many, LOW), (few, LOW)]
    shapes += [(lse, F32), (few, F32), (few, LOW), (few, LOW), (many, LOW), (many, LOW)]
    shapes += [(few, LOW), (lse, F32), (few, F32), (few, LOW)]
    outs = pl.pallas_call(
        functools.partial(open_kernel, bits, sizes),
        out_shape=[jax.ShapeDtypeStruct(*x) for x in shapes],
        in_specs=[inside] * (ARRAYS + 3),
        out_specs=[outside] * (ARRAYS + 16),
        scratch_shapes=[pltpu.VMEM(*x) for x in shapes[:INSIDE] + shapes[ARRAYS:]]
        + [
            pltpu.VMEM((count, width), LOW),
            pltpu.VMEM((H * BUCKETS, 128), F32),
            pltpu.VMEM((offs, BUCKETS, 2 * TILE), LOW),
            pltpu.VMEM((offs, 1, 2 * TILE), F32),
            pltpu.VMEM((PAIR, offs, TILE, TILE), F32),
            pltpu.VMEM((width, width), LOW),
            sems,
            sems,
            pltpu.SemaphoreType.DMA((ARRAYS,)),
            pltpu.SemaphoreType.DMA((2,)),
            pltpu.SemaphoreType.DMA((2,)),
            pltpu.SemaphoreType.DMA((INSIDE + 16,)),
        ],
        compiler_params=pltpu.CompilerParams(
            collective_id=collective_id, has_side_effects=True, vmem_limit_bytes=66_000_000
        ),
        name="open_layer",
    )(*items, hidden, encoded, buckets)
    return [out.reshape((-1,) + x.shape[-2:]) for out, x in zip(outs, items)] + list(outs[ARRAYS:])


def reversed_bits(bits, path):
    return list(reversed(sum(path_bits(bits, path), [])))


def close_kernel(bits, sizes, *refs):
    gain_size, table_size = sizes
    (ff_refs, weights, cross_refs, self_refs, (smalls_ref, buckets_ref, hidden_in),
     (layer_out, hidden_out, enc_out), outs, (small_out,)) = take(refs, (7, 8, 7, 6, 3, 3, 11, 1))
    rest = refs[46:]
    arrivals = rest[: CLOSE_ITEMS * len(bits)]
    (work_ref, ff_work, down_work, small_ref, q_buf, k_buf, pair_buf, rows_buf, grad_buf,
     res_buf, after_buf, weight_buf, enc_own, send_buf, recv_buf, dk_acc, dv_acc,
     tiles_ref, total_ref, rows_ref, flat_ref, gain_sums, hot_ref,
     mask_ref, send_sem, recv_sem, side_send, side_recv,
     fetch_sem) = rest[CLOSE_ITEMS * len(bits) :]
    steps = len(bits)
    place = coords(bits)
    seq_pos = lax.axis_index("seq")
    rows = res_buf.shape[0]
    keys = k_buf.shape[0]
    lanes = res_buf.shape[1] // (H // PAIR)
    v_buf, keys_in_buf = pair_buf.at[0], pair_buf.at[1]
    mixed_buf, query_in_buf = rows_buf.at[0], rows_buf.at[1]

    def pick(names, which, side):
        return tuple(side if name == which else slice(None) for name in names)

    def order_of(item):
        return reversed_bits(bits, CLOSE_PATHS[item])

    def part_of(item):
        if item not in (DOWN, DOWN + 1):
            return ()
        size = outs[2].shape[0] // 2
        return (pl.ds((item - DOWN) * size, size),)

    def base(item):
        if item == SMALL:
            return small_ref
        if item < DOWN:
            return ff_work.at[item % 4]
        return down_work if item < SQUARES else work_ref.at[item % SLOTS]

    def arrival(item, step):
        return arrivals[item * steps + step]

    def names_at(item, step):
        order = order_of(item)
        return [which for which in range(steps) if which not in order[:step]]

    def copy(item, step):
        which = order_of(item)[step]
        names = names_at(item, step)
        there = pick(names, which, 1 - place[which])
        if step == 0:
            source = base(item).at[there + part_of(item)]
        else:
            source = arrival(item, step - 1).at[there]
        return remote(
            bits, which, source, arrival(item, step), (send_sem.at[item, step], recv_sem.at[item, step])
        )

    def add(item, step):
        which = order_of(item)[step]
        names = names_at(item, step)
        free = [name for name in names if name != which]
        target = arrival(item, step)
        copy(item, step).wait_recv()

        def one(sub):
            here = tuple(place[which] if name == which else sub[free.index(name)] for name in names)
            if step > 0:
                mine = arrival(item, step - 1)[here]
            else:
                mine = base(item)[here + part_of(item)]
            if free:
                return mine + target[tuple(sub)]
            return mine.astype(F32) + target[tuple(sub)].astype(F32)

        if not free:
            if item == SMALL:
                small_out[...] = one(())
            elif item < DOWN:
                size = outs[0].shape[1] // FF_BLOCKS
                outs[item % 2][:, item // 2 * size : (item // 2 + 1) * size] = one(())
            elif item < SQUARES:
                outs[2][part_of(item)] = one(())
            else:
                outs[item - SQUARES + 3][...] = one(())
            return

        outer = max(0, len(free) - 2)

        def several(sub):
            sub = tuple(sub) + (slice(None),) * (len(free) - outer)
            target[sub] = one(sub)

        if outer == 0:
            several(())
            return

        @pl.loop(0, 1 << outer)
        def _(index):
            several([lax.rem(index // (1 << (outer - 1 - i)), 2) for i in range(outer)])

    def side(which):
        return remote(
            bits, 0, send_buf.at[which], recv_buf.at[which], (side_send.at[which], side_recv.at[which])
        )

    slots = {entry[:2]: entry[2] for entry in CLOSE_PLAN}
    done_slots = set()
    drained = set()

    def act(item, step):
        if item == CLOSE_ITEMS:
            side(0).start()
            return
        if item > CLOSE_ITEMS:

            @pl.when(seq_pos != 0)
            def _():
                side(1).start()

            return
        groups = list(reversed(path_bits(bits, CLOSE_PATHS[item]))) + [[None]]
        first = sum(len(group) for group in groups[:step])
        for number in range(first, first + len(groups[step])):
            if number > 0:
                add(item, number - 1)
            if number < steps:
                copy(item, number).start()

    def advance(slot):
        assert slot not in done_slots
        done_slots.add(slot)
        for item, step, planned in CLOSE_PLAN:
            if planned == slot:
                act(item, step)

    def drain(item, slot):
        assert slots[item, 1] <= slot
        copy(item, 0).wait_send()
        drained.add((item, 0))

    def fetch(source, target, sem):
        return pltpu.make_async_copy(source, target, fetch_sem.at[sem])

    def weight(number):
        return fetch(weights[number], weight_buf.at[number % 2], number % 2)

    def over_rows(count, body):
        @pl.loop(0, count // TILE)
        def _(block):
            body(lambda start=0: pl.ds(start + pl.multiple_of(block * TILE, TILE), TILE))

    def weight_grad(item, left, right):
        if item - SLOTS >= SQUARES:
            drain(item - SLOTS, max(done_slots))
        owner_grad(work_ref.at[item % SLOTS], left, right)

    def owner_grad(target, left, right):
        half = left.shape[1] // 2

        @pl.loop(0, 2)
        def _(top):
            at = pl.ds(pl.multiple_of(top * half, half), half)
            value = contract(left[:, at], right[...], 0, 0)
            target[top] = value.reshape(target.shape[1:]).astype(LOW)

    def pairs_back(lse_ref, tiles, begin):
        @pl.loop(0, H // PAIR)
        def _(pair):
            at = pl.ds(pl.multiple_of(pair * lanes, lanes), lanes)
            q_ref, k_ref, v_ref, g_ref, o_ref = (
                ref.at[:, at] for ref in (q_buf, k_buf, v_buf, grad_buf, mixed_buf)
            )
            if tiles:
                for head in range(PAIR):
                    start = pl.multiple_of((pair * PAIR + head) * BUCKETS, BUCKETS)
                    column = jnp.sum(flat_ref[pl.ds(start, BUCKETS), :], 1, keepdims=True)
                    for off in range(keys // TILE):
                        row = jnp.sum(column * hot_ref[off].astype(F32), 0, keepdims=True)
                        tiles_ref[head, off] = toeplitz(row + mask_ref[off])
            k_t = k_ref[...].T
            prod_t = (g_ref[...].astype(F32) * o_ref[...].astype(F32)).T
            main = (q_ref, k_ref, v_ref, g_ref, lse_ref.at[pl.ds(pair, 1)], q_ref, dk_acc, dv_acc)
            blocks = rows // TILE
            if not tiles:
                for block in range(blocks):
                    back_block(main, k_t, prod_t, block * TILE, None, keys, block == 0, None, None)
            else:
                for part in range(keys // rows):

                    @pl.when(seq_pos == part)
                    def _(part=part):
                        for block in range(blocks):
                            last = part * blocks + block
                            back_block(
                                main, k_t, prod_t, block * TILE, last, (last + 1) * TILE,
                                block == 0, tiles_ref, total_ref,
                            )
                        for head in range(PAIR):
                            column = jnp.zeros((BUCKETS, 1), F32)
                            for off in range((part + 1) * blocks):
                                row = skew_sum(total_ref.at[head, off])
                                column = column + jnp.sum(
                                    hot_ref[off].astype(F32) * row, 1, keepdims=True
                                )
                            start = pl.multiple_of((pair * PAIR + head) * BUCKETS, BUCKETS)
                            rows_ref[pl.ds(start, BUCKETS), :] = jnp.broadcast_to(
                                column, (BUCKETS, rows_ref.shape[1])
                            )

            k_ref[...] = dk_acc[...].astype(LOW)
            v_ref[...] = dv_acc[...].astype(LOW)
            for done in range(H // PAIR - 1):

                @pl.when(pair == done)
                def _(done=done):
                    advance(begin + done + 1)

    cq_in, ck_in, cv_in, cmixed_in, enc_in, second_in, clse_ref = cross_refs
    q_in, k_in, v_in, mixed_in, first_in, lse_ref = self_refs[:6]
    fetches = [
        fetch(cmixed_in, mixed_buf, 2), fetch(cq_in, q_buf, 3), fetch(ck_in, k_buf, 4),
        fetch(cv_in, v_buf, 5), fetch(enc_in, keys_in_buf, 6), fetch(second_in, query_in_buf, 7),
    ]
    third_in, grad_in, across_in, gate_in, up_in, down_in, after_in = ff_refs
    width = gate_in.shape[1] // FF_BLOCKS
    third_ref, grad_ref = k_buf.at[:rows], k_buf.at[rows:]
    loads = [fetch(third_in, third_ref, 2), fetch(grad_in, grad_ref, 3), fetch(across_in, after_buf, 4)]

    def ff_loads(block, slot):
        at = pl.ds(pl.multiple_of(block * width, width), width)
        return (
            fetch(gate_in.at[:, at], weight_buf.at[slot, :, pl.ds(0, width)], 8 + slot),
            fetch(up_in.at[:, at], pair_buf.at[slot, pl.ds(0, weight_buf.shape[1]), pl.ds(0, width)],
                  10 + slot),
            fetch(down_in.at[at], rows_buf.at[slot, pl.ds(0, width)], 12 + slot),
        )

    for one in ff_loads(0, 0):
        one.start()
    for one in loads:
        one.start()
    make_hot(buckets_ref, hot_ref, mask_ref)
    greet(bits)
    flat_ref[...] = table_rows(smalls_ref[...], table_size, 3)
    gain_one, gain_two, gain_three = [gain_row(smalls_ref[...], gain_size, row) for row in range(3)]
    for one in loads:
        one.wait()
    res_buf[...] = jnp.zeros_like(res_buf)
    enc_own[...] = jnp.zeros_like(enc_own)

    def ff_rows(slot, at):
        w_gate = weight_buf[slot, :, 0:width]
        w_up = pair_buf[slot, 0 : weight_buf.shape[1], 0:width]
        w_down = rows_buf[slot, 0:width, :]
        gate = contract(third_ref[at, :], w_gate, 1, 0)
        upper = contract(third_ref[at, :], w_up, 1, 0)
        grad = contract(grad_ref[at, :], w_down, 1, 1)
        square = gate * gate
        bend = jnp.tanh(GELU_SCALE * gate * (1.0 + 0.044715 * square))
        open_part = 0.5 * (1.0 + bend)
        active = gate * open_part
        slope = open_part + 0.5 * gate * (1.0 - bend * bend) * (
            GELU_SCALE * (1.0 + 3.0 * 0.044715 * square)
        )
        inner = (active * upper).astype(LOW)
        gate_grad = (grad * upper * slope).astype(LOW)
        upper_grad = (grad * active).astype(LOW)
        q_buf[at, 0:width] = inner
        grad_buf[at, 0:width] = gate_grad
        send_buf[0, at, 0:width] = upper_grad
        res_buf[at, :] += contract(inner, w_down, 1, 0)
        enc_own[at, :] += contract(gate_grad, w_gate, 1, 1) + contract(upper_grad, w_up, 1, 1)

    @pl.loop(0, FF_BLOCKS)
    def _(block):
        slot = lax.rem(block, 2)
        for one in ff_loads(block, slot):
            one.wait()

        @pl.when(block < FF_BLOCKS - 1)
        def _():
            for one in ff_loads(block + 1, 1 - slot):
                one.start()

        @pl.loop(0, rows // TILE)
        def _(part):
            ff_rows(slot, pl.ds(pl.multiple_of(part * TILE, TILE), TILE))

        for now in range(FF_BLOCKS):

            @pl.when(block == now)
            def _(now=now):
                advance(2 + 2 * now)
                if now >= 2:
                    drain(2 * now - 4, 2 + 2 * now)
                    drain(2 * now - 3, 2 + 2 * now)

        owner_grad(ff_work.at[2 * slot], third_ref, grad_buf.at[:, 0:width])
        owner_grad(ff_work.at[2 * slot + 1], third_ref, send_buf.at[0, :, 0:width])
        value = contract(q_buf[:, 0:width], grad_ref[...], 0, 0)
        down_work[lax.div(block, 2), slot] = value.reshape(down_work.shape[2:]).astype(LOW)
        for now in range(FF_BLOCKS):

            @pl.when(block == now)
            def _(now=now):
                advance(3 + 2 * now)

    weight(0).start()
    weight(1).start()
    for one in (fetches[0], fetches[1], fetches[3], fetches[4], fetches[5]):
        one.start()

    def norm_back_rows(value, gain, grad):
        scale = lax.rsqrt(jnp.mean(value * value, -1, keepdims=True) + EPSILON)
        scaled = gain * grad
        inner = jnp.mean(value * scaled, -1, keepdims=True)
        back = scale * scaled - value * (scale * scale * scale) * inner
        return back, jnp.sum(grad * value * scale, 0, keepdims=True)

    gain_sums[...] = jnp.zeros_like(gain_sums)

    def body(at):
        value = after_buf[at(), :]
        send_buf[1, at(), :] = (value + res_buf[at(), :]).astype(LOW)
        back, total = norm_back_rows(value, gain_three, enc_own[at(), :])
        gain_sums[2:3, :] += total
        res_buf[at(), :] = grad_ref[at(), :].astype(F32) + back

    over_rows(rows, body)
    layer_copy = fetch(send_buf.at[1], layer_out, 15)
    layer_copy.start()
    fetch(after_in, after_buf, 14).start()
    fetches[2].start()

    def to_mixed(number, source):
        weight(number).wait()

        def body(at):
            grad_buf[at(), :] = contract(
                source[at(), :].astype(LOW), weight_buf[number % 2], 1, 1
            ).astype(LOW)

        over_rows(rows, body)
        weight(number + 2).start()

    advance(10)
    to_mixed(0, res_buf)
    fetches[0].wait()

    def low_rows(source, target):
        def body(at):
            target[at(), :] = source[at(), :].astype(LOW)

        over_rows(rows, body)

    low_rows(res_buf, send_buf.at[0])
    weight_grad(SQUARES, mixed_buf, send_buf.at[0])
    advance(11)
    for one in fetches[1:4]:
        one.wait()
    pairs_back(clse_ref, False, 11)
    fetch(mixed_in, mixed_buf, 2).start()
    advance(17)

    def both_back(numbers, keep, count):
        def body_other(at):
            total = contract(k_buf[at(count), :], weight_buf[numbers[0] % 2], 1, 1)
            total = total + contract(v_buf[at(count), :], weight_buf[numbers[1] % 2], 1, 1)
            send_buf[keep[0], at(), :] = total.astype(LOW)
            if not count:
                gain_sums[3:4, :] += jnp.sum(
                    total * keys_in_buf[at(), :].astype(F32), 0, keepdims=True
                )

        def body_own(at):
            begin = 0 if count else rows
            total = contract(k_buf[at(begin), :], weight_buf[numbers[0] % 2], 1, 1)
            total = total + contract(v_buf[at(begin), :], weight_buf[numbers[1] % 2], 1, 1)
            keep[1][at(), :] = total

        over_rows(rows, body_other)
        return body_own

    weight(1).wait()
    weight(2).wait()
    own_part = both_back((1, 2), (0, enc_own), rows)
    for one in fetches[4:]:
        one.wait()
    advance(18)
    weight_grad(SQUARES + 1, keys_in_buf, k_buf)
    advance(19)
    weight_grad(SQUARES + 2, keys_in_buf, v_buf)
    advance(20)
    over_rows(rows, own_part)
    fetch(k_in, k_buf, 4).start()
    fetch(v_in, v_buf, 5).start()
    fetch(first_in, keys_in_buf, 6).start()
    weight(3).start()
    weight(4).start()
    advance(21)
    weight_grad(SQUARES + 3, query_in_buf, q_buf)
    advance(22)
    weight(3).wait()
    fetch(after_in, after_buf, 14).wait()

    def body(at):
        grad = contract(q_buf[at(), :], weight_buf[1], 1, 1)
        back, total = norm_back_rows(after_buf[at(), :], gain_two, grad)
        gain_sums[1:2, :] += total
        res_buf[at(), :] += back

    over_rows(rows, body)
    fetch(q_in, q_buf, 3).start()
    weight(5).start()
    weight(4).wait()

    def body(at):
        grad_buf[at(), :] = contract(res_buf[at(), :].astype(LOW), weight_buf[0], 1, 1).astype(LOW)

    over_rows(rows, body)
    weight(6).start()
    fetch(mixed_in, mixed_buf, 2).wait()
    low_rows(res_buf, query_in_buf)
    weight_grad(SQUARES + 4, mixed_buf, query_in_buf)
    advance(23)
    fetch(q_in, q_buf, 3).wait()
    fetch(k_in, k_buf, 4).wait()
    fetch(v_in, v_buf, 5).wait()
    pairs_back(lse_ref, True, 23)
    advance(29)
    side(0).wait_recv()
    side(0).wait_send()

    def body(at):
        send_buf[0, at(), :] = (enc_own[at(), :] + recv_buf[0, at(), :].astype(F32)).astype(LOW)

    over_rows(rows, body)
    enc_copy = fetch(send_buf.at[0], enc_out, 8)
    enc_copy.start()
    fetch(hidden_in, grad_buf, 9).start()
    layer_copy.wait()
    weight(5).wait()
    weight(6).wait()
    fetch(first_in, keys_in_buf, 6).wait()
    own_part = both_back((5, 6), (1, enc_own), 0)

    advance(30)
    weight_grad(SQUARES + 5, keys_in_buf, v_buf)
    advance(31)
    weight_grad(SQUARES + 6, keys_in_buf, k_buf)
    advance(32)
    weight_grad(SQUARES + 7, keys_in_buf.at[rows:], q_buf)
    advance(33)
    over_rows(rows, own_part)
    weight(7).start()
    own_low = (seq_pos == 0).astype(F32)
    fetch(hidden_in, grad_buf, 9).wait()
    weight(7).wait()

    def body(at):
        grad = contract(q_buf[at(), :], weight_buf[1], 1, 1) + enc_own[at(), :]
        grad = grad + own_low * send_buf[1, at(), :].astype(F32)
        enc_own[at(), :] = grad
        value = grad_buf[at(), :].astype(F32)
        scale = lax.rsqrt(jnp.mean(value * value, -1, keepdims=True) + EPSILON)
        gain_sums[0:1, :] += jnp.sum(grad * value * scale, 0, keepdims=True)

    over_rows(rows, body)
    gain_sums[0:1, :] += (1.0 - own_low) * gain_sums[3:4, :] / gain_one
    small_ref[...] = small_rows(
        gain_sums[0:1, :], gain_sums[1:2, :], gain_sums[2:3, :], rows_ref[...], gain_size,
        table_size, small_ref.shape
    )
    advance(34)

    @pl.when(seq_pos == 0)
    def _():
        side(1).wait_recv()

    @pl.when(seq_pos != 0)
    def _():
        side(1).wait_send()

    def body(at):
        grad = enc_own[at(), :] + jnp.where(
            seq_pos == 0, recv_buf[1, at(), :].astype(F32), 0.0
        )
        back, _ = norm_back_rows(grad_buf[at(), :].astype(F32), gain_one, grad)
        hidden_out[at(), :] = (res_buf[at(), :] + back).astype(LOW)

    over_rows(rows, body)
    advance(35)
    assert all(entry[2] in done_slots for entry in CLOSE_PLAN)
    for item in range(CLOSE_ITEMS):
        for step in range(steps):
            if (item, step) not in drained:
                copy(item, step).wait_send()
    enc_copy.wait()


def take(refs, counts):
    out = []
    begin = 0
    for count in counts:
        out.append(refs[begin : begin + count])
        begin += count
    return out


def small_rows(one, two, three, table, gain_size, table_size, shape):
    owners = one.shape[1] // gain_size

    def spread(source, size, row):
        count = owners * size
        target = lax.broadcasted_iota(jnp.int32, (owners * 8, count), 0)
        entry = lax.broadcasted_iota(jnp.int32, (owners * 8, count), 1)
        begin = (target >> 3) * size
        hot = ((target & 7) == row) & (entry >= begin) & (entry < begin + size)
        return lax.dot_general(
            hot.astype(F32), source, (((1,), (0 if row == 3 else 1,)), ((), ())),
            precision=lax.Precision.HIGHEST, preferred_element_type=F32,
        )

    def wheel(shape, axis, size):
        entry = lax.broadcasted_iota(jnp.int32, shape, axis).astype(F32)
        lane = lax.broadcasted_iota(jnp.int32, shape, 1 - axis).astype(F32)
        return lane == entry - size * jnp.floor((entry + 0.5) * (1.0 / size))

    total = jnp.zeros((owners * 8, 128), F32)
    for row, value in enumerate((one, two, three)):
        grid = (128, value.shape[1])
        total = total + spread(
            jnp.where(wheel(grid, 1, gain_size), jnp.broadcast_to(value, grid), 0.0), gain_size, row
        )
    total = total + spread(jnp.where(wheel(table.shape, 0, table_size), table, 0.0), table_size, 3)
    return total.reshape(shape)


SLOTS = 2
FF_BLOCKS = 4
DOWN = 2 * FF_BLOCKS
SQUARES = DOWN + 2
SMALL = SQUARES + 8
CLOSE_ITEMS = SMALL + 1
GELU_SCALE = 0.7978845608028654
CLOSE_PATHS = ('xzZyc', 'xyzZc', 'yzZxc', 'yxzZc', 'xzZyc', 'yzZxc', 'xzZyc', 'yxzZc', 'yzZxc', 'xzZyc', 'zZyxc', 'xyzZc', 'xzZyc', 'xzZyc', 'zZyxc', 'zZxyc', 'xyzZc', 'zZxyc', 'xyzZc')
CLOSE_PLAN = (
    (1, 0, 3), (0, 0, 3), (0, 1, 4), (1, 1, 5), (3, 0, 5), (2, 0, 5),
    (3, 1, 6), (2, 1, 6), (1, 2, 9), (6, 0, 9), (9, 0, 9), (7, 0, 9),
    (8, 0, 10), (5, 0, 10), (0, 2, 11), (9, 1, 11), (6, 1, 11), (10, 0, 11),
    (4, 0, 12), (8, 1, 12), (7, 1, 12), (3, 2, 13), (2, 2, 13), (10, 1, 15),
    (9, 2, 15), (5, 1, 16), (19, 0, 19), (11, 0, 19), (8, 2, 19), (6, 2, 19),
    (4, 1, 20), (10, 2, 20), (12, 0, 20), (3, 3, 20), (11, 1, 21), (7, 2, 21),
    (0, 3, 22), (9, 3, 22), (12, 1, 22), (5, 2, 23), (14, 0, 23), (8, 3, 24),
    (13, 0, 24), (14, 1, 26), (7, 3, 26), (10, 3, 27), (12, 2, 27), (13, 1, 27),
    (4, 2, 27), (11, 2, 27), (6, 3, 27), (20, 0, 30), (14, 2, 30), (2, 3, 31),
    (15, 0, 31), (7, 4, 31), (13, 2, 31), (16, 0, 32), (1, 3, 32), (15, 1, 32),
    (5, 3, 32), (17, 0, 33), (16, 1, 33), (4, 3, 33), (12, 3, 33), (13, 3, 33),
    (17, 1, 33), (10, 4, 33), (11, 3, 34), (7, 5, 34), (18, 0, 34), (8, 4, 34),
    (15, 2, 34), (18, 1, 34), (16, 2, 34), (17, 2, 34), (1, 4, 34), (12, 4, 34),
    (2, 4, 34), (14, 3, 34), (15, 3, 34), (5, 4, 34), (11, 4, 34), (6, 4, 34),
    (18, 2, 34), (3, 4, 34), (9, 4, 34), (8, 5, 34), (17, 3, 34), (14, 4, 34),
    (16, 3, 34), (2, 5, 34), (5, 5, 34), (3, 5, 34), (0, 4, 34), (15, 4, 34),
    (10, 5, 34), (11, 5, 34), (18, 3, 34), (13, 4, 34), (1, 5, 34), (17, 4, 34),
    (4, 4, 34), (6, 5, 34), (9, 5, 34), (16, 4, 34), (18, 4, 34), (13, 5, 35),
    (4, 5, 35), (12, 5, 35), (14, 5, 35), (15, 5, 35), (18, 5, 35), (16, 5, 35),
    (0, 5, 35), (17, 5, 35),
)


def close_layer(forward, weights, cross, own, smalls, buckets, hidden, sizes, collective_id):
    bits = bit_plan()
    steps = len(bits)
    owners = 1 << steps
    count, width = hidden.shape
    units = forward[3].shape[1]
    length = cross[1].shape[0]
    offs = length // TILE
    lanes = width // (H // PAIR)
    gate, down = (width // owners, units), (units // owners, width)
    square = (width // owners, width)
    blocks = [(gate[0], units // FF_BLOCKS)] * DOWN + [(down[0] // 2, width)] * 2 + [square] * 8
    kinds = [LOW] * SMALL + [F32]
    blocks.append((8, 128))
    arrivals = [
        pltpu.VMEM((2,) * (steps - 1 - step) + block, kind)
        for block, kind in zip(blocks, kinds)
        for step in range(steps)
    ]
    inside = pl.BlockSpec(memory_space=pltpu.VMEM)
    outside = pl.BlockSpec(memory_space=pl.ANY)
    few, many = (count, width), (length, width)
    vm = pltpu.VMEM
    sems = pltpu.SemaphoreType.DMA((CLOSE_ITEMS, steps))
    pair_sem = pltpu.SemaphoreType.DMA((2,))
    return pl.pallas_call(
        functools.partial(close_kernel, bits, sizes),
        out_shape=[jax.ShapeDtypeStruct(few, LOW)] * 3
        + [jax.ShapeDtypeStruct(block, F32) for block in (gate, gate, down)]
        + [jax.ShapeDtypeStruct(square, F32)] * 8
        + [jax.ShapeDtypeStruct((8, 128), F32)],
        in_specs=[outside] * (7 + 8) + [outside] * 6 + [inside] + [outside] * 5 + [inside]
        + [inside] * 2 + [outside],
        out_specs=[outside, inside, outside] + [inside] * 12,
        scratch_shapes=arrivals
        + [
            vm((SLOTS,) + (2,) * steps + square, LOW),
            vm((4,) + (2,) * steps + (gate[0], units // FF_BLOCKS), LOW),
            vm((2,) * steps + down, LOW),
            vm((2,) * steps + (8, 128), F32),
            vm(few, LOW), vm(many, LOW), vm((2,) + many, LOW), vm((2,) + few, LOW),
            vm(few, LOW), vm(few, F32), vm(few, F32),
            vm((2, width, width), LOW), vm(few, F32), vm((2,) + few, LOW), vm((2,) + few, LOW),
            vm((length, lanes), F32), vm((length, lanes), F32),
            vm((PAIR, offs, TILE, TILE), F32), vm((PAIR, offs, TILE, TILE), F32),
            vm((H * BUCKETS, 128), F32), vm((H * BUCKETS, 128), F32), vm((8, width), F32),
            vm((offs, BUCKETS, 2 * TILE), LOW), vm((offs, 1, 2 * TILE), F32),
            sems, sems, pair_sem, pair_sem, pltpu.SemaphoreType.DMA((16,)),
        ],
        compiler_params=pltpu.CompilerParams(
            collective_id=collective_id, has_side_effects=True, vmem_limit_bytes=67_000_000
        ),
        name="close_layer",
    )(*forward, *weights, *cross, *own, smalls, buckets, hidden)


def finish_kernel(*refs):
    count = (len(refs) - 5) // 2
    for source, target in zip(refs[: count], refs[count + 1 :]):
        target[...] = source[...]
    small = refs[count]
    for row, target in enumerate(refs[2 * count + 1 :]):
        target[...] = small[row, : target.shape[0]]


def finish(arrays, small, sizes):
    count = len(arrays)
    inside = pl.BlockSpec(memory_space=pltpu.VMEM)
    return pl.pallas_call(
        finish_kernel,
        out_shape=[jax.ShapeDtypeStruct(x.shape, x.dtype) for x in arrays]
        + [jax.ShapeDtypeStruct((size,), F32) for size in sizes],
        in_specs=[inside] * (count + 1),
        out_specs=[inside] * (count + 4),
        name="finish",
    )(*arrays, small)


def dot_low(left, right):
    return contract(left, right, 1, 0)


def dot_left(left, right):
    return contract(left, right, 0, 0)


def dot_right(left, right):
    return contract(left, right, 1, 1)


def rms_norm(value, gain):
    return value * lax.rsqrt(jnp.mean(value * value, -1, keepdims=True) + EPSILON) * gain


def norm_back(value, gain, grad):
    return jax.vjp(rms_norm, value, gain)[1](grad)


def gated(gate, upper):
    return jax.nn.gelu(gate, approximate=True) * upper


def pad_rows(rows):
    return sum(
        jnp.pad(row.astype(F32)[None], ((place, 7 - place), (0, 128 - row.shape[0])))
        for place, row in enumerate(rows)
    )


def on_device(
    hidden_in,
    encoded,
    cotangent,
    buckets,
    self_query,
    self_key,
    self_value,
    self_out,
    cross_query,
    cross_key,
    cross_value,
    cross_out,
    ff_gate,
    ff_up,
    ff_down,
    norm_self,
    norm_cross,
    norm_ff,
    bias_table,
):
    owners = lax.axis_size("seq") * lax.axis_size("shard")
    seq_pos = lax.axis_index("seq")
    seq_row = seq_pos.reshape(1).astype(jnp.int32)
    low_side = seq_pos == 0
    both = ("seq", "shard")
    width = hidden_in.shape[2]
    own_low = hidden_in[0]
    enc_own = encoded[0]
    small = pad_rows([norm_self, norm_cross, norm_ff, bias_table])
    hidden = own_low.astype(F32)
    count = hidden.shape[0]
    length = count * lax.axis_size("seq")
    gap, hot = bucket_rows(buckets, length)
    opened = open_layer(
        [small, self_query, self_key, self_value, self_out, cross_query, cross_key, cross_value,
         cross_out, ff_gate, ff_up, ff_down],
        own_low,
        enc_own,
        buckets.reshape(1, -1),
        (norm_self.shape[0], bias_table.shape[0]),
        1,
    )
    smalls = opened[0]
    (w_query, w_key, w_value, w_sout, w_cquery, w_ckey, w_cvalue, w_cout, w_gate, w_up, w_down) = [
        x.reshape(-1, x.shape[-1]) for x in opened[1:12]
    ]
    (enc_all, first_all, query, key, value, self_mixed, self_lse, after_self, second,
     cross_q, cross_k, cross_v, cross_mixed, cross_lse, after_cross, third) = opened[12:]
    gain_one, gain_two, gain_three = [
        smalls[:, i, : norm_self.shape[0]].reshape(-1) for i in range(3)
    ]
    table = smalls[:, 3, : bias_table.shape[0]].reshape(H, BUCKETS)
    rows = jnp.einsum("hb,bof->hof", table.astype(LOW), hot, preferred_element_type=F32)
    rows = jnp.where(gap[None] >= 0, rows, NEGATIVE).reshape(H // PAIR, PAIR, *gap.shape)
    first = first_all[count:]

    gains = norm_self.shape[0]
    if width // owners >= 16:
        *arrays, small_sum = close_layer(
            [third, cotangent[0], after_cross, w_gate, w_up, w_down, after_self],
            [w_cout, w_ckey, w_cvalue, w_cquery, w_sout, w_key, w_value, w_query],
            [cross_q, cross_k, cross_v, cross_mixed, enc_all, second, cross_lse],
            [query, key, value, self_mixed, first_all, self_lse],
            smalls,
            buckets.reshape(1, -1),
            own_low,
            (gains, bias_table.shape[0]),
            2,
        )
        *arrays, one, two, three, four = finish(
            arrays, small_sum, (gains,) * 3 + bias_table.shape
        )
        hidden_out, grad_hidden, grad_encoded, *sums = arrays
        return (
            hidden_out[None],
            grad_hidden[None],
            grad_encoded[None],
            sums[10],
            sums[9],
            sums[8],
            sums[7],
            sums[6],
            sums[4],
            sums[5],
            sums[3],
            sums[0],
            sums[1],
            sums[2],
            one,
            two,
            three,
            four,
        )
    gate = dot_low(third, w_gate)
    upper = dot_low(third, w_up)
    inner = gated(gate, upper).astype(LOW)
    hidden_out = (after_cross + dot_low(inner, w_down)).astype(LOW)

    grad_top = cotangent[0]
    grad_wdown = dot_left(inner, grad_top).astype(LOW)
    grad_inner = dot_right(grad_top, w_down)
    grad_gate, grad_upper = jax.vjp(gated, gate, upper)[1](grad_inner)
    gate_low = grad_gate.astype(LOW)
    upper_low = grad_upper.astype(LOW)
    grad_wgate = dot_left(third, gate_low).astype(LOW)
    grad_wup = dot_left(third, upper_low).astype(LOW)
    grad_third = dot_right(gate_low, w_gate) + dot_right(upper_low, w_up)
    norm_grad, grad_gain_three = norm_back(after_cross, gain_three, grad_third)
    grad_cross_res = grad_top.astype(F32) + norm_grad
    sum_gate, sum_up = [
        lax.psum_scatter(x, both, scatter_dimension=0, tiled=True).astype(F32)
        for x in (grad_wgate, grad_wup)
    ]
    cross_res_low = grad_cross_res.astype(LOW)
    grad_wcout = dot_left(cross_mixed, cross_res_low).astype(LOW)
    grad_cross_mix = dot_right(cross_res_low, w_cout).astype(LOW)
    grad_cq, grad_ck, grad_cv = attend_back(
        cross_q, cross_k, cross_v, grad_cross_mix, cross_mixed, cross_lse, None, None
    )
    grad_enc = dot_right(grad_ck, w_ckey) + dot_right(grad_cv, w_cvalue)
    enc_back = lax.ppermute(grad_enc[count:].astype(LOW), "seq", [(0, 1), (1, 0)])
    grad_wcquery = dot_left(second, grad_cq).astype(LOW)
    grad_wckey = dot_left(enc_all, grad_ck).astype(LOW)
    grad_wcvalue = dot_left(enc_all, grad_cv).astype(LOW)
    norm_grad, grad_gain_two = norm_back(after_self, gain_two, dot_right(grad_cq, w_cquery))
    grad_self_res = grad_cross_res + norm_grad
    self_res_low = grad_self_res.astype(LOW)
    grad_wsout = dot_left(self_mixed, self_res_low).astype(LOW)
    grad_self_mix = dot_right(self_res_low, w_sout).astype(LOW)
    grad_q, grad_k, grad_v, grad_rows = attend_back(
        query, key, value, grad_self_mix, self_mixed, self_lse, seq_row, rows
    )
    grad_part = dot_right(grad_k, w_key) + dot_right(grad_v, w_value)
    part_back = lax.ppermute(grad_part[:count].astype(LOW), "seq", [(1, 0)])
    grad_wquery = dot_left(first, grad_q).astype(LOW)
    grad_wkey = dot_left(first_all, grad_k).astype(LOW)
    grad_wvalue = dot_left(first_all, grad_v).astype(LOW)
    grad_first = (
        dot_right(grad_q, w_query)
        + grad_part[count:]
        + jnp.where(low_side, grad_part[:count], 0.0)
        + part_back.astype(F32)
    )
    norm_grad, grad_gain_one = norm_back(hidden, gain_one, grad_first)
    grad_hidden = (grad_self_res + norm_grad).astype(LOW)
    grad_encoded = (grad_enc[:count] + enc_back.astype(F32)).astype(LOW)
    table_grad = jnp.einsum(
        "hof,bof->hb", grad_rows.reshape(H, *gap.shape), hot.astype(F32),
        precision=lax.Precision.HIGHEST,
    )
    small_grads = jnp.stack(
        [
            jnp.pad(x.reshape(owners, -1), ((0, 0), (0, 128 - x.size // owners)))
            for x in (grad_gain_one, grad_gain_two, grad_gain_three, table_grad)
        ]
        + [jnp.zeros((owners, 128), F32)] * 4,
        1,
    ).reshape(owners * 8, 128)
    sums = scatter(
        [grad_wdown, grad_wcout, grad_wcquery, grad_wckey, grad_wcvalue, grad_wsout, grad_wquery,
         grad_wkey, grad_wvalue, small_grads],
        2,
    )
    small_sum = sums[9]
    return (
        hidden_out[None],
        grad_hidden[None],
        grad_encoded[None],
        sums[6],
        sums[7],
        sums[8],
        sums[5],
        sums[2],
        sums[3],
        sums[4],
        sums[1],
        sum_gate,
        sum_up,
        sums[0],
        small_sum[0, :gains],
        small_sum[1, :gains],
        small_sum[2, :gains],
        small_sum[3, : bias_table.shape[0]],
    )


def solution(mesh):
    rows = P(("seq", "shard"), None)
    flat = P(("seq", "shard"))
    tokens = P("shard", "seq", None)
    return jax.shard_map(
        on_device,
        mesh=mesh,
        in_specs=(tokens,) * 3 + (P(),) + (rows,) * 11 + (flat,) * 4,
        out_specs=(tokens,) * 3 + (rows,) * 11 + (flat,) * 4,
        check_vma=False,
    )
```

```python
import functools
import jax
import jax.numpy as jnp
from jax import lax
from jax.experimental import pallas as pl
from jax.experimental.pallas import tpu as pltpu
from jax.sharding import PartitionSpec as P

H = 12
BUCKETS = 32
NEGATIVE = -1e30
EPSILON = 1e-06
F32 = jnp.float32
LOW = jnp.bfloat16
PAIR = 2
TILE = 256


def contract(left, right, left_dim, right_dim):
    return lax.dot_general(
        left, right, (((left_dim,), (right_dim,)), ((), ())), preferred_element_type=F32
    )


def keep_head(value, head):
    size = value.shape[1] // PAIR
    lane = lax.broadcasted_iota(jnp.int32, value.shape, 1)
    inside = (lane >= head * size) & (lane < (head + 1) * size)
    return jnp.where(inside, value, jnp.zeros_like(value))


def toeplitz(row):
    wide = jnp.broadcast_to(row, (TILE, 2 * TILE))
    return pltpu.roll(wide, 0, 1, stride=1, stride_axis=0)[:, :TILE]


def skew_sum(total_ref):
    group = 8
    width = 2 * TILE
    summed = jnp.zeros((group, width), F32)
    for start in range(0, TILE, group):
        rows = total_ref[start : start + group, :]
        wide = jnp.concatenate([rows, jnp.zeros_like(rows)], 1)
        summed = summed + pltpu.roll(wide, (width - start) % width, 1)
    out = summed[0:1]
    for row in range(1, group):
        out = out + pltpu.roll(summed[row : row + 1], width - row, 1)
    return out


def scores_t(keys, query, tiles, last):
    scores = contract(keys, query, 1, 1)
    if tiles is None:
        return scores
    parts = [
        scores[place * TILE : (place + 1) * TILE] + tiles[last - place] for place in range(last + 1)
    ]
    return jnp.concatenate(parts, 0) if len(parts) > 1 else parts[0]


def attend_block(q_ref, k_ref, v_t, o_ref, lse_ref, tiles_ref, start, last, span):
    query = q_ref[start : start + TILE, :]
    size = query.shape[1] // PAIR
    mixed = []
    for head in range(PAIR):
        tiles = None if tiles_ref is None else tiles_ref.at[head]
        scores = scores_t(k_ref[:span, :], keep_head(query, head), tiles, last)
        summit = jnp.max(scores, 0, keepdims=True)
        exponent = jnp.exp(scores - summit)
        total = jnp.sum(exponent, 0, keepdims=True)
        weighted = contract(
            v_t[head * size : (head + 1) * size, :span], exponent.astype(LOW), 1, 0
        )
        mixed.append(weighted / total)
        lse_ref[0, head : head + 1, start : start + TILE] = summit + jnp.log(total)
    o_ref[start : start + TILE, :] = jnp.concatenate(mixed, 0).T.astype(LOW)


def attend_kernel(causal, *refs):
    if causal:
        seq_ref, q_ref, k_ref, v_ref, z_ref, o_ref, lse_ref, tiles_ref = refs
        make_tiles(z_ref, tiles_ref)
    else:
        q_ref, k_ref, v_ref, o_ref, lse_ref = refs
    v_t = v_ref[...].T
    blocks = q_ref.shape[0] // TILE
    keys = k_ref.shape[0]
    if not causal:
        for block in range(blocks):
            attend_block(q_ref, k_ref, v_t, o_ref, lse_ref, None, block * TILE, None, keys)
        return
    for side in range(keys // q_ref.shape[0]):

        @pl.when(seq_ref[0] == side)
        def _(side=side):
            for block in range(blocks):
                last = side * blocks + block
                attend_block(
                    q_ref, k_ref, v_t, o_ref, lse_ref, tiles_ref, block * TILE, last,
                    (last + 1) * TILE,
                )


def make_tiles(z_ref, tiles_ref):
    for head in range(PAIR):
        for off in range(z_ref.shape[2]):
            tiles_ref[head, off] = toeplitz(z_ref[0, head, off : off + 1, :])


def attend(queries, keys_all, values, seq_pos, rows):
    count, width = queries.shape
    length = keys_all.shape[0]
    pairs = H // PAIR
    lanes = width // pairs
    offs = length // TILE
    causal = rows is not None
    col = lambda size: pl.BlockSpec((size, lanes), lambda pair, *_: (0, pair))
    in_specs = [col(count), col(length), col(length)]
    args = [queries, keys_all, values]
    scratch = []
    if causal:
        in_specs.append(pl.BlockSpec((1, PAIR, offs, 2 * TILE), lambda pair, *_: (pair, 0, 0, 0)))
        args = [seq_pos] + args + [rows]
        scratch = [pltpu.VMEM((PAIR, offs, TILE, TILE), F32)]
    work = H * count * length
    return pl.pallas_call(
        functools.partial(attend_kernel, causal),
        grid_spec=pltpu.PrefetchScalarGridSpec(
            num_scalar_prefetch=1 if causal else 0,
            grid=(pairs,),
            in_specs=in_specs,
            out_specs=[
                col(count),
                pl.BlockSpec((1, PAIR, count), lambda pair, *_: (pair, 0, 0)),
            ],
            scratch_shapes=scratch,
        ),
        out_shape=[
            jax.ShapeDtypeStruct((count, width), LOW),
            jax.ShapeDtypeStruct((pairs, PAIR, count), F32),
        ],
        cost_estimate=pl.CostEstimate(
            flops=work * 256 * 2, bytes_accessed=6 * length * width, transcendentals=work
        ),
        name="attend_causal" if causal else "attend_cross",
    )(*args)


def back_block(refs, k_t, prod_t, start, last, span, first, tiles_ref, total_ref):
    q_ref, k_ref, v_ref, g_ref, lse_ref, dq_ref, dk_acc, dv_acc = refs
    query = q_ref[start : start + TILE, :]
    grad = g_ref[start : start + TILE, :]
    size = query.shape[1] // PAIR
    dq_t = []
    dk = dv = None
    for head in range(PAIR):
        own = keep_head(query, head)
        own_grad = keep_head(grad, head)
        tiles = None if tiles_ref is None else tiles_ref.at[head]
        scores = scores_t(k_ref[:span, :], own, tiles, last)
        probs = jnp.exp(scores - lse_ref[0, head : head + 1, start : start + TILE])
        grad_probs = contract(v_ref[:span, :], own_grad, 1, 1)
        delta = jnp.sum(
            prod_t[head * size : (head + 1) * size, start : start + TILE], 0, keepdims=True
        )
        grad_scores = probs * (grad_probs - delta)
        low = grad_scores.astype(LOW)
        dv_new = contract(probs.astype(LOW), own_grad, 1, 0)
        dk_new = contract(low, own, 1, 0)
        dv = dv_new if dv is None else dv + dv_new
        dk = dk_new if dk is None else dk + dk_new
        dq_t.append(contract(k_t[head * size : (head + 1) * size, :span], low, 1, 0))
        if total_ref is not None:
            for place in range(last + 1):
                off = last - place
                piece = grad_scores[place * TILE : (place + 1) * TILE]
                if first:
                    total_ref[head, off] = piece
                elif off == last:
                    total_ref[head, off] = piece
                else:
                    total_ref[head, off] += piece
    dq_ref[start : start + TILE, :] = jnp.concatenate(dq_t, 0).T.astype(LOW)
    if first:
        dk_acc[:span, :] = dk
        dv_acc[:span, :] = dv
        if span < dk_acc.shape[0]:
            dk_acc[span:, :] = jnp.zeros((dk_acc.shape[0] - span, dk_acc.shape[1]), F32)
            dv_acc[span:, :] = jnp.zeros((dv_acc.shape[0] - span, dv_acc.shape[1]), F32)
    else:
        dk_acc[:span, :] += dk
        dv_acc[:span, :] += dv


def back_kernel(causal, *refs):
    if causal:
        (seq_ref, q_ref, k_ref, v_ref, g_ref, o_ref, lse_ref, z_ref,
         dq_ref, dk_ref, dv_ref, row_ref, dk_acc, dv_acc, tiles_ref, total_ref) = refs
        make_tiles(z_ref, tiles_ref)
    else:
        (q_ref, k_ref, v_ref, g_ref, o_ref, lse_ref,
         dq_ref, dk_ref, dv_ref, dk_acc, dv_acc) = refs
        tiles_ref = total_ref = None
    k_t = k_ref[...].T
    prod_t = (g_ref[...].astype(F32) * o_ref[...].astype(F32)).T
    blocks = q_ref.shape[0] // TILE
    keys = k_ref.shape[0]
    main = (q_ref, k_ref, v_ref, g_ref, lse_ref, dq_ref, dk_acc, dv_acc)
    if not causal:
        for block in range(blocks):
            back_block(main, k_t, prod_t, block * TILE, None, keys, block == 0, None, None)
    else:
        for side in range(keys // q_ref.shape[0]):

            @pl.when(seq_ref[0] == side)
            def _(side=side):
                for block in range(blocks):
                    last = side * blocks + block
                    back_block(
                        main, k_t, prod_t, block * TILE, last, (last + 1) * TILE,
                        block == 0, tiles_ref, total_ref,
                    )
                for head in range(PAIR):
                    for off in range(keys // TILE):
                        if off < (side + 1) * blocks:
                            row_ref[0, head, off : off + 1, :] = skew_sum(total_ref.at[head, off])
                        else:
                            row_ref[0, head, off : off + 1, :] = jnp.zeros((1, 2 * TILE), F32)

    dk_ref[...] = dk_acc[...].astype(LOW)
    dv_ref[...] = dv_acc[...].astype(LOW)


def attend_back(queries, keys_all, values, grad_mixed, mixed, lse, seq_pos, rows):
    count, width = queries.shape
    length = keys_all.shape[0]
    pairs = H // PAIR
    lanes = width // pairs
    offs = length // TILE
    causal = rows is not None
    col = lambda size: pl.BlockSpec((size, lanes), lambda pair, *_: (0, pair))
    in_specs = [col(count), col(length), col(length), col(count), col(count),
                pl.BlockSpec((1, PAIR, count), lambda pair, *_: (pair, 0, 0))]
    out_specs = [col(count), col(length), col(length)]
    out_shape = [
        jax.ShapeDtypeStruct((count, width), LOW),
        jax.ShapeDtypeStruct((length, width), LOW),
        jax.ShapeDtypeStruct((length, width), LOW),
    ]
    args = [queries, keys_all, values, grad_mixed, mixed, lse]
    scratch = [pltpu.VMEM((length, lanes), F32), pltpu.VMEM((length, lanes), F32)]
    if causal:
        row_spec = pl.BlockSpec((1, PAIR, offs, 2 * TILE), lambda pair, *_: (pair, 0, 0, 0))
        in_specs.append(row_spec)
        out_specs.append(row_spec)
        out_shape.append(jax.ShapeDtypeStruct((pairs, PAIR, offs, 2 * TILE), F32))
        args = [seq_pos] + args + [rows]
        scratch += [pltpu.VMEM((PAIR, offs, TILE, TILE), F32)] * 2
    work = H * count * length
    return pl.pallas_call(
        functools.partial(back_kernel, causal),
        grid_spec=pltpu.PrefetchScalarGridSpec(
            num_scalar_prefetch=1 if causal else 0,
            grid=(pairs,),
            in_specs=in_specs,
            out_specs=out_specs,
            scratch_shapes=scratch,
        ),
        out_shape=out_shape,
        cost_estimate=pl.CostEstimate(
            flops=work * 640 * 2, bytes_accessed=12 * length * width, transcendentals=work
        ),
        name="attend_causal_back" if causal else "attend_cross_back",
    )(*args)


def bucket_rows(buckets, length):
    offs = length // TILE
    place = jnp.arange(2 * TILE, dtype=jnp.int32)
    step = jnp.where(place < TILE, place, place - 2 * TILE)
    gap = (jnp.arange(offs, dtype=jnp.int32) * TILE)[:, None] + step[None, :]
    marks = jnp.arange(BUCKETS, dtype=jnp.int32)
    begins = jnp.sum((buckets[None, :] < marks[:, None]).astype(jnp.int32), 1)
    ends = jnp.sum((buckets[None, :] <= marks[:, None]).astype(jnp.int32), 1)
    hot = (gap[None] >= begins[:, None, None]) & (gap[None] < ends[:, None, None])
    return (gap, hot.astype(LOW))


def bit_plan():
    bits = []
    for axis in ("seq", "shard"):
        size = lax.axis_size(axis)
        assert size & (size - 1) == 0
        bits += [(axis, place) for place in reversed(range(size.bit_length() - 1))]
    return bits


def bit_orders(bits):
    ends = [0, len(bits) - 2, len(bits) - 1]
    rest = [place for place in range(len(bits)) if place not in ends]
    flipped = [ends[1], ends[0], ends[2]]
    return (rest + ends, rest + flipped, ends[:2] + rest + ends[2:])


def coords(bits):
    return [lax.rem(lax.axis_index(axis) // (1 << place), 2) for axis, place in bits]


def partner(bits, which):
    axis, place = bits[which]
    index = lax.axis_index(axis)
    mine = lax.rem(index // (1 << place), 2)
    return {axis: index + (1 - 2 * mine) * (1 << place)}


def greet(bits):
    barrier = pltpu.get_barrier_semaphore()
    for which in range(len(bits)):
        pl.semaphore_signal(
            barrier, inc=1, device_id=partner(bits, which), device_id_type=pl.DeviceIdType.MESH
        )
    pl.semaphore_wait(barrier, len(bits))


def remote(bits, which, source, target, sems):
    return pltpu.make_async_remote_copy(
        src_ref=source,
        dst_ref=target,
        send_sem=sems[0],
        recv_sem=sems[1],
        device_id=partner(bits, which),
        device_id_type=pl.DeviceIdType.MESH,
    )


def send(*args):
    copy = remote(*args)
    copy.start()
    return copy


def scatter_kernel(bits, count, *refs):
    steps = len(bits)
    sources, outs, work = refs[:count], refs[count : 2 * count], refs[2 * count : 3 * count]
    arrivals = refs[3 * count : (3 + steps) * count]
    load_sem, send_sem, recv_sem = refs[(3 + steps) * count :]
    place = coords(bits)
    orders = [list(reversed(order)) for order in bit_orders(bits)[:2]]
    loads = []
    for item in range(count):
        load = pltpu.make_async_copy(sources[item], work[item], load_sem.at[item])
        load.start()
        loads.append(load)
    greet(bits)
    copies = {}

    def add(item, step):
        order = orders[item % 2]
        free = [which for which in range(steps) if which not in order[: step + 1]]
        arrived = arrivals[item * steps + step]
        copies[item, step].wait_recv()
        if not free:
            outs[item][...] = work[item][tuple(place)].astype(F32) + arrived[...].astype(F32)
            return

        @pl.loop(0, 1 << len(free))
        def _(block):
            sub = [lax.rem(block // (1 << (len(free) - 1 - i)), 2) for i in range(len(free))]
            here = tuple(
                sub[free.index(which)] if which in free else place[which] for which in range(steps)
            )
            total = work[item][here].astype(F32) + arrived[tuple(sub)].astype(F32)
            work[item][here] = total.astype(work[item].dtype)

    for turn in range(steps + 1 + (count - 1) // 2):
        for item in range(count):
            step = turn - item // 2
            if not 0 <= step <= steps:
                continue
            if step == 0:
                loads[item].wait()
            else:
                add(item, step - 1)
            if step == steps:
                continue
            order = orders[item % 2]
            there = tuple(
                1 - place[which]
                if which == order[step]
                else (place[which] if which in order[:step] else slice(None))
                for which in range(steps)
            )
            copies[item, step] = send(
                bits,
                order[step],
                work[item].at[there],
                arrivals[item * steps + step],
                (send_sem.at[item, step], recv_sem.at[item, step]),
            )
    for copy in copies.values():
        copy.wait_send()


def scatter(items, collective_id):
    bits = bit_plan()
    steps = len(bits)
    count = len(items)
    sems = pltpu.SemaphoreType.DMA((count, steps))
    owners = 1 << steps
    items = [x.reshape((2,) * steps + (x.shape[0] // owners,) + x.shape[1:]) for x in items]
    tails = [x.shape[steps:] for x in items]
    arrivals = [
        pltpu.VMEM((2,) * (steps - 1 - step) + tail, x.dtype)
        for x, tail in zip(items, tails)
        for step in range(steps)
    ]
    return pl.pallas_call(
        functools.partial(scatter_kernel, bits, count),
        out_shape=[jax.ShapeDtypeStruct(tail, F32) for tail in tails],
        in_specs=[pl.BlockSpec(memory_space=pl.ANY)] * count,
        out_specs=[pl.BlockSpec(memory_space=pltpu.VMEM)] * count,
        scratch_shapes=[pltpu.VMEM(x.shape, x.dtype) for x in items]
        + arrivals
        + [pltpu.SemaphoreType.DMA((count,)), sems, sems],
        compiler_params=pltpu.CompilerParams(collective_id=collective_id, has_side_effects=True),
        name="scatter_rows",
    )(*items)


def table_rows(smalls, table_size, row):
    flat = smalls.reshape(-1, smalls.shape[-1])
    count = table_size * flat.shape[0] // 8
    entry = lax.broadcasted_iota(jnp.int32, (count, flat.shape[0]), 0)
    source = lax.broadcasted_iota(jnp.int32, (count, flat.shape[0]), 1)
    begin = (source >> 3) * table_size
    pick = ((source & 7) == row) & (entry >= begin) & (entry < begin + table_size)
    spread = contract(pick.astype(LOW), flat.astype(LOW), 1, 0)
    lane = lax.broadcasted_iota(jnp.int32, spread.shape, 1)
    place = lax.broadcasted_iota(jnp.int32, spread.shape, 0).astype(F32)
    block = jnp.floor((place + 0.5) * (1.0 / table_size))
    return jnp.where(lane.astype(F32) == place - block * table_size, spread, 0.0)


def gain_row(smalls, size, row):
    flat = smalls.reshape(-1, smalls.shape[-1])
    count = size * flat.shape[0] // 8
    source = lax.broadcasted_iota(jnp.int32, (flat.shape[0], count), 0)
    entry = lax.broadcasted_iota(jnp.int32, (flat.shape[0], count), 1)
    begin = (source >> 3) * size
    pick = ((source & 7) == row) & (entry >= begin) & (entry < begin + size)
    spread = contract(flat.astype(LOW), pick.astype(LOW), 0, 0)
    lane = lax.broadcasted_iota(jnp.int32, spread.shape, 0).astype(F32)
    place = lax.broadcasted_iota(jnp.int32, spread.shape, 1).astype(F32)
    block = jnp.floor((place + 0.5) * (1.0 / size))
    return jnp.sum(jnp.where(lane == place - block * size, spread, 0.0), 0, keepdims=True)


def full_weight(ref):
    value = ref[...].astype(F32)
    return value.reshape(-1, value.shape[-1]).astype(LOW)


ARRAYS = 12
INSIDE = 9
ITEMS = 15
PIECES = tuple((array, None, 0) for array in range(INSIDE)) + tuple(
    (array, axis, half) for array, axis in ((9, 1), (10, 1), (11, 0)) for half in range(2)
)
PATHS = ('xzZyc', 'xzZyc', 'zZxyc', 'zZyxc', 'yxzZc', 'xzZyc', 'zZxyc', 'zZxyc', 'xyzZc', 'zZyxc', 'zZyxc', 'xzZyc', 'yzZxc', 'xzZyc', 'xyzZc')
PLAN = (
    (1, 0, 0), (3, 0, 0), (2, 0, 0), (0, 0, 0), (14, 0, 0), (15, 0, 0),
    (1, 1, 0), (3, 1, 0), (0, 1, 0), (2, 1, 0), (7, 0, 0), (6, 0, 0),
    (1, 2, 0), (3, 2, 0), (9, 0, 0), (10, 0, 0), (11, 0, 0), (2, 2, 0),
    (7, 1, 0), (4, 0, 0), (0, 2, 0), (5, 0, 0), (12, 0, 0), (9, 1, 0),
    (1, 3, 0), (12, 1, 0), (10, 1, 0), (13, 0, 0), (6, 1, 0), (0, 3, 0),
    (8, 0, 0), (4, 1, 0), (11, 1, 0), (3, 3, 0), (14, 1, 0), (1, 4, 0),
    (2, 3, 0), (0, 4, 0), (5, 1, 0), (12, 2, 0), (6, 2, 0), (8, 1, 0),
    (4, 2, 0), (7, 2, 0), (5, 2, 1), (9, 2, 1), (11, 2, 1), (10, 2, 1),
    (13, 1, 1), (2, 4, 1), (14, 2, 2), (16, 0, 2), (12, 3, 2), (3, 4, 2),
    (6, 3, 3), (4, 3, 6), (5, 3, 6), (13, 2, 7), (8, 2, 7), (10, 3, 7),
    (6, 4, 7), (7, 3, 8), (11, 3, 8), (9, 3, 8), (14, 3, 8), (4, 4, 9),
    (5, 4, 9), (8, 3, 11), (13, 3, 11), (7, 4, 11), (12, 4, 14), (11, 4, 16),
    (14, 4, 17), (10, 4, 17), (8, 4, 18), (13, 4, 18), (9, 4, 19),
)
(STAGE_GAIN, STAGE_QUERY, STAGE_KEY, STAGE_VALUE, STAGE_SELF, STAGE_OUT, STAGE_CQUERY, STAGE_CKEY,
 STAGE_CVALUE, STAGE_CROSS, STAGE_COUT, STAGE_END) = (0, 1, 2, 3, 4, 10, 11, 12, 13, 14, 20, 21)


def path_bits(bits, path):
    count = len(bits)
    rest = list(range(1, count - 2))
    groups = {"x": [0], "y": [count - 2], "c": [count - 1], "z": rest[:-1], "Z": rest[-1:]}
    return [groups[letter] for letter in path]


def open_kernel(bits, sizes, *refs):
    gain_size, table_size = sizes
    sources = refs[:ARRAYS]
    hidden_ref, enc_ref, buckets_ref = refs[ARRAYS : ARRAYS + 3]
    finals = refs[ARRAYS + 3 : 2 * ARRAYS + 19]
    kept = refs[2 * ARRAYS + 19 : 2 * ARRAYS + 35 + INSIDE]
    outs = kept[:INSIDE] + finals[INSIDE:ARRAYS]
    (enc_out, first_out, q_out, k_out, v_out, mixed_out, lse_out, after_out, second_out,
     cq_out, ck_out, cv_out, cmixed_out, clse_out, across_out, third_out) = kept[INSIDE:]
    (before_ref, flat_ref, hot_ref, mask_ref, tiles_ref, weight_ref,
     send_sem, recv_sem, own_sem, side_send, side_recv, keep_sem) = refs[2 * ARRAYS + 35 + INSIDE :]
    steps = len(bits)
    place = coords(bits)
    seq_pos = lax.axis_index("seq")
    rows = hidden_ref.shape[0]
    keys = first_out.shape[0]
    lanes = hidden_ref.shape[1] // (H // PAIR)

    def kept_copy(number):
        final = finals[number] if number < INSIDE else finals[number - INSIDE + ARRAYS]
        return pltpu.make_async_copy(kept[number], final, keep_sem.at[number])

    def keep(*numbers):
        for number in numbers:
            kept_copy(number).start()

    def keep_act(*numbers):
        keep(*(number + INSIDE for number in numbers))

    def own(array):
        return pltpu.make_async_copy(
            sources[array], outs[array].at[tuple(place)], own_sem.at[array]
        )

    def copy(item, step):
        order = sum(path_bits(bits, PATHS[item]), [])
        array, axis, half = PIECES[item]
        here = tuple(
            slice(None) if which in order[:step] else place[which] for which in range(steps)
        )
        part = ()
        if axis is not None:
            size = sources[array].shape[axis] // 2
            part = (slice(None),) * axis + (pl.ds(half * size, size),)
        target = outs[array].at[here + part]
        source = target
        if step == 0:
            source = sources[array].at[part] if part else sources[array]
        return remote(
            bits,
            order[step],
            source,
            target,
            (send_sem.at[item, step], recv_sem.at[item, step]),
        )

    def arrived(item):
        copy(item, steps - 1).wait_recv()
        if item < INSIDE:
            keep(item)

    def side(which):
        source, target = ((hidden_ref, before_ref), (enc_ref, enc_out.at[rows:]))[which]
        return remote(bits, 0, source, target, (side_send.at[which], side_recv.at[which]))

    todo = list(PLAN)
    seen = set()

    def advance(until):
        while todo and todo[0][2] <= until:
            item, step, _ = todo.pop(0)
            if item >= ITEMS:
                side(item - ITEMS).start()
                continue
            groups = path_bits(bits, PATHS[item])
            first = sum(len(group) for group in groups[:step])
            for number in range(first, first + len(groups[step])):
                if number > 0:
                    if PIECES[item][0] not in seen:
                        seen.add(PIECES[item][0])
                        own(PIECES[item][0]).wait()
                    copy(item, number - 1).wait_recv()
                copy(item, number).start()

    for array in range(ARRAYS):
        own(array).start()
    greet(bits)
    enc_out[:rows, :] = enc_ref[...]
    make_hot(buckets_ref, hot_ref, mask_ref)
    advance(STAGE_GAIN)
    arrived(0)
    gains = [gain_row(outs[0][...], gain_size, row) for row in range(3)]
    flat_ref[...] = table_rows(outs[0][...], table_size, 3)

    def normed(value, gain):
        scale = lax.rsqrt(jnp.mean(value * value, -1, keepdims=True) + EPSILON)
        return (value * scale * gain).astype(LOW)

    def over_rows(count, body):
        @pl.loop(0, count // TILE)
        def _(block):
            body(lambda base=0: pl.ds(base + pl.multiple_of(block * TILE, TILE), TILE))

    def normed_rows(source, start):
        def body(at):
            first_out[at(start), :] = normed(source[at(), :].astype(F32), gains[0])

        over_rows(rows, body)

    def project(item, source, out, begin, count):
        weight_ref[...] = full_weight(outs[item])

        def body(at):
            out[at(), :] = contract(source[at(begin), :], weight_ref[...], 1, 0).astype(LOW)

        over_rows(count, body)

    normed_rows(hidden_ref, rows)
    advance(STAGE_QUERY)
    arrived(1)
    project(1, first_out, q_out, rows, rows)
    keep_act(2)
    advance(STAGE_KEY)
    side(0).wait_recv()

    @pl.when(seq_pos == 0)
    def _():
        first_out[:rows, :] = first_out[rows:, :]

    @pl.when(seq_pos != 0)
    def _():
        normed_rows(before_ref, 0)

    arrived(2)
    project(2, first_out, k_out, 0, keys)
    keep_act(1, 3)
    advance(STAGE_VALUE)
    arrived(3)
    project(3, first_out, v_out, 0, keys)
    keep_act(4)

    advance(STAGE_SELF)

    def between(pair, begin):
        for done in range(H // PAIR - 1):

            @pl.when(pair == done)
            def _(done=done):
                advance(begin + done + 1)

    @pl.loop(0, H // PAIR)
    def _(pair):
        at = pl.ds(pl.multiple_of(pair * lanes, lanes), lanes)
        q_ref, k_ref, v_ref, o_ref = (ref.at[:, at] for ref in (q_out, k_out, v_out, mixed_out))
        for head in range(PAIR):
            column = jnp.sum(
                flat_ref[pl.ds(pl.multiple_of((pair * PAIR + head) * BUCKETS, BUCKETS), BUCKETS), :],
                1,
                keepdims=True,
            )
            for off in range(keys // TILE):
                row = jnp.sum(column * hot_ref[off].astype(F32), 0, keepdims=True)
                tiles_ref[head, off] = toeplitz(row + mask_ref[off])
        v_t = v_ref[...].T
        blocks = rows // TILE
        for part in range(keys // rows):

            @pl.when(seq_pos == part)
            def _(part=part):
                for block in range(blocks):
                    last = part * blocks + block
                    attend_block(
                        q_ref, k_ref, v_t, o_ref, lse_out.at[pl.ds(pair, 1)], tiles_ref,
                        block * TILE, last, (last + 1) * TILE,
                    )

        between(pair, STAGE_SELF)

    def residual(item, mixed, base, total, normal, gain):
        weight_ref[...] = full_weight(outs[item])

        def body(at):
            value = base[at(), :].astype(F32) + contract(mixed[at(), :], weight_ref[...], 1, 0)
            total[at(), :] = value
            normal[at(), :] = normed(value, gain)

        over_rows(rows, body)

    keep_act(5, 6)
    advance(STAGE_OUT)
    arrived(4)
    residual(4, mixed_out, hidden_ref, after_out, second_out, gains[1])
    keep_act(7, 8)
    advance(STAGE_CQUERY)
    arrived(5)
    project(5, second_out, cq_out, 0, rows)
    keep_act(9)
    advance(STAGE_CKEY)
    side(1).wait_recv()
    arrived(6)
    project(6, enc_out, ck_out, 0, keys)
    keep_act(0, 10)
    advance(STAGE_CVALUE)
    arrived(7)
    project(7, enc_out, cv_out, 0, keys)
    keep_act(11)
    advance(STAGE_CROSS)

    @pl.loop(0, H // PAIR)
    def _(pair):
        at = pl.ds(pl.multiple_of(pair * lanes, lanes), lanes)
        q_ref, k_ref, v_ref, o_ref = (ref.at[:, at] for ref in (cq_out, ck_out, cv_out, cmixed_out))
        v_t = v_ref[...].T
        for block in range(rows // TILE):
            attend_block(
                q_ref, k_ref, v_t, o_ref, clse_out.at[pl.ds(pair, 1)], None, block * TILE, None, keys
            )
        between(pair, STAGE_CROSS)

    keep_act(12, 13)
    advance(STAGE_COUT)
    arrived(8)
    residual(8, cmixed_out, after_out, across_out, third_out, gains[2])
    keep_act(14, 15)
    advance(STAGE_END)
    assert not todo
    for item in range(INSIDE, ITEMS):
        arrived(item)
    for item in range(ITEMS):
        for step in range(steps):
            copy(item, step).wait_send()
    for which in range(2):
        side(which).wait_send()
    for number in range(len(kept)):
        kept_copy(number).wait()


def make_hot(buckets_ref, hot_ref, mask_ref):
    offs, marks, width = hot_ref.shape
    bucket = buckets_ref[...].astype(F32)
    mark = lax.broadcasted_iota(jnp.int32, (marks, bucket.shape[1]), 0).astype(F32)
    begin = jnp.sum((bucket < mark).astype(F32), 1, keepdims=True)
    end = jnp.sum((bucket <= mark).astype(F32), 1, keepdims=True)
    place = lax.broadcasted_iota(jnp.int32, (marks, width), 1).astype(F32)
    step = jnp.where(place < TILE, place, place - width)
    for off in range(offs):
        gap = step + off * TILE
        hot_ref[off] = ((gap >= begin) & (gap < end)).astype(F32).astype(LOW)
        mask_ref[off] = jnp.where(gap[:1] >= 0, 0.0, NEGATIVE)


def open_layer(items, hidden, encoded, buckets, sizes, collective_id):
    bits = bit_plan()
    steps = len(bits)
    count, width = hidden.shape
    length = count * lax.axis_size("seq")
    offs = length // TILE
    sems = pltpu.SemaphoreType.DMA((ITEMS, steps))
    inside = pl.BlockSpec(memory_space=pltpu.VMEM)
    outside = pl.BlockSpec(memory_space=pl.ANY)
    few, many = (count, width), (length, width)
    lse = (H // PAIR, PAIR, count)
    shapes = [((2,) * steps + x.shape, x.dtype) for x in items]
    shapes += [(many, LOW), (many, LOW), (few, LOW), (many, LOW), (many, LOW), (few, LOW)]
    shapes += [(lse, F32), (few, F32), (few, LOW), (few, LOW), (many, LOW), (many, LOW)]
    shapes += [(few, LOW), (lse, F32), (few, F32), (few, LOW)]
    outs = pl.pallas_call(
        functools.partial(open_kernel, bits, sizes),
        out_shape=[jax.ShapeDtypeStruct(*x) for x in shapes],
        in_specs=[inside] * (ARRAYS + 3),
        out_specs=[outside] * (ARRAYS + 16),
        scratch_shapes=[pltpu.VMEM(*x) for x in shapes[:INSIDE] + shapes[ARRAYS:]]
        + [
            pltpu.VMEM((count, width), LOW),
            pltpu.VMEM((H * BUCKETS, 128), F32),
            pltpu.VMEM((offs, BUCKETS, 2 * TILE), LOW),
            pltpu.VMEM((offs, 1, 2 * TILE), F32),
            pltpu.VMEM((PAIR, offs, TILE, TILE), F32),
            pltpu.VMEM((width, width), LOW),
            sems,
            sems,
            pltpu.SemaphoreType.DMA((ARRAYS,)),
            pltpu.SemaphoreType.DMA((2,)),
            pltpu.SemaphoreType.DMA((2,)),
            pltpu.SemaphoreType.DMA((INSIDE + 16,)),
        ],
        compiler_params=pltpu.CompilerParams(
            collective_id=collective_id, has_side_effects=True, vmem_limit_bytes=66_000_000
        ),
        name="open_layer",
    )(*items, hidden, encoded, buckets)
    return [out.reshape((-1,) + x.shape[-2:]) for out, x in zip(outs, items)] + list(outs[ARRAYS:])


def reversed_bits(bits, path):
    return list(reversed(sum(path_bits(bits, path), [])))


def close_kernel(bits, sizes, *refs):
    gain_size, table_size = sizes
    (ff_refs, weights, cross_refs, self_refs, (smalls_ref, buckets_ref, hidden_in),
     (layer_out, hidden_out, enc_out), outs, (small_out,)) = take(refs, (7, 8, 7, 6, 3, 3, 11, 1))
    rest = refs[46:]
    arrivals = rest[: CLOSE_ITEMS * len(bits)]
    (work_ref, ff_work, down_work, small_ref, q_buf, k_buf, pair_buf, rows_buf, grad_buf,
     res_buf, after_buf, weight_buf, enc_own, send_buf, recv_buf, dk_acc, dv_acc,
     tiles_ref, total_ref, rows_ref, flat_ref, gain_sums, hot_ref,
     mask_ref, send_sem, recv_sem, side_send, side_recv,
     fetch_sem) = rest[CLOSE_ITEMS * len(bits) :]
    steps = len(bits)
    place = coords(bits)
    seq_pos = lax.axis_index("seq")
    rows = res_buf.shape[0]
    keys = k_buf.shape[0]
    lanes = res_buf.shape[1] // (H // PAIR)
    v_buf, keys_in_buf = pair_buf.at[0], pair_buf.at[1]
    mixed_buf, query_in_buf = rows_buf.at[0], rows_buf.at[1]

    def pick(names, which, side):
        return tuple(side if name == which else slice(None) for name in names)

    def order_of(item):
        return reversed_bits(bits, CLOSE_PATHS[item])

    def part_of(item):
        if item not in (DOWN, DOWN + 1):
            return ()
        size = outs[2].shape[0] // 2
        return (pl.ds((item - DOWN) * size, size),)

    def base(item):
        if item == SMALL:
            return small_ref
        if item < DOWN:
            return ff_work.at[item % 4]
        return down_work if item < SQUARES else work_ref.at[item % SLOTS]

    def arrival(item, step):
        return arrivals[item * steps + step]

    def names_at(item, step):
        order = order_of(item)
        return [which for which in range(steps) if which not in order[:step]]

    def copy(item, step):
        which = order_of(item)[step]
        names = names_at(item, step)
        there = pick(names, which, 1 - place[which])
        if step == 0:
            source = base(item).at[there + part_of(item)]
        else:
            source = arrival(item, step - 1).at[there]
        return remote(
            bits, which, source, arrival(item, step), (send_sem.at[item, step], recv_sem.at[item, step])
        )

    def add(item, step):
        which = order_of(item)[step]
        names = names_at(item, step)
        free = [name for name in names if name != which]
        target = arrival(item, step)
        copy(item, step).wait_recv()

        def one(sub):
            here = tuple(place[which] if name == which else sub[free.index(name)] for name in names)
            if step > 0:
                mine = arrival(item, step - 1)[here]
            else:
                mine = base(item)[here + part_of(item)]
            if free:
                return mine + target[tuple(sub)]
            return mine.astype(F32) + target[tuple(sub)].astype(F32)

        if not free:
            if item == SMALL:
                small_out[...] = one(())
            elif item < DOWN:
                size = outs[0].shape[1] // FF_BLOCKS
                outs[item % 2][:, item // 2 * size : (item // 2 + 1) * size] = one(())
            elif item < SQUARES:
                outs[2][part_of(item)] = one(())
            else:
                outs[item - SQUARES + 3][...] = one(())
            return

        outer = max(0, len(free) - 3)

        def several(sub):
            sub = tuple(sub) + (slice(None),) * (len(free) - outer)
            target[sub] = one(sub)

        if outer == 0:
            several(())
            return

        @pl.loop(0, 1 << outer)
        def _(index):
            several([lax.rem(index // (1 << (outer - 1 - i)), 2) for i in range(outer)])

    def side(which):
        return remote(
            bits, 0, send_buf.at[which], recv_buf.at[which], (side_send.at[which], side_recv.at[which])
        )

    slots = {entry[:2]: entry[2] for entry in CLOSE_PLAN}
    done_slots = set()
    drained = set()

    def act(item, step):
        if item == CLOSE_ITEMS:
            side(0).start()
            return
        if item > CLOSE_ITEMS:

            @pl.when(seq_pos != 0)
            def _():
                side(1).start()

            return
        groups = list(reversed(path_bits(bits, CLOSE_PATHS[item]))) + [[None]]
        first = sum(len(group) for group in groups[:step])
        for number in range(first, first + len(groups[step])):
            if number > 0:
                add(item, number - 1)
            if number < steps:
                copy(item, number).start()

    def advance(slot):
        assert slot not in done_slots
        done_slots.add(slot)
        for item, step, planned in CLOSE_PLAN:
            if planned == slot:
                act(item, step)

    def drain(item, slot):
        assert slots[item, 1] <= slot
        copy(item, 0).wait_send()
        drained.add((item, 0))

    def fetch(source, target, sem):
        return pltpu.make_async_copy(source, target, fetch_sem.at[sem])

    def weight(number):
        return fetch(weights[number], weight_buf.at[number % 2], number % 2)

    def over_rows(count, body):
        @pl.loop(0, count // TILE)
        def _(block):
            body(lambda start=0: pl.ds(start + pl.multiple_of(block * TILE, TILE), TILE))

    def weight_grad(item, left, right):
        if item - SLOTS >= SQUARES:
            drain(item - SLOTS, max(done_slots))
        owner_grad(work_ref.at[item % SLOTS], left, right)

    def owner_grad(target, left, right):
        half = left.shape[1] // 2

        @pl.loop(0, 2)
        def _(top):
            at = pl.ds(pl.multiple_of(top * half, half), half)
            value = contract(left[:, at], right[...], 0, 0)
            target[top] = value.reshape(target.shape[1:]).astype(LOW)

    def pairs_back(lse_ref, tiles, begin):
        @pl.loop(0, H // PAIR)
        def _(pair):
            at = pl.ds(pl.multiple_of(pair * lanes, lanes), lanes)
            q_ref, k_ref, v_ref, g_ref, o_ref = (
                ref.at[:, at] for ref in (q_buf, k_buf, v_buf, grad_buf, mixed_buf)
            )
            if tiles:
                for head in range(PAIR):
                    start = pl.multiple_of((pair * PAIR + head) * BUCKETS, BUCKETS)
                    column = jnp.sum(flat_ref[pl.ds(start, BUCKETS), :], 1, keepdims=True)
                    for off in range(keys // TILE):
                        row = jnp.sum(column * hot_ref[off].astype(F32), 0, keepdims=True)
                        tiles_ref[head, off] = toeplitz(row + mask_ref[off])
            k_t = k_ref[...].T
            prod_t = (g_ref[...].astype(F32) * o_ref[...].astype(F32)).T
            main = (q_ref, k_ref, v_ref, g_ref, lse_ref.at[pl.ds(pair, 1)], q_ref, dk_acc, dv_acc)
            blocks = rows // TILE
            if not tiles:
                for block in range(blocks):
                    back_block(main, k_t, prod_t, block * TILE, None, keys, block == 0, None, None)
            else:
                for part in range(keys // rows):

                    @pl.when(seq_pos == part)
                    def _(part=part):
                        for block in range(blocks):
                            last = part * blocks + block
                            back_block(
                                main, k_t, prod_t, block * TILE, last, (last + 1) * TILE,
                                block == 0, tiles_ref, total_ref,
                            )
                        for head in range(PAIR):
                            column = jnp.zeros((BUCKETS, 1), F32)
                            for off in range((part + 1) * blocks):
                                row = skew_sum(total_ref.at[head, off])
                                column = column + jnp.sum(
                                    hot_ref[off].astype(F32) * row, 1, keepdims=True
                                )
                            start = pl.multiple_of((pair * PAIR + head) * BUCKETS, BUCKETS)
                            rows_ref[pl.ds(start, BUCKETS), :] = jnp.broadcast_to(
                                column, (BUCKETS, rows_ref.shape[1])
                            )

            k_ref[...] = dk_acc[...].astype(LOW)
            v_ref[...] = dv_acc[...].astype(LOW)
            for done in range(H // PAIR - 1):

                @pl.when(pair == done)
                def _(done=done):
                    advance(begin + done + 1)

    cq_in, ck_in, cv_in, cmixed_in, enc_in, second_in, clse_ref = cross_refs
    q_in, k_in, v_in, mixed_in, first_in, lse_ref = self_refs[:6]
    fetches = [
        fetch(cmixed_in, mixed_buf, 2), fetch(cq_in, q_buf, 3), fetch(ck_in, k_buf, 4),
        fetch(cv_in, v_buf, 5), fetch(enc_in, keys_in_buf, 6), fetch(second_in, query_in_buf, 7),
    ]
    third_in, grad_in, across_in, gate_in, up_in, down_in, after_in = ff_refs
    width = gate_in.shape[1] // FF_BLOCKS
    third_ref, grad_ref = k_buf.at[:rows], k_buf.at[rows:]
    loads = [fetch(third_in, third_ref, 2), fetch(grad_in, grad_ref, 3), fetch(across_in, after_buf, 4)]

    def ff_loads(block, slot):
        at = pl.ds(pl.multiple_of(block * width, width), width)
        return (
            fetch(gate_in.at[:, at], weight_buf.at[slot, :, pl.ds(0, width)], 8 + slot),
            fetch(up_in.at[:, at], pair_buf.at[slot, pl.ds(0, weight_buf.shape[1]), pl.ds(0, width)],
                  10 + slot),
            fetch(down_in.at[at], rows_buf.at[slot, pl.ds(0, width)], 12 + slot),
        )

    for one in ff_loads(0, 0):
        one.start()
    for one in loads:
        one.start()
    make_hot(buckets_ref, hot_ref, mask_ref)
    greet(bits)
    flat_ref[...] = table_rows(smalls_ref[...], table_size, 3)
    gain_one, gain_two, gain_three = [gain_row(smalls_ref[...], gain_size, row) for row in range(3)]
    for one in loads:
        one.wait()
    res_buf[...] = jnp.zeros_like(res_buf)
    enc_own[...] = jnp.zeros_like(enc_own)

    def ff_rows(slot, at):
        w_gate = weight_buf[slot, :, 0:width]
        w_up = pair_buf[slot, 0 : weight_buf.shape[1], 0:width]
        w_down = rows_buf[slot, 0:width, :]
        gate = contract(third_ref[at, :], w_gate, 1, 0)
        upper = contract(third_ref[at, :], w_up, 1, 0)
        grad = contract(grad_ref[at, :], w_down, 1, 1)
        square = gate * gate
        bend = jnp.tanh(GELU_SCALE * gate * (1.0 + 0.044715 * square))
        open_part = 0.5 * (1.0 + bend)
        active = gate * open_part
        slope = open_part + 0.5 * gate * (1.0 - bend * bend) * (
            GELU_SCALE * (1.0 + 3.0 * 0.044715 * square)
        )
        inner = (active * upper).astype(LOW)
        gate_grad = (grad * upper * slope).astype(LOW)
        upper_grad = (grad * active).astype(LOW)
        q_buf[at, 0:width] = inner
        grad_buf[at, 0:width] = gate_grad
        send_buf[0, at, 0:width] = upper_grad
        res_buf[at, :] += contract(inner, w_down, 1, 0)
        enc_own[at, :] += contract(gate_grad, w_gate, 1, 1) + contract(upper_grad, w_up, 1, 1)

    @pl.loop(0, FF_BLOCKS)
    def _(block):
        slot = lax.rem(block, 2)
        for one in ff_loads(block, slot):
            one.wait()

        @pl.when(block < FF_BLOCKS - 1)
        def _():
            for one in ff_loads(block + 1, 1 - slot):
                one.start()

        @pl.loop(0, rows // TILE)
        def _(part):
            ff_rows(slot, pl.ds(pl.multiple_of(part * TILE, TILE), TILE))

        for now in range(FF_BLOCKS):

            @pl.when(block == now)
            def _(now=now):
                advance(2 + 2 * now)
                if now >= 2:
                    drain(2 * now - 4, 2 + 2 * now)
                    drain(2 * now - 3, 2 + 2 * now)

        owner_grad(ff_work.at[2 * slot], third_ref, grad_buf.at[:, 0:width])
        owner_grad(ff_work.at[2 * slot + 1], third_ref, send_buf.at[0, :, 0:width])
        value = contract(q_buf[:, 0:width], grad_ref[...], 0, 0)
        down_work[lax.div(block, 2), slot] = value.reshape(down_work.shape[2:]).astype(LOW)
        for now in range(FF_BLOCKS):

            @pl.when(block == now)
            def _(now=now):
                advance(3 + 2 * now)

    weight(0).start()
    weight(1).start()
    for one in (fetches[0], fetches[1], fetches[3], fetches[4], fetches[5]):
        one.start()

    def norm_back_rows(value, gain, grad):
        scale = lax.rsqrt(jnp.mean(value * value, -1, keepdims=True) + EPSILON)
        scaled = gain * grad
        inner = jnp.mean(value * scaled, -1, keepdims=True)
        back = scale * scaled - value * (scale * scale * scale) * inner
        return back, jnp.sum(grad * value * scale, 0, keepdims=True)

    gain_sums[...] = jnp.zeros_like(gain_sums)

    def body(at):
        value = after_buf[at(), :]
        send_buf[1, at(), :] = (value + res_buf[at(), :]).astype(LOW)
        back, total = norm_back_rows(value, gain_three, enc_own[at(), :])
        gain_sums[2:3, :] += total
        res_buf[at(), :] = grad_ref[at(), :].astype(F32) + back

    over_rows(rows, body)
    layer_copy = fetch(send_buf.at[1], layer_out, 15)
    layer_copy.start()
    fetch(after_in, after_buf, 14).start()
    fetches[2].start()

    def to_mixed(number, source):
        weight(number).wait()

        def body(at):
            grad_buf[at(), :] = contract(
                source[at(), :].astype(LOW), weight_buf[number % 2], 1, 1
            ).astype(LOW)

        over_rows(rows, body)
        weight(number + 2).start()

    advance(10)
    to_mixed(0, res_buf)
    fetches[0].wait()

    def low_rows(source, target):
        def body(at):
            target[at(), :] = source[at(), :].astype(LOW)

        over_rows(rows, body)

    low_rows(res_buf, send_buf.at[0])
    weight_grad(SQUARES, mixed_buf, send_buf.at[0])
    advance(11)
    for one in fetches[1:4]:
        one.wait()
    pairs_back(clse_ref, False, 11)
    fetch(mixed_in, mixed_buf, 2).start()
    advance(17)

    def both_back(numbers, keep, count):
        def body_other(at):
            total = contract(k_buf[at(count), :], weight_buf[numbers[0] % 2], 1, 1)
            total = total + contract(v_buf[at(count), :], weight_buf[numbers[1] % 2], 1, 1)
            send_buf[keep[0], at(), :] = total.astype(LOW)
            if not count:
                gain_sums[3:4, :] += jnp.sum(
                    total * keys_in_buf[at(), :].astype(F32), 0, keepdims=True
                )

        def body_own(at):
            begin = 0 if count else rows
            total = contract(k_buf[at(begin), :], weight_buf[numbers[0] % 2], 1, 1)
            total = total + contract(v_buf[at(begin), :], weight_buf[numbers[1] % 2], 1, 1)
            keep[1][at(), :] = total

        over_rows(rows, body_other)
        return body_own

    weight(1).wait()
    weight(2).wait()
    own_part = both_back((1, 2), (0, enc_own), rows)
    for one in fetches[4:]:
        one.wait()
    advance(18)
    weight_grad(SQUARES + 1, keys_in_buf, k_buf)
    advance(19)
    weight_grad(SQUARES + 2, keys_in_buf, v_buf)
    advance(20)
    over_rows(rows, own_part)
    fetch(k_in, k_buf, 4).start()
    fetch(v_in, v_buf, 5).start()
    fetch(first_in, keys_in_buf, 6).start()
    weight(3).start()
    weight(4).start()
    advance(21)
    weight_grad(SQUARES + 3, query_in_buf, q_buf)
    advance(22)
    weight(3).wait()
    fetch(after_in, after_buf, 14).wait()

    def body(at):
        grad = contract(q_buf[at(), :], weight_buf[1], 1, 1)
        back, total = norm_back_rows(after_buf[at(), :], gain_two, grad)
        gain_sums[1:2, :] += total
        res_buf[at(), :] += back

    over_rows(rows, body)
    fetch(q_in, q_buf, 3).start()
    weight(5).start()
    weight(4).wait()

    def body(at):
        grad_buf[at(), :] = contract(res_buf[at(), :].astype(LOW), weight_buf[0], 1, 1).astype(LOW)

    over_rows(rows, body)
    weight(6).start()
    fetch(mixed_in, mixed_buf, 2).wait()
    low_rows(res_buf, query_in_buf)
    weight_grad(SQUARES + 4, mixed_buf, query_in_buf)
    advance(23)
    fetch(q_in, q_buf, 3).wait()
    fetch(k_in, k_buf, 4).wait()
    fetch(v_in, v_buf, 5).wait()
    pairs_back(lse_ref, True, 23)
    advance(29)
    side(0).wait_recv()
    side(0).wait_send()

    def body(at):
        send_buf[0, at(), :] = (enc_own[at(), :] + recv_buf[0, at(), :].astype(F32)).astype(LOW)

    over_rows(rows, body)
    enc_copy = fetch(send_buf.at[0], enc_out, 8)
    enc_copy.start()
    fetch(hidden_in, grad_buf, 9).start()
    layer_copy.wait()
    weight(5).wait()
    weight(6).wait()
    fetch(first_in, keys_in_buf, 6).wait()
    own_part = both_back((5, 6), (1, enc_own), 0)

    advance(30)
    weight_grad(SQUARES + 5, keys_in_buf, v_buf)
    advance(31)
    weight_grad(SQUARES + 6, keys_in_buf, k_buf)
    advance(32)
    weight_grad(SQUARES + 7, keys_in_buf.at[rows:], q_buf)
    advance(33)
    over_rows(rows, own_part)
    weight(7).start()
    own_low = (seq_pos == 0).astype(F32)
    fetch(hidden_in, grad_buf, 9).wait()
    weight(7).wait()

    def body(at):
        grad = contract(q_buf[at(), :], weight_buf[1], 1, 1) + enc_own[at(), :]
        grad = grad + own_low * send_buf[1, at(), :].astype(F32)
        enc_own[at(), :] = grad
        value = grad_buf[at(), :].astype(F32)
        scale = lax.rsqrt(jnp.mean(value * value, -1, keepdims=True) + EPSILON)
        gain_sums[0:1, :] += jnp.sum(grad * value * scale, 0, keepdims=True)

    over_rows(rows, body)
    gain_sums[0:1, :] += (1.0 - own_low) * gain_sums[3:4, :] / gain_one
    small_ref[...] = small_rows(
        gain_sums[0:1, :], gain_sums[1:2, :], gain_sums[2:3, :], rows_ref[...], gain_size,
        table_size, small_ref.shape
    )
    advance(34)

    @pl.when(seq_pos == 0)
    def _():
        side(1).wait_recv()

    @pl.when(seq_pos != 0)
    def _():
        side(1).wait_send()

    def body(at):
        grad = enc_own[at(), :] + jnp.where(
            seq_pos == 0, recv_buf[1, at(), :].astype(F32), 0.0
        )
        back, _ = norm_back_rows(grad_buf[at(), :].astype(F32), gain_one, grad)
        hidden_out[at(), :] = (res_buf[at(), :] + back).astype(LOW)

    over_rows(rows, body)
    advance(35)
    assert all(entry[2] in done_slots for entry in CLOSE_PLAN)
    for item in range(CLOSE_ITEMS):
        for step in range(steps):
            if (item, step) not in drained:
                copy(item, step).wait_send()
    enc_copy.wait()


def take(refs, counts):
    out = []
    begin = 0
    for count in counts:
        out.append(refs[begin : begin + count])
        begin += count
    return out


def small_rows(one, two, three, table, gain_size, table_size, shape):
    owners = one.shape[1] // gain_size

    def spread(source, size, row):
        count = owners * size
        target = lax.broadcasted_iota(jnp.int32, (owners * 8, count), 0)
        entry = lax.broadcasted_iota(jnp.int32, (owners * 8, count), 1)
        begin = (target >> 3) * size
        hot = ((target & 7) == row) & (entry >= begin) & (entry < begin + size)
        return lax.dot_general(
            hot.astype(F32), source, (((1,), (0 if row == 3 else 1,)), ((), ())),
            precision=lax.Precision.HIGHEST, preferred_element_type=F32,
        )

    def wheel(shape, axis, size):
        entry = lax.broadcasted_iota(jnp.int32, shape, axis).astype(F32)
        lane = lax.broadcasted_iota(jnp.int32, shape, 1 - axis).astype(F32)
        return lane == entry - size * jnp.floor((entry + 0.5) * (1.0 / size))

    total = jnp.zeros((owners * 8, 128), F32)
    for row, value in enumerate((one, two, three)):
        grid = (128, value.shape[1])
        total = total + spread(
            jnp.where(wheel(grid, 1, gain_size), jnp.broadcast_to(value, grid), 0.0), gain_size, row
        )
    total = total + spread(jnp.where(wheel(table.shape, 0, table_size), table, 0.0), table_size, 3)
    return total.reshape(shape)


SLOTS = 2
FF_BLOCKS = 4
DOWN = 2 * FF_BLOCKS
SQUARES = DOWN + 2
SMALL = SQUARES + 8
CLOSE_ITEMS = SMALL + 1
GELU_SCALE = 0.7978845608028654
CLOSE_PATHS = ('xzZyc', 'xyzZc', 'yzZxc', 'yxzZc', 'xzZyc', 'yzZxc', 'xzZyc', 'yxzZc', 'yzZxc', 'xzZyc', 'zZyxc', 'xyzZc', 'xzZyc', 'xzZyc', 'zZyxc', 'zZxyc', 'xyzZc', 'zZxyc', 'xyzZc')
CLOSE_PLAN = (
    (1, 0, 3), (0, 0, 3), (0, 1, 4), (1, 1, 5), (3, 0, 5), (2, 0, 5),
    (3, 1, 6), (2, 1, 6), (1, 2, 9), (6, 0, 9), (9, 0, 9), (7, 0, 9),
    (8, 0, 10), (5, 0, 10), (0, 2, 11), (9, 1, 11), (6, 1, 11), (10, 0, 11),
    (4, 0, 12), (8, 1, 12), (7, 1, 12), (3, 2, 13), (2, 2, 13), (10, 1, 15),
    (9, 2, 15), (5, 1, 16), (19, 0, 19), (11, 0, 19), (8, 2, 19), (6, 2, 19),
    (4, 1, 20), (10, 2, 20), (12, 0, 20), (3, 3, 20), (11, 1, 21), (7, 2, 21),
    (0, 3, 22), (9, 3, 22), (12, 1, 22), (5, 2, 23), (14, 0, 23), (8, 3, 24),
    (13, 0, 24), (14, 1, 26), (7, 3, 26), (10, 3, 27), (12, 2, 27), (13, 1, 27),
    (4, 2, 27), (11, 2, 27), (6, 3, 27), (20, 0, 30), (14, 2, 30), (2, 3, 31),
    (15, 0, 31), (7, 4, 31), (13, 2, 31), (16, 0, 32), (1, 3, 32), (15, 1, 32),
    (5, 3, 32), (17, 0, 33), (16, 1, 33), (4, 3, 33), (12, 3, 33), (13, 3, 33),
    (17, 1, 33), (10, 4, 33), (11, 3, 34), (7, 5, 34), (18, 0, 34), (8, 4, 34),
    (15, 2, 34), (18, 1, 34), (16, 2, 34), (17, 2, 34), (1, 4, 34), (12, 4, 34),
    (2, 4, 34), (14, 3, 34), (15, 3, 34), (5, 4, 34), (11, 4, 34), (6, 4, 34),
    (18, 2, 34), (3, 4, 34), (9, 4, 34), (8, 5, 34), (17, 3, 34), (14, 4, 34),
    (16, 3, 34), (2, 5, 34), (5, 5, 34), (3, 5, 34), (0, 4, 34), (15, 4, 34),
    (10, 5, 34), (11, 5, 34), (18, 3, 34), (13, 4, 34), (1, 5, 34), (17, 4, 34),
    (4, 4, 34), (6, 5, 34), (9, 5, 34), (16, 4, 34), (18, 4, 34), (13, 5, 35),
    (4, 5, 35), (12, 5, 35), (14, 5, 35), (15, 5, 35), (18, 5, 35), (16, 5, 35),
    (0, 5, 35), (17, 5, 35),
)


def close_layer(forward, weights, cross, own, smalls, buckets, hidden, sizes, collective_id):
    bits = bit_plan()
    steps = len(bits)
    owners = 1 << steps
    count, width = hidden.shape
    units = forward[3].shape[1]
    length = cross[1].shape[0]
    offs = length // TILE
    lanes = width // (H // PAIR)
    gate, down = (width // owners, units), (units // owners, width)
    square = (width // owners, width)
    blocks = [(gate[0], units // FF_BLOCKS)] * DOWN + [(down[0] // 2, width)] * 2 + [square] * 8
    kinds = [LOW] * SMALL + [F32]
    blocks.append((8, 128))
    arrivals = [
        pltpu.VMEM((2,) * (steps - 1 - step) + block, kind)
        for block, kind in zip(blocks, kinds)
        for step in range(steps)
    ]
    inside = pl.BlockSpec(memory_space=pltpu.VMEM)
    outside = pl.BlockSpec(memory_space=pl.ANY)
    few, many = (count, width), (length, width)
    vm = pltpu.VMEM
    sems = pltpu.SemaphoreType.DMA((CLOSE_ITEMS, steps))
    pair_sem = pltpu.SemaphoreType.DMA((2,))
    return pl.pallas_call(
        functools.partial(close_kernel, bits, sizes),
        out_shape=[jax.ShapeDtypeStruct(few, LOW)] * 3
        + [jax.ShapeDtypeStruct(block, F32) for block in (gate, gate, down)]
        + [jax.ShapeDtypeStruct(square, F32)] * 8
        + [jax.ShapeDtypeStruct((8, 128), F32)],
        in_specs=[outside] * (7 + 8) + [outside] * 6 + [inside] + [outside] * 5 + [inside]
        + [inside] * 2 + [outside],
        out_specs=[outside, inside, outside] + [inside] * 12,
        scratch_shapes=arrivals
        + [
            vm((SLOTS,) + (2,) * steps + square, LOW),
            vm((4,) + (2,) * steps + (gate[0], units // FF_BLOCKS), LOW),
            vm((2,) * steps + down, LOW),
            vm((2,) * steps + (8, 128), F32),
            vm(few, LOW), vm(many, LOW), vm((2,) + many, LOW), vm((2,) + few, LOW),
            vm(few, LOW), vm(few, F32), vm(few, F32),
            vm((2, width, width), LOW), vm(few, F32), vm((2,) + few, LOW), vm((2,) + few, LOW),
            vm((length, lanes), F32), vm((length, lanes), F32),
            vm((PAIR, offs, TILE, TILE), F32), vm((PAIR, offs, TILE, TILE), F32),
            vm((H * BUCKETS, 128), F32), vm((H * BUCKETS, 128), F32), vm((8, width), F32),
            vm((offs, BUCKETS, 2 * TILE), LOW), vm((offs, 1, 2 * TILE), F32),
            sems, sems, pair_sem, pair_sem, pltpu.SemaphoreType.DMA((16,)),
        ],
        compiler_params=pltpu.CompilerParams(
            collective_id=collective_id, has_side_effects=True, vmem_limit_bytes=67_000_000
        ),
        name="close_layer",
    )(*forward, *weights, *cross, *own, smalls, buckets, hidden)


def finish_kernel(*refs):
    count = (len(refs) - 5) // 2
    for source, target in zip(refs[: count], refs[count + 1 :]):
        target[...] = source[...]
    small = refs[count]
    for row, target in enumerate(refs[2 * count + 1 :]):
        target[...] = small[row, : target.shape[0]]


def finish(arrays, small, sizes):
    count = len(arrays)
    inside = pl.BlockSpec(memory_space=pltpu.VMEM)
    return pl.pallas_call(
        finish_kernel,
        out_shape=[jax.ShapeDtypeStruct(x.shape, x.dtype) for x in arrays]
        + [jax.ShapeDtypeStruct((size,), F32) for size in sizes],
        in_specs=[inside] * (count + 1),
        out_specs=[inside] * (count + 4),
        name="finish",
    )(*arrays, small)


def dot_low(left, right):
    return contract(left, right, 1, 0)


def dot_left(left, right):
    return contract(left, right, 0, 0)


def dot_right(left, right):
    return contract(left, right, 1, 1)


def rms_norm(value, gain):
    return value * lax.rsqrt(jnp.mean(value * value, -1, keepdims=True) + EPSILON) * gain


def norm_back(value, gain, grad):
    return jax.vjp(rms_norm, value, gain)[1](grad)


def gated(gate, upper):
    return jax.nn.gelu(gate, approximate=True) * upper


def pad_rows(rows):
    return sum(
        jnp.pad(row.astype(F32)[None], ((place, 7 - place), (0, 128 - row.shape[0])))
        for place, row in enumerate(rows)
    )


def on_device(
    hidden_in,
    encoded,
    cotangent,
    buckets,
    self_query,
    self_key,
    self_value,
    self_out,
    cross_query,
    cross_key,
    cross_value,
    cross_out,
    ff_gate,
    ff_up,
    ff_down,
    norm_self,
    norm_cross,
    norm_ff,
    bias_table,
):
    owners = lax.axis_size("seq") * lax.axis_size("shard")
    seq_pos = lax.axis_index("seq")
    seq_row = seq_pos.reshape(1).astype(jnp.int32)
    low_side = seq_pos == 0
    both = ("seq", "shard")
    width = hidden_in.shape[2]
    own_low = hidden_in[0]
    enc_own = encoded[0]
    small = pad_rows([norm_self, norm_cross, norm_ff, bias_table])
    hidden = own_low.astype(F32)
    count = hidden.shape[0]
    length = count * lax.axis_size("seq")
    gap, hot = bucket_rows(buckets, length)
    opened = open_layer(
        [small, self_query, self_key, self_value, self_out, cross_query, cross_key, cross_value,
         cross_out, ff_gate, ff_up, ff_down],
        own_low,
        enc_own,
        buckets.reshape(1, -1),
        (norm_self.shape[0], bias_table.shape[0]),
        1,
    )
    smalls = opened[0]
    (w_query, w_key, w_value, w_sout, w_cquery, w_ckey, w_cvalue, w_cout, w_gate, w_up, w_down) = [
        x.reshape(-1, x.shape[-1]) for x in opened[1:12]
    ]
    (enc_all, first_all, query, key, value, self_mixed, self_lse, after_self, second,
     cross_q, cross_k, cross_v, cross_mixed, cross_lse, after_cross, third) = opened[12:]
    gain_one, gain_two, gain_three = [
        smalls[:, i, : norm_self.shape[0]].reshape(-1) for i in range(3)
    ]
    table = smalls[:, 3, : bias_table.shape[0]].reshape(H, BUCKETS)
    rows = jnp.einsum("hb,bof->hof", table.astype(LOW), hot, preferred_element_type=F32)
    rows = jnp.where(gap[None] >= 0, rows, NEGATIVE).reshape(H // PAIR, PAIR, *gap.shape)
    first = first_all[count:]

    gains = norm_self.shape[0]
    if width // owners >= 16:
        *arrays, small_sum = close_layer(
            [third, cotangent[0], after_cross, w_gate, w_up, w_down, after_self],
            [w_cout, w_ckey, w_cvalue, w_cquery, w_sout, w_key, w_value, w_query],
            [cross_q, cross_k, cross_v, cross_mixed, enc_all, second, cross_lse],
            [query, key, value, self_mixed, first_all, self_lse],
            smalls,
            buckets.reshape(1, -1),
            own_low,
            (gains, bias_table.shape[0]),
            2,
        )
        *arrays, one, two, three, four = finish(
            arrays, small_sum, (gains,) * 3 + bias_table.shape
        )
        hidden_out, grad_hidden, grad_encoded, *sums = arrays
        return (
            hidden_out[None],
            grad_hidden[None],
            grad_encoded[None],
            sums[10],
            sums[9],
            sums[8],
            sums[7],
            sums[6],
            sums[4],
            sums[5],
            sums[3],
            sums[0],
            sums[1],
            sums[2],
            one,
            two,
            three,
            four,
        )
    gate = dot_low(third, w_gate)
    upper = dot_low(third, w_up)
    inner = gated(gate, upper).astype(LOW)
    hidden_out = (after_cross + dot_low(inner, w_down)).astype(LOW)

    grad_top = cotangent[0]
    grad_wdown = dot_left(inner, grad_top).astype(LOW)
    grad_inner = dot_right(grad_top, w_down)
    grad_gate, grad_upper = jax.vjp(gated, gate, upper)[1](grad_inner)
    gate_low = grad_gate.astype(LOW)
    upper_low = grad_upper.astype(LOW)
    grad_wgate = dot_left(third, gate_low).astype(LOW)
    grad_wup = dot_left(third, upper_low).astype(LOW)
    grad_third = dot_right(gate_low, w_gate) + dot_right(upper_low, w_up)
    norm_grad, grad_gain_three = norm_back(after_cross, gain_three, grad_third)
    grad_cross_res = grad_top.astype(F32) + norm_grad
    sum_gate, sum_up = [
        lax.psum_scatter(x, both, scatter_dimension=0, tiled=True).astype(F32)
        for x in (grad_wgate, grad_wup)
    ]
    cross_res_low = grad_cross_res.astype(LOW)
    grad_wcout = dot_left(cross_mixed, cross_res_low).astype(LOW)
    grad_cross_mix = dot_right(cross_res_low, w_cout).astype(LOW)
    grad_cq, grad_ck, grad_cv = attend_back(
        cross_q, cross_k, cross_v, grad_cross_mix, cross_mixed, cross_lse, None, None
    )
    grad_enc = dot_right(grad_ck, w_ckey) + dot_right(grad_cv, w_cvalue)
    enc_back = lax.ppermute(grad_enc[count:].astype(LOW), "seq", [(0, 1), (1, 0)])
    grad_wcquery = dot_left(second, grad_cq).astype(LOW)
    grad_wckey = dot_left(enc_all, grad_ck).astype(LOW)
    grad_wcvalue = dot_left(enc_all, grad_cv).astype(LOW)
    norm_grad, grad_gain_two = norm_back(after_self, gain_two, dot_right(grad_cq, w_cquery))
    grad_self_res = grad_cross_res + norm_grad
    self_res_low = grad_self_res.astype(LOW)
    grad_wsout = dot_left(self_mixed, self_res_low).astype(LOW)
    grad_self_mix = dot_right(self_res_low, w_sout).astype(LOW)
    grad_q, grad_k, grad_v, grad_rows = attend_back(
        query, key, value, grad_self_mix, self_mixed, self_lse, seq_row, rows
    )
    grad_part = dot_right(grad_k, w_key) + dot_right(grad_v, w_value)
    part_back = lax.ppermute(grad_part[:count].astype(LOW), "seq", [(1, 0)])
    grad_wquery = dot_left(first, grad_q).astype(LOW)
    grad_wkey = dot_left(first_all, grad_k).astype(LOW)
    grad_wvalue = dot_left(first_all, grad_v).astype(LOW)
    grad_first = (
        dot_right(grad_q, w_query)
        + grad_part[count:]
        + jnp.where(low_side, grad_part[:count], 0.0)
        + part_back.astype(F32)
    )
    norm_grad, grad_gain_one = norm_back(hidden, gain_one, grad_first)
    grad_hidden = (grad_self_res + norm_grad).astype(LOW)
    grad_encoded = (grad_enc[:count] + enc_back.astype(F32)).astype(LOW)
    table_grad = jnp.einsum(
        "hof,bof->hb", grad_rows.reshape(H, *gap.shape), hot.astype(F32),
        precision=lax.Precision.HIGHEST,
    )
    small_grads = jnp.stack(
        [
            jnp.pad(x.reshape(owners, -1), ((0, 0), (0, 128 - x.size // owners)))
            for x in (grad_gain_one, grad_gain_two, grad_gain_three, table_grad)
        ]
        + [jnp.zeros((owners, 128), F32)] * 4,
        1,
    ).reshape(owners * 8, 128)
    sums = scatter(
        [grad_wdown, grad_wcout, grad_wcquery, grad_wckey, grad_wcvalue, grad_wsout, grad_wquery,
         grad_wkey, grad_wvalue, small_grads],
        2,
    )
    small_sum = sums[9]
    return (
        hidden_out[None],
        grad_hidden[None],
        grad_encoded[None],
        sums[6],
        sums[7],
        sums[8],
        sums[5],
        sums[2],
        sums[3],
        sums[4],
        sums[1],
        sum_gate,
        sum_up,
        sums[0],
        small_sum[0, :gains],
        small_sum[1, :gains],
        small_sum[2, :gains],
        small_sum[3, : bias_table.shape[0]],
    )


def solution(mesh):
    rows = P(("seq", "shard"), None)
    flat = P(("seq", "shard"))
    tokens = P("shard", "seq", None)
    return jax.shard_map(
        on_device,
        mesh=mesh,
        in_specs=(tokens,) * 3 + (P(),) + (rows,) * 11 + (flat,) * 4,
        out_specs=(tokens,) * 3 + (rows,) * 11 + (flat,) * 4,
        check_vma=False,
    )
```
